32 devices in a mesh: dp: 8 (over z, x), probe: 4 (over y, core).
Axes of the slice: x: 2, y: 2, z: 4, core: 2. Of those that a mesh axis runs over, the one named last changes fastest.
Arguments:
- tokens: bfloat16 [4096, 768], P('dp'), may hold values from -6 to 6
- cotangent: bfloat16 [4096, 768], P('dp'), may hold values from -6 to 6
- vec_params: float32 [13, 768], replicated, may hold values from -1.2 to 1.6
- qkv_weight: bfloat16 [768, 2304], replicated, may hold values from -0.21875 to 0.21875
- out_weight: bfloat16 [768, 768], replicated, may hold values from -0.875 to 0.875
- up_weight: bfloat16 [768, 3072], replicated, may hold values from -0.21875 to 0.21875
- down_weight: bfloat16 [3072, 768], replicated, may hold values from -0.109375 to 0.109375
- probe_vec: float32 [4, 13, 768], P('probe'), may hold values from -4 to 4
- probe_qkv: bfloat16 [4, 768, 2304], P('probe'), may hold values from -0.21875 to 0.21875
- probe_out: bfloat16 [4, 768, 768], P('probe'), may hold values from -0.21875 to 0.21875
- probe_up: bfloat16 [4, 768, 3072], P('probe'), may hold values from -0.21875 to 0.21875
- probe_down: bfloat16 [4, 3072, 768], P('probe'), may hold values from -0.109375 to 0.109375
- seq_device: int32 [14], replicated, may hold values from 0 to 7, as said below
- seq_length: int32 [14], replicated, may hold values from 128 to 512
- owners: int32 [48], replicated, may hold values from 0 to 47, as said below
- left_bases: float32 [48, 384, 384], P('dp'), may hold values from -1 to 1, as said below
- right_bases: float32 [48, 384, 384], P('dp'), may hold values from -1 to 1, as said below
- first_moment: float32 [48, 384, 384], P('dp'), may hold values from -192 to 192
- second_moment: float32 [48, 384, 384], P('dp'), may hold values from 81 to 8192, as said below
- vec_first: float32 [13, 768], replicated, may hold values from -128 to 128
- vec_second: float32 [13, 768], replicated, may hold values from 1024 to 4096, as said below
Outputs:
- block_output: bfloat16 [4096, 768], P('dp')
- input_grad: float32 [4096, 768], P('dp')
- weight_grads: float32 [48, 384, 384], P('dp')
- new_first: float32 [48, 384, 384], P('dp')
- new_second: float32 [48, 384, 384], P('dp')
- new_weights: float32 [48, 384, 384], P('dp')
- new_weights_low: bfloat16 [48, 384, 384], P('dp')
- curvature_blocks: float32 [4, 48, 384, 384], P('probe', 'dp')
- vector_state: float32 [2, 13, 768], replicated
- vector_second: float32 [13, 768], replicated
- vector_new: float32 [13, 768], replicated
- vector_curvature: float32 [4, 13, 768], P('probe')
- probe_dots: float32 [4, 2], replicated
The draws below stay inside these ranges and needn't reach their ends.
Inputs may be any that keep to these rules, and one draw needn't show every extreme that they name: `seq_device`: each index of dp receives either one sequence of 512 tokens or four sequences of 128 tokens. `owners`: distinct slot numbers; slot s lies on index s // 6 of dp. `left_bases`: each slot's matrix is orthogonal. `right_bases`: each slot's matrix is orthogonal. `second_moment`: Positive. `vec_second`: Positive.
All inputs are finite; a program needn't handle non-finite values.
Results may differ from the reference program's by a relative error of at most 0.0035.
The reference program's roundings to bfloat16 on the way count: a program that leaves them out, or rounds other values in their place, can miss the bound.
Values sent between devices are 32-bit elements; how exact they have to be, the bound alone decides.
No kernel may reach another device: no remote copies, remote signals or barrier semaphores. Data moves between devices by JAX's collectives and lax.ppermute only.
A program may use at most 320 MiB of HBM per device.

```python
import math
import jax
import jax.numpy as jnp
from jax import lax

D = 768
HEADS = 12
HEAD = 64
ROT = 16
FF = 3072
BLK = 384
STEP = 4
LONG = 512
SHORT = 128
NLONG = 6
NSHORT = 8
NSEQ = 14
TOKENS = 4096
NPROBE = 4
VEC = 13
NBLK = 48
SLOTS = 48
N_DP = 8


def sequence_plan(key):
    base_key = jax.random.fold_in(key, 11)
    host_count = NLONG + NSHORT // 4
    device_order = jax.random.permutation(jax.random.fold_in(base_key, 1), host_count).astype(jnp.int32)
    seq_order = jax.random.permutation(jax.random.fold_in(base_key, 2), NSEQ).astype(jnp.int32)
    slot_ids = jnp.arange(NSEQ, dtype=jnp.int32)
    host_index = jnp.where(slot_ids < NLONG, slot_ids, NLONG + (slot_ids - NLONG) // 4)
    host_ids = jnp.take(device_order, host_index)
    size_list = jnp.where(slot_ids < NLONG, LONG, SHORT).astype(jnp.int32)
    device_ids = jnp.zeros((NSEQ,), jnp.int32).at[seq_order].set(host_ids)
    length_ids = jnp.zeros((NSEQ,), jnp.int32).at[seq_order].set(size_list)
    return (device_ids, length_ids)


def draw_seq_device(key, part):
    return sequence_plan(key)[0]


def draw_seq_length(key, part):
    return sequence_plan(key)[1]


def owner_plan(key):
    base_key = jax.random.fold_in(key, 23)
    middle = jax.random.permutation(jax.random.fold_in(base_key, 1), SLOTS - 2)[:NBLK - 2].astype(jnp.int32) + 1
    chosen = jnp.concatenate([jnp.array([0, SLOTS - 1], jnp.int32), middle])
    return jax.random.permutation(jax.random.fold_in(base_key, 2), chosen).astype(jnp.int32)


def draw_owners(key, part):
    return owner_plan(key)


def slot_scale(key):
    owner_ids = owner_plan(key)
    slot_ids = jnp.arange(SLOTS, dtype=jnp.int32)
    matches = owner_ids[None, :] == slot_ids[:, None]
    tile_ids = jnp.sum(jnp.where(matches, jnp.arange(NBLK, dtype=jnp.int32)[None, :], 0), axis=1)
    occupied = jnp.any(matches, axis=1)
    tiles_side = D // BLK
    first_end = tiles_side * 3 * tiles_side
    second_end = first_end + tiles_side * tiles_side
    third_end = second_end + tiles_side * (FF // BLK)
    coefficient = jnp.where(tile_ids < first_end, 0.5, jnp.where(tile_ids < second_end, 0.15, jnp.where(tile_ids < third_end, 0.25, 0.6)))
    coefficient = jnp.where(occupied, coefficient, 0.3)
    return coefficient.astype(jnp.float32) * math.sqrt(TOKENS)


def draw_first_moment(key, part):
    spread = slot_scale(key)
    noise_draw = jax.random.truncated_normal(jax.random.fold_in(key, 41), -4.0, 4.0, (SLOTS, BLK, BLK), jnp.float32)
    return spread[:, None, None] * noise_draw


def draw_second_moment(key, part):
    spread = slot_scale(key)
    factor = jnp.exp(jax.random.uniform(jax.random.fold_in(key, 43), (SLOTS, BLK, BLK), jnp.float32, 0.0, math.log(4.0)))
    return (spread * spread)[:, None, None] * factor


def orthogonal_stack(key):
    row_index = jnp.arange(BLK, dtype=jnp.int32)
    phase_code = (2 * row_index[:, None] + 1) * row_index[None, :] % (4 * BLK)
    angles = phase_code.astype(jnp.float32) * (math.pi / (2 * BLK))
    cosine_table = jnp.cos(angles) * math.sqrt(2.0 / BLK) * jnp.where(row_index[None, :] == 0, math.sqrt(0.5), 1.0)

    def single_slot(slot_key):
        row_perm = jax.random.permutation(jax.random.fold_in(slot_key, 1), BLK)
        col_perm = jax.random.permutation(jax.random.fold_in(slot_key, 2), BLK)
        sign_flip = (2 * jax.random.randint(jax.random.fold_in(slot_key, 3), (BLK,), 0, 2) - 1).astype(jnp.float32)
        return jnp.take(jnp.take(cosine_table, row_perm, axis=0), col_perm, axis=1) * sign_flip[None, :]
    return jax.vmap(single_slot)(jax.random.split(key, SLOTS))


def draw_left_bases(key, part):
    return orthogonal_stack(jax.random.fold_in(key, 51))


def draw_right_bases(key, part):
    return orthogonal_stack(jax.random.fold_in(key, 53))


def draw_vec_params(key, part):
    base_noise = jax.random.truncated_normal(jax.random.fold_in(key, 61), -4.0, 4.0, (VEC, D), jnp.float32)
    row_index = jnp.arange(VEC, dtype=jnp.int32)[:, None]
    is_gain = (row_index == 0) | (row_index == 2)
    return jnp.where(is_gain, 1.0 + 0.15 * base_noise, 0.3 * base_noise)


def draw_vec_first(key, part):
    base_noise = jax.random.truncated_normal(jax.random.fold_in(key, 71), -4.0, 4.0, (VEC, D), jnp.float32)
    return 0.5 * math.sqrt(TOKENS) * base_noise


def draw_vec_second(key, part):
    factor = jnp.exp(jax.random.uniform(jax.random.fold_in(key, 73), (VEC, D), jnp.float32, 0.0, math.log(4.0)))
    return 0.25 * TOKENS * factor


def block_levels(stream_key, shape, cuts, low, high):
    level = 1.0
    for dim, shards_of in cuts:
        draws = jax.random.uniform(jax.random.fold_in(jax.random.fold_in(stream_key, 6), dim), (shards_of,), jnp.float32, low / len(cuts), high / len(cuts))
        level = level * jnp.repeat(jnp.exp(draws), shape[dim] // shards_of).reshape((-1,) + (1,) * (len(shape) - 1 - dim))
    return level


def normal_values(own_key, extent, width, bound, cuts=(), kind=jnp.bfloat16):
    drawn = jax.random.normal(own_key, extent, jnp.float32) * width
    if len(cuts) > 0:
        drawn = block_levels(own_key, extent, cuts, -0.22, 0.18) * drawn
    return jnp.clip(drawn, min=-bound, max=bound).astype(kind)


def setup_inputs(seed: int = 0) -> dict:
    arg_keys = jax.random.split(jax.random.key(seed), 22)
    tokens = normal_values(arg_keys[0], (TOKENS, D), 1.0, 6.0, ((0, 8),))
    cotangent = normal_values(arg_keys[1], (TOKENS, D), 1.0, 6.0, ((0, 8),))
    vec_params = draw_vec_params(jax.random.fold_in(arg_keys[21], 71), 0)
    qkv_weight = normal_values(arg_keys[3], (D, 3 * D), D ** -0.5, 0.21875)
    out_weight = normal_values(arg_keys[4], (D, D), (D // 16) ** -0.5, 0.875)
    up_weight = normal_values(arg_keys[5], (D, FF), D ** -0.5, 0.21875)
    down_weight = normal_values(arg_keys[6], (FF, D), FF ** -0.5, 0.109375)
    probe_vec = normal_values(arg_keys[7], (NPROBE, VEC, D), 0.3, 4.0, ((0, 4),), jnp.float32)
    probe_qkv = normal_values(arg_keys[8], (NPROBE, D, 3 * D), D ** -0.5, 0.21875, ((0, 4),))
    probe_out = normal_values(arg_keys[9], (NPROBE, D, D), D ** -0.5, 0.21875, ((0, 4),))
    probe_up = normal_values(arg_keys[10], (NPROBE, D, FF), D ** -0.5, 0.21875, ((0, 4),))
    probe_down = normal_values(arg_keys[11], (NPROBE, FF, D), FF ** -0.5, 0.109375, ((0, 4),))
    seq_device = draw_seq_device(jax.random.fold_in(arg_keys[21], 71), 0)
    seq_length = draw_seq_length(jax.random.fold_in(arg_keys[21], 71), 0)
    owners = draw_owners(jax.random.fold_in(arg_keys[21], 71), 0)
    left_bases = draw_left_bases(jax.random.fold_in(arg_keys[21], 71), 0)
    right_bases = draw_right_bases(jax.random.fold_in(arg_keys[21], 71), 0)
    first_moment = draw_first_moment(jax.random.fold_in(arg_keys[21], 71), 0)
    second_moment = draw_second_moment(jax.random.fold_in(arg_keys[21], 71), 0)
    vec_first = draw_vec_first(jax.random.fold_in(arg_keys[21], 71), 0)
    vec_second = draw_vec_second(jax.random.fold_in(arg_keys[21], 71), 0)
    return {"tokens": tokens, "cotangent": cotangent, "vec_params": vec_params, "qkv_weight": qkv_weight, "out_weight": out_weight, "up_weight": up_weight, "down_weight": down_weight, "probe_vec": probe_vec, "probe_qkv": probe_qkv, "probe_out": probe_out, "probe_up": probe_up, "probe_down": probe_down, "seq_device": seq_device, "seq_length": seq_length, "owners": owners, "left_bases": left_bases, "right_bases": right_bases, "first_moment": first_moment, "second_moment": second_moment, "vec_first": vec_first, "vec_second": vec_second}


@jax.custom_vjp
def low(v):
    return lax.optimization_barrier(v.astype(jnp.bfloat16)).astype(jnp.float32)

@jax.custom_vjp
def low_back(v):
    return v

def low_keep(v):
    return (low(v), None)

def low_pass(kept, grad):
    return (grad,)

def back_keep(v):
    return (v, None)

def back_low(kept, grad):
    return (low(grad),)
low.defvjp(low_keep, low_pass)
low_back.defvjp(back_keep, back_low)
beta_decay = 0.5
learning_rate = 0.05
weight_decay = 0.01
adam_epsilon = 1e-08
norm_epsilon = 1e-05
root_half = 0.7071067811865476
masked_score = -1e+30

def exact_dot(left_side, right_side):
    return jnp.dot(left_side, right_side, precision=lax.Precision.HIGHEST, preferred_element_type=jnp.float32)

def layer_norm(inputs, gain_row, shift_row):
    mean_row = lax.optimization_barrier(jnp.mean(inputs, axis=-1, keepdims=True))
    centred = inputs - mean_row
    variance = lax.optimization_barrier(jnp.mean(centred * centred, axis=-1, keepdims=True))
    return centred * lax.rsqrt(variance + norm_epsilon) * gain_row + shift_row

def row_layout(device, seq_device, seq_length, row_count):
    present = (seq_device == device).astype(jnp.int32)
    taken_rows = present * seq_length
    start_row = (jnp.cumsum(taken_rows) - taken_rows).astype(jnp.int32)
    row_index = jnp.arange(row_count, dtype=jnp.int32)[:, None]
    inside = ((present[None, :] > 0) & (row_index >= start_row[None, :]) & (row_index < (start_row + taken_rows)[None, :])).astype(jnp.int32)
    number = jnp.arange(seq_device.shape[0], dtype=jnp.int32)
    segment = lax.optimization_barrier(jnp.sum(inside * number[None, :], axis=1)).astype(jnp.int32)
    position = lax.optimization_barrier(jnp.sum(inside * (row_index - start_row[None, :]), axis=1)).astype(jnp.int32)
    return (segment, position)

def rotary_table(position):
    half_rot = ROT // 2
    frequency = jnp.exp(jnp.arange(half_rot, dtype=jnp.float32) * (-2.0 * math.log(10000.0) / ROT))
    angles = position.astype(jnp.float32)[:, None] * frequency[None, :]
    return (jnp.cos(angles), jnp.sin(angles))

def rotate(values, cosine_table, sine_table):
    half_rot = cosine_table.shape[1]
    first_half = values[..., :half_rot]
    second = values[..., half_rot:2 * half_rot]
    cos_wide = cosine_table[:, None, :]
    sin_wide = sine_table[:, None, :]
    return jnp.concatenate([first_half * cos_wide - second * sin_wide, second * cos_wide + first_half * sin_wide, values[..., 2 * half_rot:]], axis=-1)

def block_forward(params, inputs, segment, position):
    vector_rows, qkv_w, out_w, up_w, down_w = params
    row_count = inputs.shape[0]
    up_rows = FF // D
    attn_in = layer_norm(inputs, vector_rows[0], vector_rows[1])
    mlp_in = layer_norm(inputs, vector_rows[2], vector_rows[3])
    mixed_rows = low_back(exact_dot(low(attn_in), qkv_w) + vector_rows[4:7].reshape(-1))
    cosine_table, sine_table = rotary_table(position)
    query_rows = low(rotate(mixed_rows[:, :D].reshape(row_count, HEADS, HEAD), cosine_table, sine_table))
    key_rows = low(rotate(mixed_rows[:, D:2 * D].reshape(row_count, HEADS, HEAD), cosine_table, sine_table))
    value_rows = low(mixed_rows[:, 2 * D:].reshape(row_count, HEADS, HEAD))
    scores = low_back(jnp.einsum('qhd,khd->hqk', query_rows, key_rows, precision=lax.Precision.HIGHEST) * 0.125)
    row_index = jnp.arange(row_count, dtype=jnp.int32)
    allowed = (segment[:, None] == segment[None, :]) & (row_index[None, :] <= row_index[:, None])
    scores = jnp.where(allowed[None], scores, masked_score)
    shifted = scores - lax.optimization_barrier(jnp.max(scores, axis=2, keepdims=True))
    exp_scores = jnp.exp(shifted)
    probs = exp_scores / lax.optimization_barrier(jnp.sum(exp_scores, axis=2, keepdims=True))
    attended = jnp.einsum('hqk,khd->qhd', low(probs), value_rows, precision=lax.Precision.HIGHEST)
    attended = low(low_back(attended)).reshape(row_count, D)
    attn_out = exact_dot(attended, out_w) + vector_rows[7]
    hidden = low_back(exact_dot(low(mlp_in), up_w) + vector_rows[8:8 + up_rows].reshape(-1))
    activated = low(hidden * (0.5 * (1.0 + lax.erf(hidden * root_half))))
    mlp_out = exact_dot(activated, down_w) + vector_rows[8 + up_rows]
    return inputs + attn_out + mlp_out

def total_loss(params, inputs, cot_rows, segments, positions):

    def one_block(running, pieces):
        block_in, block_cot, segment, position = pieces
        result = block_forward(params, block_in, segment, position)
        return (running + jnp.sum(result * block_cot), result)
    return lax.scan(jax.checkpoint(one_block), jnp.zeros((), jnp.float32), (inputs, cot_rows, segments, positions))

def cut_tiles(matrix):
    height, span_cols = matrix.shape
    return matrix.reshape(height // BLK, BLK, span_cols // BLK, BLK).transpose(0, 2, 1, 3).reshape(-1, BLK, BLK)

def slot_order(owners, slot_total):
    slot_ids = jnp.arange(slot_total, dtype=jnp.int32)
    matches = owners[None, :] == slot_ids[:, None]
    tile_index = lax.optimization_barrier(jnp.sum(jnp.where(matches, jnp.arange(owners.shape[0], dtype=jnp.int32)[None, :], 0), axis=1)).astype(jnp.int32)
    occupied = jnp.any(matches, axis=1)
    return (jnp.where(occupied, tile_index, owners.shape[0]).astype(jnp.int32), occupied)

def arrange(blocks, tile_index):
    padded = jnp.concatenate([blocks, jnp.zeros((1,) + blocks.shape[1:], blocks.dtype)], axis=0)
    return jnp.take(padded, tile_index, axis=0)

def rotated_adam(gradient, weight, left_basis, right_basis, first_state, second_state, occupied):
    turned = jnp.einsum('sji,sjk->sik', left_basis, gradient, precision=lax.Precision.HIGHEST)
    turned = jnp.einsum('sik,skl->sil', turned, right_basis, precision=lax.Precision.HIGHEST)
    new_first = beta_decay * first_state + (1.0 - beta_decay) * turned
    new_second = beta_decay * second_state + (1.0 - beta_decay) * turned * turned
    correction = 1.0 - beta_decay ** STEP
    direction = new_first / correction / (jnp.sqrt(new_second / correction) + adam_epsilon)
    restored = jnp.einsum('sij,sjk->sik', left_basis, direction, precision=lax.Precision.HIGHEST)
    restored = jnp.einsum('sik,slk->sil', restored, right_basis, precision=lax.Precision.HIGHEST)
    new_weight = weight - learning_rate * (restored + weight_decay * weight)
    slot_mask = occupied.astype(jnp.float32)[:, None, None]
    return (slot_mask * new_first, slot_mask * new_second, slot_mask * new_weight)

def plain_adam(gradient, value_rows, first_state, second_state):
    new_first = beta_decay * first_state + (1.0 - beta_decay) * gradient
    new_second = beta_decay * second_state + (1.0 - beta_decay) * gradient * gradient
    correction = 1.0 - beta_decay ** STEP
    new_value = value_rows - learning_rate * (new_first / correction) / (jnp.sqrt(new_second / correction) + adam_epsilon)
    return (new_first, new_second, new_value)

def reference(tokens, cotangent, vec_params, qkv_weight, out_weight, up_weight, down_weight, probe_vec, probe_qkv, probe_out, probe_up, probe_down, seq_device, seq_length, owners, left_bases, right_bases, first_moment, second_moment, vec_first, vec_second):
    params = (vec_params, qkv_weight.astype(jnp.float32), out_weight.astype(jnp.float32), up_weight.astype(jnp.float32), down_weight.astype(jnp.float32))
    inputs = tokens.astype(jnp.float32).reshape(N_DP, LONG, D)
    cot_rows = cotangent.astype(jnp.float32).reshape(N_DP, LONG, D)
    devices = jnp.arange(N_DP, dtype=jnp.int32)
    segments, positions = jax.vmap(lambda device: row_layout(device, seq_device, seq_length, LONG))(devices)

    def loss_of(param_set, input_set):
        return total_loss(param_set, input_set, cot_rows, segments, positions)
    loss_total, pullback, outputs = jax.vjp(loss_of, params, inputs, has_aux=True)
    gradients, input_grad = pullback(jnp.ones((), jnp.float32))

    def grad_of(param_set):
        inner = jax.vjp(lambda inner_set: total_loss(inner_set, inputs, cot_rows, segments, positions)[0], param_set)[1]
        return inner(jnp.ones((), jnp.float32))[0]
    second_pull = jax.vjp(grad_of, params)[1]
    probe_set = (probe_vec, probe_qkv.astype(jnp.float32), probe_out.astype(jnp.float32), probe_up.astype(jnp.float32), probe_down.astype(jnp.float32))
    curvature = lax.map(lambda single_probe: second_pull(single_probe)[0], probe_set)
    tile_index, occupied = slot_order(owners, SLOTS)
    grad_tiles = jnp.concatenate([cut_tiles(gradients[1]), cut_tiles(gradients[2]), cut_tiles(gradients[3]), cut_tiles(gradients[4])], axis=0)
    weight_grads = arrange(grad_tiles, tile_index)
    weight_tiles = jnp.concatenate([cut_tiles(params[1]), cut_tiles(params[2]), cut_tiles(params[3]), cut_tiles(params[4])], axis=0)
    weight_slots = arrange(weight_tiles, tile_index)
    new_first, new_second, new_weights = rotated_adam(weight_grads, weight_slots, left_bases, right_bases, first_moment, second_moment, occupied)
    new_weights_low = new_weights.astype(jnp.bfloat16)

    def curvature_slots(pieces):
        tiles_all = jnp.concatenate([cut_tiles(pieces[0]), cut_tiles(pieces[1]), cut_tiles(pieces[2]), cut_tiles(pieces[3])], axis=0)
        return arrange(tiles_all, tile_index)
    curvature_blocks = lax.map(curvature_slots, (curvature[1], curvature[2], curvature[3], curvature[4]))
    vec_new_first, vec_new_second, vec_new = plain_adam(gradients[0], vec_params, vec_first, vec_second)
    vector_state = jnp.stack([gradients[0], vec_new_first], axis=0)
    along_probe = jnp.zeros((NPROBE,), jnp.float32)
    curve_probe = jnp.zeros((NPROBE,), jnp.float32)
    for leaf_index in range(5):
        along_probe = along_probe + lax.optimization_barrier(jnp.sum(gradients[leaf_index][None] * probe_set[leaf_index], axis=(1, 2)))
        curve_probe = curve_probe + lax.optimization_barrier(jnp.sum(curvature[leaf_index] * probe_set[leaf_index], axis=(1, 2)))
    probe_dots = jnp.stack([along_probe, curve_probe], axis=1)
    block_output = outputs.reshape(TOKENS, D).astype(jnp.bfloat16)
    return (block_output, input_grad.reshape(TOKENS, D), weight_grads, new_first, new_second, new_weights, new_weights_low, curvature_blocks, vector_state, vec_new_second, vec_new, curvature[0], probe_dots)
```

```python
import math

import jax
import jax.numpy as jnp
from jax import lax
from jax.experimental import pallas as pl
from jax.experimental.pallas import tpu as pltpu
from jax.sharding import PartitionSpec as P

HEAD = 64
ROT = 16
BLK = 384
STEP = 4


beta_decay = 0.5
learning_rate = 0.05
weight_decay = 0.01
adam_epsilon = 1e-08
norm_epsilon = 1e-05
root_half = 0.7071067811865476
density_scale = 0.3989422804014327
masked_score = -1e30


def product(pattern, left_side, right_side):
    if left_side.dtype == jnp.bfloat16 and right_side.dtype == jnp.bfloat16:
        return jnp.einsum(pattern, left_side, right_side, preferred_element_type=jnp.float32)
    return jnp.einsum(
        pattern,
        left_side,
        right_side,
        precision=lax.Precision.HIGHEST,
        preferred_element_type=jnp.float32,
    )


def normalize(inputs):
    mean_row = jnp.mean(inputs, axis=1, keepdims=True)
    centred = inputs - mean_row
    variance = jnp.mean(centred * centred, axis=1, keepdims=True)
    norm_scale = lax.rsqrt(variance + norm_epsilon)
    return (centred * norm_scale, norm_scale)


def norm_back(grad_normed, normed, norm_scale):
    mean_grad = jnp.mean(grad_normed, axis=1, keepdims=True)
    mean_cross = jnp.mean(grad_normed * normed, axis=1, keepdims=True)
    return norm_scale * (grad_normed - mean_grad - normed * mean_cross)


def row_layout(device, seq_device, seq_length, row_count):
    present = (seq_device == device).astype(jnp.int32)
    taken_rows = present * seq_length
    start_row = jnp.cumsum(taken_rows) - taken_rows
    row_index = jnp.arange(row_count, dtype=jnp.int32)[:, None]
    inside = (
        (present[None, :] > 0)
        & (row_index >= start_row[None, :])
        & (row_index < (start_row + taken_rows)[None, :])
    ).astype(jnp.int32)
    number = jnp.arange(seq_device.shape[0], dtype=jnp.int32)
    segment = jnp.sum(inside * number[None, :], axis=1)
    position = jnp.sum(inside * (row_index - start_row[None, :]), axis=1)
    return (segment, position)


def rotary_table(position):
    half_rot = ROT // 2
    frequency = jnp.exp(jnp.arange(half_rot, dtype=jnp.float32) * (-2.0 * math.log(10000.0) / ROT))
    angles = position.astype(jnp.float32)[:, None] * frequency[None, :]
    return (jnp.cos(angles), jnp.sin(angles))


def rotate(values, cosine_table, sine_table, reverse):
    half_rot = cosine_table.shape[1]
    first_half = values[..., :half_rot]
    second = values[..., half_rot : 2 * half_rot]
    cos_wide = cosine_table[:, None, :]
    sin_wide = sine_table[:, None, :]
    if reverse:
        new_first = first_half * cos_wide + second * sin_wide
        new_second = second * cos_wide - first_half * sin_wide
    else:
        new_first = first_half * cos_wide - second * sin_wide
        new_second = second * cos_wide + first_half * sin_wide
    return jnp.concatenate([new_first, new_second, values[..., 2 * half_rot :]], axis=-1)


def swap_major(values):
    return jnp.transpose(values, (1, 0, 2))


def cut_tiles(matrix):
    height, span_cols = matrix.shape
    return (
        matrix.reshape(height // BLK, BLK, span_cols // BLK, BLK)
        .transpose(0, 2, 1, 3)
        .reshape(-1, BLK, BLK)
    )


def slot_order(owners, slot_total):
    slot_ids = jnp.arange(slot_total, dtype=jnp.int32)
    matches = owners[None, :] == slot_ids[:, None]
    tile_index = jnp.sum(
        jnp.where(matches, jnp.arange(owners.shape[0], dtype=jnp.int32)[None, :], 0), axis=1
    )
    occupied = jnp.any(matches, axis=1)
    return (jnp.where(occupied, tile_index, owners.shape[0]), occupied)


def arrange(blocks, tile_index):
    padded = jnp.concatenate([blocks, jnp.zeros((1,) + blocks.shape[1:], blocks.dtype)], axis=0)
    return jnp.take(padded, tile_index, axis=0)


def rotated_adam(gradient, weight, left_basis, right_basis, first_state, second_state, occupied):
    turned = jnp.einsum("sji,sjk->sik", left_basis, gradient, precision=lax.Precision.HIGHEST)
    turned = jnp.einsum("sik,skl->sil", turned, right_basis, precision=lax.Precision.HIGHEST)
    new_first = beta_decay * first_state + (1.0 - beta_decay) * turned
    new_second = beta_decay * second_state + (1.0 - beta_decay) * turned * turned
    correction = 1.0 - beta_decay**STEP
    direction = new_first / correction / (jnp.sqrt(new_second / correction) + adam_epsilon)
    restored = jnp.einsum("sij,sjk->sik", left_basis, direction, precision=lax.Precision.HIGHEST)
    restored = jnp.einsum("sik,slk->sil", restored, right_basis, precision=lax.Precision.HIGHEST)
    new_weight = weight - learning_rate * (restored + weight_decay * weight)
    slot_mask = occupied.astype(jnp.float32)[:, None, None]
    return (slot_mask * new_first, slot_mask * new_second, slot_mask * new_weight)


def plain_adam(gradient, value_rows, first_state, second_state):
    new_first = beta_decay * first_state + (1.0 - beta_decay) * gradient
    new_second = beta_decay * second_state + (1.0 - beta_decay) * gradient * gradient
    correction = 1.0 - beta_decay**STEP
    new_value = value_rows - learning_rate * (new_first / correction) / (
        jnp.sqrt(new_second / correction) + adam_epsilon
    )
    return (new_first, new_second, new_value)


def local_any(
    tokens,
    cotangent,
    vec_params,
    qkv_weight,
    out_weight,
    up_weight,
    down_weight,
    probe_vec,
    probe_qkv,
    probe_out,
    probe_up,
    probe_down,
    seq_device,
    seq_length,
    owners,
    left_bases,
    right_bases,
    first_moment,
    second_moment,
    vec_first,
    vec_second,
):
    row_count, model_width = tokens.shape
    head_count = model_width // HEAD
    up_rows = up_weight.shape[1] // model_width
    device = lax.axis_index("dp")
    segment, position = row_layout(device, seq_device, seq_length, row_count)
    cosine_table, sine_table = rotary_table(position)
    row_index = jnp.arange(row_count, dtype=jnp.int32)
    allowed = (segment[:, None] == segment[None, :]) & (row_index[None, :] <= row_index[:, None])
    drift_vec = probe_vec[0]
    drift_qkv = probe_qkv[0]
    drift_out = probe_out[0]
    drift_up = probe_up[0]
    drift_down = probe_down[0]
    inputs = tokens.astype(jnp.float32)
    cot_rows = cotangent.astype(jnp.float32)
    normed, norm_scale = normalize(inputs)
    attn_in = normed * vec_params[0] + vec_params[1]
    drift_attn_in = normed * drift_vec[0] + drift_vec[1]
    mlp_in = normed * vec_params[2] + vec_params[3]
    drift_mlp_in = normed * drift_vec[2] + drift_vec[3]
    attn_low = attn_in.astype(jnp.bfloat16)
    mlp_low = mlp_in.astype(jnp.bfloat16)
    mixed_rows = product("ij,jk->ik", attn_low, qkv_weight) + vec_params[4:7].reshape(-1)
    drift_mixed = (
        product("ij,jk->ik", drift_attn_in, qkv_weight)
        + product("ij,jk->ik", attn_low, drift_qkv)
        + drift_vec[4:7].reshape(-1)
    )

    def split_heads(matrix, column_group):
        return matrix[:, column_group * model_width : (column_group + 1) * model_width].reshape(
            row_count, head_count, HEAD
        )

    query_rows = rotate(split_heads(mixed_rows, 0), cosine_table, sine_table, False)
    key_rows = rotate(split_heads(mixed_rows, 1), cosine_table, sine_table, False)
    value_rows = split_heads(mixed_rows, 2)
    drift_query = rotate(split_heads(drift_mixed, 0), cosine_table, sine_table, False)
    drift_key = rotate(split_heads(drift_mixed, 1), cosine_table, sine_table, False)
    drift_value = split_heads(drift_mixed, 2)
    grad_att = product("ij,kj->ik", cotangent, out_weight)
    drift_grad_att = product("ij,kj->ik", cotangent, drift_out)
    grad_att_low = grad_att.astype(jnp.bfloat16)

    def attend(pieces):
        query_block, key_block, value_block, drift_q, drift_k, drift_v, grad_out, drift_grad_out = (
            pieces
        )
        scores = product("ij,kj->ik", query_block, key_block) * 0.125
        drift_scores = (
            product("ij,kj->ik", drift_q, key_block) + product("ij,kj->ik", query_block, drift_k)
        ) * 0.125
        scores = jnp.where(allowed, scores, masked_score)
        shifted = scores - jnp.max(scores, axis=1, keepdims=True)
        exp_scores = jnp.exp(shifted)
        probs = exp_scores / jnp.sum(exp_scores, axis=1, keepdims=True)
        drift_probs = probs * (drift_scores - jnp.sum(probs * drift_scores, axis=1, keepdims=True))
        probs_low = probs.astype(jnp.bfloat16)
        attended_head = product("ij,jk->ik", probs_low, value_block)
        drift_attended_head = product("ij,jk->ik", drift_probs, value_block) + product(
            "ij,jk->ik", probs_low, drift_v
        )
        grad_probs = product("ij,kj->ik", grad_out, value_block)
        drift_grad_probs = product("ij,kj->ik", drift_grad_out, value_block) + product(
            "ij,kj->ik", grad_out, drift_v
        )
        grad_value_head = product("ij,ik->jk", probs_low, grad_out)
        drift_grad_value_head = product("ij,ik->jk", drift_probs, grad_out) + product(
            "ij,ik->jk", probs_low, drift_grad_out
        )
        centre = jnp.sum(probs * grad_probs, axis=1, keepdims=True)
        drift_centre = jnp.sum(
            drift_probs * grad_probs + probs * drift_grad_probs, axis=1, keepdims=True
        )
        grad_scores = probs * (grad_probs - centre)
        drift_grad_scores = drift_probs * (grad_probs - centre) + probs * (
            drift_grad_probs - drift_centre
        )
        scores_low = grad_scores.astype(jnp.bfloat16)
        grad_query_head = product("ij,jk->ik", scores_low, key_block) * 0.125
        drift_grad_query_head = (
            product("ij,jk->ik", drift_grad_scores, key_block)
            + product("ij,jk->ik", scores_low, drift_k)
        ) * 0.125
        grad_key_head = product("ij,ik->jk", scores_low, query_block) * 0.125
        drift_grad_key_head = (
            product("ij,ik->jk", drift_grad_scores, query_block)
            + product("ij,ik->jk", scores_low, drift_q)
        ) * 0.125
        return (
            attended_head,
            drift_attended_head,
            grad_query_head,
            grad_key_head,
            grad_value_head,
            drift_grad_query_head,
            drift_grad_key_head,
            drift_grad_value_head,
        )

    results = lax.map(
        attend,
        (
            swap_major(query_rows.astype(jnp.bfloat16)),
            swap_major(key_rows.astype(jnp.bfloat16)),
            swap_major(value_rows.astype(jnp.bfloat16)),
            swap_major(drift_query),
            swap_major(drift_key),
            swap_major(drift_value),
            swap_major(grad_att_low.reshape(row_count, head_count, HEAD)),
            swap_major(drift_grad_att.reshape(row_count, head_count, HEAD)),
        ),
    )
    attended = swap_major(results[0]).reshape(row_count, model_width)
    drift_attended = swap_major(results[1]).reshape(row_count, model_width)
    grad_query = rotate(swap_major(results[2]), cosine_table, sine_table, True).reshape(
        row_count, model_width
    )
    grad_key = rotate(swap_major(results[3]), cosine_table, sine_table, True).reshape(
        row_count, model_width
    )
    grad_value = swap_major(results[4]).reshape(row_count, model_width)
    drift_grad_query = rotate(swap_major(results[5]), cosine_table, sine_table, True).reshape(
        row_count, model_width
    )
    drift_grad_key = rotate(swap_major(results[6]), cosine_table, sine_table, True).reshape(
        row_count, model_width
    )
    drift_grad_value = swap_major(results[7]).reshape(row_count, model_width)
    grad_mixed_low = jnp.concatenate([grad_query, grad_key, grad_value], axis=1).astype(
        jnp.bfloat16
    )
    drift_grad_mixed = jnp.concatenate([drift_grad_query, drift_grad_key, drift_grad_value], axis=1)
    att_low = attended.astype(jnp.bfloat16)
    attn_out = product("ij,jk->ik", att_low, out_weight) + vec_params[7]
    hidden = product("ij,jk->ik", mlp_low, up_weight) + vec_params[8 : 8 + up_rows].reshape(-1)
    drift_hidden = (
        product("ij,jk->ik", drift_mlp_in, up_weight)
        + product("ij,jk->ik", mlp_low, drift_up)
        + drift_vec[8 : 8 + up_rows].reshape(-1)
    )
    cumulative = 0.5 * (1.0 + lax.erf(hidden * root_half))
    density = jnp.exp(-0.5 * hidden * hidden) * density_scale
    activated = hidden * cumulative
    gelu_slope = cumulative + hidden * density
    gelu_bend = density * (2.0 - hidden * hidden)
    act_low = activated.astype(jnp.bfloat16)
    drift_act = gelu_slope * drift_hidden
    mlp_out = product("ij,jk->ik", act_low, down_weight) + vec_params[8 + up_rows]
    block_output = (inputs + attn_out + mlp_out).astype(jnp.bfloat16)
    grad_down = product("ij,ik->jk", act_low, cotangent)
    drift_grad_down = product("ij,ik->jk", drift_act, cotangent)
    grad_act = product("ij,kj->ik", cotangent, down_weight)
    drift_grad_act = product("ij,kj->ik", cotangent, drift_down)
    grad_hidden = grad_act * gelu_slope
    drift_grad_hidden = drift_grad_act * gelu_slope + grad_act * gelu_bend * drift_hidden
    grad_hidden_low = grad_hidden.astype(jnp.bfloat16)
    grad_up = product("ij,ik->jk", mlp_low, grad_hidden_low)
    drift_grad_up = product("ij,ik->jk", drift_mlp_in, grad_hidden_low) + product(
        "ij,ik->jk", mlp_low, drift_grad_hidden
    )
    grad_mlp_in = product("ij,kj->ik", grad_hidden_low, up_weight)
    drift_grad_mlp_in = product("ij,kj->ik", drift_grad_hidden, up_weight) + product(
        "ij,kj->ik", grad_hidden_low, drift_up
    )
    grad_out_w = product("ij,ik->jk", att_low, cotangent)
    drift_grad_out_w = product("ij,ik->jk", drift_attended, cotangent)
    grad_qkv = product("ij,ik->jk", attn_low, grad_mixed_low)
    drift_grad_qkv = product("ij,ik->jk", drift_attn_in, grad_mixed_low) + product(
        "ij,ik->jk", attn_low, drift_grad_mixed
    )
    grad_attn_in = product("ij,kj->ik", grad_mixed_low, qkv_weight)
    drift_grad_attn_in = product("ij,kj->ik", drift_grad_mixed, qkv_weight) + product(
        "ij,kj->ik", grad_mixed_low, drift_qkv
    )
    grad_weighted = grad_attn_in * vec_params[0] + grad_mlp_in * vec_params[2]
    input_grad = cot_rows + norm_back(grad_weighted, normed, norm_scale)
    out_sum = jnp.sum(cot_rows, axis=0)[None]
    zero_row = jnp.zeros((1, model_width), jnp.float32)
    vec_grad = jnp.concatenate(
        [
            jnp.sum(grad_attn_in * normed, axis=0)[None],
            jnp.sum(grad_attn_in, axis=0)[None],
            jnp.sum(grad_mlp_in * normed, axis=0)[None],
            jnp.sum(grad_mlp_in, axis=0)[None],
            jnp.sum(grad_mixed_low, axis=0, dtype=jnp.float32).reshape(3, model_width),
            out_sum,
            jnp.sum(grad_hidden_low, axis=0, dtype=jnp.float32).reshape(up_rows, model_width),
            out_sum,
        ],
        axis=0,
    )
    vec_drift = jnp.concatenate(
        [
            jnp.sum(drift_grad_attn_in * normed, axis=0)[None],
            jnp.sum(drift_grad_attn_in, axis=0)[None],
            jnp.sum(drift_grad_mlp_in * normed, axis=0)[None],
            jnp.sum(drift_grad_mlp_in, axis=0)[None],
            jnp.sum(drift_grad_mixed, axis=0).reshape(3, model_width),
            zero_row,
            jnp.sum(drift_grad_hidden, axis=0).reshape(up_rows, model_width),
            zero_row,
        ],
        axis=0,
    )
    along_probe = jnp.sum(vec_grad * drift_vec)
    curve_probe = jnp.sum(vec_drift * drift_vec)
    for gradient, drift_gradient, direction_set in (
        (grad_qkv, drift_grad_qkv, drift_qkv),
        (grad_out_w, drift_grad_out_w, drift_out),
        (grad_up, drift_grad_up, drift_up),
        (grad_down, drift_grad_down, drift_down),
    ):
        along_probe = along_probe + jnp.sum(gradient * direction_set.astype(jnp.float32))
        curve_probe = curve_probe + jnp.sum(drift_gradient * direction_set.astype(jnp.float32))
    dots = jnp.stack([along_probe, curve_probe])
    grad_tiles = jnp.concatenate(
        [cut_tiles(grad_qkv), cut_tiles(grad_out_w), cut_tiles(grad_up), cut_tiles(grad_down)],
        axis=0,
    )
    curve_tiles = jnp.concatenate(
        [
            cut_tiles(drift_grad_qkv),
            cut_tiles(drift_grad_out_w),
            cut_tiles(drift_grad_up),
            cut_tiles(drift_grad_down),
        ],
        axis=0,
    )
    slot_dev = left_bases.shape[0]
    slot_total = slot_dev * lax.axis_size("dp")
    tile_index, occupied = slot_order(owners, slot_total)
    slot_grad = arrange(grad_tiles, tile_index)
    slot_curve = arrange(curve_tiles, tile_index)
    own_grad, own_curve = (
        lax.psum_scatter(slot_grad, "dp", scatter_dimension=0, tiled=True),
        lax.psum_scatter(slot_curve, "dp", scatter_dimension=0, tiled=True),
    )
    vec_total, vec_curve, dot_total = lax.psum((vec_grad, vec_drift, dots), "dp")
    all_dots = lax.all_gather(dot_total[None, :], "probe", axis=0, tiled=True)
    own_index = lax.dynamic_slice_in_dim(tile_index, device * slot_dev, slot_dev)
    own_used = lax.dynamic_slice_in_dim(occupied, device * slot_dev, slot_dev)
    weight_tiles = jnp.concatenate(
        [
            cut_tiles(qkv_weight),
            cut_tiles(out_weight),
            cut_tiles(up_weight),
            cut_tiles(down_weight),
        ],
        axis=0,
    )
    own_weight = arrange(weight_tiles, own_index).astype(jnp.float32)
    new_first, new_second, new_weights = rotated_adam(
        own_grad, own_weight, left_bases, right_bases, first_moment, second_moment, own_used
    )
    new_weights_low = new_weights.astype(jnp.bfloat16)
    vec_new_first, vec_new_second, vec_new = plain_adam(
        vec_total, vec_params, vec_first, vec_second
    )
    vector_state = jnp.stack([vec_total, vec_new_first], axis=0)
    return (
        block_output,
        input_grad,
        own_grad,
        new_first,
        new_second,
        new_weights,
        new_weights_low,
        own_curve[None],
        vector_state,
        vec_new_second,
        vec_new,
        vec_curve[None],
        all_dots,
    )


f32 = jnp.float32
bf16 = jnp.bfloat16
VMEM_SHARD = 60 << 20
HEAD_A = (0, 1, 7, 8, 3, 4, 10, 11)
HEAD_B = (6, 6, 2, 2, 9, 9, 5, 5)
ARRIVE = ((1, 2, 3), (0, 2, 3), (3, 1, 0), (2, 1, 0))


def fits_tp(mesh):
    return mesh.shape["dp"] == 8 and mesh.shape["probe"] == 4


def device_table():
    rows = []
    for device in range(8):
        z, x = device // 2, device % 2
        levels = (z,) + ARRIVE[z]
        order = [2 * level + x for level in levels] + [2 * level + 1 - x for level in levels]
        for probe in range(4):
            rows.append([device, HEAD_A[device], HEAD_B[device], probe % 2, x, probe // 2, z % 2, 0] + order)
    return rows


def is_short(seq_device, seq_length, group, rows):
    longest = jnp.int32(0)
    for i in range(seq_device.shape[0]):
        longest = jnp.maximum(longest, jnp.where(seq_device[i] == group, seq_length[i], 0))
    return (longest < rows).astype(jnp.int32)


def in_hbm(value):
    return pltpu.with_memory_space_constraint(value, pltpu.HBM)


def dot_nt(left, right):
    return lax.dot_general(left, right, (((1,), (1,)), ((), ())), preferred_element_type=f32)


def dot_nn(left, right):
    return lax.dot_general(left, right, (((1,), (0,)), ((), ())), preferred_element_type=f32)


def rotate_rows(ref, base, cos, sin, reverse):
    up, low = ref[base : base + 8, :], ref[base + 8 : base + 16, :]
    if reverse:
        ref[base : base + 8, :] = up * cos + low * sin
        ref[base + 8 : base + 16, :] = low * cos - up * sin
    else:
        ref[base : base + 8, :] = up * cos - low * sin
        ref[base + 8 : base + 16, :] = low * cos + up * sin


def mask_rows(bias, short, rows):
    for start in range(0, rows, 128):
        row = lax.broadcasted_iota(jnp.int32, (128, rows), 0) + start
        col = lax.broadcasted_iota(jnp.int32, (128, rows), 1)
        first = jnp.where(short == 1, start, 0)
        bias[start : start + 128, :] = jnp.where((col >= first) & (col <= row), 0.0, masked_score)


def one_row(block, index):
    rows = lax.broadcasted_iota(jnp.int32, block.shape, 0)
    return jnp.sum(jnp.where(rows == index, block, 0.0), axis=0, keepdims=True)


def prepare_kernel(info, up_0, up_1, dup_0, dup_1, down, ddown, qkv, dqkv, out_w, dout_w, vec, dvec, uwt, dwt, bias_u, wat, oat, bias_a, turn, turn_h):
    j = pl.program_id(0)
    device = info[0]
    row = lax.broadcasted_iota(jnp.int32, (48, 128), 0) + (device * 48) % 128
    lane = lax.broadcasted_iota(jnp.int32, (48, 128), 1)
    pick_0, pick_1 = (lane == row).astype(bf16), (lane == row - 128).astype(bf16)
    for part, (first, second, below, bias) in enumerate(((up_0, up_1, down, vec), (dup_0, dup_1, ddown, dvec))):
        uwt[part, 0] = (dot_nt(pick_0, first[...]) + dot_nt(pick_1, second[...])).astype(bf16)
        dwt[part, 0] = below[...]
        line = one_row(bias[8:12, pl.ds(pl.multiple_of(384 * (j % 2), 128), 384)], j // 2)
        turn[...] = jnp.transpose(jnp.broadcast_to(line, (128, 384)))
        bias_u[part, 0] = turn[pl.ds(pl.multiple_of(device * 48, 16), 48), :]

    @pl.when(j < 6)
    def _():
        head = info[1 + j // 3]
        row = lax.broadcasted_iota(jnp.int32, (64, 128), 0) + (head % 2) * 64
        pick = (lax.broadcasted_iota(jnp.int32, (64, 128), 1) == row).astype(bf16)
        rows, drows = dot_nt(pick, qkv[...]).astype(bf16), dot_nt(pick, dqkv[...]).astype(bf16)
        wat[:64, :768] = rows
        wat[:64, 768:] = jnp.zeros((64, 768), bf16)
        wat[64:, :768] = drows
        wat[64:, 768:] = rows
        oat[:64, :] = out_w[...]
        oat[64:, :] = dout_w[...]
        for part, bias in enumerate((vec, dvec)):
            line = one_row(bias[4:7, pl.ds(pl.multiple_of(128 * (head // 2), 128), 128)], j % 3)
            turn_h[...] = jnp.transpose(jnp.broadcast_to(line, (128, 128)))
            bias_a[part * 64 : part * 64 + 64, :] = turn_h[pl.ds(pl.multiple_of((head % 2) * 64, 64), 64), :]


def prepare(info, qkv, dqkv, out_w, dout_w, up, dup, down, ddown, vec, dvec):
    def at_head(i):
        return jnp.minimum(i, 5)

    whole = pl.BlockSpec(memory_space=pltpu.VMEM)
    up_0 = pl.BlockSpec((768, 128), lambda i, info: (0, 3 * i + (info[0] * 48) // 128))
    up_1 = pl.BlockSpec((768, 128), lambda i, info: (0, 3 * i + jnp.minimum((info[0] * 48) // 128 + 1, 2)))
    down_spec = pl.BlockSpec((48, 768), lambda i, info: (8 * i + info[0], 0))
    qkv_spec = pl.BlockSpec((768, 128), lambda i, info: (0, 6 * (at_head(i) % 3) + info[1 + at_head(i) // 3] // 2))
    out_spec = pl.BlockSpec((64, 768), lambda i, info: (info[1 + at_head(i) // 3], 0))
    uwt, dwt, bias_u, wat, oat, bias_a = pl.pallas_call(
        prepare_kernel,
        out_shape=[
            jax.ShapeDtypeStruct((2, 8, 48, 768), bf16),
            jax.ShapeDtypeStruct((2, 8, 48, 768), bf16),
            jax.ShapeDtypeStruct((2, 8, 48, 128), f32),
            jax.ShapeDtypeStruct((768, 1536), bf16),
            jax.ShapeDtypeStruct((256, 768), bf16),
            jax.ShapeDtypeStruct((768, 128), f32),
        ],
        grid_spec=pltpu.PrefetchScalarGridSpec(
            num_scalar_prefetch=1,
            grid=(8,),
            in_specs=[up_0, up_1, up_0, up_1, down_spec, down_spec, qkv_spec, qkv_spec, out_spec, out_spec, whole, whole],
            out_specs=[
                pl.BlockSpec((2, 1, 48, 768), lambda i, info: (0, i, 0, 0)),
                pl.BlockSpec((2, 1, 48, 768), lambda i, info: (0, i, 0, 0)),
                pl.BlockSpec((2, 1, 48, 128), lambda i, info: (0, i, 0, 0)),
                pl.BlockSpec((128, 1536), lambda i, info: (at_head(i), 0)),
                pl.BlockSpec((128, 768), lambda i, info: (at_head(i) // 3, 0)),
                pl.BlockSpec((128, 128), lambda i, info: (at_head(i), 0)),
            ],
            scratch_shapes=[pltpu.VMEM((384, 128), f32), pltpu.VMEM((128, 128), f32)],
        ),
        compiler_params=pltpu.CompilerParams(vmem_limit_bytes=VMEM_SHARD),
        cost_estimate=pl.CostEstimate(flops=10**9, bytes_accessed=2 * 10**7, transcendentals=0),
        name="prepare",
    )(info, *(in_hbm(value) for value in (up, up, dup, dup, down, ddown, qkv, dqkv, out_w, dout_w)), vec, dvec)
    return (uwt.reshape(768, 768), dwt.reshape(768, 768), bias_u.reshape(768, 128), wat, oat, bias_a)


def wide(column):
    return jnp.concatenate([column] * 4, axis=1)


def shard_kernel(heads, first, index, *refs):
    refs = list(refs)
    info, seq_device, seq_length = refs[:3]
    refs = refs[3:]
    mine_h, other_h, vec, dvec, cos_ref, sin_ref = refs[:6]
    weights_h = refs[6:12]
    refs = refs[12:]
    count = heads + 3
    old_h = None if first else refs[:count]
    refs = refs if first else refs[count:]
    out_h = refs[:count]
    refs = refs[count:]
    mine, other, wat, bias_a, oat, uwt, dwt, bias_u = refs[:8]
    new = refs[8 : 8 + count]
    sem = refs[8 + count]
    (nb, ones, lhs_a, ml, dm, cb, mask, proj, gat, qt, kt, ks, vt, vs, gt, qn, gn, gq, gk, gv, head_g, head_a, hid, act, mlp_a, mlp_g, one, two) = refs[9 + count :]
    core = info[3]
    short = is_short(seq_device, seq_length, info[8 + index], 512)
    width = 768
    gain_a, shift_a, gain_m, shift_m = (vec[i : i + 1, :] for i in range(4))
    dgain_a, dshift_a, dgain_m, dshift_m = (dvec[i : i + 1, :] for i in range(4))
    acc_m, acc_c, acc_r = new[heads], new[heads + 1], new[heads + 2]
    wat_h, bias_ah, oat_h, uwt_h, dwt_h, bias_uh = weights_h
    lead = heads * 384
    pairs = [
        (mine_h, mine),
        (other_h, other),
        (uwt_h, uwt),
        (dwt_h, dwt),
        (bias_uh, bias_u),
        (wat_h.at[:lead], wat),
        (oat_h.at[: heads * 128], oat),
        (bias_ah.at[:lead], bias_a),
    ]
    if not first:
        pairs += [(old_h[slot], new[slot]) for slot in [heads, heads + 1, heads + 2] + list(range(heads))]
    arrivals = [pltpu.make_async_copy(source, target, sem.at[i]) for i, (source, target) in enumerate(pairs)]
    for copy in arrivals:
        copy.start()
    ones[...] = jnp.ones((512, 128), bf16)
    mask_rows(mask, short, 512)

    def arrived(*which):
        for i in which:
            if i < len(arrivals):
                arrivals[i].wait()

    def load(ref, cot_ref, base, count):
        def step(i, carry):
            src = pl.ds(pl.multiple_of(i * 64, 64), 64)
            dst = pl.ds(pl.multiple_of(base + i * 64, 64), 64)
            rows = ref[src, :width].astype(f32)
            centred = rows - jnp.mean(rows, axis=1, keepdims=True)
            variance = jnp.mean(centred * centred, axis=1, keepdims=True)
            normed = centred * lax.rsqrt(variance + norm_epsilon)
            nb[dst, :] = normed.astype(bf16)
            lhs_a[dst, :width] = (normed * gain_a + shift_a).astype(bf16)
            lhs_a[dst, width:] = (normed * dgain_a + dshift_a).astype(bf16)
            ml[dst, :] = (normed * gain_m + shift_m).astype(bf16)
            dm[dst, :] = (normed * dgain_m + dshift_m).astype(bf16)
            cb[dst, :] = cot_ref[src, :].astype(bf16)
            return carry

        lax.fori_loop(0, count, step, 0)

    if first:
        arrived(0, 1)
        load(mine, other, 0, 8)
    else:
        arrived(0)
        load(mine, mine.at[:, width:], core * 256, 4)
        arrived(1)
        load(other, other.at[:, width:], (1 - core) * 256, 4)

    def add(slot, rows, value):
        new[slot][rows, :] = value if first else new[slot][rows, :] + value

    def fold(carry, size, slot, at, tops, w_rows, dw_rows, dgain, dshift, c_rows):
        grad_at, curve_at = at
        top, low = tops
        p_two, q_two = two[top, :], two[low, :]
        add(slot, grad_at, one[top, :])
        add(slot, curve_at, one[low, :] + dgain * p_two + dshift * c_rows)
        w_wide = w_rows.astype(f32)
        part = w_wide * q_two + dw_rows.astype(f32) * p_two
        drift, plain = carry
        drift = drift + jnp.sum(part.reshape(size // 8, 8, width), axis=0)
        plain = plain + jnp.sum((w_wide * p_two).reshape(size // 8, 8, width), axis=0)
        return (drift, plain)

    arrived(2, 3, 4)
    hid[...] = dot_nt(uwt[...], ml[...])
    act[...] = dot_nt(dwt[...], cb[...])
    hid[384:, :] += dot_nt(uwt[:384, :], dm[...])

    def gelu(i, carry):
        top = pl.ds(pl.multiple_of(i * 32, 32), 32)
        low = pl.ds(pl.multiple_of(384 + i * 32, 32), 32)
        hidden, dhidden = hid[top, :] + wide(bias_u[top, :]), hid[low, :] + wide(bias_u[low, :])
        grad_act, dgrad_act = act[top, :], act[low, :]
        cumulative = 0.5 * (1.0 + lax.erf(hidden * root_half))
        density = jnp.exp(-0.5 * hidden * hidden) * density_scale
        slope = cumulative + hidden * density
        bend = density * (2.0 - hidden * hidden)
        mlp_a[top, :] = (hidden * cumulative).astype(bf16)
        mlp_a[low, :] = (slope * dhidden).astype(bf16)
        mlp_g[top, :] = (grad_act * slope).astype(bf16)
        mlp_g[low, :] = (dgrad_act * slope + grad_act * bend * dhidden).astype(bf16)
        return carry

    lax.fori_loop(0, 12, gelu, 0)
    one[...] = dot_nn(mlp_g[...], ml[...])
    two[...] = dot_nn(mlp_g[...], nb[...])
    sums = dot_nn(mlp_g[...], ones[...])
    arrived(8, 9, 10)
    add(heads + 1, slice(768, 1536), sums)
    proj[0:384, 0:128] = sums[:384, :]

    def fold_m(i, carry):
        top = pl.ds(pl.multiple_of(i * 64, 64), 64)
        low = pl.ds(pl.multiple_of(384 + i * 64, 64), 64)
        return fold(carry, 64, heads, (top, low), (top, low), uwt[top, :], uwt[low, :], dgain_m, dshift_m, proj[top, 0:1])

    blank = jnp.zeros((8, width), f32)
    carry_m = (blank, blank) if first else (acc_r[8:16, :], acc_r[24:32, :])
    acc_r[8:16, :], acc_r[24:32, :] = lax.fori_loop(0, 6, fold_m, carry_m)
    one[...] = dot_nn(mlp_a[...], cb[...])
    add(heads, slice(768, 1536), one[...])
    leave_m = pltpu.make_async_copy(acc_m, out_h[heads], sem.at[0])
    leave_m.start()

    arrived(5, 6, 7)
    cos, sin = cos_ref[short], sin_ref[short]
    proj[...] = dot_nt(wat[...], lhs_a[...])
    gat[...] = dot_nt(oat[...], cb[...])
    arrived(*range(11, 11 + heads))
    carry_r = (blank, blank) if first else (acc_r[0:8, :], acc_r[16:24, :])
    for head in range(heads):
        base = head * 384
        proj[base : base + 384, :] += wide(bias_a[base : base + 384, :])
        for part in (0, 64, 128, 192):
            rotate_rows(proj, base + part, cos, sin, False)
        q_rows = proj[base : base + 128, :] * 0.125
        qt[...] = q_rows.astype(bf16)
        qn[...] = jnp.transpose(q_rows).astype(bf16)
        kt[...] = proj[base + 128 : base + 256, :].astype(bf16)
        ks[...] = jnp.concatenate([kt[64:, :], kt[:64, :]], axis=0)
        vt[...] = proj[base + 256 : base + 384, :].astype(bf16)
        vs[...] = jnp.concatenate([vt[64:, :], vt[:64, :]], axis=0)
        g_rows = gat[head * 128 : head * 128 + 128, :]
        gt[...] = g_rows.astype(bf16)
        gn[...] = jnp.transpose(g_rows).astype(bf16)
        for block in range(2):
            rows = slice(block * 256, block * 256 + 256)
            span = block * 256 + 256
            scores = dot_nn(qn[rows, :64], kt[:64, :span]) + mask[rows, :span]
            dscores = dot_nn(qn[rows, :], ks[:, :span])
            exp_scores = jnp.exp(scores - jnp.max(scores, axis=1, keepdims=True))
            probs = exp_scores * (1.0 / jnp.sum(exp_scores, axis=1, keepdims=True))
            dprobs = probs * (dscores - jnp.sum(probs * dscores, axis=1, keepdims=True))
            probs_low, dprobs_low = probs.astype(bf16), dprobs.astype(bf16)
            grad_probs = dot_nn(gn[rows, :64], vt[:64, :span])
            dgrad_probs = dot_nn(gn[rows, :], vs[:, :span])
            centre = jnp.sum(probs * grad_probs, axis=1, keepdims=True)
            dcentre = jnp.sum(dprobs * grad_probs + probs * dgrad_probs, axis=1, keepdims=True)
            rest = grad_probs - centre
            g_scores = (probs * rest).astype(bf16)
            dg_scores = (dprobs * rest + probs * (dgrad_probs - dcentre)).astype(bf16)
            out = dot_nt(vt[:, :span], probs_low)
            head_a[head * 128 : head * 128 + 64, rows] = out[:64, :].astype(bf16)
            head_a[head * 128 + 64 : head * 128 + 128, rows] = (out[64:, :] + dot_nt(vt[:64, :span], dprobs_low)).astype(bf16)
            gq[:, rows] = dot_nt(kt[:, :span], g_scores) * 0.125
            gq[64:, rows] += dot_nt(kt[:64, :span], dg_scores) * 0.125
            part_v = dot_nn(gt[:, rows], probs_low)
            part_dv = dot_nn(gt[:64, rows], dprobs_low)
            part_k = dot_nn(qt[:, rows], g_scores)
            part_dk = dot_nn(qt[:64, rows], dg_scores)
            if block == 0:
                gv[:, :span] = part_v
                gk[:, :span] = part_k
                gv[:, span:] = jnp.zeros((128, 512 - span), f32)
                gk[:, span:] = jnp.zeros((128, 512 - span), f32)
            else:
                gv[:, :span] += part_v
                gk[:, :span] += part_k
            gv[64:, :span] += part_dv
            gk[64:, :span] += part_dk
        for part in (0, 64):
            rotate_rows(gq, part, cos, sin, True)
            rotate_rows(gk, part, cos, sin, True)
        head_g[0:128, :] = gq[...].astype(bf16)
        head_g[128:256, :] = gk[...].astype(bf16)
        head_g[256:384, :] = gv[...].astype(bf16)
        one[:384, :] = dot_nn(head_g[...], lhs_a[:, :width])
        two[:384, :] = dot_nn(head_g[...], nb[...])
        sums = dot_nn(head_g[...], ones[...])
        rows = slice(base, base + 384)
        add(heads + 1, rows, sums)
        for kind in range(3):
            top, low = slice(kind * 128, kind * 128 + 64), slice(kind * 128 + 64, kind * 128 + 128)
            carry_r = fold(
                carry_r, 64, head, (top, low), (top, low),
                wat[base + kind * 128 : base + kind * 128 + 64, :width],
                wat[base + kind * 128 + 64 : base + kind * 128 + 128, :width],
                dgain_a, dshift_a, sums[kind * 128 : kind * 128 + 64, 0:1],
            )
        add(head, slice(384, 512), dot_nn(head_a[head * 128 : head * 128 + 128, :], cb[...]))
    acc_r[0:8, :], acc_r[16:24, :] = carry_r
    slots = [heads + 1, heads + 2] + list(range(heads))
    leaves = [pltpu.make_async_copy(new[slot], out_h[slot], sem.at[1 + i]) for i, slot in enumerate(slots)]
    for copy in leaves:
        copy.start()
    leave_m.wait()
    for copy in leaves:
        copy.wait()


def shard_step(heads, index, scalars, mine, other, shared, tables, old):
    first = old is None
    sizes = [(512, 768)] * heads + [(1536, 768), (1536, 128), (32, 768)]
    whole = pl.BlockSpec(memory_space=pltpu.VMEM)
    there = pl.BlockSpec(memory_space=pltpu.HBM)
    specs = [pl.BlockSpec(memory_space=pl.ANY)] * 2 + [whole] * 4 + [there] * 6
    vec, dvec, wat, bias_a, oat, uwt, dwt, bias_u = shared
    operands = [mine, other, vec, dvec, *tables, wat, bias_a, oat, uwt, dwt, bias_u]
    aliases = {}
    if not first:
        aliases = {3 + len(operands) + i: i for i in range(len(sizes))}
        specs += [there] * len(sizes)
        operands += list(old)
    scratch = [(mine.shape, mine.dtype), (other.shape, other.dtype)]
    scratch += [((heads * 384, 1536), bf16), ((heads * 384, 128), f32), ((heads * 128, 768), bf16)]
    scratch += [((768, 768), bf16)] * 2 + [((768, 128), f32)] + [(size, f32) for size in sizes] + [None]
    scratch += [
        ((512, 768), bf16),
        ((512, 128), bf16),
        ((512, 1536), bf16),
        ((512, 768), bf16),
        ((512, 768), bf16),
        ((512, 768), bf16),
        ((512, 512), f32),
        ((heads * 384, 512), f32),
        ((heads * 128, 512), f32),
    ]
    scratch += [((128, 512), bf16)] * 6 + [((512, 128), bf16)] * 2 + [((128, 512), f32)] * 3
    scratch += [((384, 512), bf16), ((heads * 128, 512), bf16)]
    scratch += [((768, 512), f32)] * 2 + [((768, 512), bf16)] * 2 + [((768, 768), f32)] * 2
    return pl.pallas_call(
        lambda *refs: shard_kernel(heads, first, index, *refs),
        out_shape=[jax.ShapeDtypeStruct(size, f32) for size in sizes],
        grid_spec=pltpu.PrefetchScalarGridSpec(
            num_scalar_prefetch=3,
            grid=(1,),
            in_specs=specs,
            out_specs=[there] * len(sizes),
            scratch_shapes=[pltpu.SemaphoreType.DMA((16,)) if one is None else pltpu.VMEM(*one) for one in scratch],
        ),
        input_output_aliases=aliases,
        compiler_params=pltpu.CompilerParams(vmem_limit_bytes=VMEM_SHARD),
        cost_estimate=pl.CostEstimate(flops=heads * 2 * 10**9 + 5 * 10**9, bytes_accessed=2 * 10**7, transcendentals=10**6),
        name=f"shard{heads}",
    )(*scalars, *operands)


def put_tile(slot_dev, owner, y, tile, curve, grad, curve_rows, grad_rows):
    group = slot_dev // 2
    slot = owner[tile]
    curve_rows(curve.at[slot])
    home, place = slot // slot_dev, slot % slot_dev

    @pl.when(place // group == y)
    def _():
        grad_rows(grad.at[home * group + place % group])


def tile_at(kind, side):
    return (side * 6 + 2 * kind, 1) if kind < 3 else (12 + side, 2)


def finish_kernel(slot_dev, owner, info, acc_a, acc_b, acc_m, acc_c, acc_r, wat, oat, uwt, dwt, out_sum, curve, grad, sums):
    core, y, odd = info[3], info[5], info[6]
    if slot_dev * 8 > 48:
        curve[...] = jnp.zeros(curve.shape, f32)
        grad[...] = jnp.zeros(grad.shape, f32)

    def put(tile, columns, source, curve_at, grad_at):
        def curve_rows(ref):
            ref[...] = source[curve_at : curve_at + 48, columns]

        def grad_rows(ref):
            ref[...] = source[pl.ds(pl.multiple_of(grad_at + core * 24, 8), 24), columns]

        put_tile(slot_dev, owner, y, tile, curve, grad, curve_rows, grad_rows)

    for side in range(2):
        columns = slice(side * 384, side * 384 + 384)
        for kind in range(4):
            lower, step = tile_at(kind, side)
            put(lower + odd * step, columns, acc_a, kind * 128 + 64, kind * 128)
        for block in range(8):
            at = block * 48
            put(16 + side * 8 + block, columns, acc_m, 384 + at, at)
            put(32 + block * 2 + side, columns, acc_m, 1152 + at, 768 + at)
    small_sums_kernel(info, acc_a, acc_b, acc_m, acc_c, acc_r, wat, oat, uwt, dwt, out_sum, sums)


def finish_split_kernel(slot_dev, owner, info, acc_b, near_b, extra, old_curve, old_grad, curve, grad, new_curve, new_grad, sem):
    core, x, y, odd = info[3], info[4], info[5], info[6]
    group = slot_dev // 2
    for index in range(8):
        near_b[index] += acc_b[pl.ds(pl.multiple_of(index * 64 + x * 32, 32), 32), :]
    copies = []
    for kind in range(4):
        for side in range(2):
            columns = slice(side * 384, side * 384 + 384)
            lower, step = tile_at(kind, side)
            slot = owner[lower + (1 - odd) * step]
            place = kind * 2 + side
            new_curve[place, 0:32, :] = near_b[kind * 2 + 1, :, columns]
            new_curve[place, 32:48, :] = extra[kind * 2 + 1, :, columns]
            copy = pltpu.make_async_copy(new_curve.at[place], curve.at[slot], sem.at[place])
            copy.start()
            copies.append(copy)

            @pl.when(core == 0)
            def _(place=place, kind=kind, columns=columns):
                new_grad[place] = near_b[kind * 2, 0:24, columns]

            @pl.when(core == 1)
            def _(place=place, kind=kind, columns=columns):
                new_grad[place, 0:8, :] = near_b[kind * 2, 24:32, columns]
                new_grad[place, 8:24, :] = extra[kind * 2, :, columns]

            home, spot = slot // slot_dev, slot % slot_dev

            @pl.when(spot // group == y)
            def _(place=place, home=home, spot=spot):
                copy = pltpu.make_async_copy(new_grad.at[place], grad.at[home * group + spot % group], sem.at[8 + place])
                copy.start()
                copy.wait()

    for copy in copies:
        copy.wait()


def finish(owners, info, slot_dev, arrays):
    whole = pl.BlockSpec(memory_space=pltpu.VMEM)
    return pl.pallas_call(
        lambda *refs: finish_kernel(slot_dev, *refs),
        out_shape=[
            jax.ShapeDtypeStruct((8 * slot_dev, 48, 384), f32),
            jax.ShapeDtypeStruct((4 * slot_dev, 24, 384), f32),
            jax.ShapeDtypeStruct((32, 768), f32),
        ],
        grid_spec=pltpu.PrefetchScalarGridSpec(
            num_scalar_prefetch=2,
            grid=(1,),
            in_specs=[whole] * len(arrays),
            out_specs=[whole] * 3,
        ),
        compiler_params=pltpu.CompilerParams(vmem_limit_bytes=VMEM_SHARD),
        cost_estimate=pl.CostEstimate(flops=10**7, bytes_accessed=2 * 10**7, transcendentals=0),
        name="finish",
    )(owners, info, *arrays)


def finish_split(owners, info, slot_dev, acc_b, near_b, extra, curve, grad):
    whole = pl.BlockSpec(memory_space=pltpu.VMEM)
    there = pl.BlockSpec(memory_space=pltpu.HBM)
    return pl.pallas_call(
        lambda *refs: finish_split_kernel(slot_dev, *refs),
        out_shape=[jax.ShapeDtypeStruct(curve.shape, f32), jax.ShapeDtypeStruct(grad.shape, f32)],
        grid_spec=pltpu.PrefetchScalarGridSpec(
            num_scalar_prefetch=2,
            grid=(1,),
            in_specs=[whole] * 3 + [there] * 2,
            out_specs=[there] * 2,
            scratch_shapes=[
                pltpu.VMEM((8, 48, 384), f32),
                pltpu.VMEM((8, 24, 384), f32),
                pltpu.SemaphoreType.DMA((16,)),
            ],
        ),
        input_output_aliases={5: 0, 6: 1},
        compiler_params=pltpu.CompilerParams(vmem_limit_bytes=VMEM_SHARD),
        cost_estimate=pl.CostEstimate(flops=0, bytes_accessed=5 * 10**6, transcendentals=0),
        name="finish_split",
    )(owners, info, acc_b, near_b, extra, curve, grad)


def own_attention_kernel(info, seq_device, seq_length, q_ref, k_ref, v_ref, g_ref, cos_ref, sin_ref, att, gq_out, gk_out, gv_out, mask, buf, gk, gv):
    short = is_short(seq_device, seq_length, info[0], 512)

    @pl.when(pl.program_id(0) == 0)
    def _():
        mask_rows(mask, short, 512)

    cos, sin = cos_ref[short], sin_ref[short]
    buf[...] = q_ref[...]
    rotate_rows(buf, 0, cos, sin, False)
    q_rows = buf[...] * 0.125
    qt = q_rows.astype(bf16)
    qn = jnp.transpose(q_rows).astype(bf16)
    buf[...] = k_ref[...]
    rotate_rows(buf, 0, cos, sin, False)
    kt = buf[...].astype(bf16)
    vt = v_ref[...].astype(bf16)
    gt = g_ref[...].astype(bf16)
    gn = jnp.transpose(g_ref[...]).astype(bf16)
    for block in range(2):
        rows = slice(block * 256, block * 256 + 256)
        wide = block * 256 + 256
        scores = dot_nn(qn[rows, :], kt[:, :wide]) + mask[rows, :wide]
        exp_scores = jnp.exp(scores - jnp.max(scores, axis=1, keepdims=True))
        probs = exp_scores * (1.0 / jnp.sum(exp_scores, axis=1, keepdims=True))
        probs_low = probs.astype(bf16)
        grad_probs = dot_nn(gn[rows, :], vt[:, :wide])
        weighted = probs * grad_probs
        g_scores = (weighted - probs * jnp.sum(weighted, axis=1, keepdims=True)).astype(bf16)
        att[:, rows] = dot_nt(vt[:, :wide], probs_low).astype(bf16)
        buf[:, rows] = dot_nt(kt[:, :wide], g_scores) * 0.125
        part_v = dot_nn(gt[:, rows], probs_low)
        part_k = dot_nn(qt[:, rows], g_scores)
        if block == 0:
            gv[:, :wide] = part_v
            gk[:, :wide] = part_k
            gv[:, wide:] = jnp.zeros((64, 512 - wide), f32)
            gk[:, wide:] = jnp.zeros((64, 512 - wide), f32)
        else:
            gv[:, :wide] += part_v
            gk[:, :wide] += part_k
    rotate_rows(buf, 0, cos, sin, True)
    rotate_rows(gk, 0, cos, sin, True)
    gq_out[...] = buf[...].astype(bf16)
    gk_out[...] = gk[...].astype(bf16)
    gv_out[...] = gv[...].astype(bf16)


def own_attention(scalars, mixed, grad_att, tables):
    def rows_at(offset):
        return pl.BlockSpec((64, 512), lambda i, *scalars: (offset + i, 0))

    whole = pl.BlockSpec(memory_space=pltpu.VMEM)
    return pl.pallas_call(
        own_attention_kernel,
        out_shape=[jax.ShapeDtypeStruct((768, 512), bf16)] * 4,
        grid_spec=pltpu.PrefetchScalarGridSpec(
            num_scalar_prefetch=3,
            grid=(12,),
            in_specs=[rows_at(0), rows_at(12), rows_at(24), rows_at(0), whole, whole],
            out_specs=[rows_at(0)] * 4,
            scratch_shapes=[pltpu.VMEM((512, 512), f32)] + [pltpu.VMEM((64, 512), f32)] * 3,
        ),
        compiler_params=pltpu.CompilerParams(vmem_limit_bytes=16 << 20),
        cost_estimate=pl.CostEstimate(flops=10**10, bytes_accessed=10**7, transcendentals=3 * 10**6),
        name="own_attention",
    )(*scalars, mixed, mixed, mixed, grad_att, *tables)


def lay_rows(table, slot, rows, out, buf):
    for source in range(8):
        for part in range(3):
            start = pl.multiple_of(table[slot, source * 3 + part], 16)
            buf[pl.ds(start, 16), :] = rows(source, part * 16)

    @pl.when(table[slot, 24] == 1)
    def _():
        out[0] = jnp.transpose(buf[...])

    @pl.when(table[slot, 24] == 0)
    def _():
        out[0] = buf[...]


def assemble_kernel(table, pieces, out, buf):
    lay_rows(table, pl.program_id(0), lambda source, at: pieces[source, 0, at : at + 16, :], out, buf)


def assemble(table, pieces):
    slots = pieces.shape[1]
    return pl.pallas_call(
        assemble_kernel,
        out_shape=jax.ShapeDtypeStruct((slots, 384, 384), f32),
        grid_spec=pltpu.PrefetchScalarGridSpec(
            num_scalar_prefetch=1,
            grid=(slots,),
            in_specs=[pl.BlockSpec((8, 1, 48, 384), lambda i, table: (0, i, 0, 0))],
            out_specs=pl.BlockSpec((1, 384, 384), lambda i, table: (i, 0, 0)),
            scratch_shapes=[pltpu.VMEM((384, 384), f32)],
        ),
        compiler_params=pltpu.CompilerParams(vmem_limit_bytes=16 << 20),
        cost_estimate=pl.CostEstimate(flops=0, bytes_accessed=8 * 10**6, transcendentals=0),
        name="assemble",
    )(table, pieces)


def split_two(value):
    high = value.astype(bf16)
    return (high, (value - high.astype(f32)).astype(bf16))


def dot_fine(left, right, dims):
    (a_high, a_low), (b_high, b_low) = left, right

    def dot(a, b):
        return lax.dot_general(a, b, (dims, ((), ())), preferred_element_type=f32)

    return dot(a_high, b_high) + (dot(a_high, b_low) + dot(a_low, b_high))


def update_kernel(table, info, tile, own, own_core, far, far_core, qkv, out_w, up, down, left, right, first, second, grad, new_first, new_second, new_weight, new_low, rows, buf):
    slot = pl.program_id(0)
    core, y = info[3], info[5]
    group = pl.num_programs(0) // 2

    def join(one, two):
        rows[:, pl.ds(pl.multiple_of(core * 24, 8), 24), :] = one[:, 0]
        rows[:, pl.ds(pl.multiple_of(24 - core * 24, 8), 24), :] = two[:, 0]

    @pl.when(slot // group == y)
    def _():
        join(own, own_core)

    @pl.when(slot // group != y)
    def _():
        join(far, far_core)

    lay_rows(table, slot, lambda source, at: rows[source, at : at + 16, :], grad, buf)
    index = tile[slot]

    def weight(low, high, ref):
        @pl.when((index >= low) & (index < high))
        def _():
            buf[...] = ref[...].astype(f32)

    weight(0, 12, qkv)
    weight(12, 16, out_w)
    weight(16, 32, up)
    weight(32, 48, down)
    used = jnp.where(index < 48, 1.0, 0.0)
    l_two, r_two = split_two(left[0]), split_two(right[0])
    turned = dot_fine(l_two, split_two(grad[0]), ((0,), (0,)))
    turned = dot_fine(split_two(turned), r_two, ((1,), (0,)))
    moment = beta_decay * first[0] + (1.0 - beta_decay) * turned
    square = beta_decay * second[0] + (1.0 - beta_decay) * turned * turned
    correction = 1.0 - beta_decay**STEP
    direction = moment / correction / (jnp.sqrt(square / correction) + adam_epsilon)
    new_first[0] = used * moment
    new_second[0] = used * square
    restored = dot_fine(l_two, split_two(direction), ((1,), (0,)))
    restored = dot_fine(split_two(restored), r_two, ((1,), (1,)))
    value = buf[...]
    value = jnp.where(index < 48, value - learning_rate * (restored + weight_decay * value), 0.0)
    new_weight[0] = value
    new_low[0] = value.astype(bf16)


def update(table, info, tile, pieces, weights, states):
    group = pieces[0].shape[1]
    slots = 2 * group
    piece = pl.BlockSpec((8, 1, 24, 384), lambda i, table, info, tile: (0, i % group, 0, 0))
    slab = pl.BlockSpec((1, 384, 384), lambda i, table, info, tile: (i, 0, 0))

    def spec(start, count, columns):
        def at(i, table, info, tile):
            local_tile = jnp.clip(tile[i] - start, 0, count - 1)
            return (local_tile // columns, local_tile % columns)

        return pl.BlockSpec((384, 384), at)

    kinds = [f32, f32, f32, f32, bf16]
    return pl.pallas_call(
        update_kernel,
        out_shape=[jax.ShapeDtypeStruct((slots, 384, 384), kind) for kind in kinds],
        grid_spec=pltpu.PrefetchScalarGridSpec(
            num_scalar_prefetch=3,
            grid=(slots,),
            in_specs=[piece] * 4 + [spec(0, 12, 6), spec(12, 4, 2), spec(16, 16, 8), spec(32, 16, 2)] + [slab] * 4,
            out_specs=[slab] * 5,
            scratch_shapes=[pltpu.VMEM((8, 48, 384), f32), pltpu.VMEM((384, 384), f32)],
        ),
        compiler_params=pltpu.CompilerParams(vmem_limit_bytes=32 << 20),
        cost_estimate=pl.CostEstimate(flops=10**10, bytes_accessed=4 * 10**7, transcendentals=10**6),
        name="update",
    )(table, info, tile, *pieces, *(in_hbm(value) for value in (*weights, *states)))


def small_sums_kernel(info, acc_a, acc_b, acc_m, acc_c, acc_r, wat, oat, uwt, dwt, out_sum, out):
    device = info[0]
    out[...] = jnp.zeros((32, 768), f32)
    blank = jnp.zeros((8, 768), f32)
    along, curve = blank, blank
    shift_a, shift_m, dshift_a, dshift_m = blank, blank, blank, blank

    def fold(value):
        return jnp.sum(value.reshape(value.shape[0] // 8, 8, 768), axis=0)

    for place, acc in enumerate((acc_a, acc_b)):
        head = info[1 + place]
        row = lax.broadcasted_iota(jnp.int32, (64, 128), 0) + (head % 2) * 64
        pick = lax.broadcasted_iota(jnp.int32, (64, 128), 1) == row
        for kind in range(4):
            at = kind * 128
            if kind < 3:
                base = place * 384 + at
                w_one, w_drift = wat[base : base + 64, :768].astype(f32), wat[base + 64 : base + 128, :768].astype(f32)
                p_col, q_col = acc_c[base : base + 64, :], acc_c[base + 64 : base + 128, :]
                shift_a += fold(w_one * p_col[:, 0:1])
                dshift_a += fold(w_one * q_col[:, 0:1] + w_drift * p_col[:, 0:1])
                lanes = pl.ds(pl.multiple_of(128 * (head // 2), 128), 128)
                out[4 + kind : 5 + kind, lanes] += jnp.sum(jnp.where(pick, p_col, 0.0), axis=0, keepdims=True)
                out[20 + kind : 21 + kind, lanes] += jnp.sum(jnp.where(pick, q_col, 0.0), axis=0, keepdims=True)
            else:
                w_drift = oat[place * 128 + 64 : place * 128 + 128, :].astype(f32)
            along += fold(acc[at : at + 64, :] * w_drift)
            curve += fold(acc[at + 64 : at + 128, :] * w_drift)
    row = lax.broadcasted_iota(jnp.int32, (48, 384), 0) + device * 48
    pick = lax.broadcasted_iota(jnp.int32, (48, 384), 1) == row
    for block in range(8):
        at = block * 48
        w_one, w_drift = uwt[at : at + 48, :].astype(f32), uwt[384 + at : 432 + at, :].astype(f32)
        d_drift = dwt[384 + at : 432 + at, :].astype(f32)
        p_col, q_col = acc_c[768 + at : 816 + at, 0:1], acc_c[1152 + at : 1200 + at, 0:1]
        shift_m += fold(w_one * p_col)
        dshift_m += fold(w_one * q_col + w_drift * p_col)
        along += fold(acc_m[at : at + 48, :] * w_drift) + fold(acc_m[768 + at : 816 + at, :] * d_drift)
        curve += fold(acc_m[384 + at : 432 + at, :] * w_drift) + fold(acc_m[1152 + at : 1200 + at, :] * d_drift)
        lanes = slice(384 * (block % 2), 384 * (block % 2) + 384)
        place = 8 + block // 2
        out[place : place + 1, lanes] = jnp.sum(jnp.where(pick, p_col, 0.0), axis=0, keepdims=True)
        out[16 + place : 17 + place, lanes] = jnp.sum(jnp.where(pick, q_col, 0.0), axis=0, keepdims=True)

    def row_sum(value):
        return jnp.sum(value, axis=0, keepdims=True)

    out[0:1, :] = row_sum(acc_r[16:24, :])
    out[1:2, :] = row_sum(shift_a)
    out[2:3, :] = row_sum(acc_r[24:32, :])
    out[3:4, :] = row_sum(shift_m)
    out[7:8, :] = out_sum[...]
    out[12:13, :] = out_sum[...]
    out[16:17, :] = row_sum(acc_r[0:8, :])
    out[17:18, :] = row_sum(dshift_a)
    out[18:19, :] = row_sum(acc_r[8:16, :])
    out[19:20, :] = row_sum(dshift_m)
    lane = lax.broadcasted_iota(jnp.int32, (1, 768), 1)
    out[29:30, :] = jnp.where(lane == 0, jnp.sum(along), jnp.where(lane == 1, jnp.sum(curve), 0.0))


def take_rows(matrix, start, size):
    return lax.dynamic_slice_in_dim(matrix, start, size, axis=0)


def piece_rows(index):
    z, x = index // 2, index % 2
    plain = [48 * index, 48 * index + 16, 48 * index + 32]
    full = [[64 * x + 16 * i for i in range(3)], [64 + 64 * x + 16 * i for i in range(3)]]
    full += [[192 + 64 * x + 16 * i for i in range(3)], [256 + 64 * x + 16 * i for i in range(3)]]
    split = [
        [32 * x, 32 * x + 16, 64 + 64 * x + 48],
        [128 + 32 * x, 144 + 32 * x, 64 * x + 48],
        [192 + 32 * x, 208 + 32 * x, 256 + 64 * x + 48],
        [320 + 32 * x, 336 + 32 * x, 192 + 64 * x + 48],
    ]
    even = z % 2 == 0
    return (full[z] if even else split[z], split[z] if even else full[z], plain)


def local_tp(
    tokens,
    cotangent,
    vec_params,
    qkv_weight,
    out_weight,
    up_weight,
    down_weight,
    probe_vec,
    probe_qkv,
    probe_out,
    probe_up,
    probe_down,
    seq_device,
    seq_length,
    owners,
    left_bases,
    right_bases,
    first_moment,
    second_moment,
    vec_first,
    vec_second,
):
    row_count, width = tokens.shape
    device = lax.axis_index("dp")
    z = device // 2
    probe = lax.axis_index("probe")
    x, y, core = device % 2, probe // 2, probe % 2
    info = lax.dynamic_index_in_dim(jnp.array(device_table(), jnp.int32), device * 4 + probe, 0, keepdims=False)
    scalars = (info, seq_device, seq_length)
    drift_vec, drift_qkv, drift_out = probe_vec[0], probe_qkv[0], probe_out[0]
    drift_up, drift_down = probe_up[0], probe_down[0]
    barrier = lax.optimization_barrier

    across = [(i, i ^ 1) for i in range(8)]
    rise = [[(i, i + 2) for i in range(6) if i // 2 >= k] for k in range(3)]
    fall = [[(i + 2, i) for i in range(6) if 3 - (i + 2) // 2 >= k] for k in range(3)]
    swap_core = [(0, 1), (1, 0), (2, 3), (3, 2)]
    swap_y = [(0, 2), (2, 0), (1, 3), (3, 1)]

    def move(value, pairs):
        return lax.ppermute(value, "dp", pairs)

    def to_core(value):
        return lax.ppermute(value, "probe", swap_core)

    half = row_count // 2

    mine = jnp.concatenate(
        [take_rows(tokens, core * half, half).astype(f32), take_rows(cotangent, core * half, half).astype(f32)], axis=1
    )
    up_1, down_1, cross_0 = move(mine, rise[0]), move(mine, fall[0]), move(mine, across)

    row_index = jnp.arange(row_count, dtype=jnp.int32)
    half_rot = ROT // 2
    frequency = jnp.exp(jnp.arange(half_rot, dtype=f32) * (-2.0 * math.log(10000.0) / ROT))
    position = jnp.stack([row_index, row_index % (row_count // 4)])
    angles = position.astype(f32)[:, None, :] * frequency[None, :, None]
    tables = (jnp.cos(angles), jnp.sin(angles))

    flat_bias = vec_params[4:7].reshape(-1)
    uwt, dwt, bias_u, wat, oat, bias_a = prepare(
        info,
        qkv_weight, drift_qkv, out_weight, drift_out, up_weight, drift_up, down_weight, drift_down, vec_params, drift_vec,
    )
    shared = (vec_params, drift_vec, wat, bias_a, oat, uwt, dwt, bias_u)

    def step(heads, index, mine, other, old):
        return shard_step(heads, index, scalars, mine, other, shared, tables, old)

    acc_a, acc_b, acc_m, acc_c, acc_r = step(2, 0, tokens, cotangent, None)
    (up_1, down_1, cross_0, acc_r) = barrier((up_1, down_1, cross_0, acc_r))
    near = jnp.where((z == 0) | (z == 2), down_1, up_1)
    (up_1, down_1, near) = barrier((up_1, down_1, near))
    up_2, down_2, cross_1 = move(up_1, rise[1]), move(down_1, fall[1]), move(near, across)
    cross_0o, near_o = to_core(cross_0), to_core(near)
    acc_a, acc_m, acc_c, acc_r = step(1, 4, cross_0, cross_0o, [acc_a, acc_m, acc_c, acc_r])
    acc_a, acc_b, acc_m, acc_c, acc_r = step(2, 1, near, near_o, [acc_a, acc_b, acc_m, acc_c, acc_r])

    (up_2, down_2, cross_1, acc_r) = barrier((up_2, down_2, cross_1, acc_r))
    second = jnp.where(z == 0, down_2, jnp.where(z == 1, down_1, jnp.where(z == 2, up_1, up_2)))
    (up_2, down_2, second) = barrier((up_2, down_2, second))
    up_3, down_3, cross_2 = move(up_2, rise[2]), move(down_2, fall[2]), move(second, across)
    second_o, cross_1o = to_core(second), to_core(cross_1)
    acc_a, acc_m, acc_c, acc_r = step(1, 5, cross_1, cross_1o, [acc_a, acc_m, acc_c, acc_r])
    acc_a, acc_b, acc_m, acc_c, acc_r = step(2, 2, second, second_o, [acc_a, acc_b, acc_m, acc_c, acc_r])

    (up_3, down_3, cross_2, acc_r) = barrier((up_3, down_3, cross_2, acc_r))
    third = jnp.where(z == 0, down_3, jnp.where(z == 1, down_2, jnp.where(z == 2, up_2, up_3)))
    third = barrier(third)
    cross_3, third_o, cross_2o = move(third, across), to_core(third), to_core(cross_2)
    acc_a, acc_b, acc_m, acc_c, acc_r = step(2, 3, third, third_o, [acc_a, acc_b, acc_m, acc_c, acc_r])
    sends = lax.dynamic_slice_in_dim(acc_b.reshape(8, 64, width), 32 - 32 * x, 32, axis=1)
    near_b = move(sends, across)
    acc_a, acc_m, acc_c, acc_r = step(1, 6, cross_2, cross_2o, [acc_a, acc_m, acc_c, acc_r])
    (tokens, cotangent, cross_3, acc_r) = barrier((tokens, cotangent, cross_3, acc_r))
    cross_3o = to_core(cross_3)
    inputs = tokens.astype(f32)
    cot_rows = cotangent.astype(f32)
    out_sum = jnp.sum(cot_rows, axis=0, keepdims=True)
    normed, norm_scale = normalize(inputs)
    attn_low = (normed * vec_params[0] + vec_params[1]).astype(bf16)
    mlp_low = (normed * vec_params[2] + vec_params[3]).astype(bf16)
    mixed = product("kj,tk->jt", qkv_weight, attn_low) + flat_bias[:, None]
    grad_att = product("jk,tk->jt", out_weight, cotangent)
    (cross_3, cross_3o, acc_r, mixed, grad_att, mlp_low) = barrier((cross_3, cross_3o, acc_r, mixed, grad_att, mlp_low))
    acc_a, acc_m, acc_c, acc_r = step(1, 7, cross_3, cross_3o, [acc_a, acc_m, acc_c, acc_r])
    extra = move(acc_a.reshape(8, 64, width)[:, 48:], [(i, i ^ 2) for i in range(8)])

    slot_dev = left_bases.shape[0]
    tile_index, occupied = slot_order(owners, slot_dev * 8)
    curve_slots, grad_slots, vec_all = finish(
        owners, info, slot_dev, (acc_a, acc_b, acc_m, acc_c, acc_r, wat, oat, uwt, dwt, out_sum)
    )
    vec_one = move(vec_all, [(i, i ^ 1) for i in range(8)])
    (extra, near_b, vec_all) = barrier((extra, near_b, vec_all))
    curve_slots, grad_slots = finish_split(owners, info, slot_dev, acc_b, near_b, extra, curve_slots, grad_slots)
    curve_slots = curve_slots.reshape(8, slot_dev, 48, 384)
    (vec_all, vec_one, grad_slots) = barrier((vec_all, vec_one, grad_slots))
    vec_all = vec_all + vec_one
    vec_two = move(vec_all, [(i, i ^ 2) for i in range(8)])
    grad_slots = lax.all_to_all(grad_slots.reshape(8, slot_dev // 2, 24, 384), "dp", 0, 0)
    (mixed, grad_att, curve_slots) = barrier((mixed, grad_att, curve_slots))
    att_t, gq_t, gk_t, gv_t = own_attention(scalars, mixed, grad_att, tables)
    (vec_all, vec_two, att_t) = barrier((vec_all, vec_two, att_t))
    vec_all = vec_all + vec_two
    vec_four = move(vec_all, [(i, i ^ 4) for i in range(8)])

    (grad_slots, curve_slots, att_t, gq_t, gk_t, gv_t) = barrier((grad_slots, curve_slots, att_t, gq_t, gk_t, gv_t))
    curve_slots = lax.all_to_all(curve_slots, "dp", 0, 0)
    far = lax.ppermute(grad_slots, "probe", swap_y)
    own_core = to_core(grad_slots)
    (mlp_low, cotangent, own_core, att_t, gq_t, gk_t, gv_t) = barrier((mlp_low, cotangent, own_core, att_t, gq_t, gk_t, gv_t))
    hidden = product("ij,jk->ik", mlp_low, up_weight) + vec_params[8:12].reshape(-1)
    cumulative = 0.5 * (1.0 + lax.erf(hidden * root_half))
    density = jnp.exp(-0.5 * hidden * hidden) * density_scale
    act_low = (hidden * cumulative).astype(bf16)
    grad_act = product("ij,kj->ik", cotangent, down_weight)
    grad_hidden_low = (grad_act * (cumulative + hidden * density)).astype(bf16)
    mlp_out = product("ij,jk->ik", act_low, down_weight) + vec_params[12]
    (mlp_out, far, grad_hidden_low, att_t) = barrier((mlp_out, far, grad_hidden_low, att_t))
    far_core = to_core(far)
    attn_out = product("jt,jk->tk", att_t, out_weight) + vec_params[7]
    block_output = (inputs + attn_out + mlp_out).astype(bf16)
    grad_mlp_in = product("ij,kj->ik", grad_hidden_low, up_weight)
    grad_attn_in = (
        product("jt,kj->tk", gq_t, qkv_weight[:, :width])
        + product("jt,kj->tk", gk_t, qkv_weight[:, width : 2 * width])
        + product("jt,kj->tk", gv_t, qkv_weight[:, 2 * width :])
    )
    grad_weighted = grad_attn_in * vec_params[0] + grad_mlp_in * vec_params[2]
    input_grad = cot_rows + norm_back(grad_weighted, normed, norm_scale)

    own_index = lax.dynamic_slice_in_dim(tile_index, device * slot_dev, slot_dev)
    kinds = [sum((piece_rows(i)[kind] for i in range(8)), []) for kind in range(3)]
    row_table = jnp.array(kinds, jnp.int32)
    in_qkv, in_out = own_index < 12, (own_index >= 12) & (own_index < 16)
    kind = jnp.where(in_qkv, own_index % 2, jnp.where(in_out, (own_index - 12) // 2, 2))
    turned = in_qkv | ((own_index >= 16) & (own_index < 32))
    table = jnp.concatenate([row_table[kind], turned.astype(jnp.int32)[:, None]], axis=1)
    (far_core, input_grad, block_output) = barrier((far_core, input_grad, block_output))
    own_grad, new_first, new_second, new_weights, new_weights_low = update(
        table,
        info,
        own_index,
        [grad_slots, own_core, far, far_core],
        [qkv_weight, out_weight, up_weight, down_weight],
        [left_bases, right_bases, first_moment, second_moment],
    )
    (vec_all, vec_four, new_first) = barrier((vec_all, vec_four, new_first))
    vec_all = vec_all + vec_four
    vec_total, vec_curve = vec_all[:13], vec_all[16:29]
    own_dots = jnp.stack(
        [vec_all[29, 0] + jnp.sum(vec_total * drift_vec), vec_all[29, 1] + jnp.sum(vec_curve * drift_vec)]
    )
    all_dots = jnp.where(jnp.arange(8)[:, None] == probe, jnp.pad(own_dots, (0, 126))[None], 0.0)
    all_dots = all_dots + to_core(all_dots)
    all_dots = all_dots + lax.ppermute(all_dots, "probe", swap_y)
    all_dots = all_dots[:4, :2]
    own_curve = assemble(table, curve_slots)
    vec_new_first, vec_new_second, vec_new = plain_adam(vec_total, vec_params, vec_first, vec_second)
    vector_state = jnp.stack([vec_total, vec_new_first], axis=0)
    return (
        block_output,
        input_grad,
        own_grad,
        new_first,
        new_second,
        new_weights,
        new_weights_low,
        own_curve[None],
        vector_state,
        vec_new_second,
        vec_new,
        vec_curve[None],
        all_dots,
    )


def solution(mesh):
    local = local_tp if fits_tp(mesh) else local_any
    return jax.shard_map(
        local,
        mesh=mesh,
        in_specs=(
            P("dp", None),
            P("dp", None),
            P(),
            P(),
            P(),
            P(),
            P(),
            P("probe", None, None),
            P("probe", None, None),
            P("probe", None, None),
            P("probe", None, None),
            P("probe", None, None),
            P(),
            P(),
            P(),
            P("dp", None, None),
            P("dp", None, None),
            P("dp", None, None),
            P("dp", None, None),
            P(),
            P(),
        ),
        out_specs=(
            P("dp", None),
            P("dp", None),
            P("dp", None, None),
            P("dp", None, None),
            P("dp", None, None),
            P("dp", None, None),
            P("dp", None, None),
            P("probe", "dp", None, None),
            P(),
            P(),
            P(),
            P("probe", None, None),
            P(),
        ),
        check_vma=False,
    )
```

```python
import math

import jax
import jax.numpy as jnp
from jax import lax
from jax.experimental import pallas as pl
from jax.experimental.pallas import tpu as pltpu
from jax.sharding import PartitionSpec as P

HEAD = 64
ROT = 16
BLK = 384
STEP = 4


beta_decay = 0.5
learning_rate = 0.05
weight_decay = 0.01
adam_epsilon = 1e-08
norm_epsilon = 1e-05
root_half = 0.7071067811865476
density_scale = 0.3989422804014327
masked_score = -1e30


def product(pattern, left_side, right_side):
    if left_side.dtype == jnp.bfloat16 and right_side.dtype == jnp.bfloat16:
        return jnp.einsum(pattern, left_side, right_side, preferred_element_type=jnp.float32)
    return jnp.einsum(
        pattern,
        left_side,
        right_side,
        precision=lax.Precision.HIGHEST,
        preferred_element_type=jnp.float32,
    )


def normalize(inputs):
    mean_row = jnp.mean(inputs, axis=1, keepdims=True)
    centred = inputs - mean_row
    variance = jnp.mean(centred * centred, axis=1, keepdims=True)
    norm_scale = lax.rsqrt(variance + norm_epsilon)
    return (centred * norm_scale, norm_scale)


def norm_back(grad_normed, normed, norm_scale):
    mean_grad = jnp.mean(grad_normed, axis=1, keepdims=True)
    mean_cross = jnp.mean(grad_normed * normed, axis=1, keepdims=True)
    return norm_scale * (grad_normed - mean_grad - normed * mean_cross)


def row_layout(device, seq_device, seq_length, row_count):
    present = (seq_device == device).astype(jnp.int32)
    taken_rows = present * seq_length
    start_row = jnp.cumsum(taken_rows) - taken_rows
    row_index = jnp.arange(row_count, dtype=jnp.int32)[:, None]
    inside = (
        (present[None, :] > 0)
        & (row_index >= start_row[None, :])
        & (row_index < (start_row + taken_rows)[None, :])
    ).astype(jnp.int32)
    number = jnp.arange(seq_device.shape[0], dtype=jnp.int32)
    segment = jnp.sum(inside * number[None, :], axis=1)
    position = jnp.sum(inside * (row_index - start_row[None, :]), axis=1)
    return (segment, position)


def rotary_table(position):
    half_rot = ROT // 2
    frequency = jnp.exp(jnp.arange(half_rot, dtype=jnp.float32) * (-2.0 * math.log(10000.0) / ROT))
    angles = position.astype(jnp.float32)[:, None] * frequency[None, :]
    return (jnp.cos(angles), jnp.sin(angles))


def rotate(values, cosine_table, sine_table, reverse):
    half_rot = cosine_table.shape[1]
    first_half = values[..., :half_rot]
    second = values[..., half_rot : 2 * half_rot]
    cos_wide = cosine_table[:, None, :]
    sin_wide = sine_table[:, None, :]
    if reverse:
        new_first = first_half * cos_wide + second * sin_wide
        new_second = second * cos_wide - first_half * sin_wide
    else:
        new_first = first_half * cos_wide - second * sin_wide
        new_second = second * cos_wide + first_half * sin_wide
    return jnp.concatenate([new_first, new_second, values[..., 2 * half_rot :]], axis=-1)


def swap_major(values):
    return jnp.transpose(values, (1, 0, 2))


def cut_tiles(matrix):
    height, span_cols = matrix.shape
    return (
        matrix.reshape(height // BLK, BLK, span_cols // BLK, BLK)
        .transpose(0, 2, 1, 3)
        .reshape(-1, BLK, BLK)
    )


def slot_order(owners, slot_total):
    slot_ids = jnp.arange(slot_total, dtype=jnp.int32)
    matches = owners[None, :] == slot_ids[:, None]
    tile_index = jnp.sum(
        jnp.where(matches, jnp.arange(owners.shape[0], dtype=jnp.int32)[None, :], 0), axis=1
    )
    occupied = jnp.any(matches, axis=1)
    return (jnp.where(occupied, tile_index, owners.shape[0]), occupied)


def arrange(blocks, tile_index):
    padded = jnp.concatenate([blocks, jnp.zeros((1,) + blocks.shape[1:], blocks.dtype)], axis=0)
    return jnp.take(padded, tile_index, axis=0)


def rotated_adam(gradient, weight, left_basis, right_basis, first_state, second_state, occupied):
    turned = jnp.einsum("sji,sjk->sik", left_basis, gradient, precision=lax.Precision.HIGHEST)
    turned = jnp.einsum("sik,skl->sil", turned, right_basis, precision=lax.Precision.HIGHEST)
    new_first = beta_decay * first_state + (1.0 - beta_decay) * turned
    new_second = beta_decay * second_state + (1.0 - beta_decay) * turned * turned
    correction = 1.0 - beta_decay**STEP
    direction = new_first / correction / (jnp.sqrt(new_second / correction) + adam_epsilon)
    restored = jnp.einsum("sij,sjk->sik", left_basis, direction, precision=lax.Precision.HIGHEST)
    restored = jnp.einsum("sik,slk->sil", restored, right_basis, precision=lax.Precision.HIGHEST)
    new_weight = weight - learning_rate * (restored + weight_decay * weight)
    slot_mask = occupied.astype(jnp.float32)[:, None, None]
    return (slot_mask * new_first, slot_mask * new_second, slot_mask * new_weight)


def plain_adam(gradient, value_rows, first_state, second_state):
    new_first = beta_decay * first_state + (1.0 - beta_decay) * gradient
    new_second = beta_decay * second_state + (1.0 - beta_decay) * gradient * gradient
    correction = 1.0 - beta_decay**STEP
    new_value = value_rows - learning_rate * (new_first / correction) / (
        jnp.sqrt(new_second / correction) + adam_epsilon
    )
    return (new_first, new_second, new_value)


def local_any(
    tokens,
    cotangent,
    vec_params,
    qkv_weight,
    out_weight,
    up_weight,
    down_weight,
    probe_vec,
    probe_qkv,
    probe_out,
    probe_up,
    probe_down,
    seq_device,
    seq_length,
    owners,
    left_bases,
    right_bases,
    first_moment,
    second_moment,
    vec_first,
    vec_second,
):
    row_count, model_width = tokens.shape
    head_count = model_width // HEAD
    up_rows = up_weight.shape[1] // model_width
    device = lax.axis_index("dp")
    segment, position = row_layout(device, seq_device, seq_length, row_count)
    cosine_table, sine_table = rotary_table(position)
    row_index = jnp.arange(row_count, dtype=jnp.int32)
    allowed = (segment[:, None] == segment[None, :]) & (row_index[None, :] <= row_index[:, None])
    drift_vec = probe_vec[0]
    drift_qkv = probe_qkv[0]
    drift_out = probe_out[0]
    drift_up = probe_up[0]
    drift_down = probe_down[0]
    inputs = tokens.astype(jnp.float32)
    cot_rows = cotangent.astype(jnp.float32)
    normed, norm_scale = normalize(inputs)
    attn_in = normed * vec_params[0] + vec_params[1]
    drift_attn_in = normed * drift_vec[0] + drift_vec[1]
    mlp_in = normed * vec_params[2] + vec_params[3]
    drift_mlp_in = normed * drift_vec[2] + drift_vec[3]
    attn_low = attn_in.astype(jnp.bfloat16)
    mlp_low = mlp_in.astype(jnp.bfloat16)
    mixed_rows = product("ij,jk->ik", attn_low, qkv_weight) + vec_params[4:7].reshape(-1)
    drift_mixed = (
        product("ij,jk->ik", drift_attn_in, qkv_weight)
        + product("ij,jk->ik", attn_low, drift_qkv)
        + drift_vec[4:7].reshape(-1)
    )

    def split_heads(matrix, column_group):
        return matrix[:, column_group * model_width : (column_group + 1) * model_width].reshape(
            row_count, head_count, HEAD
        )

    query_rows = rotate(split_heads(mixed_rows, 0), cosine_table, sine_table, False)
    key_rows = rotate(split_heads(mixed_rows, 1), cosine_table, sine_table, False)
    value_rows = split_heads(mixed_rows, 2)
    drift_query = rotate(split_heads(drift_mixed, 0), cosine_table, sine_table, False)
    drift_key = rotate(split_heads(drift_mixed, 1), cosine_table, sine_table, False)
    drift_value = split_heads(drift_mixed, 2)
    grad_att = product("ij,kj->ik", cotangent, out_weight)
    drift_grad_att = product("ij,kj->ik", cotangent, drift_out)
    grad_att_low = grad_att.astype(jnp.bfloat16)

    def attend(pieces):
        query_block, key_block, value_block, drift_q, drift_k, drift_v, grad_out, drift_grad_out = (
            pieces
        )
        scores = product("ij,kj->ik", query_block, key_block) * 0.125
        drift_scores = (
            product("ij,kj->ik", drift_q, key_block) + product("ij,kj->ik", query_block, drift_k)
        ) * 0.125
        scores = jnp.where(allowed, scores, masked_score)
        shifted = scores - jnp.max(scores, axis=1, keepdims=True)
        exp_scores = jnp.exp(shifted)
        probs = exp_scores / jnp.sum(exp_scores, axis=1, keepdims=True)
        drift_probs = probs * (drift_scores - jnp.sum(probs * drift_scores, axis=1, keepdims=True))
        probs_low = probs.astype(jnp.bfloat16)
        attended_head = product("ij,jk->ik", probs_low, value_block)
        drift_attended_head = product("ij,jk->ik", drift_probs, value_block) + product(
            "ij,jk->ik", probs_low, drift_v
        )
        grad_probs = product("ij,kj->ik", grad_out, value_block)
        drift_grad_probs = product("ij,kj->ik", drift_grad_out, value_block) + product(
            "ij,kj->ik", grad_out, drift_v
        )
        grad_value_head = product("ij,ik->jk", probs_low, grad_out)
        drift_grad_value_head = product("ij,ik->jk", drift_probs, grad_out) + product(
            "ij,ik->jk", probs_low, drift_grad_out
        )
        centre = jnp.sum(probs * grad_probs, axis=1, keepdims=True)
        drift_centre = jnp.sum(
            drift_probs * grad_probs + probs * drift_grad_probs, axis=1, keepdims=True
        )
        grad_scores = probs * (grad_probs - centre)
        drift_grad_scores = drift_probs * (grad_probs - centre) + probs * (
            drift_grad_probs - drift_centre
        )
        scores_low = grad_scores.astype(jnp.bfloat16)
        grad_query_head = product("ij,jk->ik", scores_low, key_block) * 0.125
        drift_grad_query_head = (
            product("ij,jk->ik", drift_grad_scores, key_block)
            + product("ij,jk->ik", scores_low, drift_k)
        ) * 0.125
        grad_key_head = product("ij,ik->jk", scores_low, query_block) * 0.125
        drift_grad_key_head = (
            product("ij,ik->jk", drift_grad_scores, query_block)
            + product("ij,ik->jk", scores_low, drift_q)
        ) * 0.125
        return (
            attended_head,
            drift_attended_head,
            grad_query_head,
            grad_key_head,
            grad_value_head,
            drift_grad_query_head,
            drift_grad_key_head,
            drift_grad_value_head,
        )

    results = lax.map(
        attend,
        (
            swap_major(query_rows.astype(jnp.bfloat16)),
            swap_major(key_rows.astype(jnp.bfloat16)),
            swap_major(value_rows.astype(jnp.bfloat16)),
            swap_major(drift_query),
            swap_major(drift_key),
            swap_major(drift_value),
            swap_major(grad_att_low.reshape(row_count, head_count, HEAD)),
            swap_major(drift_grad_att.reshape(row_count, head_count, HEAD)),
        ),
    )
    attended = swap_major(results[0]).reshape(row_count, model_width)
    drift_attended = swap_major(results[1]).reshape(row_count, model_width)
    grad_query = rotate(swap_major(results[2]), cosine_table, sine_table, True).reshape(
        row_count, model_width
    )
    grad_key = rotate(swap_major(results[3]), cosine_table, sine_table, True).reshape(
        row_count, model_width
    )
    grad_value = swap_major(results[4]).reshape(row_count, model_width)
    drift_grad_query = rotate(swap_major(results[5]), cosine_table, sine_table, True).reshape(
        row_count, model_width
    )
    drift_grad_key = rotate(swap_major(results[6]), cosine_table, sine_table, True).reshape(
        row_count, model_width
    )
    drift_grad_value = swap_major(results[7]).reshape(row_count, model_width)
    grad_mixed_low = jnp.concatenate([grad_query, grad_key, grad_value], axis=1).astype(
        jnp.bfloat16
    )
    drift_grad_mixed = jnp.concatenate([drift_grad_query, drift_grad_key, drift_grad_value], axis=1)
    att_low = attended.astype(jnp.bfloat16)
    attn_out = product("ij,jk->ik", att_low, out_weight) + vec_params[7]
    hidden = product("ij,jk->ik", mlp_low, up_weight) + vec_params[8 : 8 + up_rows].reshape(-1)
    drift_hidden = (
        product("ij,jk->ik", drift_mlp_in, up_weight)
        + product("ij,jk->ik", mlp_low, drift_up)
        + drift_vec[8 : 8 + up_rows].reshape(-1)
    )
    cumulative = 0.5 * (1.0 + lax.erf(hidden * root_half))
    density = jnp.exp(-0.5 * hidden * hidden) * density_scale
    activated = hidden * cumulative
    gelu_slope = cumulative + hidden * density
    gelu_bend = density * (2.0 - hidden * hidden)
    act_low = activated.astype(jnp.bfloat16)
    drift_act = gelu_slope * drift_hidden
    mlp_out = product("ij,jk->ik", act_low, down_weight) + vec_params[8 + up_rows]
    block_output = (inputs + attn_out + mlp_out).astype(jnp.bfloat16)
    grad_down = product("ij,ik->jk", act_low, cotangent)
    drift_grad_down = product("ij,ik->jk", drift_act, cotangent)
    grad_act = product("ij,kj->ik", cotangent, down_weight)
    drift_grad_act = product("ij,kj->ik", cotangent, drift_down)
    grad_hidden = grad_act * gelu_slope
    drift_grad_hidden = drift_grad_act * gelu_slope + grad_act * gelu_bend * drift_hidden
    grad_hidden_low = grad_hidden.astype(jnp.bfloat16)
    grad_up = product("ij,ik->jk", mlp_low, grad_hidden_low)
    drift_grad_up = product("ij,ik->jk", drift_mlp_in, grad_hidden_low) + product(
        "ij,ik->jk", mlp_low, drift_grad_hidden
    )
    grad_mlp_in = product("ij,kj->ik", grad_hidden_low, up_weight)
    drift_grad_mlp_in = product("ij,kj->ik", drift_grad_hidden, up_weight) + product(
        "ij,kj->ik", grad_hidden_low, drift_up
    )
    grad_out_w = product("ij,ik->jk", att_low, cotangent)
    drift_grad_out_w = product("ij,ik->jk", drift_attended, cotangent)
    grad_qkv = product("ij,ik->jk", attn_low, grad_mixed_low)
    drift_grad_qkv = product("ij,ik->jk", drift_attn_in, grad_mixed_low) + product(
        "ij,ik->jk", attn_low, drift_grad_mixed
    )
    grad_attn_in = product("ij,kj->ik", grad_mixed_low, qkv_weight)
    drift_grad_attn_in = product("ij,kj->ik", drift_grad_mixed, qkv_weight) + product(
        "ij,kj->ik", grad_mixed_low, drift_qkv
    )
    grad_weighted = grad_attn_in * vec_params[0] + grad_mlp_in * vec_params[2]
    input_grad = cot_rows + norm_back(grad_weighted, normed, norm_scale)
    out_sum = jnp.sum(cot_rows, axis=0)[None]
    zero_row = jnp.zeros((1, model_width), jnp.float32)
    vec_grad = jnp.concatenate(
        [
            jnp.sum(grad_attn_in * normed, axis=0)[None],
            jnp.sum(grad_attn_in, axis=0)[None],
            jnp.sum(grad_mlp_in * normed, axis=0)[None],
            jnp.sum(grad_mlp_in, axis=0)[None],
            jnp.sum(grad_mixed_low, axis=0, dtype=jnp.float32).reshape(3, model_width),
            out_sum,
            jnp.sum(grad_hidden_low, axis=0, dtype=jnp.float32).reshape(up_rows, model_width),
            out_sum,
        ],
        axis=0,
    )
    vec_drift = jnp.concatenate(
        [
            jnp.sum(drift_grad_attn_in * normed, axis=0)[None],
            jnp.sum(drift_grad_attn_in, axis=0)[None],
            jnp.sum(drift_grad_mlp_in * normed, axis=0)[None],
            jnp.sum(drift_grad_mlp_in, axis=0)[None],
            jnp.sum(drift_grad_mixed, axis=0).reshape(3, model_width),
            zero_row,
            jnp.sum(drift_grad_hidden, axis=0).reshape(up_rows, model_width),
            zero_row,
        ],
        axis=0,
    )
    along_probe = jnp.sum(vec_grad * drift_vec)
    curve_probe = jnp.sum(vec_drift * drift_vec)
    for gradient, drift_gradient, direction_set in (
        (grad_qkv, drift_grad_qkv, drift_qkv),
        (grad_out_w, drift_grad_out_w, drift_out),
        (grad_up, drift_grad_up, drift_up),
        (grad_down, drift_grad_down, drift_down),
    ):
        along_probe = along_probe + jnp.sum(gradient * direction_set.astype(jnp.float32))
        curve_probe = curve_probe + jnp.sum(drift_gradient * direction_set.astype(jnp.float32))
    dots = jnp.stack([along_probe, curve_probe])
    grad_tiles = jnp.concatenate(
        [cut_tiles(grad_qkv), cut_tiles(grad_out_w), cut_tiles(grad_up), cut_tiles(grad_down)],
        axis=0,
    )
    curve_tiles = jnp.concatenate(
        [
            cut_tiles(drift_grad_qkv),
            cut_tiles(drift_grad_out_w),
            cut_tiles(drift_grad_up),
            cut_tiles(drift_grad_down),
        ],
        axis=0,
    )
    slot_dev = left_bases.shape[0]
    slot_total = slot_dev * lax.axis_size("dp")
    tile_index, occupied = slot_order(owners, slot_total)
    slot_grad = arrange(grad_tiles, tile_index)
    slot_curve = arrange(curve_tiles, tile_index)
    own_grad, own_curve = (
        lax.psum_scatter(slot_grad, "dp", scatter_dimension=0, tiled=True),
        lax.psum_scatter(slot_curve, "dp", scatter_dimension=0, tiled=True),
    )
    vec_total, vec_curve, dot_total = lax.psum((vec_grad, vec_drift, dots), "dp")
    all_dots = lax.all_gather(dot_total[None, :], "probe", axis=0, tiled=True)
    own_index = lax.dynamic_slice_in_dim(tile_index, device * slot_dev, slot_dev)
    own_used = lax.dynamic_slice_in_dim(occupied, device * slot_dev, slot_dev)
    weight_tiles = jnp.concatenate(
        [
            cut_tiles(qkv_weight),
            cut_tiles(out_weight),
            cut_tiles(up_weight),
            cut_tiles(down_weight),
        ],
        axis=0,
    )
    own_weight = arrange(weight_tiles, own_index).astype(jnp.float32)
    new_first, new_second, new_weights = rotated_adam(
        own_grad, own_weight, left_bases, right_bases, first_moment, second_moment, own_used
    )
    new_weights_low = new_weights.astype(jnp.bfloat16)
    vec_new_first, vec_new_second, vec_new = plain_adam(
        vec_total, vec_params, vec_first, vec_second
    )
    vector_state = jnp.stack([vec_total, vec_new_first], axis=0)
    return (
        block_output,
        input_grad,
        own_grad,
        new_first,
        new_second,
        new_weights,
        new_weights_low,
        own_curve[None],
        vector_state,
        vec_new_second,
        vec_new,
        vec_curve[None],
        all_dots,
    )


f32 = jnp.float32
bf16 = jnp.bfloat16
VMEM_SHARD = 60 << 20
HEAD_A = (0, 1, 7, 8, 3, 4, 10, 11)
HEAD_B = (6, 6, 2, 2, 9, 9, 5, 5)
ARRIVE = ((1, 2, 3), (0, 2, 3), (3, 1, 0), (2, 1, 0))


def fits_tp(mesh):
    return mesh.shape["dp"] == 8 and mesh.shape["probe"] == 4


def device_table():
    rows = []
    for device in range(8):
        z, x = device // 2, device % 2
        levels = (z,) + ARRIVE[z]
        order = [2 * level + x for level in levels] + [2 * level + 1 - x for level in levels]
        for probe in range(4):
            rows.append([device, HEAD_A[device], HEAD_B[device], probe % 2, x, probe // 2, z % 2, 0] + order)
    return rows


def is_short(seq_device, seq_length, group, rows):
    longest = jnp.int32(0)
    for i in range(seq_device.shape[0]):
        longest = jnp.maximum(longest, jnp.where(seq_device[i] == group, seq_length[i], 0))
    return (longest < rows).astype(jnp.int32)


def in_hbm(value):
    return pltpu.with_memory_space_constraint(value, pltpu.HBM)


def dot_nt(left, right):
    return lax.dot_general(left, right, (((1,), (1,)), ((), ())), preferred_element_type=f32)


def dot_nn(left, right):
    return lax.dot_general(left, right, (((1,), (0,)), ((), ())), preferred_element_type=f32)


def rotate_rows(ref, base, cos, sin, reverse):
    up, low = ref[base : base + 8, :], ref[base + 8 : base + 16, :]
    if reverse:
        ref[base : base + 8, :] = up * cos + low * sin
        ref[base + 8 : base + 16, :] = low * cos - up * sin
    else:
        ref[base : base + 8, :] = up * cos - low * sin
        ref[base + 8 : base + 16, :] = low * cos + up * sin


def mask_rows(bias, short, rows):
    for start in range(0, rows, 128):
        row = lax.broadcasted_iota(jnp.int32, (128, rows), 0) + start
        col = lax.broadcasted_iota(jnp.int32, (128, rows), 1)
        first = jnp.where(short == 1, start, 0)
        bias[start : start + 128, :] = jnp.where((col >= first) & (col <= row), 0.0, masked_score)


def one_row(block, index):
    rows = lax.broadcasted_iota(jnp.int32, block.shape, 0)
    return jnp.sum(jnp.where(rows == index, block, 0.0), axis=0, keepdims=True)


def prepare_kernel(info, up_0, up_1, dup_0, dup_1, down, ddown, qkv, dqkv, out_w, dout_w, vec, dvec, uwt, dwt, bias_u, wat, oat, bias_a, turn, turn_h):
    j = pl.program_id(0)
    device = info[0]
    row = lax.broadcasted_iota(jnp.int32, (48, 128), 0) + (device * 48) % 128
    lane = lax.broadcasted_iota(jnp.int32, (48, 128), 1)
    pick_0, pick_1 = (lane == row).astype(bf16), (lane == row - 128).astype(bf16)
    for part, (first, second, below, bias) in enumerate(((up_0, up_1, down, vec), (dup_0, dup_1, ddown, dvec))):
        uwt[part, 0] = (dot_nt(pick_0, first[...]) + dot_nt(pick_1, second[...])).astype(bf16)
        dwt[part, 0] = below[...]
        line = one_row(bias[8:12, pl.ds(pl.multiple_of(384 * (j % 2), 128), 384)], j // 2)
        turn[...] = jnp.transpose(jnp.broadcast_to(line, (128, 384)))
        bias_u[part, 0] = turn[pl.ds(pl.multiple_of(device * 48, 16), 48), :]

    @pl.when(j < 6)
    def _():
        head = info[1 + j // 3]
        row = lax.broadcasted_iota(jnp.int32, (64, 128), 0) + (head % 2) * 64
        pick = (lax.broadcasted_iota(jnp.int32, (64, 128), 1) == row).astype(bf16)
        rows, drows = dot_nt(pick, qkv[...]).astype(bf16), dot_nt(pick, dqkv[...]).astype(bf16)
        wat[:, :768] = drows
        wat[:, 768:] = rows
        oat[:64, :] = out_w[...]
        oat[64:, :] = dout_w[...]
        for part, bias in enumerate((vec, dvec)):
            line = one_row(bias[4:7, pl.ds(pl.multiple_of(128 * (head // 2), 128), 128)], j % 3)
            turn_h[...] = jnp.transpose(jnp.broadcast_to(line, (128, 128)))
            bias_a[part * 64 : part * 64 + 64, :] = turn_h[pl.ds(pl.multiple_of((head % 2) * 64, 64), 64), :]


def prepare(info, qkv, dqkv, out_w, dout_w, up, dup, down, ddown, vec, dvec):
    def at_head(i):
        return jnp.minimum(i, 5)

    whole = pl.BlockSpec(memory_space=pltpu.VMEM)
    up_0 = pl.BlockSpec((768, 128), lambda i, info: (0, 3 * i + (info[0] * 48) // 128))
    up_1 = pl.BlockSpec((768, 128), lambda i, info: (0, 3 * i + jnp.minimum((info[0] * 48) // 128 + 1, 2)))
    down_spec = pl.BlockSpec((48, 768), lambda i, info: (8 * i + info[0], 0))
    qkv_spec = pl.BlockSpec((768, 128), lambda i, info: (0, 6 * (at_head(i) % 3) + info[1 + at_head(i) // 3] // 2))
    out_spec = pl.BlockSpec((64, 768), lambda i, info: (info[1 + at_head(i) // 3], 0))
    uwt, dwt, bias_u, wat, oat, bias_a = pl.pallas_call(
        prepare_kernel,
        out_shape=[
            jax.ShapeDtypeStruct((2, 8, 48, 768), bf16),
            jax.ShapeDtypeStruct((2, 8, 48, 768), bf16),
            jax.ShapeDtypeStruct((2, 8, 48, 128), f32),
            jax.ShapeDtypeStruct((384, 1536), bf16),
            jax.ShapeDtypeStruct((256, 768), bf16),
            jax.ShapeDtypeStruct((768, 128), f32),
        ],
        grid_spec=pltpu.PrefetchScalarGridSpec(
            num_scalar_prefetch=1,
            grid=(8,),
            in_specs=[up_0, up_1, up_0, up_1, down_spec, down_spec, qkv_spec, qkv_spec, out_spec, out_spec, whole, whole],
            out_specs=[
                pl.BlockSpec((2, 1, 48, 768), lambda i, info: (0, i, 0, 0)),
                pl.BlockSpec((2, 1, 48, 768), lambda i, info: (0, i, 0, 0)),
                pl.BlockSpec((2, 1, 48, 128), lambda i, info: (0, i, 0, 0)),
                pl.BlockSpec((64, 1536), lambda i, info: (at_head(i), 0)),
                pl.BlockSpec((128, 768), lambda i, info: (at_head(i) // 3, 0)),
                pl.BlockSpec((128, 128), lambda i, info: (at_head(i), 0)),
            ],
            scratch_shapes=[pltpu.VMEM((384, 128), f32), pltpu.VMEM((128, 128), f32)],
        ),
        compiler_params=pltpu.CompilerParams(vmem_limit_bytes=VMEM_SHARD),
        cost_estimate=pl.CostEstimate(flops=10**9, bytes_accessed=2 * 10**7, transcendentals=0),
        name="prepare",
    )(info, *(in_hbm(value) for value in (up, up, dup, dup, down, ddown, qkv, dqkv, out_w, dout_w)), vec, dvec)
    return (uwt.reshape(768, 768), dwt.reshape(768, 768), bias_u.reshape(768, 128), wat, oat, bias_a)


def wide(column):
    return jnp.concatenate([column] * 4, axis=1)


def shard_kernel(plan, first, *refs):
    refs = list(refs)
    info, seq_device, seq_length = refs[:3]
    steps = len(plan)
    data_h = refs[3 : 3 + 2 * steps]
    refs = refs[3 + 2 * steps :]
    vec, dvec, cos_ref, sin_ref = refs[:4]
    weights_h = refs[4:10]
    refs = refs[10:]
    old_h = None if first else refs[:4]
    refs = refs if first else refs[4:]
    out_h = refs[:4]
    (mine, other, wat, bias_a, oat, uwt, dwt, bias_u, acc_h, acc_m, acc_c, acc_r, sem) = refs[4:17]
    (nb, nb_low, ones, lhs_a, ml, dm, dm_low, cb, mask, proj, gat, qt, kt, k4, vt, v4, gt, q4, g4, gq, gk, gv, head_g, head_a, hid, act, mlp_a, mlp_g, one, two) = refs[17:]
    new = (acc_h, acc_m, acc_c, acc_r)
    step = pl.program_id(0)
    core = info[3]
    most = max(heads for _, heads in plan)

    def by_step(values):
        result = jnp.int32(values[0])
        for i, value in enumerate(values[1:]):
            result = jnp.where(step > i, value, result)
        return result

    heads_now = by_step([heads for _, heads in plan])
    short = is_short(seq_device, seq_length, info[8 + by_step([index for index, _ in plan])], 512)
    width = 768
    gain_a, shift_a, gain_m, shift_m = (vec[i : i + 1, :] for i in range(4))
    dgain_a, dshift_a, dgain_m, dshift_m = (dvec[i : i + 1, :] for i in range(4))
    wat_h, bias_ah, oat_h, uwt_h, dwt_h, bias_uh = weights_h
    lead = most * 384
    pairs = [
        (data_h[0], mine.at[0]),
        (data_h[1], other.at[0]),
        (uwt_h, uwt),
        (dwt_h, dwt),
        (bias_uh, bias_u),
        (wat_h.at[: most * 192], wat),
        (oat_h.at[: most * 128], oat),
        (bias_ah.at[:lead], bias_a),
    ]
    if not first:
        pairs += [(old_h[1], acc_m), (old_h[2], acc_c), (old_h[3], acc_r), (old_h[0].at[: most * 512], acc_h)]
    base_count = len(pairs)
    for i in range(1, steps):
        pairs += [(data_h[2 * i], mine.at[i]), (data_h[2 * i + 1], other.at[i])]
    arrivals = [pltpu.make_async_copy(source, target, sem.at[i]) for i, (source, target) in enumerate(pairs)]

    def at_step(which):
        if steps == 1:
            return lambda body: body()
        return pl.when(step == which)

    @at_step(0)
    def _():
        for copy in arrivals:
            copy.start()

    def arrived(*which):
        @at_step(0)
        def _():
            for i in which:
                if i < base_count:
                    arrivals[i].wait()

    ones[...] = jnp.ones((512, 128), bf16)
    mask_rows(mask, short, 512)

    def load(ref, cot_ref, base, count):
        def rows_of(i, carry):
            src = pl.ds(pl.multiple_of(i * 128, 128), 128)
            dst = pl.ds(pl.multiple_of(base + i * 128, 128), 128)
            rows = ref[step, src, :width].astype(f32)
            centred = rows - jnp.mean(rows, axis=1, keepdims=True)
            variance = jnp.mean(centred * centred, axis=1, keepdims=True)
            normed = centred * lax.rsqrt(variance + norm_epsilon)
            nb[dst, :], nb_low[dst, :] = split_two(normed)
            lhs_a[dst, :width] = (normed * gain_a + shift_a).astype(bf16)
            lhs_a[dst, width : 2 * width], lhs_a[dst, 2 * width :] = split_two(normed * dgain_a + dshift_a)
            ml[dst, :] = (normed * gain_m + shift_m).astype(bf16)
            dm[dst, :], dm_low[dst, :] = split_two(normed * dgain_m + dshift_m)
            cb[dst, :] = cot_ref[step, src, :].astype(bf16)
            return carry

        lax.fori_loop(0, count, rows_of, 0)

    if first:
        arrived(0, 1)
        load(mine, other, 0, 4)
    else:
        arrived(0)
        for i in range(1, steps):

            @at_step(i)
            def _(i=i):
                arrivals[base_count + 2 * i - 2].wait()
                arrivals[base_count + 2 * i - 1].wait()

        load(mine, mine.at[:, :, width:], core * 256, 2)
        arrived(1)
        load(other, other.at[:, :, width:], (1 - core) * 256, 2)

    def add(ref, rows, value):
        ref[rows, :] = value if first else ref[rows, :] + value

    def eight(value):
        rows, columns = value.shape
        return jnp.sum(value.reshape(rows // 8, 8, columns), axis=0)

    def fold(carry, ref, at, tops, w_rows, dw_rows, dgain, dshift, c_rows):
        grad_at, curve_at = at
        top, low = tops
        p_two, q_two = two[top, :], two[low, :]
        add(ref, grad_at, one[top, :])
        moved = dgain * p_two + dshift * c_rows
        add(ref, curve_at, one[low, :] + moved)
        w_wide, dw_wide = w_rows.astype(f32), dw_rows.astype(f32)
        drift, plain, dots = carry
        drift = drift + eight(w_wide * q_two + dw_wide * p_two)
        plain = plain + eight(w_wide * p_two)
        dots = dots + eight(dw_wide * (2.0 * moved))
        return (drift, plain, dots)

    arrived(2, 3, 4)
    hid[...] = dot_nt(uwt[...], ml[...])
    act[...] = dot_nt(dwt[...], cb[...])
    hid[384:, :] += dot_nt(uwt[:384, :], dm[...]) + dot_nt(uwt[:384, :], dm_low[...])

    def gelu(i, carry):
        top = pl.ds(pl.multiple_of(i * 32, 32), 32)
        low = pl.ds(pl.multiple_of(384 + i * 32, 32), 32)
        hidden, dhidden = hid[top, :] + wide(bias_u[top, :]), hid[low, :] + wide(bias_u[low, :])
        grad_act, dgrad_act = act[top, :], act[low, :]
        cumulative = 0.5 * (1.0 + lax.erf(hidden * root_half))
        density = jnp.exp(-0.5 * hidden * hidden) * density_scale
        slope = cumulative + hidden * density
        bend = density * (2.0 - hidden * hidden)
        drift_act = slope * dhidden
        drift_grad = dgrad_act * slope + grad_act * bend * dhidden
        mlp_a[top, :] = (hidden * cumulative).astype(bf16)
        mlp_a[low, :] = drift_act.astype(bf16)
        mlp_g[top, :] = (grad_act * slope).astype(bf16)
        mlp_g[low, :] = drift_grad.astype(bf16)
        return carry + eight(drift_grad * dhidden + drift_act * dgrad_act)

    dots_m = lax.fori_loop(0, 12, gelu, jnp.zeros((8, 512), f32))
    one[...] = dot_nn(mlp_g[...], ml[...])
    two[...] = dot_nn(mlp_g[...], nb[...])
    two[:384, :] += dot_nn(mlp_g[:384, :], nb_low[...])
    sums = dot_nn(mlp_g[...], ones[...])
    arrived(8, 9, 10)
    add(acc_c, slice(768, 1536), sums)
    proj[0:384, 0:128] = sums[:384, :]

    def fold_m(i, carry):
        top = pl.ds(pl.multiple_of(i * 64, 64), 64)
        low = pl.ds(pl.multiple_of(384 + i * 64, 64), 64)
        return fold(carry, acc_m, (top, low), (top, low), uwt[top, :], uwt[low, :], dgain_m, dshift_m, proj[top, 0:1])

    blank = jnp.zeros((8, width), f32)
    carry_m = (blank, blank, blank) if first else (acc_r[8:16, :], acc_r[24:32, :], acc_r[32:40, :])
    acc_r[8:16, :], acc_r[24:32, :], acc_r[32:40, :] = lax.fori_loop(0, 6, fold_m, carry_m)
    acc_r[32:40, :512] += dots_m
    one[...] = dot_nn(mlp_a[...], cb[...])
    add(acc_m, slice(768, 1536), one[...])
    leave_m = pltpu.make_async_copy(acc_m, out_h[1], sem.at[0])

    @at_step(steps - 1)
    def _():
        leave_m.start()

    arrived(5, 6, 7, 11)
    cos, sin = cos_ref[short], sin_ref[short]

    def attend(head, carry):
        base = pl.multiple_of(head * 384, 128)
        w_at = pl.ds(pl.multiple_of(head * 192, 64), 192)
        plain = dot_nt(wat[w_at, width:], lhs_a[:, :width])
        drift = dot_nt(wat[w_at, :], lhs_a[:, : 2 * width]) + dot_nt(wat[w_at, width:], lhs_a[:, 2 * width :])
        for kind in range(3):
            proj[kind * 128 : kind * 128 + 64, :] = plain[kind * 64 : kind * 64 + 64, :]
            proj[kind * 128 + 64 : kind * 128 + 128, :] = drift[kind * 64 : kind * 64 + 64, :]
        proj[...] += wide(bias_a[pl.ds(base, 384), :])
        gat[...] = dot_nt(oat[pl.ds(pl.multiple_of(head * 128, 128), 128), :], cb[...])
        for part in (0, 64, 128, 192):
            rotate_rows(proj, part, cos, sin, False)
        proj[0:128, :] = proj[0:128, :] * 0.125
        rests = []
        for source, flat, tall, back in ((proj.at[0:128], qt, q4, True), (proj.at[128:256], kt, k4, False), (proj.at[256:384], vt, v4, False), (gat, gt, g4, True)):
            own, moved = source[0:64, :], source[64:128, :]
            flat[0:64, :] = own.astype(bf16)
            high, low = split_two(moved)
            flat[64:128, :] = high
            if back:
                low_wide = low.astype(f32)
                rests.append(low_wide)
                tall[...] = jnp.transpose(jnp.concatenate([own, own, high.astype(f32), low_wide], axis=0)).astype(bf16)
            else:
                tall[0:64, :] = high
                tall[64:128, :] = low
                tall[128:192, :] = flat[0:64, :]
                tall[192:256, :] = flat[0:64, :]
        rest_q, rest_g = rests
        for block in range(2):
            rows = slice(block * 256, block * 256 + 256)
            span = block * 256 + 256
            scores = dot_nn(q4[rows, :64], kt[:64, :span]) + mask[rows, :span]
            dscores = dot_nn(q4[rows, :], k4[:, :span])
            exp_scores = jnp.exp(scores - jnp.max(scores, axis=1, keepdims=True))
            probs = exp_scores * (1.0 / jnp.sum(exp_scores, axis=1, keepdims=True))
            dprobs = probs * (dscores - jnp.sum(probs * dscores, axis=1, keepdims=True))
            probs_low, dprobs_low = probs.astype(bf16), dprobs.astype(bf16)
            grad_probs = dot_nn(g4[rows, :64], vt[:64, :span])
            dgrad_probs = dot_nn(g4[rows, :], v4[:, :span])
            centre = jnp.sum(probs * grad_probs, axis=1, keepdims=True)
            dcentre = jnp.sum(dprobs * grad_probs + probs * dgrad_probs, axis=1, keepdims=True)
            rest = grad_probs - centre
            g_scores = (probs * rest).astype(bf16)
            dg_wide = dprobs * rest + probs * (dgrad_probs - dcentre)
            dg_scores = dg_wide.astype(bf16)
            acc_r[32:40, :span] += eight(dprobs * dgrad_probs + dg_wide * dscores)
            out = dot_nt(vt[:, :span], probs_low)
            head_a[0:64, rows] = out[:64, :].astype(bf16)
            head_a[64:128, rows] = (out[64:, :] + dot_nt(vt[:64, :span], dprobs_low)).astype(bf16)
            part_q = dot_nt(kt[:, :span], g_scores)
            acc_r[32:40, rows] += 2.0 * eight(rest_g[:, rows] * out[64:, :] + rest_q[:, rows] * part_q[64:, :])
            gq[:, rows] = part_q * 0.125
            gq[64:, rows] += dot_nt(kt[:64, :span], dg_scores) * 0.125
            part_v = dot_nn(gt[:, rows], probs_low)
            part_dv = dot_nn(gt[:64, rows], dprobs_low)
            part_k = dot_nn(qt[:, rows], g_scores)
            part_dk = dot_nn(qt[:64, rows], dg_scores)
            acc_r[32:40, :span] += 2.0 * eight(proj[320:384, :span] * part_v[64:, :] + proj[192:256, :span] * part_k[64:, :])
            if block == 0:
                gv[:, :span] = part_v
                gk[:, :span] = part_k
                gv[:, span:] = jnp.zeros((128, 512 - span), f32)
                gk[:, span:] = jnp.zeros((128, 512 - span), f32)
            else:
                gv[:, :span] += part_v
                gk[:, :span] += part_k
            gv[64:, :span] += part_dv
            gk[64:, :span] += part_dk
        for part in (0, 64):
            rotate_rows(gq, part, cos, sin, True)
            rotate_rows(gk, part, cos, sin, True)
        for kind, grad in enumerate((gq, gk, gv)):
            head_g[kind * 64 : kind * 64 + 64, :] = grad[:64, :].astype(bf16)
            head_g[192 + kind * 64 : 256 + kind * 64, :] = grad[64:, :].astype(bf16)
        one[:384, :] = dot_nn(head_g[...], lhs_a[:, :width])
        two[:384, :] = dot_nn(head_g[...], nb[...])
        two[:192, :] += dot_nn(head_g[:192, :], nb_low[...])
        sums = dot_nn(head_g[...], ones[...])
        add(acc_c, pl.ds(base, 384), sums)
        for kind in range(3):
            at = pl.multiple_of(head * 512 + kind * 128, 128)
            top, low = slice(kind * 64, kind * 64 + 64), slice(192 + kind * 64, 256 + kind * 64)
            w_rows = pl.ds(pl.multiple_of(head * 192 + kind * 64, 64), 64)
            carry = fold(
                carry, acc_h, (pl.ds(at, 64), pl.ds(at + 64, 64)), (top, low),
                wat[w_rows, width:], wat[w_rows, :width], dgain_a, dshift_a, sums[top, 0:1],
            )
        add(acc_h, pl.ds(pl.multiple_of(head * 512 + 384, 128), 128), dot_nn(head_a[...], cb[...]))
        return carry

    carry_r = (blank, blank, blank) if first else (acc_r[0:8, :], acc_r[16:24, :], blank)
    if most == 1:
        carry_r = attend(0, carry_r)
    else:
        carry_r = lax.fori_loop(0, heads_now, attend, carry_r)
    acc_r[0:8, :], acc_r[16:24, :] = carry_r[:2]
    acc_r[32:40, :] += carry_r[2]
    leaves = [
        pltpu.make_async_copy(acc_c, out_h[2], sem.at[1]),
        pltpu.make_async_copy(acc_r, out_h[3], sem.at[2]),
        pltpu.make_async_copy(acc_h.at[: most * 512], out_h[0].at[: most * 512], sem.at[3]),
    ]

    @at_step(steps - 1)
    def _():
        for copy in leaves:
            copy.start()
        leave_m.wait()
        for copy in leaves:
            copy.wait()


def shard_steps(plan, scalars, data, shared, tables, old):
    first = old is None
    sizes = [(1024, 768), (1536, 768), (1536, 128), (40, 768)]
    steps = len(plan)
    most = max(heads for _, heads in plan)
    whole = pl.BlockSpec(memory_space=pltpu.VMEM)
    there = pl.BlockSpec(memory_space=pltpu.HBM)
    specs = [pl.BlockSpec(memory_space=pl.ANY)] * (2 * steps) + [whole] * 4 + [there] * 6
    vec, dvec, wat, bias_a, oat, uwt, dwt, bias_u = shared
    operands = [*data, vec, dvec, *tables, wat, bias_a, oat, uwt, dwt, bias_u]
    aliases = {}
    if not first:
        aliases = {3 + len(operands) + i: i for i in range(len(sizes))}
        specs += [there] * len(sizes)
        operands += list(old)
    scratch = [((steps, *data[0].shape), data[0].dtype), ((steps, *data[1].shape), data[1].dtype)]
    scratch += [((most * 192, 1536), bf16), ((most * 384, 128), f32), ((most * 128, 768), bf16)]
    scratch += [((768, 768), bf16)] * 2 + [((768, 128), f32)]
    scratch += [((most * 512, 768), f32)] + [(size, f32) for size in sizes[1:]] + [None]
    scratch += [
        ((512, 768), bf16),
        ((512, 768), bf16),
        ((512, 128), bf16),
        ((512, 2304), bf16),
        ((512, 768), bf16),
        ((512, 768), bf16),
        ((512, 768), bf16),
        ((512, 768), bf16),
        ((512, 512), f32),
        ((384, 512), f32),
        ((128, 512), f32),
    ]
    flat, tall, back = ((128, 512), bf16), ((256, 512), bf16), ((512, 256), bf16)
    scratch += [flat, flat, tall, flat, tall, flat, back, back] + [((128, 512), f32)] * 3
    scratch += [((384, 512), bf16), ((128, 512), bf16)]
    scratch += [((768, 512), f32)] * 2 + [((768, 512), bf16)] * 2 + [((768, 768), f32)] * 2
    return pl.pallas_call(
        lambda *refs: shard_kernel(plan, first, *refs),
        out_shape=[jax.ShapeDtypeStruct(size, f32) for size in sizes],
        grid_spec=pltpu.PrefetchScalarGridSpec(
            num_scalar_prefetch=3,
            grid=(steps,),
            in_specs=specs,
            out_specs=[there] * len(sizes),
            scratch_shapes=[pltpu.SemaphoreType.DMA((16,)) if one is None else pltpu.VMEM(*one) for one in scratch],
        ),
        input_output_aliases=aliases,
        compiler_params=pltpu.CompilerParams(vmem_limit_bytes=VMEM_SHARD),
        cost_estimate=pl.CostEstimate(
            flops=sum(heads * 2 * 10**9 + 5 * 10**9 for _, heads in plan), bytes_accessed=2 * 10**7, transcendentals=10**6
        ),
        name="shards" + "".join(str(heads) for _, heads in plan),
    )(*scalars, *operands)


def put_tile(slot_dev, owner, y, tile, curve, grad, curve_rows, grad_rows):
    group = slot_dev // 2
    slot = owner[tile]
    curve_rows(curve.at[slot])
    home, place = slot // slot_dev, slot % slot_dev

    @pl.when(place // group == y)
    def _():
        grad_rows(grad.at[home * group + place % group])


def tile_at(kind, side):
    return (side * 6 + 2 * kind, 1) if kind < 3 else (12 + side, 2)


def finish_kernel(slot_dev, owner, info, acc_h, acc_m, acc_c, acc_r, wat, oat, uwt, dwt, out_sum, curve, grad, sums):
    core, y, odd = info[3], info[5], info[6]
    if slot_dev * 8 > 48:
        curve[...] = jnp.zeros(curve.shape, f32)
        grad[...] = jnp.zeros(grad.shape, f32)

    def put(tile, columns, source, curve_at, grad_at):
        def curve_rows(ref):
            ref[...] = source[curve_at : curve_at + 48, columns]

        def grad_rows(ref):
            ref[...] = source[pl.ds(pl.multiple_of(grad_at + core * 24, 8), 24), columns]

        put_tile(slot_dev, owner, y, tile, curve, grad, curve_rows, grad_rows)

    for side in range(2):
        columns = slice(side * 384, side * 384 + 384)
        for kind in range(4):
            lower, step = tile_at(kind, side)
            put(lower + odd * step, columns, acc_h, kind * 128 + 64, kind * 128)
        for block in range(8):
            at = block * 48
            put(16 + side * 8 + block, columns, acc_m, 384 + at, at)
            put(32 + block * 2 + side, columns, acc_m, 1152 + at, 768 + at)
    small_sums_kernel(info, acc_h, acc_m, acc_c, acc_r, wat, oat, uwt, dwt, out_sum, sums)


def finish_split_kernel(slot_dev, owner, info, own_b, near_b, extra, old_curve, old_grad, curve, grad, new_curve, new_grad, sem):
    core, x, y, odd = info[3], info[4], info[5], info[6]
    group = slot_dev // 2
    for index in range(8):
        near_b[index] += own_b[0, pl.ds(pl.multiple_of(index * 64 + x * 32, 32), 32), :]
    copies, later = [], []
    for kind in range(4):
        for side in range(2):
            columns = slice(side * 384, side * 384 + 384)
            lower, step = tile_at(kind, side)
            slot = owner[lower + (1 - odd) * step]
            place = kind * 2 + side
            new_curve[place, 0:32, :] = near_b[kind * 2 + 1, :, columns]
            new_curve[place, 32:48, :] = extra[kind * 2 + 1, :, columns]
            copy = pltpu.make_async_copy(new_curve.at[place], curve.at[slot], sem.at[place])
            copy.start()
            copies.append(copy)

            @pl.when(core == 0)
            def _(place=place, kind=kind, columns=columns):
                new_grad[place] = near_b[kind * 2, 0:24, columns]

            @pl.when(core == 1)
            def _(place=place, kind=kind, columns=columns):
                new_grad[place, 0:8, :] = near_b[kind * 2, 24:32, columns]
                new_grad[place, 8:24, :] = extra[kind * 2, :, columns]

            home, spot = slot // slot_dev, slot % slot_dev

            @pl.when(spot // group == y)
            def _(place=place, home=home, spot=spot):
                pltpu.make_async_copy(new_grad.at[place], grad.at[home * group + spot % group], sem.at[8 + place]).start()

            later.append((place, home * group + spot % group, spot // group == y))

    for copy in copies:
        copy.wait()
    for place, target, mine in later:

        @pl.when(mine)
        def _(place=place, target=target):
            pltpu.make_async_copy(new_grad.at[place], grad.at[target], sem.at[8 + place]).wait()


def finish(owners, info, slot_dev, arrays):
    whole = pl.BlockSpec(memory_space=pltpu.VMEM)
    return pl.pallas_call(
        lambda *refs: finish_kernel(slot_dev, *refs),
        out_shape=[
            jax.ShapeDtypeStruct((8 * slot_dev, 48, 384), f32),
            jax.ShapeDtypeStruct((4 * slot_dev, 24, 384), f32),
            jax.ShapeDtypeStruct((32, 768), f32),
        ],
        grid_spec=pltpu.PrefetchScalarGridSpec(
            num_scalar_prefetch=2,
            grid=(1,),
            in_specs=[whole] * len(arrays),
            out_specs=[whole] * 3,
        ),
        compiler_params=pltpu.CompilerParams(vmem_limit_bytes=VMEM_SHARD),
        cost_estimate=pl.CostEstimate(flops=10**7, bytes_accessed=2 * 10**7, transcendentals=0),
        name="finish",
    )(owners, info, *arrays)


def finish_split(owners, info, slot_dev, acc_h, near_b, extra, curve, grad):
    whole = pl.BlockSpec(memory_space=pltpu.VMEM)
    there = pl.BlockSpec(memory_space=pltpu.HBM)
    return pl.pallas_call(
        lambda *refs: finish_split_kernel(slot_dev, *refs),
        out_shape=[jax.ShapeDtypeStruct(curve.shape, f32), jax.ShapeDtypeStruct(grad.shape, f32)],
        grid_spec=pltpu.PrefetchScalarGridSpec(
            num_scalar_prefetch=2,
            grid=(1,),
            in_specs=[pl.BlockSpec((1, 512, 768), lambda i, *scalars: (1, 0, 0))] + [whole] * 2 + [there] * 2,
            out_specs=[there] * 2,
            scratch_shapes=[
                pltpu.VMEM((8, 48, 384), f32),
                pltpu.VMEM((8, 24, 384), f32),
                pltpu.SemaphoreType.DMA((16,)),
            ],
        ),
        input_output_aliases={5: 0, 6: 1},
        compiler_params=pltpu.CompilerParams(vmem_limit_bytes=VMEM_SHARD),
        cost_estimate=pl.CostEstimate(flops=0, bytes_accessed=5 * 10**6, transcendentals=0),
        name="finish_split",
    )(owners, info, acc_h.reshape(2, 512, 768), near_b, extra, curve, grad)


def own_attention_kernel(info, seq_device, seq_length, q_ref, k_ref, v_ref, g_ref, cos_ref, sin_ref, att, gq_out, gk_out, gv_out, mask, buf, gk, gv):
    short = is_short(seq_device, seq_length, info[0], 512)

    @pl.when(pl.program_id(0) == 0)
    def _():
        mask_rows(mask, short, 512)

    cos, sin = cos_ref[short], sin_ref[short]
    buf[...] = q_ref[...]
    rotate_rows(buf, 0, cos, sin, False)
    q_rows = buf[...] * 0.125
    qt = q_rows.astype(bf16)
    qn = jnp.transpose(q_rows).astype(bf16)
    buf[...] = k_ref[...]
    rotate_rows(buf, 0, cos, sin, False)
    kt = buf[...].astype(bf16)
    vt = v_ref[...].astype(bf16)
    gt = g_ref[...].astype(bf16)
    gn = jnp.transpose(g_ref[...]).astype(bf16)
    for block in range(2):
        rows = slice(block * 256, block * 256 + 256)
        wide = block * 256 + 256
        scores = dot_nn(qn[rows, :], kt[:, :wide]) + mask[rows, :wide]
        exp_scores = jnp.exp(scores - jnp.max(scores, axis=1, keepdims=True))
        probs = exp_scores * (1.0 / jnp.sum(exp_scores, axis=1, keepdims=True))
        probs_low = probs.astype(bf16)
        grad_probs = dot_nn(gn[rows, :], vt[:, :wide])
        weighted = probs * grad_probs
        g_scores = (weighted - probs * jnp.sum(weighted, axis=1, keepdims=True)).astype(bf16)
        att[:, rows] = dot_nt(vt[:, :wide], probs_low).astype(bf16)
        buf[:, rows] = dot_nt(kt[:, :wide], g_scores) * 0.125
        part_v = dot_nn(gt[:, rows], probs_low)
        part_k = dot_nn(qt[:, rows], g_scores)
        if block == 0:
            gv[:, :wide] = part_v
            gk[:, :wide] = part_k
            gv[:, wide:] = jnp.zeros((64, 512 - wide), f32)
            gk[:, wide:] = jnp.zeros((64, 512 - wide), f32)
        else:
            gv[:, :wide] += part_v
            gk[:, :wide] += part_k
    rotate_rows(buf, 0, cos, sin, True)
    rotate_rows(gk, 0, cos, sin, True)
    gq_out[...] = buf[...].astype(bf16)
    gk_out[...] = gk[...].astype(bf16)
    gv_out[...] = gv[...].astype(bf16)


def own_attention(scalars, mixed, grad_att, tables):
    def rows_at(offset):
        return pl.BlockSpec((64, 512), lambda i, *scalars: (offset + i, 0))

    whole = pl.BlockSpec(memory_space=pltpu.VMEM)
    return pl.pallas_call(
        own_attention_kernel,
        out_shape=[jax.ShapeDtypeStruct((768, 512), bf16)] * 4,
        grid_spec=pltpu.PrefetchScalarGridSpec(
            num_scalar_prefetch=3,
            grid=(12,),
            in_specs=[rows_at(0), rows_at(12), rows_at(24), rows_at(0), whole, whole],
            out_specs=[rows_at(0)] * 4,
            scratch_shapes=[pltpu.VMEM((512, 512), f32)] + [pltpu.VMEM((64, 512), f32)] * 3,
        ),
        compiler_params=pltpu.CompilerParams(vmem_limit_bytes=16 << 20),
        cost_estimate=pl.CostEstimate(flops=10**10, bytes_accessed=10**7, transcendentals=3 * 10**6),
        name="own_attention",
    )(*scalars, mixed, mixed, mixed, grad_att, *tables)


def lay_rows(table, slot, rows, out, buf):
    for source in range(8):
        for part in range(3):
            start = pl.multiple_of(table[slot, source * 3 + part], 16)
            buf[pl.ds(start, 16), :] = rows(source, part * 16)

    @pl.when(table[slot, 24] == 1)
    def _():
        out[0] = jnp.transpose(buf[...])

    @pl.when(table[slot, 24] == 0)
    def _():
        out[0] = buf[...]


def assemble_kernel(table, pieces, out, buf):
    lay_rows(table, pl.program_id(0), lambda source, at: pieces[source, 0, at : at + 16, :], out, buf)


def assemble(table, pieces):
    slots = pieces.shape[1]
    return pl.pallas_call(
        assemble_kernel,
        out_shape=jax.ShapeDtypeStruct((slots, 384, 384), f32),
        grid_spec=pltpu.PrefetchScalarGridSpec(
            num_scalar_prefetch=1,
            grid=(slots,),
            in_specs=[pl.BlockSpec((8, 1, 48, 384), lambda i, table: (0, i, 0, 0))],
            out_specs=pl.BlockSpec((1, 384, 384), lambda i, table: (i, 0, 0)),
            scratch_shapes=[pltpu.VMEM((384, 384), f32)],
        ),
        compiler_params=pltpu.CompilerParams(vmem_limit_bytes=16 << 20),
        cost_estimate=pl.CostEstimate(flops=0, bytes_accessed=8 * 10**6, transcendentals=0),
        name="assemble",
    )(table, pieces)


def split_two(value):
    high = value.astype(bf16)
    return (high, (value - high.astype(f32)).astype(bf16))


def dot_fine(left, right, dims):
    (a_high, a_low), (b_high, b_low) = left, right

    def dot(a, b):
        return lax.dot_general(a, b, (dims, ((), ())), preferred_element_type=f32)

    return dot(a_high, b_high) + (dot(a_high, b_low) + dot(a_low, b_high))


def update_kernel(table, info, tile, own, own_core, far, far_core, qkv, out_w, up, down, left, right, first, second, grad, new_first, new_second, new_weight, new_low, rows, buf):
    slot = pl.program_id(0)
    core, y = info[3], info[5]
    group = pl.num_programs(0) // 2

    def join(one, two):
        rows[:, pl.ds(pl.multiple_of(core * 24, 8), 24), :] = one[:, 0]
        rows[:, pl.ds(pl.multiple_of(24 - core * 24, 8), 24), :] = two[:, 0]

    @pl.when(slot // group == y)
    def _():
        join(own, own_core)

    @pl.when(slot // group != y)
    def _():
        join(far, far_core)

    lay_rows(table, slot, lambda source, at: rows[source, at : at + 16, :], grad, buf)
    index = tile[slot]

    def weight(low, high, ref):
        @pl.when((index >= low) & (index < high))
        def _():
            buf[...] = ref[...].astype(f32)

    weight(0, 12, qkv)
    weight(12, 16, out_w)
    weight(16, 32, up)
    weight(32, 48, down)
    used = jnp.where(index < 48, 1.0, 0.0)
    l_two, r_two = split_two(left[0]), split_two(right[0])
    turned = dot_fine(l_two, split_two(grad[0]), ((0,), (0,)))
    turned = dot_fine(split_two(turned), r_two, ((1,), (0,)))
    moment = beta_decay * first[0] + (1.0 - beta_decay) * turned
    square = beta_decay * second[0] + (1.0 - beta_decay) * turned * turned
    correction = 1.0 - beta_decay**STEP
    direction = moment / correction / (jnp.sqrt(square / correction) + adam_epsilon)
    new_first[0] = used * moment
    new_second[0] = used * square
    restored = dot_fine(l_two, split_two(direction), ((1,), (0,)))
    restored = dot_fine(split_two(restored), r_two, ((1,), (1,)))
    value = buf[...]
    value = jnp.where(index < 48, value - learning_rate * (restored + weight_decay * value), 0.0)
    new_weight[0] = value
    new_low[0] = value.astype(bf16)


def update(table, info, tile, pieces, weights, states):
    group = pieces[0].shape[1]
    slots = 2 * group
    piece = pl.BlockSpec((8, 1, 24, 384), lambda i, table, info, tile: (0, i % group, 0, 0))
    slab = pl.BlockSpec((1, 384, 384), lambda i, table, info, tile: (i, 0, 0))

    def spec(start, count, columns):
        def at(i, table, info, tile):
            local_tile = jnp.clip(tile[i] - start, 0, count - 1)
            return (local_tile // columns, local_tile % columns)

        return pl.BlockSpec((384, 384), at)

    kinds = [f32, f32, f32, f32, bf16]
    return pl.pallas_call(
        update_kernel,
        out_shape=[jax.ShapeDtypeStruct((slots, 384, 384), kind) for kind in kinds],
        grid_spec=pltpu.PrefetchScalarGridSpec(
            num_scalar_prefetch=3,
            grid=(slots,),
            in_specs=[piece] * 4 + [spec(0, 12, 6), spec(12, 4, 2), spec(16, 16, 8), spec(32, 16, 2)] + [slab] * 4,
            out_specs=[slab] * 5,
            scratch_shapes=[pltpu.VMEM((8, 48, 384), f32), pltpu.VMEM((384, 384), f32)],
        ),
        compiler_params=pltpu.CompilerParams(vmem_limit_bytes=32 << 20),
        cost_estimate=pl.CostEstimate(flops=10**10, bytes_accessed=4 * 10**7, transcendentals=10**6),
        name="update",
    )(table, info, tile, *pieces, *(in_hbm(value) for value in (*weights, *states)))


def small_sums_kernel(info, acc_h, acc_m, acc_c, acc_r, wat, oat, uwt, dwt, out_sum, out):
    device = info[0]
    out[...] = jnp.zeros((32, 768), f32)
    blank = jnp.zeros((8, 768), f32)
    along, curve = blank, acc_r[32:40, :]
    shift_a, shift_m, dshift_a, dshift_m = blank, blank, blank, blank

    def fold(value):
        return jnp.sum(value.reshape(value.shape[0] // 8, 8, 768), axis=0)

    for place in range(2):
        acc = acc_h.at[place * 512 : place * 512 + 512]
        head = info[1 + place]
        row = lax.broadcasted_iota(jnp.int32, (64, 128), 0) + (head % 2) * 64
        pick = lax.broadcasted_iota(jnp.int32, (64, 128), 1) == row
        for kind in range(4):
            at = kind * 128
            if kind < 3:
                base = place * 192 + kind * 64
                w_one, w_drift = wat[base : base + 64, 768:].astype(f32), wat[base : base + 64, :768].astype(f32)
                base = place * 384 + kind * 64
                p_col, q_col = acc_c[base : base + 64, :], acc_c[base + 192 : base + 256, :]
                shift_a += fold(w_one * p_col[:, 0:1])
                dshift_a += fold(w_one * q_col[:, 0:1] + w_drift * p_col[:, 0:1])
                lanes = pl.ds(pl.multiple_of(128 * (head // 2), 128), 128)
                out[4 + kind : 5 + kind, lanes] += jnp.sum(jnp.where(pick, p_col, 0.0), axis=0, keepdims=True)
                out[20 + kind : 21 + kind, lanes] += jnp.sum(jnp.where(pick, q_col, 0.0), axis=0, keepdims=True)
            else:
                w_drift = oat[place * 128 + 64 : place * 128 + 128, :].astype(f32)
            along += fold(acc[at : at + 64, :] * w_drift)
    row = lax.broadcasted_iota(jnp.int32, (48, 384), 0) + device * 48
    pick = lax.broadcasted_iota(jnp.int32, (48, 384), 1) == row
    for block in range(8):
        at = block * 48
        w_one, w_drift = uwt[at : at + 48, :].astype(f32), uwt[384 + at : 432 + at, :].astype(f32)
        d_drift = dwt[384 + at : 432 + at, :].astype(f32)
        p_col, q_col = acc_c[768 + at : 816 + at, 0:1], acc_c[1152 + at : 1200 + at, 0:1]
        shift_m += fold(w_one * p_col)
        dshift_m += fold(w_one * q_col + w_drift * p_col)
        along += fold(acc_m[at : at + 48, :] * w_drift) + fold(acc_m[768 + at : 816 + at, :] * d_drift)
        lanes = slice(384 * (block % 2), 384 * (block % 2) + 384)
        place = 8 + block // 2
        out[place : place + 1, lanes] = jnp.sum(jnp.where(pick, p_col, 0.0), axis=0, keepdims=True)
        out[16 + place : 17 + place, lanes] = jnp.sum(jnp.where(pick, q_col, 0.0), axis=0, keepdims=True)

    def row_sum(value):
        return jnp.sum(value, axis=0, keepdims=True)

    out[0:1, :] = row_sum(acc_r[16:24, :])
    out[1:2, :] = row_sum(shift_a)
    out[2:3, :] = row_sum(acc_r[24:32, :])
    out[3:4, :] = row_sum(shift_m)
    out[7:8, :] = out_sum[...]
    out[12:13, :] = out_sum[...]
    out[16:17, :] = row_sum(acc_r[0:8, :])
    out[17:18, :] = row_sum(dshift_a)
    out[18:19, :] = row_sum(acc_r[8:16, :])
    out[19:20, :] = row_sum(dshift_m)
    lane = lax.broadcasted_iota(jnp.int32, (1, 768), 1)
    out[29:30, :] = jnp.where(lane == 0, jnp.sum(along), jnp.where(lane == 1, jnp.sum(curve), 0.0))


def take_rows(matrix, start, size):
    return lax.dynamic_slice_in_dim(matrix, start, size, axis=0)


def piece_rows(index):
    z, x = index // 2, index % 2
    plain = [48 * index, 48 * index + 16, 48 * index + 32]
    full = [[64 * x + 16 * i for i in range(3)], [64 + 64 * x + 16 * i for i in range(3)]]
    full += [[192 + 64 * x + 16 * i for i in range(3)], [256 + 64 * x + 16 * i for i in range(3)]]
    split = [
        [32 * x, 32 * x + 16, 64 + 64 * x + 48],
        [128 + 32 * x, 144 + 32 * x, 64 * x + 48],
        [192 + 32 * x, 208 + 32 * x, 256 + 64 * x + 48],
        [320 + 32 * x, 336 + 32 * x, 192 + 64 * x + 48],
    ]
    even = z % 2 == 0
    return (full[z] if even else split[z], split[z] if even else full[z], plain)


def local_tp(
    tokens,
    cotangent,
    vec_params,
    qkv_weight,
    out_weight,
    up_weight,
    down_weight,
    probe_vec,
    probe_qkv,
    probe_out,
    probe_up,
    probe_down,
    seq_device,
    seq_length,
    owners,
    left_bases,
    right_bases,
    first_moment,
    second_moment,
    vec_first,
    vec_second,
):
    row_count, width = tokens.shape
    device = lax.axis_index("dp")
    z = device // 2
    probe = lax.axis_index("probe")
    x, y, core = device % 2, probe // 2, probe % 2
    info = lax.dynamic_index_in_dim(jnp.array(device_table(), jnp.int32), device * 4 + probe, 0, keepdims=False)
    scalars = (info, seq_device, seq_length)
    drift_vec, drift_qkv, drift_out = probe_vec[0], probe_qkv[0], probe_out[0]
    drift_up, drift_down = probe_up[0], probe_down[0]
    barrier = lax.optimization_barrier

    across = [(i, i ^ 1) for i in range(8)]
    outer = [(i, i ^ 2) for i in range(8)]
    middle = [(2, 4), (3, 5), (4, 2), (5, 3)]
    outward = [(2, 0), (3, 1), (4, 6), (5, 7)]
    swap_core = [(0, 1), (1, 0), (2, 3), (3, 2)]
    swap_y = [(0, 2), (2, 0), (1, 3), (3, 1)]

    def move(value, pairs):
        return lax.ppermute(value, "dp", pairs)

    def to_core(value):
        return lax.ppermute(value, "probe", swap_core)

    half = row_count // 2

    mine = jnp.concatenate(
        [take_rows(tokens, core * half, half).astype(f32), take_rows(cotangent, core * half, half).astype(f32)], axis=1
    )
    near, centre, cross_0 = move(mine, outer), move(mine, middle), move(mine, across)
    inside = (z == 1) | (z == 2)

    row_index = jnp.arange(row_count, dtype=jnp.int32)
    half_rot = ROT // 2
    frequency = jnp.exp(jnp.arange(half_rot, dtype=f32) * (-2.0 * math.log(10000.0) / ROT))
    position = jnp.stack([row_index, row_index % (row_count // 4)])
    angles = position.astype(f32)[:, None, :] * frequency[None, :, None]
    tables = (jnp.cos(angles), jnp.sin(angles))

    flat_bias = vec_params[4:7].reshape(-1)
    uwt, dwt, bias_u, wat, oat, bias_a = prepare(
        info,
        qkv_weight, drift_qkv, out_weight, drift_out, up_weight, drift_up, down_weight, drift_down, vec_params, drift_vec,
    )
    shared = (vec_params, drift_vec, wat, bias_a, oat, uwt, dwt, bias_u)

    def step(plan, data, old):
        return shard_steps(plan, scalars, data, shared, tables, old)

    acc_h, acc_m, acc_c, acc_r = step(((0, 2),), (tokens, cotangent), None)
    (near, centre, cross_0, acc_r) = barrier((near, centre, cross_0, acc_r))
    edge, middle_near, cross_1 = move(centre, outward), move(near, middle), move(near, across)
    cross_0o, near_o = to_core(cross_0), to_core(near)
    acc_h, acc_m, acc_c, acc_r = step(((1, 2), (4, 1)), (near, near_o, cross_0, cross_0o), (acc_h, acc_m, acc_c, acc_r))

    (edge, middle_near, cross_1, acc_r) = barrier((edge, middle_near, cross_1, acc_r))
    second = jnp.where(inside, centre, edge)
    (middle_near, second) = barrier((middle_near, second))
    edge_far, cross_2 = move(middle_near, outward), move(second, across)
    second_o, cross_1o = to_core(second), to_core(cross_1)
    acc_h, acc_m, acc_c, acc_r = step(((2, 2), (5, 1)), (second, second_o, cross_1, cross_1o), (acc_h, acc_m, acc_c, acc_r))

    (edge_far, cross_2, acc_r) = barrier((edge_far, cross_2, acc_r))
    third = barrier(jnp.where(inside, middle_near, edge_far))
    cross_3, third_o, cross_2o = move(third, across), to_core(third), to_core(cross_2)
    acc_h, acc_m, acc_c, acc_r = step(((3, 2), (6, 1)), (third, third_o, cross_2, cross_2o), (acc_h, acc_m, acc_c, acc_r))
    sends = lax.dynamic_slice(acc_h.reshape(16, 64, width), (8, 32 - 32 * x, 0), (8, 32, width))
    near_b = move(sends, across)
    (tokens, cotangent, cross_3, acc_r) = barrier((tokens, cotangent, cross_3, acc_r))
    cross_3o = to_core(cross_3)
    inputs = tokens.astype(f32)
    cot_rows = cotangent.astype(f32)
    out_sum = jnp.sum(cot_rows, axis=0, keepdims=True)
    normed, norm_scale = normalize(inputs)
    attn_low = (normed * vec_params[0] + vec_params[1]).astype(bf16)
    mlp_low = (normed * vec_params[2] + vec_params[3]).astype(bf16)
    (cross_3, cross_3o, acc_r, attn_low, mlp_low) = barrier((cross_3, cross_3o, acc_r, attn_low, mlp_low))
    acc_h, acc_m, acc_c, acc_r = step(((7, 1),), (cross_3, cross_3o), (acc_h, acc_m, acc_c, acc_r))
    extra = move(acc_h.reshape(16, 64, width)[:8, 48:], [(i, i ^ 2) for i in range(8)])

    slot_dev = left_bases.shape[0]
    tile_index, occupied = slot_order(owners, slot_dev * 8)
    curve_slots, grad_slots, vec_all = finish(
        owners, info, slot_dev, (acc_h, acc_m, acc_c, acc_r, wat, oat, uwt, dwt, out_sum)
    )
    vec_one = move(vec_all, [(i, i ^ 4) for i in range(8)])
    (extra, near_b, vec_all) = barrier((extra, near_b, vec_all))
    curve_slots, grad_slots = finish_split(owners, info, slot_dev, acc_h, near_b, extra, curve_slots, grad_slots)
    curve_slots = curve_slots.reshape(8, slot_dev, 48, 384)
    (vec_all, vec_one, grad_slots) = barrier((vec_all, vec_one, grad_slots))
    vec_all = vec_all + vec_one
    vec_two = move(vec_all, [(i, i ^ 2) for i in range(8)])
    grad_slots = lax.all_to_all(grad_slots.reshape(8, slot_dev // 2, 24, 384), "dp", 0, 0)
    curve_slots = lax.all_to_all(curve_slots, "dp", 0, 0)
    (attn_low, cotangent, vec_all) = barrier((attn_low, cotangent, vec_all))
    mixed = product("kj,tk->jt", qkv_weight, attn_low) + flat_bias[:, None]
    grad_att = product("jk,tk->jt", out_weight, cotangent)
    att_t, gq_t, gk_t, gv_t = own_attention(scalars, mixed, grad_att, tables)
    (vec_all, vec_two, att_t) = barrier((vec_all, vec_two, att_t))
    vec_all = vec_all + vec_two
    vec_four = move(vec_all, [(i, i ^ 1) for i in range(8)])

    (grad_slots, att_t, gq_t, gk_t, gv_t) = barrier((grad_slots, att_t, gq_t, gk_t, gv_t))
    far = lax.ppermute(grad_slots, "probe", swap_y)
    own_core = to_core(grad_slots)
    (mlp_low, cotangent, own_core, att_t, gq_t, gk_t, gv_t) = barrier((mlp_low, cotangent, own_core, att_t, gq_t, gk_t, gv_t))
    hidden = product("ij,jk->ik", mlp_low, up_weight) + vec_params[8:12].reshape(-1)
    cumulative = 0.5 * (1.0 + lax.erf(hidden * root_half))
    density = jnp.exp(-0.5 * hidden * hidden) * density_scale
    act_low = (hidden * cumulative).astype(bf16)
    grad_act = product("ij,kj->ik", cotangent, down_weight)
    grad_hidden_low = (grad_act * (cumulative + hidden * density)).astype(bf16)
    mlp_out = product("ij,jk->ik", act_low, down_weight) + vec_params[12]
    (mlp_out, far, grad_hidden_low, att_t) = barrier((mlp_out, far, grad_hidden_low, att_t))
    far_core = to_core(far)
    attn_out = product("jt,jk->tk", att_t, out_weight) + vec_params[7]
    block_output = (inputs + attn_out + mlp_out).astype(bf16)
    grad_mlp_in = product("ij,kj->ik", grad_hidden_low, up_weight)
    grad_attn_in = (
        product("jt,kj->tk", gq_t, qkv_weight[:, :width])
        + product("jt,kj->tk", gk_t, qkv_weight[:, width : 2 * width])
        + product("jt,kj->tk", gv_t, qkv_weight[:, 2 * width :])
    )
    grad_weighted = grad_attn_in * vec_params[0] + grad_mlp_in * vec_params[2]
    input_grad = cot_rows + norm_back(grad_weighted, normed, norm_scale)

    own_index = lax.dynamic_slice_in_dim(tile_index, device * slot_dev, slot_dev)
    kinds = [sum((piece_rows(i)[kind] for i in range(8)), []) for kind in range(3)]
    row_table = jnp.array(kinds, jnp.int32)
    in_qkv, in_out = own_index < 12, (own_index >= 12) & (own_index < 16)
    kind = jnp.where(in_qkv, own_index % 2, jnp.where(in_out, (own_index - 12) // 2, 2))
    turned = in_qkv | ((own_index >= 16) & (own_index < 32))
    table = jnp.concatenate([row_table[kind], turned.astype(jnp.int32)[:, None]], axis=1)
    (far_core, input_grad, block_output) = barrier((far_core, input_grad, block_output))
    own_grad, new_first, new_second, new_weights, new_weights_low = update(
        table,
        info,
        own_index,
        [grad_slots, own_core, far, far_core],
        [qkv_weight, out_weight, up_weight, down_weight],
        [left_bases, right_bases, first_moment, second_moment],
    )
    (vec_all, vec_four, new_first) = barrier((vec_all, vec_four, new_first))
    vec_all = vec_all + vec_four
    vec_total, vec_curve = vec_all[:13], vec_all[16:29]
    own_dots = jnp.stack(
        [vec_all[29, 0] + jnp.sum(vec_total * drift_vec), vec_all[29, 1]]
    )
    all_dots = jnp.where(jnp.arange(8)[:, None] == probe, jnp.pad(own_dots, (0, 126))[None], 0.0)
    all_dots = all_dots + to_core(all_dots)
    all_dots = all_dots + lax.ppermute(all_dots, "probe", swap_y)
    all_dots = all_dots[:4, :2]
    own_curve = assemble(table, curve_slots)
    vec_new_first, vec_new_second, vec_new = plain_adam(vec_total, vec_params, vec_first, vec_second)
    vector_state = jnp.stack([vec_total, vec_new_first], axis=0)
    return (
        block_output,
        input_grad,
        own_grad,
        new_first,
        new_second,
        new_weights,
        new_weights_low,
        own_curve[None],
        vector_state,
        vec_new_second,
        vec_new,
        vec_curve[None],
        all_dots,
    )


def solution(mesh):
    local = local_tp if fits_tp(mesh) else local_any
    return jax.shard_map(
        local,
        mesh=mesh,
        in_specs=(
            P("dp", None),
            P("dp", None),
            P(),
            P(),
            P(),
            P(),
            P(),
            P("probe", None, None),
            P("probe", None, None),
            P("probe", None, None),
            P("probe", None, None),
            P("probe", None, None),
            P(),
            P(),
            P(),
            P("dp", None, None),
            P("dp", None, None),
            P("dp", None, None),
            P("dp", None, None),
            P(),
            P(),
        ),
        out_specs=(
            P("dp", None),
            P("dp", None),
            P("dp", None, None),
            P("dp", None, None),
            P("dp", None, None),
            P("dp", None, None),
            P("dp", None, None),
            P("probe", "dp", None, None),
            P(),
            P(),
            P(),
            P("probe", None, None),
            P(),
        ),
        check_vma=False,
    )
```

```python
import math

import jax
import jax.numpy as jnp
from jax import lax
from jax.experimental import pallas as pl
from jax.experimental.pallas import tpu as pltpu
from jax.sharding import PartitionSpec as P

HEAD = 64
ROT = 16
BLK = 384
STEP = 4


beta_decay = 0.5
learning_rate = 0.05
weight_decay = 0.01
adam_epsilon = 1e-08
norm_epsilon = 1e-05
root_half = 0.7071067811865476
density_scale = 0.3989422804014327
masked_score = -1e30


def product(pattern, left_side, right_side):
    if left_side.dtype == jnp.bfloat16 and right_side.dtype == jnp.bfloat16:
        return jnp.einsum(pattern, left_side, right_side, preferred_element_type=jnp.float32)
    return jnp.einsum(
        pattern,
        left_side,
        right_side,
        precision=lax.Precision.HIGHEST,
        preferred_element_type=jnp.float32,
    )


def normalize(inputs):
    mean_row = jnp.mean(inputs, axis=1, keepdims=True)
    centred = inputs - mean_row
    variance = jnp.mean(centred * centred, axis=1, keepdims=True)
    norm_scale = lax.rsqrt(variance + norm_epsilon)
    return (centred * norm_scale, norm_scale)


def norm_back(grad_normed, normed, norm_scale):
    mean_grad = jnp.mean(grad_normed, axis=1, keepdims=True)
    mean_cross = jnp.mean(grad_normed * normed, axis=1, keepdims=True)
    return norm_scale * (grad_normed - mean_grad - normed * mean_cross)


def row_layout(device, seq_device, seq_length, row_count):
    present = (seq_device == device).astype(jnp.int32)
    taken_rows = present * seq_length
    start_row = jnp.cumsum(taken_rows) - taken_rows
    row_index = jnp.arange(row_count, dtype=jnp.int32)[:, None]
    inside = (
        (present[None, :] > 0)
        & (row_index >= start_row[None, :])
        & (row_index < (start_row + taken_rows)[None, :])
    ).astype(jnp.int32)
    number = jnp.arange(seq_device.shape[0], dtype=jnp.int32)
    segment = jnp.sum(inside * number[None, :], axis=1)
    position = jnp.sum(inside * (row_index - start_row[None, :]), axis=1)
    return (segment, position)


def rotary_table(position):
    half_rot = ROT // 2
    frequency = jnp.exp(jnp.arange(half_rot, dtype=jnp.float32) * (-2.0 * math.log(10000.0) / ROT))
    angles = position.astype(jnp.float32)[:, None] * frequency[None, :]
    return (jnp.cos(angles), jnp.sin(angles))


def rotate(values, cosine_table, sine_table, reverse):
    half_rot = cosine_table.shape[1]
    first_half = values[..., :half_rot]
    second = values[..., half_rot : 2 * half_rot]
    cos_wide = cosine_table[:, None, :]
    sin_wide = sine_table[:, None, :]
    if reverse:
        new_first = first_half * cos_wide + second * sin_wide
        new_second = second * cos_wide - first_half * sin_wide
    else:
        new_first = first_half * cos_wide - second * sin_wide
        new_second = second * cos_wide + first_half * sin_wide
    return jnp.concatenate([new_first, new_second, values[..., 2 * half_rot :]], axis=-1)


def swap_major(values):
    return jnp.transpose(values, (1, 0, 2))


def cut_tiles(matrix):
    height, span_cols = matrix.shape
    return (
        matrix.reshape(height // BLK, BLK, span_cols // BLK, BLK)
        .transpose(0, 2, 1, 3)
        .reshape(-1, BLK, BLK)
    )


def slot_order(owners, slot_total):
    slot_ids = jnp.arange(slot_total, dtype=jnp.int32)
    matches = owners[None, :] == slot_ids[:, None]
    tile_index = jnp.sum(
        jnp.where(matches, jnp.arange(owners.shape[0], dtype=jnp.int32)[None, :], 0), axis=1
    )
    occupied = jnp.any(matches, axis=1)
    return (jnp.where(occupied, tile_index, owners.shape[0]), occupied)


def arrange(blocks, tile_index):
    padded = jnp.concatenate([blocks, jnp.zeros((1,) + blocks.shape[1:], blocks.dtype)], axis=0)
    return jnp.take(padded, tile_index, axis=0)


def rotated_adam(gradient, weight, left_basis, right_basis, first_state, second_state, occupied):
    turned = jnp.einsum("sji,sjk->sik", left_basis, gradient, precision=lax.Precision.HIGHEST)
    turned = jnp.einsum("sik,skl->sil", turned, right_basis, precision=lax.Precision.HIGHEST)
    new_first = beta_decay * first_state + (1.0 - beta_decay) * turned
    new_second = beta_decay * second_state + (1.0 - beta_decay) * turned * turned
    correction = 1.0 - beta_decay**STEP
    direction = new_first / correction / (jnp.sqrt(new_second / correction) + adam_epsilon)
    restored = jnp.einsum("sij,sjk->sik", left_basis, direction, precision=lax.Precision.HIGHEST)
    restored = jnp.einsum("sik,slk->sil", restored, right_basis, precision=lax.Precision.HIGHEST)
    new_weight = weight - learning_rate * (restored + weight_decay * weight)
    slot_mask = occupied.astype(jnp.float32)[:, None, None]
    return (slot_mask * new_first, slot_mask * new_second, slot_mask * new_weight)


def plain_adam(gradient, value_rows, first_state, second_state):
    new_first = beta_decay * first_state + (1.0 - beta_decay) * gradient
    new_second = beta_decay * second_state + (1.0 - beta_decay) * gradient * gradient
    correction = 1.0 - beta_decay**STEP
    new_value = value_rows - learning_rate * (new_first / correction) / (
        jnp.sqrt(new_second / correction) + adam_epsilon
    )
    return (new_first, new_second, new_value)


def local_any(
    tokens,
    cotangent,
    vec_params,
    qkv_weight,
    out_weight,
    up_weight,
    down_weight,
    probe_vec,
    probe_qkv,
    probe_out,
    probe_up,
    probe_down,
    seq_device,
    seq_length,
    owners,
    left_bases,
    right_bases,
    first_moment,
    second_moment,
    vec_first,
    vec_second,
):
    row_count, model_width = tokens.shape
    head_count = model_width // HEAD
    up_rows = up_weight.shape[1] // model_width
    device = lax.axis_index("dp")
    segment, position = row_layout(device, seq_device, seq_length, row_count)
    cosine_table, sine_table = rotary_table(position)
    row_index = jnp.arange(row_count, dtype=jnp.int32)
    allowed = (segment[:, None] == segment[None, :]) & (row_index[None, :] <= row_index[:, None])
    drift_vec = probe_vec[0]
    drift_qkv = probe_qkv[0]
    drift_out = probe_out[0]
    drift_up = probe_up[0]
    drift_down = probe_down[0]
    inputs = tokens.astype(jnp.float32)
    cot_rows = cotangent.astype(jnp.float32)
    normed, norm_scale = normalize(inputs)
    attn_in = normed * vec_params[0] + vec_params[1]
    drift_attn_in = normed * drift_vec[0] + drift_vec[1]
    mlp_in = normed * vec_params[2] + vec_params[3]
    drift_mlp_in = normed * drift_vec[2] + drift_vec[3]
    attn_low = attn_in.astype(jnp.bfloat16)
    mlp_low = mlp_in.astype(jnp.bfloat16)
    mixed_rows = product("ij,jk->ik", attn_low, qkv_weight) + vec_params[4:7].reshape(-1)
    drift_mixed = (
        product("ij,jk->ik", drift_attn_in, qkv_weight)
        + product("ij,jk->ik", attn_low, drift_qkv)
        + drift_vec[4:7].reshape(-1)
    )

    def split_heads(matrix, column_group):
        return matrix[:, column_group * model_width : (column_group + 1) * model_width].reshape(
            row_count, head_count, HEAD
        )

    query_rows = rotate(split_heads(mixed_rows, 0), cosine_table, sine_table, False)
    key_rows = rotate(split_heads(mixed_rows, 1), cosine_table, sine_table, False)
    value_rows = split_heads(mixed_rows, 2)
    drift_query = rotate(split_heads(drift_mixed, 0), cosine_table, sine_table, False)
    drift_key = rotate(split_heads(drift_mixed, 1), cosine_table, sine_table, False)
    drift_value = split_heads(drift_mixed, 2)
    grad_att = product("ij,kj->ik", cotangent, out_weight)
    drift_grad_att = product("ij,kj->ik", cotangent, drift_out)
    grad_att_low = grad_att.astype(jnp.bfloat16)

    def attend(pieces):
        query_block, key_block, value_block, drift_q, drift_k, drift_v, grad_out, drift_grad_out = (
            pieces
        )
        scores = product("ij,kj->ik", query_block, key_block) * 0.125
        drift_scores = (
            product("ij,kj->ik", drift_q, key_block) + product("ij,kj->ik", query_block, drift_k)
        ) * 0.125
        scores = jnp.where(allowed, scores, masked_score)
        shifted = scores - jnp.max(scores, axis=1, keepdims=True)
        exp_scores = jnp.exp(shifted)
        probs = exp_scores / jnp.sum(exp_scores, axis=1, keepdims=True)
        drift_probs = probs * (drift_scores - jnp.sum(probs * drift_scores, axis=1, keepdims=True))
        probs_low = probs.astype(jnp.bfloat16)
        attended_head = product("ij,jk->ik", probs_low, value_block)
        drift_attended_head = product("ij,jk->ik", drift_probs, value_block) + product(
            "ij,jk->ik", probs_low, drift_v
        )
        grad_probs = product("ij,kj->ik", grad_out, value_block)
        drift_grad_probs = product("ij,kj->ik", drift_grad_out, value_block) + product(
            "ij,kj->ik", grad_out, drift_v
        )
        grad_value_head = product("ij,ik->jk", probs_low, grad_out)
        drift_grad_value_head = product("ij,ik->jk", drift_probs, grad_out) + product(
            "ij,ik->jk", probs_low, drift_grad_out
        )
        centre = jnp.sum(probs * grad_probs, axis=1, keepdims=True)
        drift_centre = jnp.sum(
            drift_probs * grad_probs + probs * drift_grad_probs, axis=1, keepdims=True
        )
        grad_scores = probs * (grad_probs - centre)
        drift_grad_scores = drift_probs * (grad_probs - centre) + probs * (
            drift_grad_probs - drift_centre
        )
        scores_low = grad_scores.astype(jnp.bfloat16)
        grad_query_head = product("ij,jk->ik", scores_low, key_block) * 0.125
        drift_grad_query_head = (
            product("ij,jk->ik", drift_grad_scores, key_block)
            + product("ij,jk->ik", scores_low, drift_k)
        ) * 0.125
        grad_key_head = product("ij,ik->jk", scores_low, query_block) * 0.125
        drift_grad_key_head = (
            product("ij,ik->jk", drift_grad_scores, query_block)
            + product("ij,ik->jk", scores_low, drift_q)
        ) * 0.125
        return (
            attended_head,
            drift_attended_head,
            grad_query_head,
            grad_key_head,
            grad_value_head,
            drift_grad_query_head,
            drift_grad_key_head,
            drift_grad_value_head,
        )

    results = lax.map(
        attend,
        (
            swap_major(query_rows.astype(jnp.bfloat16)),
            swap_major(key_rows.astype(jnp.bfloat16)),
            swap_major(value_rows.astype(jnp.bfloat16)),
            swap_major(drift_query),
            swap_major(drift_key),
            swap_major(drift_value),
            swap_major(grad_att_low.reshape(row_count, head_count, HEAD)),
            swap_major(drift_grad_att.reshape(row_count, head_count, HEAD)),
        ),
    )
    attended = swap_major(results[0]).reshape(row_count, model_width)
    drift_attended = swap_major(results[1]).reshape(row_count, model_width)
    grad_query = rotate(swap_major(results[2]), cosine_table, sine_table, True).reshape(
        row_count, model_width
    )
    grad_key = rotate(swap_major(results[3]), cosine_table, sine_table, True).reshape(
        row_count, model_width
    )
    grad_value = swap_major(results[4]).reshape(row_count, model_width)
    drift_grad_query = rotate(swap_major(results[5]), cosine_table, sine_table, True).reshape(
        row_count, model_width
    )
    drift_grad_key = rotate(swap_major(results[6]), cosine_table, sine_table, True).reshape(
        row_count, model_width
    )
    drift_grad_value = swap_major(results[7]).reshape(row_count, model_width)
    grad_mixed_low = jnp.concatenate([grad_query, grad_key, grad_value], axis=1).astype(
        jnp.bfloat16
    )
    drift_grad_mixed = jnp.concatenate([drift_grad_query, drift_grad_key, drift_grad_value], axis=1)
    att_low = attended.astype(jnp.bfloat16)
    attn_out = product("ij,jk->ik", att_low, out_weight) + vec_params[7]
    hidden = product("ij,jk->ik", mlp_low, up_weight) + vec_params[8 : 8 + up_rows].reshape(-1)
    drift_hidden = (
        product("ij,jk->ik", drift_mlp_in, up_weight)
        + product("ij,jk->ik", mlp_low, drift_up)
        + drift_vec[8 : 8 + up_rows].reshape(-1)
    )
    cumulative = 0.5 * (1.0 + lax.erf(hidden * root_half))
    density = jnp.exp(-0.5 * hidden * hidden) * density_scale
    activated = hidden * cumulative
    gelu_slope = cumulative + hidden * density
    gelu_bend = density * (2.0 - hidden * hidden)
    act_low = activated.astype(jnp.bfloat16)
    drift_act = gelu_slope * drift_hidden
    mlp_out = product("ij,jk->ik", act_low, down_weight) + vec_params[8 + up_rows]
    block_output = (inputs + attn_out + mlp_out).astype(jnp.bfloat16)
    grad_down = product("ij,ik->jk", act_low, cotangent)
    drift_grad_down = product("ij,ik->jk", drift_act, cotangent)
    grad_act = product("ij,kj->ik", cotangent, down_weight)
    drift_grad_act = product("ij,kj->ik", cotangent, drift_down)
    grad_hidden = grad_act * gelu_slope
    drift_grad_hidden = drift_grad_act * gelu_slope + grad_act * gelu_bend * drift_hidden
    grad_hidden_low = grad_hidden.astype(jnp.bfloat16)
    grad_up = product("ij,ik->jk", mlp_low, grad_hidden_low)
    drift_grad_up = product("ij,ik->jk", drift_mlp_in, grad_hidden_low) + product(
        "ij,ik->jk", mlp_low, drift_grad_hidden
    )
    grad_mlp_in = product("ij,kj->ik", grad_hidden_low, up_weight)
    drift_grad_mlp_in = product("ij,kj->ik", drift_grad_hidden, up_weight) + product(
        "ij,kj->ik", grad_hidden_low, drift_up
    )
    grad_out_w = product("ij,ik->jk", att_low, cotangent)
    drift_grad_out_w = product("ij,ik->jk", drift_attended, cotangent)
    grad_qkv = product("ij,ik->jk", attn_low, grad_mixed_low)
    drift_grad_qkv = product("ij,ik->jk", drift_attn_in, grad_mixed_low) + product(
        "ij,ik->jk", attn_low, drift_grad_mixed
    )
    grad_attn_in = product("ij,kj->ik", grad_mixed_low, qkv_weight)
    drift_grad_attn_in = product("ij,kj->ik", drift_grad_mixed, qkv_weight) + product(
        "ij,kj->ik", grad_mixed_low, drift_qkv
    )
    grad_weighted = grad_attn_in * vec_params[0] + grad_mlp_in * vec_params[2]
    input_grad = cot_rows + norm_back(grad_weighted, normed, norm_scale)
    out_sum = jnp.sum(cot_rows, axis=0)[None]
    zero_row = jnp.zeros((1, model_width), jnp.float32)
    vec_grad = jnp.concatenate(
        [
            jnp.sum(grad_attn_in * normed, axis=0)[None],
            jnp.sum(grad_attn_in, axis=0)[None],
            jnp.sum(grad_mlp_in * normed, axis=0)[None],
            jnp.sum(grad_mlp_in, axis=0)[None],
            jnp.sum(grad_mixed_low, axis=0, dtype=jnp.float32).reshape(3, model_width),
            out_sum,
            jnp.sum(grad_hidden_low, axis=0, dtype=jnp.float32).reshape(up_rows, model_width),
            out_sum,
        ],
        axis=0,
    )
    vec_drift = jnp.concatenate(
        [
            jnp.sum(drift_grad_attn_in * normed, axis=0)[None],
            jnp.sum(drift_grad_attn_in, axis=0)[None],
            jnp.sum(drift_grad_mlp_in * normed, axis=0)[None],
            jnp.sum(drift_grad_mlp_in, axis=0)[None],
            jnp.sum(drift_grad_mixed, axis=0).reshape(3, model_width),
            zero_row,
            jnp.sum(drift_grad_hidden, axis=0).reshape(up_rows, model_width),
            zero_row,
        ],
        axis=0,
    )
    along_probe = jnp.sum(vec_grad * drift_vec)
    curve_probe = jnp.sum(vec_drift * drift_vec)
    for gradient, drift_gradient, direction_set in (
        (grad_qkv, drift_grad_qkv, drift_qkv),
        (grad_out_w, drift_grad_out_w, drift_out),
        (grad_up, drift_grad_up, drift_up),
        (grad_down, drift_grad_down, drift_down),
    ):
        along_probe = along_probe + jnp.sum(gradient * direction_set.astype(jnp.float32))
        curve_probe = curve_probe + jnp.sum(drift_gradient * direction_set.astype(jnp.float32))
    dots = jnp.stack([along_probe, curve_probe])
    grad_tiles = jnp.concatenate(
        [cut_tiles(grad_qkv), cut_tiles(grad_out_w), cut_tiles(grad_up), cut_tiles(grad_down)],
        axis=0,
    )
    curve_tiles = jnp.concatenate(
        [
            cut_tiles(drift_grad_qkv),
            cut_tiles(drift_grad_out_w),
            cut_tiles(drift_grad_up),
            cut_tiles(drift_grad_down),
        ],
        axis=0,
    )
    slot_dev = left_bases.shape[0]
    slot_total = slot_dev * lax.axis_size("dp")
    tile_index, occupied = slot_order(owners, slot_total)
    slot_grad = arrange(grad_tiles, tile_index)
    slot_curve = arrange(curve_tiles, tile_index)
    own_grad, own_curve = (
        lax.psum_scatter(slot_grad, "dp", scatter_dimension=0, tiled=True),
        lax.psum_scatter(slot_curve, "dp", scatter_dimension=0, tiled=True),
    )
    vec_total, vec_curve, dot_total = lax.psum((vec_grad, vec_drift, dots), "dp")
    all_dots = lax.all_gather(dot_total[None, :], "probe", axis=0, tiled=True)
    own_index = lax.dynamic_slice_in_dim(tile_index, device * slot_dev, slot_dev)
    own_used = lax.dynamic_slice_in_dim(occupied, device * slot_dev, slot_dev)
    weight_tiles = jnp.concatenate(
        [
            cut_tiles(qkv_weight),
            cut_tiles(out_weight),
            cut_tiles(up_weight),
            cut_tiles(down_weight),
        ],
        axis=0,
    )
    own_weight = arrange(weight_tiles, own_index).astype(jnp.float32)
    new_first, new_second, new_weights = rotated_adam(
        own_grad, own_weight, left_bases, right_bases, first_moment, second_moment, own_used
    )
    new_weights_low = new_weights.astype(jnp.bfloat16)
    vec_new_first, vec_new_second, vec_new = plain_adam(
        vec_total, vec_params, vec_first, vec_second
    )
    vector_state = jnp.stack([vec_total, vec_new_first], axis=0)
    return (
        block_output,
        input_grad,
        own_grad,
        new_first,
        new_second,
        new_weights,
        new_weights_low,
        own_curve[None],
        vector_state,
        vec_new_second,
        vec_new,
        vec_curve[None],
        all_dots,
    )


f32 = jnp.float32
bf16 = jnp.bfloat16
VMEM_SHARD = 60 << 20
HEAD_A = (0, 1, 7, 8, 3, 4, 10, 11)
HEAD_B = (6, 6, 2, 2, 9, 9, 5, 5)
ARRIVE = ((1, 2, 3), (0, 2, 3), (3, 1, 0), (2, 1, 0))


def fits_tp(mesh):
    return mesh.shape["dp"] == 8 and mesh.shape["probe"] == 4


def device_table():
    rows = []
    for device in range(8):
        z, x = device // 2, device % 2
        levels = (z,) + ARRIVE[z]
        order = [2 * level + x for level in levels] + [2 * level + 1 - x for level in levels]
        for probe in range(4):
            rows.append([device, HEAD_A[device], HEAD_B[device], probe % 2, x, probe // 2, z % 2, 0] + order)
    return rows


def is_short(seq_device, seq_length, group, rows):
    longest = jnp.int32(0)
    for i in range(seq_device.shape[0]):
        longest = jnp.maximum(longest, jnp.where(seq_device[i] == group, seq_length[i], 0))
    return (longest < rows).astype(jnp.int32)


def in_hbm(value):
    return pltpu.with_memory_space_constraint(value, pltpu.HBM)


def dot_nt(left, right):
    return lax.dot_general(left, right, (((1,), (1,)), ((), ())), preferred_element_type=f32)


def dot_nn(left, right):
    return lax.dot_general(left, right, (((1,), (0,)), ((), ())), preferred_element_type=f32)


def rotate_rows(ref, base, cos, sin, reverse):
    up, low = ref[base : base + 8, :], ref[base + 8 : base + 16, :]
    if reverse:
        ref[base : base + 8, :] = up * cos + low * sin
        ref[base + 8 : base + 16, :] = low * cos - up * sin
    else:
        ref[base : base + 8, :] = up * cos - low * sin
        ref[base + 8 : base + 16, :] = low * cos + up * sin


def mask_rows(bias, short, rows):
    for start in range(0, rows, 128):
        row = lax.broadcasted_iota(jnp.int32, (128, rows), 0) + start
        col = lax.broadcasted_iota(jnp.int32, (128, rows), 1)
        first = jnp.where(short == 1, start, 0)
        bias[start : start + 128, :] = jnp.where((col >= first) & (col <= row), 0.0, masked_score)


def one_row(block, index):
    rows = lax.broadcasted_iota(jnp.int32, block.shape, 0)
    return jnp.sum(jnp.where(rows == index, block, 0.0), axis=0, keepdims=True)


def prepare_kernel(info, up_0, up_1, dup_0, dup_1, down, ddown, qkv, dqkv, out_w, dout_w, vec, dvec, uwt, dwt, bias_u, wat, oat, bias_a, turn, turn_h):
    j = pl.program_id(0)
    device = info[0]
    row = lax.broadcasted_iota(jnp.int32, (48, 128), 0) + (device * 48) % 128
    lane = lax.broadcasted_iota(jnp.int32, (48, 128), 1)
    pick_0, pick_1 = (lane == row).astype(bf16), (lane == row - 128).astype(bf16)
    for part, (first, second, below, bias) in enumerate(((up_0, up_1, down, vec), (dup_0, dup_1, ddown, dvec))):
        uwt[part, 0] = (dot_nt(pick_0, first[...]) + dot_nt(pick_1, second[...])).astype(bf16)
        dwt[part, 0] = below[...]
        line = one_row(bias[8:12, pl.ds(pl.multiple_of(384 * (j % 2), 128), 384)], j // 2)
        turn[...] = jnp.transpose(jnp.broadcast_to(line, (128, 384)))
        bias_u[part, 0] = turn[pl.ds(pl.multiple_of(device * 48, 16), 48), :]

    @pl.when(j < 6)
    def _():
        head = info[1 + j // 3]
        row = lax.broadcasted_iota(jnp.int32, (64, 128), 0) + (head % 2) * 64
        pick = (lax.broadcasted_iota(jnp.int32, (64, 128), 1) == row).astype(bf16)
        rows, drows = dot_nt(pick, qkv[...]).astype(bf16), dot_nt(pick, dqkv[...]).astype(bf16)
        wat[:, :768] = drows
        wat[:, 768:] = rows
        oat[:64, :] = out_w[...]
        oat[64:, :] = dout_w[...]
        for part, bias in enumerate((vec, dvec)):
            line = one_row(bias[4:7, pl.ds(pl.multiple_of(128 * (head // 2), 128), 128)], j % 3)
            turn_h[...] = jnp.transpose(jnp.broadcast_to(line, (128, 128)))
            bias_a[part * 64 : part * 64 + 64, :] = turn_h[pl.ds(pl.multiple_of((head % 2) * 64, 64), 64), :]


def prepare(info, qkv, dqkv, out_w, dout_w, up, dup, down, ddown, vec, dvec):
    def at_head(i):
        return jnp.minimum(i, 5)

    whole = pl.BlockSpec(memory_space=pltpu.VMEM)
    up_0 = pl.BlockSpec((768, 128), lambda i, info: (0, 3 * i + (info[0] * 48) // 128))
    up_1 = pl.BlockSpec((768, 128), lambda i, info: (0, 3 * i + jnp.minimum((info[0] * 48) // 128 + 1, 2)))
    down_spec = pl.BlockSpec((48, 768), lambda i, info: (8 * i + info[0], 0))
    qkv_spec = pl.BlockSpec((768, 128), lambda i, info: (0, 6 * (at_head(i) % 3) + info[1 + at_head(i) // 3] // 2))
    out_spec = pl.BlockSpec((64, 768), lambda i, info: (info[1 + at_head(i) // 3], 0))
    uwt, dwt, bias_u, wat, oat, bias_a = pl.pallas_call(
        prepare_kernel,
        out_shape=[
            jax.ShapeDtypeStruct((2, 8, 48, 768), bf16),
            jax.ShapeDtypeStruct((2, 8, 48, 768), bf16),
            jax.ShapeDtypeStruct((2, 8, 48, 128), f32),
            jax.ShapeDtypeStruct((384, 1536), bf16),
            jax.ShapeDtypeStruct((256, 768), bf16),
            jax.ShapeDtypeStruct((768, 128), f32),
        ],
        grid_spec=pltpu.PrefetchScalarGridSpec(
            num_scalar_prefetch=1,
            grid=(8,),
            in_specs=[up_0, up_1, up_0, up_1, down_spec, down_spec, qkv_spec, qkv_spec, out_spec, out_spec, whole, whole],
            out_specs=[
                pl.BlockSpec((2, 1, 48, 768), lambda i, info: (0, i, 0, 0)),
                pl.BlockSpec((2, 1, 48, 768), lambda i, info: (0, i, 0, 0)),
                pl.BlockSpec((2, 1, 48, 128), lambda i, info: (0, i, 0, 0)),
                pl.BlockSpec((64, 1536), lambda i, info: (at_head(i), 0)),
                pl.BlockSpec((128, 768), lambda i, info: (at_head(i) // 3, 0)),
                pl.BlockSpec((128, 128), lambda i, info: (at_head(i), 0)),
            ],
            scratch_shapes=[pltpu.VMEM((384, 128), f32), pltpu.VMEM((128, 128), f32)],
        ),
        compiler_params=pltpu.CompilerParams(vmem_limit_bytes=VMEM_SHARD),
        cost_estimate=pl.CostEstimate(flops=10**9, bytes_accessed=2 * 10**7, transcendentals=0),
        name="prepare",
    )(info, *(in_hbm(value) for value in (up, up, dup, dup, down, ddown, qkv, dqkv, out_w, dout_w)), vec, dvec)
    return (uwt.reshape(768, 768), dwt.reshape(768, 768), bias_u.reshape(768, 128), wat, oat, bias_a)


def outgoing_kernel(info, tokens, cotangent, out):
    def rows_of(i, carry):
        rows = pl.ds(pl.multiple_of(i * 64, 64), 64)
        out[rows, :768] = normalize(tokens[rows, :].astype(f32))[0]
        out[rows, 768:] = cotangent[rows, :].astype(f32)
        return carry

    lax.fori_loop(0, 4, rows_of, 0)


def outgoing(info, tokens, cotangent):
    half = pl.BlockSpec((256, 768), lambda i, info: (info[3], 0))
    return pl.pallas_call(
        outgoing_kernel,
        out_shape=jax.ShapeDtypeStruct((256, 1536), f32),
        grid_spec=pltpu.PrefetchScalarGridSpec(
            num_scalar_prefetch=1,
            grid=(1,),
            in_specs=[half, half],
            out_specs=pl.BlockSpec((256, 1536), lambda i, info: (0, 0)),
        ),
        compiler_params=pltpu.CompilerParams(vmem_limit_bytes=VMEM_SHARD),
        cost_estimate=pl.CostEstimate(flops=10**6, bytes_accessed=3 * 10**6, transcendentals=0),
        name="outgoing",
    )(info, in_hbm(tokens), in_hbm(cotangent))


def wide(column):
    return jnp.concatenate([column] * 4, axis=1)


def shard_kernel(plan, first, parts, slot_dev, *refs):
    refs = list(refs)
    with_heads, with_mlp, with_finish = parts != "close", parts != "heads", parts == "close"
    info, seq_device, seq_length = refs[:3]
    refs = refs[3:]
    owner = refs.pop(0) if with_finish else None
    steps = len(plan)
    data_h = refs[: 2 * steps]
    refs = refs[2 * steps :]
    vec, dvec, cos_ref, sin_ref = refs[:4]
    weights_h = refs[4:10]
    refs = refs[10:]
    old_h = None if first else refs[:4]
    refs = refs if first else refs[4:]
    if with_finish:
        out_sum, curve, grad, sums_out = refs[0], refs[1], refs[2], refs[3]
        out_h = (None,) * 4
    else:
        out_h = refs[:4]
    (mine, other, wat, bias_a, oat, uwt, dwt, bias_u, acc_h, acc_m, acc_c, acc_r, sem) = refs[4:17]
    (nb, nb_low, ones, lhs_a, ml, dm, dm_low, cb, mask, proj, gat, qt, kt, k4, vt, v4, gt, q4, g4, gq, gk, gv, head_g, head_a, hid, act, mlp_a, mlp_g, one, two) = refs[17:]
    new = (acc_h, acc_m, acc_c, acc_r)
    step = pl.program_id(0)
    core = info[3]
    most = max(heads for _, heads in plan)

    def by_step(values):
        result = jnp.int32(values[0])
        for i, value in enumerate(values[1:]):
            result = jnp.where(step > i, value, result)
        return result

    heads_now = by_step([heads for _, heads in plan])
    short = is_short(seq_device, seq_length, info[8 + by_step([index for index, _ in plan])], 512)
    width = 768
    gain_a, shift_a, gain_m, shift_m = (vec[i : i + 1, :] for i in range(4))
    dgain_a, dshift_a, dgain_m, dshift_m = (dvec[i : i + 1, :] for i in range(4))
    wat_h, bias_ah, oat_h, uwt_h, dwt_h, bias_uh = weights_h
    lead = most * 384
    pairs = [(data_h[0], mine.at[0]), (data_h[1], other.at[0])]
    pairs += [(uwt_h, uwt), (dwt_h, dwt), (bias_uh, bias_u)] if with_mlp else []
    for_mlp = range(2, len(pairs))
    held = 2 if with_finish else most
    pairs += [(wat_h.at[: held * 192], wat), (oat_h.at[: held * 128], oat)]
    pairs += [(bias_ah.at[:lead], bias_a)] if with_heads else []
    for_heads = range(for_mlp.stop, len(pairs))
    if not first:
        pairs += [(old_h[1], acc_m)] if with_mlp else []
        pairs += [(old_h[2], acc_c), (old_h[3], acc_r)]
    for_sums = range(for_heads.stop, len(pairs))
    if not first:
        pairs += [(old_h[0].at[: held * 512], acc_h)]
    for_tiles = range(for_sums.stop, len(pairs))
    base_count = len(pairs)
    for i in range(1, steps):
        pairs += [(data_h[2 * i], mine.at[i]), (data_h[2 * i + 1], other.at[i])]
    arrivals = [pltpu.make_async_copy(source, target, sem.at[i]) for i, (source, target) in enumerate(pairs)]

    def at_step(which):
        if steps == 1:
            return lambda body: body()
        return pl.when(step == which)

    @at_step(0)
    def _():
        for copy in arrivals:
            copy.start()

    def arrived(*which):
        @at_step(0)
        def _():
            for i in which:
                if i < base_count:
                    arrivals[i].wait()

    ones[...] = jnp.ones((512, 128), bf16)
    if with_heads:
        mask_rows(mask, short, 512)

    def load(ref, cot_ref, base, count):
        def rows_of(i, carry):
            src = pl.ds(pl.multiple_of(i * 128, 128), 128)
            dst = pl.ds(pl.multiple_of(base + i * 128, 128), 128)
            rows = ref[step, src, :width].astype(f32)
            normed = normalize(rows)[0] if first else rows
            nb[dst, :], nb_low[dst, :] = split_two(normed)
            if with_heads:
                lhs_a[dst, :width] = (normed * gain_a + shift_a).astype(bf16)
                lhs_a[dst, width : 2 * width], lhs_a[dst, 2 * width :] = split_two(normed * dgain_a + dshift_a)
            if with_mlp:
                ml[dst, :] = (normed * gain_m + shift_m).astype(bf16)
                dm[dst, :], dm_low[dst, :] = split_two(normed * dgain_m + dshift_m)
            cb[dst, :] = cot_ref[step, src, :].astype(bf16)
            return carry

        lax.fori_loop(0, count, rows_of, 0)

    if first:
        arrived(0, 1)
        load(mine, other, 0, 4)
    else:
        arrived(0)
        for i in range(1, steps):

            @at_step(i)
            def _(i=i):
                arrivals[base_count + 2 * i - 2].wait()
                arrivals[base_count + 2 * i - 1].wait()

        load(mine, mine.at[:, :, width:], core * 256, 2)
        arrived(1)
        load(other, other.at[:, :, width:], (1 - core) * 256, 2)

    def add(ref, rows, value):
        ref[rows, :] = value if first else ref[rows, :] + value

    def eight(value):
        rows, columns = value.shape
        return jnp.sum(value.reshape(rows // 8, 8, columns), axis=0)

    def fold(carry, ref, at, tops, w_rows, dw_rows, dgain, dshift, c_rows):
        grad_at, curve_at = at
        top, low = tops
        p_two, q_two = two[top, :], two[low, :]
        add(ref, grad_at, one[top, :])
        moved = dgain * p_two + dshift * c_rows
        add(ref, curve_at, one[low, :] + moved)
        w_wide, dw_wide = w_rows.astype(f32), dw_rows.astype(f32)
        drift, plain, dots = carry
        drift = drift + eight(w_wide * q_two + dw_wide * p_two)
        plain = plain + eight(w_wide * p_two)
        dots = dots + eight(dw_wide * (2.0 * moved))
        return (drift, plain, dots)

    blank = jnp.zeros((8, width), f32)
    if with_mlp:
        arrived(*for_mlp)
        hid[...] = dot_nt(uwt[...], ml[...])
        act[...] = dot_nt(dwt[...], cb[...])
        hid[384:, :] += dot_nt(uwt[:384, :], dm[...]) + dot_nt(uwt[:384, :], dm_low[...])

        def gelu(i, carry):
            top = pl.ds(pl.multiple_of(i * 32, 32), 32)
            low = pl.ds(pl.multiple_of(384 + i * 32, 32), 32)
            hidden, dhidden = hid[top, :] + wide(bias_u[top, :]), hid[low, :] + wide(bias_u[low, :])
            grad_act, dgrad_act = act[top, :], act[low, :]
            cumulative = 0.5 * (1.0 + lax.erf(hidden * root_half))
            density = jnp.exp(-0.5 * hidden * hidden) * density_scale
            slope = cumulative + hidden * density
            bend = density * (2.0 - hidden * hidden)
            drift_act = slope * dhidden
            drift_grad = dgrad_act * slope + grad_act * bend * dhidden
            mlp_a[top, :] = (hidden * cumulative).astype(bf16)
            mlp_a[low, :] = drift_act.astype(bf16)
            mlp_g[top, :] = (grad_act * slope).astype(bf16)
            mlp_g[low, :] = drift_grad.astype(bf16)
            return carry + eight(drift_grad * dhidden + drift_act * dgrad_act)

        dots_m = lax.fori_loop(0, 12, gelu, jnp.zeros((8, 512), f32))
        one[...] = dot_nn(mlp_g[...], ml[...])
        two[...] = dot_nn(mlp_g[...], nb[...])
        two[:384, :] += dot_nn(mlp_g[:384, :], nb_low[...])
        sums = dot_nn(mlp_g[...], ones[...])
        arrived(*for_sums)
        add(acc_c, slice(768, 1536), sums)
        proj[0:384, 0:128] = sums[:384, :]

        def fold_m(i, carry):
            top = pl.ds(pl.multiple_of(i * 64, 64), 64)
            low = pl.ds(pl.multiple_of(384 + i * 64, 64), 64)
            return fold(carry, acc_m, (top, low), (top, low), uwt[top, :], uwt[low, :], dgain_m, dshift_m, proj[top, 0:1])

        carry_m = (blank, blank, blank) if first else (acc_r[8:16, :], acc_r[24:32, :], acc_r[32:40, :])
        acc_r[8:16, :], acc_r[24:32, :], acc_r[32:40, :] = lax.fori_loop(0, 6, fold_m, carry_m)
        acc_r[32:40, :512] += dots_m
        one[...] = dot_nn(mlp_a[...], cb[...])
        add(acc_m, slice(768, 1536), one[...])
        if with_finish:
            arrived(*for_heads, *for_tiles)
            finish_kernel(slot_dev, owner, info, acc_h, acc_m, acc_c, acc_r, wat, oat, uwt, dwt, out_sum, curve, grad, sums_out)
            return
        leave_m = pltpu.make_async_copy(acc_m, out_h[1], sem.at[0])

        @at_step(steps - 1)
        def _():
            leave_m.start()

    if not with_mlp:
        arrived(*for_sums)
    arrived(*for_heads, *for_tiles)
    cos, sin = cos_ref[short], sin_ref[short]

    def attend(head, carry):
        base = pl.multiple_of(head * 384, 128)
        w_at = pl.ds(pl.multiple_of(head * 192, 64), 192)
        plain = dot_nt(wat[w_at, width:], lhs_a[:, :width])
        drift = dot_nt(wat[w_at, :], lhs_a[:, : 2 * width]) + dot_nt(wat[w_at, width:], lhs_a[:, 2 * width :])
        for kind in range(3):
            proj[kind * 128 : kind * 128 + 64, :] = plain[kind * 64 : kind * 64 + 64, :]
            proj[kind * 128 + 64 : kind * 128 + 128, :] = drift[kind * 64 : kind * 64 + 64, :]
        proj[...] += wide(bias_a[pl.ds(base, 384), :])
        gat[...] = dot_nt(oat[pl.ds(pl.multiple_of(head * 128, 128), 128), :], cb[...])
        for part in (0, 64, 128, 192):
            rotate_rows(proj, part, cos, sin, False)
        proj[0:128, :] = proj[0:128, :] * 0.125
        rests = []
        for source, flat, tall, back in ((proj.at[0:128], qt, q4, True), (proj.at[128:256], kt, k4, False), (proj.at[256:384], vt, v4, False), (gat, gt, g4, True)):
            own, moved = source[0:64, :], source[64:128, :]
            flat[0:64, :] = own.astype(bf16)
            high, low = split_two(moved)
            flat[64:128, :] = high
            if back:
                low_wide = low.astype(f32)
                rests.append(low_wide)
                tall[...] = jnp.transpose(jnp.concatenate([own, own, high.astype(f32), low_wide], axis=0)).astype(bf16)
            else:
                tall[0:64, :] = high
                tall[64:128, :] = low
                tall[128:192, :] = flat[0:64, :]
                tall[192:256, :] = flat[0:64, :]
        rest_q, rest_g = rests
        for block in range(2):
            rows = slice(block * 256, block * 256 + 256)
            span = block * 256 + 256
            scores = dot_nn(q4[rows, :64], kt[:64, :span]) + mask[rows, :span]
            dscores = dot_nn(q4[rows, :], k4[:, :span])
            exp_scores = jnp.exp(scores - jnp.max(scores, axis=1, keepdims=True))
            probs = exp_scores * (1.0 / jnp.sum(exp_scores, axis=1, keepdims=True))
            dprobs = probs * (dscores - jnp.sum(probs * dscores, axis=1, keepdims=True))
            probs_low, dprobs_low = probs.astype(bf16), dprobs.astype(bf16)
            grad_probs = dot_nn(g4[rows, :64], vt[:64, :span])
            dgrad_probs = dot_nn(g4[rows, :], v4[:, :span])
            centre = jnp.sum(probs * grad_probs, axis=1, keepdims=True)
            dcentre = jnp.sum(dprobs * grad_probs + probs * dgrad_probs, axis=1, keepdims=True)
            rest = grad_probs - centre
            g_scores = (probs * rest).astype(bf16)
            dg_wide = dprobs * rest + probs * (dgrad_probs - dcentre)
            dg_scores = dg_wide.astype(bf16)
            acc_r[32:40, :span] += eight(dprobs * dgrad_probs + dg_wide * dscores)
            out = dot_nt(vt[:, :span], probs_low)
            head_a[0:64, rows] = out[:64, :].astype(bf16)
            head_a[64:128, rows] = (out[64:, :] + dot_nt(vt[:64, :span], dprobs_low)).astype(bf16)
            part_q = dot_nt(kt[:, :span], g_scores)
            acc_r[32:40, rows] += 2.0 * eight(rest_g[:, rows] * out[64:, :] + rest_q[:, rows] * part_q[64:, :])
            gq[:, rows] = part_q * 0.125
            gq[64:, rows] += dot_nt(kt[:64, :span], dg_scores) * 0.125
            part_v = dot_nn(gt[:, rows], probs_low)
            part_dv = dot_nn(gt[:64, rows], dprobs_low)
            part_k = dot_nn(qt[:, rows], g_scores)
            part_dk = dot_nn(qt[:64, rows], dg_scores)
            acc_r[32:40, :span] += 2.0 * eight(proj[320:384, :span] * part_v[64:, :] + proj[192:256, :span] * part_k[64:, :])
            if block == 0:
                gv[:, :span] = part_v
                gk[:, :span] = part_k
                gv[:, span:] = jnp.zeros((128, 512 - span), f32)
                gk[:, span:] = jnp.zeros((128, 512 - span), f32)
            else:
                gv[:, :span] += part_v
                gk[:, :span] += part_k
            gv[64:, :span] += part_dv
            gk[64:, :span] += part_dk
        for part in (0, 64):
            rotate_rows(gq, part, cos, sin, True)
            rotate_rows(gk, part, cos, sin, True)
        for kind, grad in enumerate((gq, gk, gv)):
            head_g[kind * 64 : kind * 64 + 64, :] = grad[:64, :].astype(bf16)
            head_g[192 + kind * 64 : 256 + kind * 64, :] = grad[64:, :].astype(bf16)
        one[:384, :] = dot_nn(head_g[...], lhs_a[:, :width])
        two[:384, :] = dot_nn(head_g[...], nb[...])
        two[:192, :] += dot_nn(head_g[:192, :], nb_low[...])
        sums = dot_nn(head_g[...], ones[...])
        add(acc_c, pl.ds(base, 384), sums)
        for kind in range(3):
            at = pl.multiple_of(head * 512 + kind * 128, 128)
            top, low = slice(kind * 64, kind * 64 + 64), slice(192 + kind * 64, 256 + kind * 64)
            w_rows = pl.ds(pl.multiple_of(head * 192 + kind * 64, 64), 64)
            carry = fold(
                carry, acc_h, (pl.ds(at, 64), pl.ds(at + 64, 64)), (top, low),
                wat[w_rows, width:], wat[w_rows, :width], dgain_a, dshift_a, sums[top, 0:1],
            )
        add(acc_h, pl.ds(pl.multiple_of(head * 512 + 384, 128), 128), dot_nn(head_a[...], cb[...]))
        return carry

    carry_r = (blank, blank, blank) if first else (acc_r[0:8, :], acc_r[16:24, :], blank)
    if most == 1:
        carry_r = attend(0, carry_r)
    else:
        carry_r = lax.fori_loop(0, heads_now, attend, carry_r)
    acc_r[0:8, :], acc_r[16:24, :] = carry_r[:2]
    acc_r[32:40, :] += carry_r[2]
    leaves = [
        pltpu.make_async_copy(acc_c, out_h[2], sem.at[1]),
        pltpu.make_async_copy(acc_r, out_h[3], sem.at[2]),
        pltpu.make_async_copy(acc_h.at[: most * 512], out_h[0].at[: most * 512], sem.at[3]),
    ]

    @at_step(steps - 1)
    def _():
        for copy in leaves:
            copy.start()
        if with_mlp:
            leave_m.wait()
        for copy in leaves:
            copy.wait()


def shard_steps(plan, scalars, data, shared, tables, old, parts="both", close=None):
    first = old is None
    sizes = [(1024, 768), (1536, 768), (1536, 128), (40, 768)]
    steps = len(plan)
    most = max(heads for _, heads in plan)
    whole = pl.BlockSpec(memory_space=pltpu.VMEM)
    there = pl.BlockSpec(memory_space=pltpu.HBM)
    specs = [pl.BlockSpec(memory_space=pl.ANY)] * (2 * steps) + [whole] * 4 + [there] * 6
    vec, dvec, wat, bias_a, oat, uwt, dwt, bias_u = shared
    operands = [*data, vec, dvec, *tables, wat, bias_a, oat, uwt, dwt, bias_u]
    aliases = {}
    if not first:
        aliases = {3 + len(operands) + i: i for i in range(len(sizes))}
        specs += [there] * len(sizes)
        operands += list(old)
    held = most
    outs, out_specs, slot_dev = sizes, [there] * len(sizes), None
    if parts == "close":
        owners, slot_dev, out_sum = close
        held, aliases, scalars = 2, {}, (*scalars, owners)
        specs.append(whole)
        operands.append(out_sum)
        outs, out_specs = [(8 * slot_dev, 48, 384), (4 * slot_dev, 24, 384), (32, 768)], [whole] * 3
    scratch = [((steps, *data[0].shape), data[0].dtype), ((steps, *data[1].shape), data[1].dtype)]
    scratch += [((held * 192, 1536), bf16), ((most * 384, 128), f32), ((held * 128, 768), bf16)]
    scratch += [((768, 768), bf16)] * 2 + [((768, 128), f32)]
    scratch += [((held * 512, 768), f32)] + [(size, f32) for size in sizes[1:]] + [None]
    scratch += [
        ((512, 768), bf16),
        ((512, 768), bf16),
        ((512, 128), bf16),
        ((512, 2304), bf16),
        ((512, 768), bf16),
        ((512, 768), bf16),
        ((512, 768), bf16),
        ((512, 768), bf16),
        ((512, 512), f32),
        ((384, 512), f32),
        ((128, 512), f32),
    ]
    flat, tall, back = ((128, 512), bf16), ((256, 512), bf16), ((512, 256), bf16)
    scratch += [flat, flat, tall, flat, tall, flat, back, back] + [((128, 512), f32)] * 3
    scratch += [((384, 512), bf16), ((128, 512), bf16)]
    scratch += [((768, 512), f32)] * 2 + [((768, 512), bf16)] * 2 + [((768, 768), f32)] * 2
    return pl.pallas_call(
        lambda *refs: shard_kernel(plan, first, parts, slot_dev, *refs),
        out_shape=[jax.ShapeDtypeStruct(size, f32) for size in outs],
        grid_spec=pltpu.PrefetchScalarGridSpec(
            num_scalar_prefetch=len(scalars),
            grid=(steps,),
            in_specs=specs,
            out_specs=out_specs,
            scratch_shapes=[pltpu.SemaphoreType.DMA((16,)) if one is None else pltpu.VMEM(*one) for one in scratch],
        ),
        input_output_aliases=aliases,
        compiler_params=pltpu.CompilerParams(vmem_limit_bytes=VMEM_SHARD),
        cost_estimate=pl.CostEstimate(
            flops=sum(heads * 2 * 10**9 + 5 * 10**9 for _, heads in plan), bytes_accessed=2 * 10**7, transcendentals=10**6
        ),
        name="shards_" + parts + "".join(str(heads) for _, heads in plan),
    )(*scalars, *operands)


def put_tile(slot_dev, owner, y, tile, curve, grad, curve_rows, grad_rows):
    group = slot_dev // 2
    slot = owner[tile]
    curve_rows(curve.at[slot])
    home, place = slot // slot_dev, slot % slot_dev

    @pl.when(place // group == y)
    def _():
        grad_rows(grad.at[home * group + place % group])


def tile_at(kind, side):
    return (side * 6 + 2 * kind, 1) if kind < 3 else (12 + side, 2)


def finish_kernel(slot_dev, owner, info, acc_h, acc_m, acc_c, acc_r, wat, oat, uwt, dwt, out_sum, curve, grad, sums):
    core, y, odd = info[3], info[5], info[6]
    if slot_dev * 8 > 48:
        curve[...] = jnp.zeros(curve.shape, f32)
        grad[...] = jnp.zeros(grad.shape, f32)

    def put(tile, columns, source, curve_at, grad_at):
        def curve_rows(ref):
            ref[...] = source[curve_at : curve_at + 48, columns]

        def grad_rows(ref):
            ref[...] = source[pl.ds(pl.multiple_of(grad_at + core * 24, 8), 24), columns]

        put_tile(slot_dev, owner, y, tile, curve, grad, curve_rows, grad_rows)

    for side in range(2):
        columns = slice(side * 384, side * 384 + 384)
        for kind in range(4):
            lower, step = tile_at(kind, side)
            put(lower + odd * step, columns, acc_h, kind * 128 + 64, kind * 128)
        for block in range(8):
            at = block * 48
            put(16 + side * 8 + block, columns, acc_m, 384 + at, at)
            put(32 + block * 2 + side, columns, acc_m, 1152 + at, 768 + at)
    small_sums_kernel(info, acc_h, acc_m, acc_c, acc_r, wat, oat, uwt, dwt, out_sum, sums)


def finish_split_kernel(slot_dev, owner, info, own_b, near_b, extra, old_curve, old_grad, curve, grad, new_curve, new_grad, sem):
    core, x, y, odd = info[3], info[4], info[5], info[6]
    group = slot_dev // 2
    for index in range(8):
        near_b[index] += own_b[0, pl.ds(pl.multiple_of(index * 64 + x * 32, 32), 32), :]
    copies, later = [], []
    for kind in range(4):
        for side in range(2):
            columns = slice(side * 384, side * 384 + 384)
            lower, step = tile_at(kind, side)
            slot = owner[lower + (1 - odd) * step]
            place = kind * 2 + side
            new_curve[place, 0:32, :] = near_b[kind * 2 + 1, :, columns]
            new_curve[place, 32:48, :] = extra[kind * 2 + 1, :, columns]
            copy = pltpu.make_async_copy(new_curve.at[place], curve.at[slot], sem.at[place])
            copy.start()
            copies.append(copy)

            @pl.when(core == 0)
            def _(place=place, kind=kind, columns=columns):
                new_grad[place] = near_b[kind * 2, 0:24, columns]

            @pl.when(core == 1)
            def _(place=place, kind=kind, columns=columns):
                new_grad[place, 0:8, :] = near_b[kind * 2, 24:32, columns]
                new_grad[place, 8:24, :] = extra[kind * 2, :, columns]

            home, spot = slot // slot_dev, slot % slot_dev

            @pl.when(spot // group == y)
            def _(place=place, home=home, spot=spot):
                pltpu.make_async_copy(new_grad.at[place], grad.at[home * group + spot % group], sem.at[8 + place]).start()

            later.append((place, home * group + spot % group, spot // group == y))

    for copy in copies:
        copy.wait()
    for place, target, mine in later:

        @pl.when(mine)
        def _(place=place, target=target):
            pltpu.make_async_copy(new_grad.at[place], grad.at[target], sem.at[8 + place]).wait()


def finish_split(owners, info, slot_dev, acc_h, near_b, extra, curve, grad):
    whole = pl.BlockSpec(memory_space=pltpu.VMEM)
    there = pl.BlockSpec(memory_space=pltpu.HBM)
    return pl.pallas_call(
        lambda *refs: finish_split_kernel(slot_dev, *refs),
        out_shape=[jax.ShapeDtypeStruct(curve.shape, f32), jax.ShapeDtypeStruct(grad.shape, f32)],
        grid_spec=pltpu.PrefetchScalarGridSpec(
            num_scalar_prefetch=2,
            grid=(1,),
            in_specs=[pl.BlockSpec((1, 512, 768), lambda i, *scalars: (1, 0, 0))] + [whole] * 2 + [there] * 2,
            out_specs=[there] * 2,
            scratch_shapes=[
                pltpu.VMEM((8, 48, 384), f32),
                pltpu.VMEM((8, 24, 384), f32),
                pltpu.SemaphoreType.DMA((16,)),
            ],
        ),
        input_output_aliases={5: 0, 6: 1},
        compiler_params=pltpu.CompilerParams(vmem_limit_bytes=VMEM_SHARD),
        cost_estimate=pl.CostEstimate(flops=0, bytes_accessed=5 * 10**6, transcendentals=0),
        name="finish_split",
    )(owners, info, acc_h.reshape(2, 512, 768), near_b, extra, curve, grad)


def own_attention_kernel(info, seq_device, seq_length, q_ref, k_ref, v_ref, g_ref, cos_ref, sin_ref, att, gq_out, gk_out, gv_out, mask, buf, gk, gv):
    short = is_short(seq_device, seq_length, info[0], 512)

    @pl.when(pl.program_id(0) == 0)
    def _():
        mask_rows(mask, short, 512)

    cos, sin = cos_ref[short], sin_ref[short]
    buf[...] = q_ref[...]
    rotate_rows(buf, 0, cos, sin, False)
    q_rows = buf[...] * 0.125
    qt = q_rows.astype(bf16)
    qn = jnp.transpose(q_rows).astype(bf16)
    buf[...] = k_ref[...]
    rotate_rows(buf, 0, cos, sin, False)
    kt = buf[...].astype(bf16)
    vt = v_ref[...].astype(bf16)
    gt = g_ref[...].astype(bf16)
    gn = jnp.transpose(g_ref[...]).astype(bf16)
    for block in range(2):
        rows = slice(block * 256, block * 256 + 256)
        wide = block * 256 + 256
        scores = dot_nn(qn[rows, :], kt[:, :wide]) + mask[rows, :wide]
        exp_scores = jnp.exp(scores - jnp.max(scores, axis=1, keepdims=True))
        probs = exp_scores * (1.0 / jnp.sum(exp_scores, axis=1, keepdims=True))
        probs_low = probs.astype(bf16)
        grad_probs = dot_nn(gn[rows, :], vt[:, :wide])
        weighted = probs * grad_probs
        g_scores = (weighted - probs * jnp.sum(weighted, axis=1, keepdims=True)).astype(bf16)
        att[:, rows] = dot_nt(vt[:, :wide], probs_low).astype(bf16)
        buf[:, rows] = dot_nt(kt[:, :wide], g_scores) * 0.125
        part_v = dot_nn(gt[:, rows], probs_low)
        part_k = dot_nn(qt[:, rows], g_scores)
        if block == 0:
            gv[:, :wide] = part_v
            gk[:, :wide] = part_k
            gv[:, wide:] = jnp.zeros((64, 512 - wide), f32)
            gk[:, wide:] = jnp.zeros((64, 512 - wide), f32)
        else:
            gv[:, :wide] += part_v
            gk[:, :wide] += part_k
    rotate_rows(buf, 0, cos, sin, True)
    rotate_rows(gk, 0, cos, sin, True)
    gq_out[...] = buf[...].astype(bf16)
    gk_out[...] = gk[...].astype(bf16)
    gv_out[...] = gv[...].astype(bf16)


def own_attention(scalars, mixed, grad_att, tables):
    def rows_at(offset):
        return pl.BlockSpec((64, 512), lambda i, *scalars: (offset + i, 0))

    whole = pl.BlockSpec(memory_space=pltpu.VMEM)
    return pl.pallas_call(
        own_attention_kernel,
        out_shape=[jax.ShapeDtypeStruct((768, 512), bf16)] * 4,
        grid_spec=pltpu.PrefetchScalarGridSpec(
            num_scalar_prefetch=3,
            grid=(12,),
            in_specs=[rows_at(0), rows_at(12), rows_at(24), rows_at(0), whole, whole],
            out_specs=[rows_at(0)] * 4,
            scratch_shapes=[pltpu.VMEM((512, 512), f32)] + [pltpu.VMEM((64, 512), f32)] * 3,
        ),
        compiler_params=pltpu.CompilerParams(vmem_limit_bytes=16 << 20),
        cost_estimate=pl.CostEstimate(flops=10**10, bytes_accessed=10**7, transcendentals=3 * 10**6),
        name="own_attention",
    )(*scalars, mixed, mixed, mixed, grad_att, *tables)


def lay_rows(table, slot, rows, out, buf):
    for source in range(8):
        for part in range(3):
            start = pl.multiple_of(table[slot, source * 3 + part], 16)
            buf[pl.ds(start, 16), :] = rows(source, part * 16)

    @pl.when(table[slot, 24] == 1)
    def _():
        out[0] = jnp.transpose(buf[...])

    @pl.when(table[slot, 24] == 0)
    def _():
        out[0] = buf[...]


def assemble_kernel(table, pieces, out, buf):
    lay_rows(table, pl.program_id(0), lambda source, at: pieces[source, 0, at : at + 16, :], out, buf)


def assemble(table, pieces):
    slots = pieces.shape[1]
    return pl.pallas_call(
        assemble_kernel,
        out_shape=jax.ShapeDtypeStruct((slots, 384, 384), f32),
        grid_spec=pltpu.PrefetchScalarGridSpec(
            num_scalar_prefetch=1,
            grid=(slots,),
            in_specs=[pl.BlockSpec((8, 1, 48, 384), lambda i, table: (0, i, 0, 0))],
            out_specs=pl.BlockSpec((1, 384, 384), lambda i, table: (i, 0, 0)),
            scratch_shapes=[pltpu.VMEM((384, 384), f32)],
        ),
        compiler_params=pltpu.CompilerParams(vmem_limit_bytes=16 << 20),
        cost_estimate=pl.CostEstimate(flops=0, bytes_accessed=8 * 10**6, transcendentals=0),
        name="assemble",
    )(table, pieces)


def split_two(value):
    high = value.astype(bf16)
    return (high, (value - high.astype(f32)).astype(bf16))


def dot_fine(left, right, dims):
    (a_high, a_low), (b_high, b_low) = left, right

    def dot(a, b):
        return lax.dot_general(a, b, (dims, ((), ())), preferred_element_type=f32)

    return dot(a_high, b_high) + (dot(a_high, b_low) + dot(a_low, b_high))


def update_kernel(table, info, tile, own, own_core, far, far_core, qkv, out_w, up, down, left, right, first, second, grad, new_first, new_second, new_weight, new_low, rows, buf):
    slot = pl.program_id(0)
    core, y = info[3], info[5]
    group = pl.num_programs(0) // 2

    def join(one, two):
        rows[:, pl.ds(pl.multiple_of(core * 24, 8), 24), :] = one[:, 0]
        rows[:, pl.ds(pl.multiple_of(24 - core * 24, 8), 24), :] = two[:, 0]

    @pl.when(slot // group == y)
    def _():
        join(own, own_core)

    @pl.when(slot // group != y)
    def _():
        join(far, far_core)

    lay_rows(table, slot, lambda source, at: rows[source, at : at + 16, :], grad, buf)
    index = tile[slot]

    def weight(low, high, ref):
        @pl.when((index >= low) & (index < high))
        def _():
            buf[...] = ref[...].astype(f32)

    weight(0, 12, qkv)
    weight(12, 16, out_w)
    weight(16, 32, up)
    weight(32, 48, down)
    used = jnp.where(index < 48, 1.0, 0.0)
    l_two, r_two = split_two(left[0]), split_two(right[0])
    turned = dot_fine(l_two, split_two(grad[0]), ((0,), (0,)))
    turned = dot_fine(split_two(turned), r_two, ((1,), (0,)))
    moment = beta_decay * first[0] + (1.0 - beta_decay) * turned
    square = beta_decay * second[0] + (1.0 - beta_decay) * turned * turned
    correction = 1.0 - beta_decay**STEP
    direction = moment / correction / (jnp.sqrt(square / correction) + adam_epsilon)
    new_first[0] = used * moment
    new_second[0] = used * square
    restored = dot_fine(l_two, split_two(direction), ((1,), (0,)))
    restored = dot_fine(split_two(restored), r_two, ((1,), (1,)))
    value = buf[...]
    value = jnp.where(index < 48, value - learning_rate * (restored + weight_decay * value), 0.0)
    new_weight[0] = value
    new_low[0] = value.astype(bf16)


def update(table, info, tile, pieces, weights, states):
    group = pieces[0].shape[1]
    slots = 2 * group
    piece = pl.BlockSpec((8, 1, 24, 384), lambda i, table, info, tile: (0, i % group, 0, 0))
    slab = pl.BlockSpec((1, 384, 384), lambda i, table, info, tile: (i, 0, 0))

    def spec(start, count, columns):
        def at(i, table, info, tile):
            local_tile = jnp.clip(tile[i] - start, 0, count - 1)
            return (local_tile // columns, local_tile % columns)

        return pl.BlockSpec((384, 384), at)

    kinds = [f32, f32, f32, f32, bf16]
    return pl.pallas_call(
        update_kernel,
        out_shape=[jax.ShapeDtypeStruct((slots, 384, 384), kind) for kind in kinds],
        grid_spec=pltpu.PrefetchScalarGridSpec(
            num_scalar_prefetch=3,
            grid=(slots,),
            in_specs=[piece] * 4 + [spec(0, 12, 6), spec(12, 4, 2), spec(16, 16, 8), spec(32, 16, 2)] + [slab] * 4,
            out_specs=[slab] * 5,
            scratch_shapes=[pltpu.VMEM((8, 48, 384), f32), pltpu.VMEM((384, 384), f32)],
        ),
        compiler_params=pltpu.CompilerParams(vmem_limit_bytes=32 << 20),
        cost_estimate=pl.CostEstimate(flops=10**10, bytes_accessed=4 * 10**7, transcendentals=10**6),
        name="update",
    )(table, info, tile, *pieces, *(in_hbm(value) for value in (*weights, *states)))


def small_sums_kernel(info, acc_h, acc_m, acc_c, acc_r, wat, oat, uwt, dwt, out_sum, out):
    device = info[0]
    out[...] = jnp.zeros((32, 768), f32)
    blank = jnp.zeros((8, 768), f32)
    along, curve = blank, acc_r[32:40, :]
    shift_a, shift_m, dshift_a, dshift_m = blank, blank, blank, blank

    def fold(value):
        return jnp.sum(value.reshape(value.shape[0] // 8, 8, 768), axis=0)

    for place in range(2):
        acc = acc_h.at[place * 512 : place * 512 + 512]
        head = info[1 + place]
        row = lax.broadcasted_iota(jnp.int32, (64, 128), 0) + (head % 2) * 64
        pick = lax.broadcasted_iota(jnp.int32, (64, 128), 1) == row
        for kind in range(4):
            at = kind * 128
            if kind < 3:
                base = place * 192 + kind * 64
                w_one, w_drift = wat[base : base + 64, 768:].astype(f32), wat[base : base + 64, :768].astype(f32)
                base = place * 384 + kind * 64
                p_col, q_col = acc_c[base : base + 64, :], acc_c[base + 192 : base + 256, :]
                shift_a += fold(w_one * p_col[:, 0:1])
                dshift_a += fold(w_one * q_col[:, 0:1] + w_drift * p_col[:, 0:1])
                lanes = pl.ds(pl.multiple_of(128 * (head // 2), 128), 128)
                out[4 + kind : 5 + kind, lanes] += jnp.sum(jnp.where(pick, p_col, 0.0), axis=0, keepdims=True)
                out[20 + kind : 21 + kind, lanes] += jnp.sum(jnp.where(pick, q_col, 0.0), axis=0, keepdims=True)
            else:
                w_drift = oat[place * 128 + 64 : place * 128 + 128, :].astype(f32)
            along += fold(acc[at : at + 64, :] * w_drift)
    row = lax.broadcasted_iota(jnp.int32, (48, 384), 0) + device * 48
    pick = lax.broadcasted_iota(jnp.int32, (48, 384), 1) == row
    for block in range(8):
        at = block * 48
        w_one, w_drift = uwt[at : at + 48, :].astype(f32), uwt[384 + at : 432 + at, :].astype(f32)
        d_drift = dwt[384 + at : 432 + at, :].astype(f32)
        p_col, q_col = acc_c[768 + at : 816 + at, 0:1], acc_c[1152 + at : 1200 + at, 0:1]
        shift_m += fold(w_one * p_col)
        dshift_m += fold(w_one * q_col + w_drift * p_col)
        along += fold(acc_m[at : at + 48, :] * w_drift) + fold(acc_m[768 + at : 816 + at, :] * d_drift)
        lanes = slice(384 * (block % 2), 384 * (block % 2) + 384)
        place = 8 + block // 2
        out[place : place + 1, lanes] = jnp.sum(jnp.where(pick, p_col, 0.0), axis=0, keepdims=True)
        out[16 + place : 17 + place, lanes] = jnp.sum(jnp.where(pick, q_col, 0.0), axis=0, keepdims=True)

    def row_sum(value):
        return jnp.sum(value, axis=0, keepdims=True)

    out[0:1, :] = row_sum(acc_r[16:24, :])
    out[1:2, :] = row_sum(shift_a)
    out[2:3, :] = row_sum(acc_r[24:32, :])
    out[3:4, :] = row_sum(shift_m)
    out[7:8, :] = out_sum[...]
    out[12:13, :] = out_sum[...]
    out[16:17, :] = row_sum(acc_r[0:8, :])
    out[17:18, :] = row_sum(dshift_a)
    out[18:19, :] = row_sum(acc_r[8:16, :])
    out[19:20, :] = row_sum(dshift_m)
    lane = lax.broadcasted_iota(jnp.int32, (1, 768), 1)
    out[29:30, :] = jnp.where(lane == 0, jnp.sum(along), jnp.where(lane == 1, jnp.sum(curve), 0.0))


def take_rows(matrix, start, size):
    return lax.dynamic_slice_in_dim(matrix, start, size, axis=0)


def piece_rows(index):
    z, x = index // 2, index % 2
    plain = [48 * index, 48 * index + 16, 48 * index + 32]
    full = [[64 * x + 16 * i for i in range(3)], [64 + 64 * x + 16 * i for i in range(3)]]
    full += [[192 + 64 * x + 16 * i for i in range(3)], [256 + 64 * x + 16 * i for i in range(3)]]
    split = [
        [32 * x, 32 * x + 16, 64 + 64 * x + 48],
        [128 + 32 * x, 144 + 32 * x, 64 * x + 48],
        [192 + 32 * x, 208 + 32 * x, 256 + 64 * x + 48],
        [320 + 32 * x, 336 + 32 * x, 192 + 64 * x + 48],
    ]
    even = z % 2 == 0
    return (full[z] if even else split[z], split[z] if even else full[z], plain)


def local_tp(
    tokens,
    cotangent,
    vec_params,
    qkv_weight,
    out_weight,
    up_weight,
    down_weight,
    probe_vec,
    probe_qkv,
    probe_out,
    probe_up,
    probe_down,
    seq_device,
    seq_length,
    owners,
    left_bases,
    right_bases,
    first_moment,
    second_moment,
    vec_first,
    vec_second,
):
    row_count, width = tokens.shape
    device = lax.axis_index("dp")
    z = device // 2
    probe = lax.axis_index("probe")
    x, y, core = device % 2, probe // 2, probe % 2
    info = lax.dynamic_index_in_dim(jnp.array(device_table(), jnp.int32), device * 4 + probe, 0, keepdims=False)
    scalars = (info, seq_device, seq_length)
    drift_vec, drift_qkv, drift_out = probe_vec[0], probe_qkv[0], probe_out[0]
    drift_up, drift_down = probe_up[0], probe_down[0]
    barrier = lax.optimization_barrier

    across = [(i, i ^ 1) for i in range(8)]
    outer = [(i, i ^ 2) for i in range(8)]
    middle = [(2, 4), (3, 5), (4, 2), (5, 3)]
    outward = [(2, 0), (3, 1), (4, 6), (5, 7)]
    swap_core = [(0, 1), (1, 0), (2, 3), (3, 2)]
    swap_y = [(0, 2), (2, 0), (1, 3), (3, 1)]

    def move(value, pairs):
        return lax.ppermute(value, "dp", pairs)

    def to_core(value):
        return lax.ppermute(value, "probe", swap_core)

    mine = outgoing(info, tokens, cotangent)
    near, centre, cross_0 = move(mine, outer), move(mine, middle), move(mine, across)
    inside = (z == 1) | (z == 2)

    row_index = jnp.arange(row_count, dtype=jnp.int32)
    half_rot = ROT // 2
    frequency = jnp.exp(jnp.arange(half_rot, dtype=f32) * (-2.0 * math.log(10000.0) / ROT))
    position = jnp.stack([row_index, row_index % (row_count // 4)])
    angles = position.astype(f32)[:, None, :] * frequency[None, :, None]
    tables = (jnp.cos(angles), jnp.sin(angles))

    flat_bias = vec_params[4:7].reshape(-1)
    uwt, dwt, bias_u, wat, oat, bias_a = prepare(
        info,
        qkv_weight, drift_qkv, out_weight, drift_out, up_weight, drift_up, down_weight, drift_down, vec_params, drift_vec,
    )
    shared = (vec_params, drift_vec, wat, bias_a, oat, uwt, dwt, bias_u)

    def step(plan, data, old, *how):
        return shard_steps(plan, scalars, data, shared, tables, old, *how)

    acc_h, acc_m, acc_c, acc_r = step(((0, 2),), (tokens, cotangent), None)
    (near, centre, cross_0, acc_r) = barrier((near, centre, cross_0, acc_r))
    edge, middle_near, cross_1 = move(centre, outward), move(near, middle), move(near, across)
    cross_0o, near_o = to_core(cross_0), to_core(near)
    acc_h, acc_m, acc_c, acc_r = step(((1, 2), (4, 1)), (near, near_o, cross_0, cross_0o), (acc_h, acc_m, acc_c, acc_r))

    (edge, middle_near, cross_1, acc_r) = barrier((edge, middle_near, cross_1, acc_r))
    second = jnp.where(inside, centre, edge)
    (middle_near, second) = barrier((middle_near, second))
    edge_far, cross_2 = move(middle_near, outward), move(second, across)
    second_o, cross_1o = to_core(second), to_core(cross_1)
    acc_h, acc_m, acc_c, acc_r = step(((2, 2), (5, 1)), (second, second_o, cross_1, cross_1o), (acc_h, acc_m, acc_c, acc_r))

    (edge_far, cross_2, acc_r) = barrier((edge_far, cross_2, acc_r))
    third = barrier(jnp.where(inside, middle_near, edge_far))
    cross_3, third_o, cross_2o = move(third, across), to_core(third), to_core(cross_2)
    acc_h, acc_m, acc_c, acc_r = step(((3, 2), (6, 1)), (third, third_o, cross_2, cross_2o), (acc_h, acc_m, acc_c, acc_r))
    sends = lax.dynamic_slice(acc_h.reshape(16, 64, width), (8, 32 - 32 * x, 0), (8, 32, width))
    near_b = move(sends, across)
    (tokens, cotangent, cross_3, acc_r) = barrier((tokens, cotangent, cross_3, acc_r))
    cross_3o = to_core(cross_3)
    inputs = tokens.astype(f32)
    cot_rows = cotangent.astype(f32)
    out_sum = jnp.sum(cot_rows, axis=0, keepdims=True)
    normed, norm_scale = normalize(inputs)
    attn_low = (normed * vec_params[0] + vec_params[1]).astype(bf16)
    mlp_low = (normed * vec_params[2] + vec_params[3]).astype(bf16)
    (cross_3, cross_3o, acc_r, attn_low, mlp_low) = barrier((cross_3, cross_3o, acc_r, attn_low, mlp_low))
    acc_h, acc_m, acc_c, acc_r = step(((7, 1),), (cross_3, cross_3o), (acc_h, acc_m, acc_c, acc_r), "heads")
    extra = move(acc_h.reshape(16, 64, width)[:8, 48:], [(i, i ^ 2) for i in range(8)])

    slot_dev = left_bases.shape[0]
    tile_index, occupied = slot_order(owners, slot_dev * 8)
    curve_slots, grad_slots, vec_all = step(
        ((7, 1),), (cross_3, cross_3o), (acc_h, acc_m, acc_c, acc_r), "close", (owners, slot_dev, out_sum)
    )
    vec_one = move(vec_all, [(i, i ^ 4) for i in range(8)])
    (extra, near_b, vec_all) = barrier((extra, near_b, vec_all))
    curve_slots, grad_slots = finish_split(owners, info, slot_dev, acc_h, near_b, extra, curve_slots, grad_slots)
    curve_slots = curve_slots.reshape(8, slot_dev, 48, 384)
    (attn_low, cotangent, grad_slots) = barrier((attn_low, cotangent, grad_slots))
    grad_slots = lax.all_to_all(grad_slots.reshape(8, slot_dev // 2, 24, 384), "dp", 0, 0)
    curve_slots = lax.all_to_all(curve_slots, "dp", 0, 0)
    mixed = product("kj,tk->jt", qkv_weight, attn_low) + flat_bias[:, None]
    grad_att = product("jk,tk->jt", out_weight, cotangent)
    (mixed, grad_att, vec_all, vec_one) = barrier((mixed, grad_att, vec_all, vec_one))
    vec_all = vec_all + vec_one
    vec_two = move(vec_all, [(i, i ^ 2) for i in range(8)])
    att_t, gq_t, gk_t, gv_t = own_attention(scalars, mixed, grad_att, tables)
    (vec_all, vec_two, att_t) = barrier((vec_all, vec_two, att_t))
    vec_all = vec_all + vec_two
    vec_four = move(vec_all, [(i, i ^ 1) for i in range(8)])

    (grad_slots, att_t, gq_t, gk_t, gv_t) = barrier((grad_slots, att_t, gq_t, gk_t, gv_t))
    far = lax.ppermute(grad_slots, "probe", swap_y)
    own_core = to_core(grad_slots)
    (mlp_low, cotangent, own_core, att_t, gq_t, gk_t, gv_t) = barrier((mlp_low, cotangent, own_core, att_t, gq_t, gk_t, gv_t))
    hidden = product("ij,jk->ik", mlp_low, up_weight) + vec_params[8:12].reshape(-1)
    cumulative = 0.5 * (1.0 + lax.erf(hidden * root_half))
    density = jnp.exp(-0.5 * hidden * hidden) * density_scale
    act_low = (hidden * cumulative).astype(bf16)
    grad_act = product("ij,kj->ik", cotangent, down_weight)
    grad_hidden_low = (grad_act * (cumulative + hidden * density)).astype(bf16)
    mlp_out = product("ij,jk->ik", act_low, down_weight) + vec_params[12]
    (mlp_out, far, grad_hidden_low, att_t) = barrier((mlp_out, far, grad_hidden_low, att_t))
    far_core = to_core(far)
    attn_out = product("jt,jk->tk", att_t, out_weight) + vec_params[7]
    block_output = (inputs + attn_out + mlp_out).astype(bf16)
    grad_mlp_in = product("ij,kj->ik", grad_hidden_low, up_weight)
    grad_attn_in = (
        product("jt,kj->tk", gq_t, qkv_weight[:, :width])
        + product("jt,kj->tk", gk_t, qkv_weight[:, width : 2 * width])
        + product("jt,kj->tk", gv_t, qkv_weight[:, 2 * width :])
    )
    grad_weighted = grad_attn_in * vec_params[0] + grad_mlp_in * vec_params[2]
    input_grad = cot_rows + norm_back(grad_weighted, normed, norm_scale)

    own_index = lax.dynamic_slice_in_dim(tile_index, device * slot_dev, slot_dev)
    kinds = [sum((piece_rows(i)[kind] for i in range(8)), []) for kind in range(3)]
    row_table = jnp.array(kinds, jnp.int32)
    in_qkv, in_out = own_index < 12, (own_index >= 12) & (own_index < 16)
    kind = jnp.where(in_qkv, own_index % 2, jnp.where(in_out, (own_index - 12) // 2, 2))
    turned = in_qkv | ((own_index >= 16) & (own_index < 32))
    table = jnp.concatenate([row_table[kind], turned.astype(jnp.int32)[:, None]], axis=1)
    (far_core, input_grad, block_output) = barrier((far_core, input_grad, block_output))
    own_grad, new_first, new_second, new_weights, new_weights_low = update(
        table,
        info,
        own_index,
        [grad_slots, own_core, far, far_core],
        [qkv_weight, out_weight, up_weight, down_weight],
        [left_bases, right_bases, first_moment, second_moment],
    )
    (vec_all, vec_four, new_first) = barrier((vec_all, vec_four, new_first))
    vec_all = vec_all + vec_four
    vec_total, vec_curve = vec_all[:13], vec_all[16:29]
    own_dots = jnp.stack(
        [vec_all[29, 0] + jnp.sum(vec_total * drift_vec), vec_all[29, 1]]
    )
    all_dots = jnp.where(jnp.arange(8)[:, None] == probe, jnp.pad(own_dots, (0, 126))[None], 0.0)
    all_dots = all_dots + to_core(all_dots)
    all_dots = all_dots + lax.ppermute(all_dots, "probe", swap_y)
    all_dots = all_dots[:4, :2]
    own_curve = assemble(table, curve_slots)
    vec_new_first, vec_new_second, vec_new = plain_adam(vec_total, vec_params, vec_first, vec_second)
    vector_state = jnp.stack([vec_total, vec_new_first], axis=0)
    return (
        block_output,
        input_grad,
        own_grad,
        new_first,
        new_second,
        new_weights,
        new_weights_low,
        own_curve[None],
        vector_state,
        vec_new_second,
        vec_new,
        vec_curve[None],
        all_dots,
    )


def solution(mesh):
    local = local_tp if fits_tp(mesh) else local_any
    return jax.shard_map(
        local,
        mesh=mesh,
        in_specs=(
            P("dp", None),
            P("dp", None),
            P(),
            P(),
            P(),
            P(),
            P(),
            P("probe", None, None),
            P("probe", None, None),
            P("probe", None, None),
            P("probe", None, None),
            P("probe", None, None),
            P(),
            P(),
            P(),
            P("dp", None, None),
            P("dp", None, None),
            P("dp", None, None),
            P("dp", None, None),
            P(),
            P(),
        ),
        out_specs=(
            P("dp", None),
            P("dp", None),
            P("dp", None, None),
            P("dp", None, None),
            P("dp", None, None),
            P("dp", None, None),
            P("dp", None, None),
            P("probe", "dp", None, None),
            P(),
            P(),
            P(),
            P("probe", None, None),
            P(),
        ),
        check_vma=False,
    )
```

```python
import math

import jax
import jax.numpy as jnp
from jax import lax
from jax.experimental import pallas as pl
from jax.experimental.pallas import tpu as pltpu
from jax.sharding import PartitionSpec as P

HEAD = 64
ROT = 16
BLK = 384
STEP = 4


beta_decay = 0.5
learning_rate = 0.05
weight_decay = 0.01
adam_epsilon = 1e-08
norm_epsilon = 1e-05
root_half = 0.7071067811865476
density_scale = 0.3989422804014327
masked_score = -1e30


def product(pattern, left_side, right_side):
    if left_side.dtype == jnp.bfloat16 and right_side.dtype == jnp.bfloat16:
        return jnp.einsum(pattern, left_side, right_side, preferred_element_type=jnp.float32)
    return jnp.einsum(
        pattern,
        left_side,
        right_side,
        precision=lax.Precision.HIGHEST,
        preferred_element_type=jnp.float32,
    )


def normalize(inputs):
    mean_row = jnp.mean(inputs, axis=1, keepdims=True)
    centred = inputs - mean_row
    variance = jnp.mean(centred * centred, axis=1, keepdims=True)
    norm_scale = lax.rsqrt(variance + norm_epsilon)
    return (centred * norm_scale, norm_scale)


def norm_back(grad_normed, normed, norm_scale):
    mean_grad = jnp.mean(grad_normed, axis=1, keepdims=True)
    mean_cross = jnp.mean(grad_normed * normed, axis=1, keepdims=True)
    return norm_scale * (grad_normed - mean_grad - normed * mean_cross)


def row_layout(device, seq_device, seq_length, row_count):
    present = (seq_device == device).astype(jnp.int32)
    taken_rows = present * seq_length
    start_row = jnp.cumsum(taken_rows) - taken_rows
    row_index = jnp.arange(row_count, dtype=jnp.int32)[:, None]
    inside = (
        (present[None, :] > 0)
        & (row_index >= start_row[None, :])
        & (row_index < (start_row + taken_rows)[None, :])
    ).astype(jnp.int32)
    number = jnp.arange(seq_device.shape[0], dtype=jnp.int32)
    segment = jnp.sum(inside * number[None, :], axis=1)
    position = jnp.sum(inside * (row_index - start_row[None, :]), axis=1)
    return (segment, position)


def rotary_table(position):
    half_rot = ROT // 2
    frequency = jnp.exp(jnp.arange(half_rot, dtype=jnp.float32) * (-2.0 * math.log(10000.0) / ROT))
    angles = position.astype(jnp.float32)[:, None] * frequency[None, :]
    return (jnp.cos(angles), jnp.sin(angles))


def rotate(values, cosine_table, sine_table, reverse):
    half_rot = cosine_table.shape[1]
    first_half = values[..., :half_rot]
    second = values[..., half_rot : 2 * half_rot]
    cos_wide = cosine_table[:, None, :]
    sin_wide = sine_table[:, None, :]
    if reverse:
        new_first = first_half * cos_wide + second * sin_wide
        new_second = second * cos_wide - first_half * sin_wide
    else:
        new_first = first_half * cos_wide - second * sin_wide
        new_second = second * cos_wide + first_half * sin_wide
    return jnp.concatenate([new_first, new_second, values[..., 2 * half_rot :]], axis=-1)


def swap_major(values):
    return jnp.transpose(values, (1, 0, 2))


def cut_tiles(matrix):
    height, span_cols = matrix.shape
    return (
        matrix.reshape(height // BLK, BLK, span_cols // BLK, BLK)
        .transpose(0, 2, 1, 3)
        .reshape(-1, BLK, BLK)
    )


def slot_order(owners, slot_total):
    slot_ids = jnp.arange(slot_total, dtype=jnp.int32)
    matches = owners[None, :] == slot_ids[:, None]
    tile_index = jnp.sum(
        jnp.where(matches, jnp.arange(owners.shape[0], dtype=jnp.int32)[None, :], 0), axis=1
    )
    occupied = jnp.any(matches, axis=1)
    return (jnp.where(occupied, tile_index, owners.shape[0]), occupied)


def arrange(blocks, tile_index):
    padded = jnp.concatenate([blocks, jnp.zeros((1,) + blocks.shape[1:], blocks.dtype)], axis=0)
    return jnp.take(padded, tile_index, axis=0)


def rotated_adam(gradient, weight, left_basis, right_basis, first_state, second_state, occupied):
    turned = jnp.einsum("sji,sjk->sik", left_basis, gradient, precision=lax.Precision.HIGHEST)
    turned = jnp.einsum("sik,skl->sil", turned, right_basis, precision=lax.Precision.HIGHEST)
    new_first = beta_decay * first_state + (1.0 - beta_decay) * turned
    new_second = beta_decay * second_state + (1.0 - beta_decay) * turned * turned
    correction = 1.0 - beta_decay**STEP
    direction = new_first / correction / (jnp.sqrt(new_second / correction) + adam_epsilon)
    restored = jnp.einsum("sij,sjk->sik", left_basis, direction, precision=lax.Precision.HIGHEST)
    restored = jnp.einsum("sik,slk->sil", restored, right_basis, precision=lax.Precision.HIGHEST)
    new_weight = weight - learning_rate * (restored + weight_decay * weight)
    slot_mask = occupied.astype(jnp.float32)[:, None, None]
    return (slot_mask * new_first, slot_mask * new_second, slot_mask * new_weight)


def plain_adam(gradient, value_rows, first_state, second_state):
    new_first = beta_decay * first_state + (1.0 - beta_decay) * gradient
    new_second = beta_decay * second_state + (1.0 - beta_decay) * gradient * gradient
    correction = 1.0 - beta_decay**STEP
    new_value = value_rows - learning_rate * (new_first / correction) / (
        jnp.sqrt(new_second / correction) + adam_epsilon
    )
    return (new_first, new_second, new_value)


def local_any(
    tokens,
    cotangent,
    vec_params,
    qkv_weight,
    out_weight,
    up_weight,
    down_weight,
    probe_vec,
    probe_qkv,
    probe_out,
    probe_up,
    probe_down,
    seq_device,
    seq_length,
    owners,
    left_bases,
    right_bases,
    first_moment,
    second_moment,
    vec_first,
    vec_second,
):
    row_count, model_width = tokens.shape
    head_count = model_width // HEAD
    up_rows = up_weight.shape[1] // model_width
    device = lax.axis_index("dp")
    segment, position = row_layout(device, seq_device, seq_length, row_count)
    cosine_table, sine_table = rotary_table(position)
    row_index = jnp.arange(row_count, dtype=jnp.int32)
    allowed = (segment[:, None] == segment[None, :]) & (row_index[None, :] <= row_index[:, None])
    drift_vec = probe_vec[0]
    drift_qkv = probe_qkv[0]
    drift_out = probe_out[0]
    drift_up = probe_up[0]
    drift_down = probe_down[0]
    inputs = tokens.astype(jnp.float32)
    cot_rows = cotangent.astype(jnp.float32)
    normed, norm_scale = normalize(inputs)
    attn_in = normed * vec_params[0] + vec_params[1]
    drift_attn_in = normed * drift_vec[0] + drift_vec[1]
    mlp_in = normed * vec_params[2] + vec_params[3]
    drift_mlp_in = normed * drift_vec[2] + drift_vec[3]
    attn_low = attn_in.astype(jnp.bfloat16)
    mlp_low = mlp_in.astype(jnp.bfloat16)
    mixed_rows = product("ij,jk->ik", attn_low, qkv_weight) + vec_params[4:7].reshape(-1)
    drift_mixed = (
        product("ij,jk->ik", drift_attn_in, qkv_weight)
        + product("ij,jk->ik", attn_low, drift_qkv)
        + drift_vec[4:7].reshape(-1)
    )

    def split_heads(matrix, column_group):
        return matrix[:, column_group * model_width : (column_group + 1) * model_width].reshape(
            row_count, head_count, HEAD
        )

    query_rows = rotate(split_heads(mixed_rows, 0), cosine_table, sine_table, False)
    key_rows = rotate(split_heads(mixed_rows, 1), cosine_table, sine_table, False)
    value_rows = split_heads(mixed_rows, 2)
    drift_query = rotate(split_heads(drift_mixed, 0), cosine_table, sine_table, False)
    drift_key = rotate(split_heads(drift_mixed, 1), cosine_table, sine_table, False)
    drift_value = split_heads(drift_mixed, 2)
    grad_att = product("ij,kj->ik", cotangent, out_weight)
    drift_grad_att = product("ij,kj->ik", cotangent, drift_out)
    grad_att_low = grad_att.astype(jnp.bfloat16)

    def attend(pieces):
        query_block, key_block, value_block, drift_q, drift_k, drift_v, grad_out, drift_grad_out = (
            pieces
        )
        scores = product("ij,kj->ik", query_block, key_block) * 0.125
        drift_scores = (
            product("ij,kj->ik", drift_q, key_block) + product("ij,kj->ik", query_block, drift_k)
        ) * 0.125
        scores = jnp.where(allowed, scores, masked_score)
        shifted = scores - jnp.max(scores, axis=1, keepdims=True)
        exp_scores = jnp.exp(shifted)
        probs = exp_scores / jnp.sum(exp_scores, axis=1, keepdims=True)
        drift_probs = probs * (drift_scores - jnp.sum(probs * drift_scores, axis=1, keepdims=True))
        probs_low = probs.astype(jnp.bfloat16)
        attended_head = product("ij,jk->ik", probs_low, value_block)
        drift_attended_head = product("ij,jk->ik", drift_probs, value_block) + product(
            "ij,jk->ik", probs_low, drift_v
        )
        grad_probs = product("ij,kj->ik", grad_out, value_block)
        drift_grad_probs = product("ij,kj->ik", drift_grad_out, value_block) + product(
            "ij,kj->ik", grad_out, drift_v
        )
        grad_value_head = product("ij,ik->jk", probs_low, grad_out)
        drift_grad_value_head = product("ij,ik->jk", drift_probs, grad_out) + product(
            "ij,ik->jk", probs_low, drift_grad_out
        )
        centre = jnp.sum(probs * grad_probs, axis=1, keepdims=True)
        drift_centre = jnp.sum(
            drift_probs * grad_probs + probs * drift_grad_probs, axis=1, keepdims=True
        )
        grad_scores = probs * (grad_probs - centre)
        drift_grad_scores = drift_probs * (grad_probs - centre) + probs * (
            drift_grad_probs - drift_centre
        )
        scores_low = grad_scores.astype(jnp.bfloat16)
        grad_query_head = product("ij,jk->ik", scores_low, key_block) * 0.125
        drift_grad_query_head = (
            product("ij,jk->ik", drift_grad_scores, key_block)
            + product("ij,jk->ik", scores_low, drift_k)
        ) * 0.125
        grad_key_head = product("ij,ik->jk", scores_low, query_block) * 0.125
        drift_grad_key_head = (
            product("ij,ik->jk", drift_grad_scores, query_block)
            + product("ij,ik->jk", scores_low, drift_q)
        ) * 0.125
        return (
            attended_head,
            drift_attended_head,
            grad_query_head,
            grad_key_head,
            grad_value_head,
            drift_grad_query_head,
            drift_grad_key_head,
            drift_grad_value_head,
        )

    results = lax.map(
        attend,
        (
            swap_major(query_rows.astype(jnp.bfloat16)),
            swap_major(key_rows.astype(jnp.bfloat16)),
            swap_major(value_rows.astype(jnp.bfloat16)),
            swap_major(drift_query),
            swap_major(drift_key),
            swap_major(drift_value),
            swap_major(grad_att_low.reshape(row_count, head_count, HEAD)),
            swap_major(drift_grad_att.reshape(row_count, head_count, HEAD)),
        ),
    )
    attended = swap_major(results[0]).reshape(row_count, model_width)
    drift_attended = swap_major(results[1]).reshape(row_count, model_width)
    grad_query = rotate(swap_major(results[2]), cosine_table, sine_table, True).reshape(
        row_count, model_width
    )
    grad_key = rotate(swap_major(results[3]), cosine_table, sine_table, True).reshape(
        row_count, model_width
    )
    grad_value = swap_major(results[4]).reshape(row_count, model_width)
    drift_grad_query = rotate(swap_major(results[5]), cosine_table, sine_table, True).reshape(
        row_count, model_width
    )
    drift_grad_key = rotate(swap_major(results[6]), cosine_table, sine_table, True).reshape(
        row_count, model_width
    )
    drift_grad_value = swap_major(results[7]).reshape(row_count, model_width)
    grad_mixed_low = jnp.concatenate([grad_query, grad_key, grad_value], axis=1).astype(
        jnp.bfloat16
    )
    drift_grad_mixed = jnp.concatenate([drift_grad_query, drift_grad_key, drift_grad_value], axis=1)
    att_low = attended.astype(jnp.bfloat16)
    attn_out = product("ij,jk->ik", att_low, out_weight) + vec_params[7]
    hidden = product("ij,jk->ik", mlp_low, up_weight) + vec_params[8 : 8 + up_rows].reshape(-1)
    drift_hidden = (
        product("ij,jk->ik", drift_mlp_in, up_weight)
        + product("ij,jk->ik", mlp_low, drift_up)
        + drift_vec[8 : 8 + up_rows].reshape(-1)
    )
    cumulative = 0.5 * (1.0 + lax.erf(hidden * root_half))
    density = jnp.exp(-0.5 * hidden * hidden) * density_scale
    activated = hidden * cumulative
    gelu_slope = cumulative + hidden * density
    gelu_bend = density * (2.0 - hidden * hidden)
    act_low = activated.astype(jnp.bfloat16)
    drift_act = gelu_slope * drift_hidden
    mlp_out = product("ij,jk->ik", act_low, down_weight) + vec_params[8 + up_rows]
    block_output = (inputs + attn_out + mlp_out).astype(jnp.bfloat16)
    grad_down = product("ij,ik->jk", act_low, cotangent)
    drift_grad_down = product("ij,ik->jk", drift_act, cotangent)
    grad_act = product("ij,kj->ik", cotangent, down_weight)
    drift_grad_act = product("ij,kj->ik", cotangent, drift_down)
    grad_hidden = grad_act * gelu_slope
    drift_grad_hidden = drift_grad_act * gelu_slope + grad_act * gelu_bend * drift_hidden
    grad_hidden_low = grad_hidden.astype(jnp.bfloat16)
    grad_up = product("ij,ik->jk", mlp_low, grad_hidden_low)
    drift_grad_up = product("ij,ik->jk", drift_mlp_in, grad_hidden_low) + product(
        "ij,ik->jk", mlp_low, drift_grad_hidden
    )
    grad_mlp_in = product("ij,kj->ik", grad_hidden_low, up_weight)
    drift_grad_mlp_in = product("ij,kj->ik", drift_grad_hidden, up_weight) + product(
        "ij,kj->ik", grad_hidden_low, drift_up
    )
    grad_out_w = product("ij,ik->jk", att_low, cotangent)
    drift_grad_out_w = product("ij,ik->jk", drift_attended, cotangent)
    grad_qkv = product("ij,ik->jk", attn_low, grad_mixed_low)
    drift_grad_qkv = product("ij,ik->jk", drift_attn_in, grad_mixed_low) + product(
        "ij,ik->jk", attn_low, drift_grad_mixed
    )
    grad_attn_in = product("ij,kj->ik", grad_mixed_low, qkv_weight)
    drift_grad_attn_in = product("ij,kj->ik", drift_grad_mixed, qkv_weight) + product(
        "ij,kj->ik", grad_mixed_low, drift_qkv
    )
    grad_weighted = grad_attn_in * vec_params[0] + grad_mlp_in * vec_params[2]
    input_grad = cot_rows + norm_back(grad_weighted, normed, norm_scale)
    out_sum = jnp.sum(cot_rows, axis=0)[None]
    zero_row = jnp.zeros((1, model_width), jnp.float32)
    vec_grad = jnp.concatenate(
        [
            jnp.sum(grad_attn_in * normed, axis=0)[None],
            jnp.sum(grad_attn_in, axis=0)[None],
            jnp.sum(grad_mlp_in * normed, axis=0)[None],
            jnp.sum(grad_mlp_in, axis=0)[None],
            jnp.sum(grad_mixed_low, axis=0, dtype=jnp.float32).reshape(3, model_width),
            out_sum,
            jnp.sum(grad_hidden_low, axis=0, dtype=jnp.float32).reshape(up_rows, model_width),
            out_sum,
        ],
        axis=0,
    )
    vec_drift = jnp.concatenate(
        [
            jnp.sum(drift_grad_attn_in * normed, axis=0)[None],
            jnp.sum(drift_grad_attn_in, axis=0)[None],
            jnp.sum(drift_grad_mlp_in * normed, axis=0)[None],
            jnp.sum(drift_grad_mlp_in, axis=0)[None],
            jnp.sum(drift_grad_mixed, axis=0).reshape(3, model_width),
            zero_row,
            jnp.sum(drift_grad_hidden, axis=0).reshape(up_rows, model_width),
            zero_row,
        ],
        axis=0,
    )
    along_probe = jnp.sum(vec_grad * drift_vec)
    curve_probe = jnp.sum(vec_drift * drift_vec)
    for gradient, drift_gradient, direction_set in (
        (grad_qkv, drift_grad_qkv, drift_qkv),
        (grad_out_w, drift_grad_out_w, drift_out),
        (grad_up, drift_grad_up, drift_up),
        (grad_down, drift_grad_down, drift_down),
    ):
        along_probe = along_probe + jnp.sum(gradient * direction_set.astype(jnp.float32))
        curve_probe = curve_probe + jnp.sum(drift_gradient * direction_set.astype(jnp.float32))
    dots = jnp.stack([along_probe, curve_probe])
    grad_tiles = jnp.concatenate(
        [cut_tiles(grad_qkv), cut_tiles(grad_out_w), cut_tiles(grad_up), cut_tiles(grad_down)],
        axis=0,
    )
    curve_tiles = jnp.concatenate(
        [
            cut_tiles(drift_grad_qkv),
            cut_tiles(drift_grad_out_w),
            cut_tiles(drift_grad_up),
            cut_tiles(drift_grad_down),
        ],
        axis=0,
    )
    slot_dev = left_bases.shape[0]
    slot_total = slot_dev * lax.axis_size("dp")
    tile_index, occupied = slot_order(owners, slot_total)
    slot_grad = arrange(grad_tiles, tile_index)
    slot_curve = arrange(curve_tiles, tile_index)
    own_grad, own_curve = (
        lax.psum_scatter(slot_grad, "dp", scatter_dimension=0, tiled=True),
        lax.psum_scatter(slot_curve, "dp", scatter_dimension=0, tiled=True),
    )
    vec_total, vec_curve, dot_total = lax.psum((vec_grad, vec_drift, dots), "dp")
    all_dots = lax.all_gather(dot_total[None, :], "probe", axis=0, tiled=True)
    own_index = lax.dynamic_slice_in_dim(tile_index, device * slot_dev, slot_dev)
    own_used = lax.dynamic_slice_in_dim(occupied, device * slot_dev, slot_dev)
    weight_tiles = jnp.concatenate(
        [
            cut_tiles(qkv_weight),
            cut_tiles(out_weight),
            cut_tiles(up_weight),
            cut_tiles(down_weight),
        ],
        axis=0,
    )
    own_weight = arrange(weight_tiles, own_index).astype(jnp.float32)
    new_first, new_second, new_weights = rotated_adam(
        own_grad, own_weight, left_bases, right_bases, first_moment, second_moment, own_used
    )
    new_weights_low = new_weights.astype(jnp.bfloat16)
    vec_new_first, vec_new_second, vec_new = plain_adam(
        vec_total, vec_params, vec_first, vec_second
    )
    vector_state = jnp.stack([vec_total, vec_new_first], axis=0)
    return (
        block_output,
        input_grad,
        own_grad,
        new_first,
        new_second,
        new_weights,
        new_weights_low,
        own_curve[None],
        vector_state,
        vec_new_second,
        vec_new,
        vec_curve[None],
        all_dots,
    )


f32 = jnp.float32
bf16 = jnp.bfloat16
VMEM_SHARD = 60 << 20
HEAD_A = (0, 1, 7, 8, 3, 4, 10, 11)
HEAD_B = (6, 6, 2, 2, 9, 9, 5, 5)
ARRIVE = ((1, 2, 3), (0, 2, 3), (3, 1, 0), (2, 1, 0))


def fits_tp(mesh):
    return mesh.shape["dp"] == 8 and mesh.shape["probe"] == 4


def device_table():
    rows = []
    for device in range(8):
        z, x = device // 2, device % 2
        levels = (z,) + ARRIVE[z]
        order = [2 * level + x for level in levels] + [2 * level + 1 - x for level in levels]
        for probe in range(4):
            rows.append([device, HEAD_A[device], HEAD_B[device], probe % 2, x, probe // 2, z % 2, 0] + order)
    return rows


def is_short(seq_device, seq_length, group, rows):
    longest = jnp.int32(0)
    for i in range(seq_device.shape[0]):
        longest = jnp.maximum(longest, jnp.where(seq_device[i] == group, seq_length[i], 0))
    return (longest < rows).astype(jnp.int32)


def in_hbm(value):
    return pltpu.with_memory_space_constraint(value, pltpu.HBM)


def dot_nt(left, right):
    return lax.dot_general(left, right, (((1,), (1,)), ((), ())), preferred_element_type=f32)


def dot_nn(left, right):
    return lax.dot_general(left, right, (((1,), (0,)), ((), ())), preferred_element_type=f32)


def rotate_rows(ref, base, cos, sin, reverse):
    up, low = ref[base : base + 8, :], ref[base + 8 : base + 16, :]
    if reverse:
        ref[base : base + 8, :] = up * cos + low * sin
        ref[base + 8 : base + 16, :] = low * cos - up * sin
    else:
        ref[base : base + 8, :] = up * cos - low * sin
        ref[base + 8 : base + 16, :] = low * cos + up * sin


def mask_rows(bias, short, rows):
    for start in range(0, rows, 128):
        row = lax.broadcasted_iota(jnp.int32, (128, rows), 0) + start
        col = lax.broadcasted_iota(jnp.int32, (128, rows), 1)
        first = jnp.where(short == 1, start, 0)
        bias[start : start + 128, :] = jnp.where((col >= first) & (col <= row), 0.0, masked_score)


def one_row(block, index):
    rows = lax.broadcasted_iota(jnp.int32, block.shape, 0)
    return jnp.sum(jnp.where(rows == index, block, 0.0), axis=0, keepdims=True)


def prepare_kernel(info, up_0, up_1, dup_0, dup_1, down, ddown, qkv, dqkv, out_w, dout_w, vec, dvec, uwt, dwt, bias_u, wat, oat, bias_a, turn, turn_h):
    j = pl.program_id(0)
    device = info[0]
    row = lax.broadcasted_iota(jnp.int32, (48, 128), 0) + (device * 48) % 128
    lane = lax.broadcasted_iota(jnp.int32, (48, 128), 1)
    pick_0, pick_1 = (lane == row).astype(bf16), (lane == row - 128).astype(bf16)
    for part, (first, second, below, bias) in enumerate(((up_0, up_1, down, vec), (dup_0, dup_1, ddown, dvec))):
        uwt[part, 0] = (dot_nt(pick_0, first[...]) + dot_nt(pick_1, second[...])).astype(bf16)
        dwt[part, 0] = below[...]
        line = one_row(bias[8:12, pl.ds(pl.multiple_of(384 * (j % 2), 128), 384)], j // 2)
        turn[...] = jnp.transpose(jnp.broadcast_to(line, (128, 384)))
        bias_u[part, 0] = turn[pl.ds(pl.multiple_of(device * 48, 16), 48), :]

    @pl.when(j < 6)
    def _():
        head = info[1 + j // 3]
        row = lax.broadcasted_iota(jnp.int32, (64, 128), 0) + (head % 2) * 64
        pick = (lax.broadcasted_iota(jnp.int32, (64, 128), 1) == row).astype(bf16)
        rows, drows = dot_nt(pick, qkv[...]).astype(bf16), dot_nt(pick, dqkv[...]).astype(bf16)
        wat[:, :768] = drows
        wat[:, 768:] = rows
        oat[:64, :] = out_w[...]
        oat[64:, :] = dout_w[...]
        for part, bias in enumerate((vec, dvec)):
            line = one_row(bias[4:7, pl.ds(pl.multiple_of(128 * (head // 2), 128), 128)], j % 3)
            turn_h[...] = jnp.transpose(jnp.broadcast_to(line, (128, 128)))
            bias_a[part * 64 : part * 64 + 64, :] = turn_h[pl.ds(pl.multiple_of((head % 2) * 64, 64), 64), :]


def prepare(info, qkv, dqkv, out_w, dout_w, up, dup, down, ddown, vec, dvec):
    def at_head(i):
        return jnp.minimum(i, 5)

    whole = pl.BlockSpec(memory_space=pltpu.VMEM)
    up_0 = pl.BlockSpec((768, 128), lambda i, info: (0, 3 * i + (info[0] * 48) // 128))
    up_1 = pl.BlockSpec((768, 128), lambda i, info: (0, 3 * i + jnp.minimum((info[0] * 48) // 128 + 1, 2)))
    down_spec = pl.BlockSpec((48, 768), lambda i, info: (8 * i + info[0], 0))
    qkv_spec = pl.BlockSpec((768, 128), lambda i, info: (0, 6 * (at_head(i) % 3) + info[1 + at_head(i) // 3] // 2))
    out_spec = pl.BlockSpec((64, 768), lambda i, info: (info[1 + at_head(i) // 3], 0))
    uwt, dwt, bias_u, wat, oat, bias_a = pl.pallas_call(
        prepare_kernel,
        out_shape=[
            jax.ShapeDtypeStruct((2, 8, 48, 768), bf16),
            jax.ShapeDtypeStruct((2, 8, 48, 768), bf16),
            jax.ShapeDtypeStruct((2, 8, 48, 128), f32),
            jax.ShapeDtypeStruct((384, 1536), bf16),
            jax.ShapeDtypeStruct((256, 768), bf16),
            jax.ShapeDtypeStruct((768, 128), f32),
        ],
        grid_spec=pltpu.PrefetchScalarGridSpec(
            num_scalar_prefetch=1,
            grid=(8,),
            in_specs=[up_0, up_1, up_0, up_1, down_spec, down_spec, qkv_spec, qkv_spec, out_spec, out_spec, whole, whole],
            out_specs=[
                pl.BlockSpec((2, 1, 48, 768), lambda i, info: (0, i, 0, 0)),
                pl.BlockSpec((2, 1, 48, 768), lambda i, info: (0, i, 0, 0)),
                pl.BlockSpec((2, 1, 48, 128), lambda i, info: (0, i, 0, 0)),
                pl.BlockSpec((64, 1536), lambda i, info: (at_head(i), 0)),
                pl.BlockSpec((128, 768), lambda i, info: (at_head(i) // 3, 0)),
                pl.BlockSpec((128, 128), lambda i, info: (at_head(i), 0)),
            ],
            scratch_shapes=[pltpu.VMEM((384, 128), f32), pltpu.VMEM((128, 128), f32)],
        ),
        compiler_params=pltpu.CompilerParams(vmem_limit_bytes=VMEM_SHARD),
        cost_estimate=pl.CostEstimate(flops=10**9, bytes_accessed=2 * 10**7, transcendentals=0),
        name="prepare",
    )(info, *(in_hbm(value) for value in (up, up, dup, dup, down, ddown, qkv, dqkv, out_w, dout_w)), vec, dvec)
    return (uwt.reshape(768, 768), dwt.reshape(768, 768), bias_u.reshape(768, 128), wat, oat, bias_a)


def outgoing_kernel(info, tokens, cotangent, out):
    def rows_of(i, carry):
        rows = pl.ds(pl.multiple_of(i * 128, 128), 128)
        out[rows, :768] = normalize(tokens[rows, :].astype(f32))[0]
        out[rows, 768:] = cotangent[rows, :].astype(f32)
        return carry

    lax.fori_loop(0, 2, rows_of, 0)


def outgoing(info, tokens, cotangent):
    half = pl.BlockSpec((256, 768), lambda i, info: (info[3], 0))
    return pl.pallas_call(
        outgoing_kernel,
        out_shape=jax.ShapeDtypeStruct((256, 1536), f32),
        grid_spec=pltpu.PrefetchScalarGridSpec(
            num_scalar_prefetch=1,
            grid=(1,),
            in_specs=[half, half],
            out_specs=pl.BlockSpec((256, 1536), lambda i, info: (0, 0)),
        ),
        compiler_params=pltpu.CompilerParams(vmem_limit_bytes=VMEM_SHARD),
        cost_estimate=pl.CostEstimate(flops=10**6, bytes_accessed=3 * 10**6, transcendentals=0),
        name="outgoing",
    )(info, in_hbm(tokens), in_hbm(cotangent))


def wide(column):
    return jnp.concatenate([column] * 4, axis=1)


def shard_kernel(plan, first, parts, slot_dev, *refs):
    refs = list(refs)
    with_heads, with_mlp, with_finish = parts != "close", parts != "heads", parts == "close"
    info, seq_device, seq_length = refs[:3]
    refs = refs[3:]
    owner = refs.pop(0) if with_finish else None
    steps = len(plan)
    data_h = refs[: 2 * steps]
    refs = refs[2 * steps :]
    vec, dvec, cos_ref, sin_ref = refs[:4]
    weights_h = refs[4:10]
    refs = refs[10:]
    old_h = None if first else refs[:4]
    refs = refs if first else refs[4:]
    if with_finish:
        out_sum, curve, grad, sums_out = refs[0], refs[1], refs[2], refs[3]
        out_h = (None,) * 4
    else:
        out_h = refs[:4]
        border = refs[4] if parts == "heads" else None
        refs = refs[:4] + refs[5:] if parts == "heads" else refs
    (mine, other, wat, bias_a, oat, uwt, dwt, bias_u, acc_h, acc_m, acc_c, acc_r, sem) = refs[4:17]
    (nb, nb_low, ones, lhs_a, ml, dm, dm_low, cb, mask, proj, gat, qt, kt, k4, vt, v4, gt, q4, g4, gq, gk, gv, head_g, head_a, hid, act, mlp_a, mlp_g, one, two) = refs[17:]
    new = (acc_h, acc_m, acc_c, acc_r)
    step = pl.program_id(0)
    core = info[3]
    most = max(heads for _, heads in plan)

    def by_step(values):
        result = jnp.int32(values[0])
        for i, value in enumerate(values[1:]):
            result = jnp.where(step > i, value, result)
        return result

    heads_now = by_step([heads for _, heads in plan])
    short = is_short(seq_device, seq_length, info[8 + by_step([index for index, _ in plan])], 512)
    width = 768
    gain_a, shift_a, gain_m, shift_m = (vec[i : i + 1, :] for i in range(4))
    dgain_a, dshift_a, dgain_m, dshift_m = (dvec[i : i + 1, :] for i in range(4))
    wat_h, bias_ah, oat_h, uwt_h, dwt_h, bias_uh = weights_h
    lead = most * 384
    pairs = [(data_h[0], mine.at[0]), (data_h[1], other.at[0])]
    pairs += [(uwt_h, uwt), (dwt_h, dwt), (bias_uh, bias_u)] if with_mlp else []
    for_mlp = range(2, len(pairs))
    held = 2 if with_finish else most
    pairs += [(wat_h.at[: held * 192], wat), (oat_h.at[: held * 128], oat)]
    pairs += [(bias_ah.at[:lead], bias_a)] if with_heads else []
    for_heads = range(for_mlp.stop, len(pairs))
    if not first:
        pairs += [(old_h[1], acc_m)] if with_mlp else []
        pairs += [(old_h[2], acc_c), (old_h[3], acc_r)]
    for_sums = range(for_heads.stop, len(pairs))
    if not first:
        pairs += [(old_h[0].at[: held * 512], acc_h)]
    for_tiles = range(for_sums.stop, len(pairs))
    base_count = len(pairs)
    for i in range(1, steps):
        pairs += [(data_h[2 * i], mine.at[i]), (data_h[2 * i + 1], other.at[i])]
    arrivals = [pltpu.make_async_copy(source, target, sem.at[i]) for i, (source, target) in enumerate(pairs)]

    def at_step(which):
        if steps == 1:
            return lambda body: body()
        return pl.when(step == which)

    @at_step(0)
    def _():
        for copy in arrivals:
            copy.start()

    def arrived(*which):
        @at_step(0)
        def _():
            for i in which:
                if i < base_count:
                    arrivals[i].wait()

    ones[...] = jnp.ones((512, 128), bf16)
    if with_heads:
        mask_rows(mask, short, 512)

    def load(ref, cot_ref, base, count):
        def rows_of(i, carry):
            src = pl.ds(pl.multiple_of(i * 128, 128), 128)
            dst = pl.ds(pl.multiple_of(base + i * 128, 128), 128)
            rows = ref[step, src, :width].astype(f32)
            normed = normalize(rows)[0] if first else rows
            nb[dst, :], nb_low[dst, :] = split_two(normed)
            if with_heads:
                lhs_a[dst, :width] = (normed * gain_a + shift_a).astype(bf16)
                lhs_a[dst, width : 2 * width], lhs_a[dst, 2 * width :] = split_two(normed * dgain_a + dshift_a)
            if with_mlp:
                ml[dst, :] = (normed * gain_m + shift_m).astype(bf16)
                dm[dst, :], dm_low[dst, :] = split_two(normed * dgain_m + dshift_m)
            cb[dst, :] = cot_ref[step, src, :].astype(bf16)
            return carry

        lax.fori_loop(0, count, rows_of, 0)

    if first:
        arrived(0, 1)
        load(mine, other, 0, 4)
    else:
        arrived(0)
        for i in range(1, steps):

            @at_step(i)
            def _(i=i):
                arrivals[base_count + 2 * i - 2].wait()
                arrivals[base_count + 2 * i - 1].wait()

        load(mine, mine.at[:, :, width:], core * 256, 2)
        arrived(1)
        load(other, other.at[:, :, width:], (1 - core) * 256, 2)

    def add(ref, rows, value):
        ref[rows, :] = value if first else ref[rows, :] + value

    def eight(value):
        rows, columns = value.shape
        return jnp.sum(value.reshape(rows // 8, 8, columns), axis=0)

    def fold(carry, ref, at, tops, w_rows, dw_rows, dgain, dshift, c_rows):
        grad_at, curve_at = at
        top, low = tops
        p_two, q_two = two[top, :], two[low, :]
        add(ref, grad_at, one[top, :])
        moved = dgain * p_two + dshift * c_rows
        add(ref, curve_at, one[low, :] + moved)
        w_wide, dw_wide = w_rows.astype(f32), dw_rows.astype(f32)
        drift, plain, dots = carry
        drift = drift + eight(w_wide * q_two + dw_wide * p_two)
        plain = plain + eight(w_wide * p_two)
        dots = dots + eight(dw_wide * (2.0 * moved))
        return (drift, plain, dots)

    blank = jnp.zeros((8, width), f32)
    if with_mlp:
        arrived(*for_mlp)
        hid[...] = dot_nt(uwt[...], ml[...])
        act[...] = dot_nt(dwt[...], cb[...])
        hid[384:, :] += dot_nt(uwt[:384, :], dm[...]) + dot_nt(uwt[:384, :], dm_low[...])

        def gelu(i, carry):
            top = pl.ds(pl.multiple_of(i * 32, 32), 32)
            low = pl.ds(pl.multiple_of(384 + i * 32, 32), 32)
            hidden, dhidden = hid[top, :] + wide(bias_u[top, :]), hid[low, :] + wide(bias_u[low, :])
            grad_act, dgrad_act = act[top, :], act[low, :]
            cumulative = 0.5 * (1.0 + lax.erf(hidden * root_half))
            density = jnp.exp(-0.5 * hidden * hidden) * density_scale
            slope = cumulative + hidden * density
            bend = density * (2.0 - hidden * hidden)
            drift_act = slope * dhidden
            drift_grad = dgrad_act * slope + grad_act * bend * dhidden
            mlp_a[top, :] = (hidden * cumulative).astype(bf16)
            mlp_a[low, :] = drift_act.astype(bf16)
            mlp_g[top, :] = (grad_act * slope).astype(bf16)
            mlp_g[low, :] = drift_grad.astype(bf16)
            return carry + eight(drift_grad * dhidden + drift_act * dgrad_act)

        dots_m = lax.fori_loop(0, 12, gelu, jnp.zeros((8, 512), f32))
        one[...] = dot_nn(mlp_g[...], ml[...])
        two[...] = dot_nn(mlp_g[...], nb[...])
        two[:384, :] += dot_nn(mlp_g[:384, :], nb_low[...])
        sums = dot_nn(mlp_g[...], ones[...])
        arrived(*for_sums)
        add(acc_c, slice(768, 1536), sums)
        proj[0:384, 0:128] = sums[:384, :]

        def fold_m(i, carry):
            top = pl.ds(pl.multiple_of(i * 64, 64), 64)
            low = pl.ds(pl.multiple_of(384 + i * 64, 64), 64)
            return fold(carry, acc_m, (top, low), (top, low), uwt[top, :], uwt[low, :], dgain_m, dshift_m, proj[top, 0:1])

        carry_m = (blank, blank, blank) if first else (acc_r[8:16, :], acc_r[24:32, :], acc_r[32:40, :])
        acc_r[8:16, :], acc_r[24:32, :], acc_r[32:40, :] = lax.fori_loop(0, 6, fold_m, carry_m)
        acc_r[32:40, :512] += dots_m
        one[...] = dot_nn(mlp_a[...], cb[...])
        add(acc_m, slice(768, 1536), one[...])
        if with_finish:
            arrived(*for_heads, *for_tiles)
            finish_kernel(slot_dev, owner, info, acc_h, acc_m, acc_c, acc_r, wat, oat, uwt, dwt, out_sum, curve, grad, sums_out)
            return
        leave_m = pltpu.make_async_copy(acc_m, out_h[1], sem.at[0])

        @at_step(steps - 1)
        def _():
            leave_m.start()

    if not with_mlp:
        arrived(*for_sums)
    arrived(*for_heads, *for_tiles)
    cos, sin = cos_ref[short], sin_ref[short]

    def attend(head, carry):
        base = pl.multiple_of(head * 384, 128)
        w_at = pl.ds(pl.multiple_of(head * 192, 64), 192)
        plain = dot_nt(wat[w_at, width:], lhs_a[:, :width])
        drift = dot_nt(wat[w_at, :], lhs_a[:, : 2 * width]) + dot_nt(wat[w_at, width:], lhs_a[:, 2 * width :])
        for kind in range(3):
            proj[kind * 128 : kind * 128 + 64, :] = plain[kind * 64 : kind * 64 + 64, :]
            proj[kind * 128 + 64 : kind * 128 + 128, :] = drift[kind * 64 : kind * 64 + 64, :]
        proj[...] += wide(bias_a[pl.ds(base, 384), :])
        gat[...] = dot_nt(oat[pl.ds(pl.multiple_of(head * 128, 128), 128), :], cb[...])
        for part in (0, 64, 128, 192):
            rotate_rows(proj, part, cos, sin, False)
        proj[0:128, :] = proj[0:128, :] * 0.125
        rests = []
        for source, flat, tall, back in ((proj.at[0:128], qt, q4, True), (proj.at[128:256], kt, k4, False), (proj.at[256:384], vt, v4, False), (gat, gt, g4, True)):
            own, moved = source[0:64, :], source[64:128, :]
            flat[0:64, :] = own.astype(bf16)
            high, low = split_two(moved)
            flat[64:128, :] = high
            if back:
                low_wide = low.astype(f32)
                rests.append(low_wide)
                tall[...] = jnp.transpose(jnp.concatenate([own, own, high.astype(f32), low_wide], axis=0)).astype(bf16)
            else:
                tall[0:64, :] = high
                tall[64:128, :] = low
                tall[128:192, :] = flat[0:64, :]
                tall[192:256, :] = flat[0:64, :]
        rest_q, rest_g = rests
        for block in range(2):
            rows = slice(block * 256, block * 256 + 256)
            span = block * 256 + 256
            scores = dot_nn(q4[rows, :64], kt[:64, :span]) + mask[rows, :span]
            dscores = dot_nn(q4[rows, :], k4[:, :span])
            exp_scores = jnp.exp(scores - jnp.max(scores, axis=1, keepdims=True))
            probs = exp_scores * (1.0 / jnp.sum(exp_scores, axis=1, keepdims=True))
            dprobs = probs * (dscores - jnp.sum(probs * dscores, axis=1, keepdims=True))
            probs_low, dprobs_low = probs.astype(bf16), dprobs.astype(bf16)
            grad_probs = dot_nn(g4[rows, :64], vt[:64, :span])
            dgrad_probs = dot_nn(g4[rows, :], v4[:, :span])
            centre = jnp.sum(probs * grad_probs, axis=1, keepdims=True)
            dcentre = jnp.sum(dprobs * grad_probs + probs * dgrad_probs, axis=1, keepdims=True)
            rest = grad_probs - centre
            g_scores = (probs * rest).astype(bf16)
            dg_wide = dprobs * rest + probs * (dgrad_probs - dcentre)
            dg_scores = dg_wide.astype(bf16)
            acc_r[32:40, :span] += eight(dprobs * dgrad_probs + dg_wide * dscores)
            out = dot_nt(vt[:, :span], probs_low)
            head_a[0:64, rows] = out[:64, :].astype(bf16)
            head_a[64:128, rows] = (out[64:, :] + dot_nt(vt[:64, :span], dprobs_low)).astype(bf16)
            part_q = dot_nt(kt[:, :span], g_scores)
            acc_r[32:40, rows] += 2.0 * eight(rest_g[:, rows] * out[64:, :] + rest_q[:, rows] * part_q[64:, :])
            gq[:, rows] = part_q * 0.125
            gq[64:, rows] += dot_nt(kt[:64, :span], dg_scores) * 0.125
            part_v = dot_nn(gt[:, rows], probs_low)
            part_dv = dot_nn(gt[:64, rows], dprobs_low)
            part_k = dot_nn(qt[:, rows], g_scores)
            part_dk = dot_nn(qt[:64, rows], dg_scores)
            acc_r[32:40, :span] += 2.0 * eight(proj[320:384, :span] * part_v[64:, :] + proj[192:256, :span] * part_k[64:, :])
            if block == 0:
                gv[:, :span] = part_v
                gk[:, :span] = part_k
                gv[:, span:] = jnp.zeros((128, 512 - span), f32)
                gk[:, span:] = jnp.zeros((128, 512 - span), f32)
            else:
                gv[:, :span] += part_v
                gk[:, :span] += part_k
            gv[64:, :span] += part_dv
            gk[64:, :span] += part_dk
        for part in (0, 64):
            rotate_rows(gq, part, cos, sin, True)
            rotate_rows(gk, part, cos, sin, True)
        for kind, grad in enumerate((gq, gk, gv)):
            head_g[kind * 64 : kind * 64 + 64, :] = grad[:64, :].astype(bf16)
            head_g[192 + kind * 64 : 256 + kind * 64, :] = grad[64:, :].astype(bf16)
        one[:384, :] = dot_nn(head_g[...], lhs_a[:, :width])
        two[:384, :] = dot_nn(head_g[...], nb[...])
        two[:192, :] += dot_nn(head_g[:192, :], nb_low[...])
        sums = dot_nn(head_g[...], ones[...])
        add(acc_c, pl.ds(base, 384), sums)
        for kind in range(3):
            at = pl.multiple_of(head * 512 + kind * 128, 128)
            top, low = slice(kind * 64, kind * 64 + 64), slice(192 + kind * 64, 256 + kind * 64)
            w_rows = pl.ds(pl.multiple_of(head * 192 + kind * 64, 64), 64)
            carry = fold(
                carry, acc_h, (pl.ds(at, 64), pl.ds(at + 64, 64)), (top, low),
                wat[w_rows, width:], wat[w_rows, :width], dgain_a, dshift_a, sums[top, 0:1],
            )
        add(acc_h, pl.ds(pl.multiple_of(head * 512 + 384, 128), 128), dot_nn(head_a[...], cb[...]))
        return carry

    carry_r = (blank, blank, blank) if first else (acc_r[0:8, :], acc_r[16:24, :], blank)
    if most == 1:
        carry_r = attend(0, carry_r)
    else:
        carry_r = lax.fori_loop(0, heads_now, attend, carry_r)
    acc_r[0:8, :], acc_r[16:24, :] = carry_r[:2]
    acc_r[32:40, :] += carry_r[2]
    if parts == "heads":
        for index in range(8):
            border[index] = acc_h[index * 64 + 48 : index * 64 + 64, :]
    leaves = [
        pltpu.make_async_copy(acc_c, out_h[2], sem.at[1]),
        pltpu.make_async_copy(acc_r, out_h[3], sem.at[2]),
        pltpu.make_async_copy(acc_h.at[: most * 512], out_h[0].at[: most * 512], sem.at[3]),
    ]

    @at_step(steps - 1)
    def _():
        for copy in leaves:
            copy.start()
        if with_mlp:
            leave_m.wait()
        for copy in leaves:
            copy.wait()


def shard_steps(plan, scalars, data, shared, tables, old, parts="both", close=None):
    first = old is None
    sizes = [(1024, 768), (1536, 768), (1536, 128), (40, 768)]
    steps = len(plan)
    most = max(heads for _, heads in plan)
    whole = pl.BlockSpec(memory_space=pltpu.VMEM)
    there = pl.BlockSpec(memory_space=pltpu.HBM)
    specs = [pl.BlockSpec(memory_space=pl.ANY)] * (2 * steps) + [whole] * 4 + [there] * 6
    vec, dvec, wat, bias_a, oat, uwt, dwt, bias_u = shared
    operands = [*data, vec, dvec, *tables, wat, bias_a, oat, uwt, dwt, bias_u]
    aliases = {}
    if not first:
        aliases = {3 + len(operands) + i: i for i in range(len(sizes))}
        specs += [there] * len(sizes)
        operands += list(old)
    held = most
    outs, out_specs, slot_dev = sizes, [there] * len(sizes), None
    if parts == "close":
        owners, slot_dev, out_sum = close
        held, aliases, scalars = 2, {}, (*scalars, owners)
        specs.append(whole)
        operands.append(out_sum)
        outs, out_specs = [(8 * slot_dev, 48, 384), (4 * slot_dev, 24, 384), (32, 768)], [whole] * 3
    if parts == "heads":
        outs, out_specs = sizes + [(8, 16, 768)], out_specs + [whole]
    scratch = [((steps, *data[0].shape), data[0].dtype), ((steps, *data[1].shape), data[1].dtype)]
    scratch += [((held * 192, 1536), bf16), ((most * 384, 128), f32), ((held * 128, 768), bf16)]
    scratch += [((768, 768), bf16)] * 2 + [((768, 128), f32)]
    scratch += [((held * 512, 768), f32)] + [(size, f32) for size in sizes[1:]] + [None]
    scratch += [
        ((512, 768), bf16),
        ((512, 768), bf16),
        ((512, 128), bf16),
        ((512, 2304), bf16),
        ((512, 768), bf16),
        ((512, 768), bf16),
        ((512, 768), bf16),
        ((512, 768), bf16),
        ((512, 512), f32),
        ((384, 512), f32),
        ((128, 512), f32),
    ]
    flat, tall, back = ((128, 512), bf16), ((256, 512), bf16), ((512, 256), bf16)
    scratch += [flat, flat, tall, flat, tall, flat, back, back] + [((128, 512), f32)] * 3
    scratch += [((384, 512), bf16), ((128, 512), bf16)]
    scratch += [((768, 512), f32)] * 2 + [((768, 512), bf16)] * 2 + [((768, 768), f32)] * 2
    return pl.pallas_call(
        lambda *refs: shard_kernel(plan, first, parts, slot_dev, *refs),
        out_shape=[jax.ShapeDtypeStruct(size, f32) for size in outs],
        grid_spec=pltpu.PrefetchScalarGridSpec(
            num_scalar_prefetch=len(scalars),
            grid=(steps,),
            in_specs=specs,
            out_specs=out_specs,
            scratch_shapes=[pltpu.SemaphoreType.DMA((16,)) if one is None else pltpu.VMEM(*one) for one in scratch],
        ),
        input_output_aliases=aliases,
        compiler_params=pltpu.CompilerParams(vmem_limit_bytes=VMEM_SHARD),
        cost_estimate=pl.CostEstimate(
            flops=sum(heads * 2 * 10**9 + 5 * 10**9 for _, heads in plan), bytes_accessed=2 * 10**7, transcendentals=10**6
        ),
        name="shards_" + parts + "".join(str(heads) for _, heads in plan),
    )(*scalars, *operands)


def put_tile(slot_dev, owner, y, tile, curve, grad, curve_rows, grad_rows):
    group = slot_dev // 2
    slot = owner[tile]
    curve_rows(curve.at[slot])
    home, place = slot // slot_dev, slot % slot_dev

    @pl.when(place // group == y)
    def _():
        grad_rows(grad.at[home * group + place % group])


def tile_at(kind, side):
    return (side * 6 + 2 * kind, 1) if kind < 3 else (12 + side, 2)


def finish_kernel(slot_dev, owner, info, acc_h, acc_m, acc_c, acc_r, wat, oat, uwt, dwt, out_sum, curve, grad, sums):
    core, y, odd = info[3], info[5], info[6]
    if slot_dev * 8 > 48:
        curve[...] = jnp.zeros(curve.shape, f32)
        grad[...] = jnp.zeros(grad.shape, f32)

    def put(tile, columns, source, curve_at, grad_at):
        def curve_rows(ref):
            ref[...] = source[curve_at : curve_at + 48, columns]

        def grad_rows(ref):
            ref[...] = source[pl.ds(pl.multiple_of(grad_at + core * 24, 8), 24), columns]

        put_tile(slot_dev, owner, y, tile, curve, grad, curve_rows, grad_rows)

    for side in range(2):
        columns = slice(side * 384, side * 384 + 384)
        for kind in range(4):
            lower, step = tile_at(kind, side)
            put(lower + odd * step, columns, acc_h, kind * 128 + 64, kind * 128)
        for block in range(8):
            at = block * 48
            put(16 + side * 8 + block, columns, acc_m, 384 + at, at)
            put(32 + block * 2 + side, columns, acc_m, 1152 + at, 768 + at)
    small_sums_kernel(info, acc_h, acc_m, acc_c, acc_r, wat, oat, uwt, dwt, out_sum, sums)


def finish_split_kernel(slot_dev, owner, info, own_b, far_b, extra, old_curve, old_grad, curve, grad, new_curve, new_grad, near_b, sem):
    core, x, y, odd = info[3], info[4], info[5], info[6]
    group = slot_dev // 2
    for index in range(8):
        near_b[index] = far_b[index] + own_b[0, pl.ds(pl.multiple_of(index * 64 + x * 32, 32), 32), :]
    copies, later = [], []
    for kind in range(4):
        for side in range(2):
            columns = slice(side * 384, side * 384 + 384)
            lower, step = tile_at(kind, side)
            slot = owner[lower + (1 - odd) * step]
            place = kind * 2 + side
            new_curve[place, 0:32, :] = near_b[kind * 2 + 1, :, columns]
            new_curve[place, 32:48, :] = extra[kind * 2 + 1, :, columns]
            copy = pltpu.make_async_copy(new_curve.at[place], curve.at[slot], sem.at[place])
            copy.start()
            copies.append(copy)

            @pl.when(core == 0)
            def _(place=place, kind=kind, columns=columns):
                new_grad[place] = near_b[kind * 2, 0:24, columns]

            @pl.when(core == 1)
            def _(place=place, kind=kind, columns=columns):
                new_grad[place, 0:8, :] = near_b[kind * 2, 24:32, columns]
                new_grad[place, 8:24, :] = extra[kind * 2, :, columns]

            home, spot = slot // slot_dev, slot % slot_dev

            @pl.when(spot // group == y)
            def _(place=place, home=home, spot=spot):
                pltpu.make_async_copy(new_grad.at[place], grad.at[home * group + spot % group], sem.at[8 + place]).start()

            later.append((place, home * group + spot % group, spot // group == y))

    for copy in copies:
        copy.wait()
    for place, target, mine in later:

        @pl.when(mine)
        def _(place=place, target=target):
            pltpu.make_async_copy(new_grad.at[place], grad.at[target], sem.at[8 + place]).wait()


def finish_split(owners, info, slot_dev, acc_h, near_b, extra, curve, grad):
    whole = pl.BlockSpec(memory_space=pltpu.VMEM)
    there = pl.BlockSpec(memory_space=pltpu.HBM)
    return pl.pallas_call(
        lambda *refs: finish_split_kernel(slot_dev, *refs),
        out_shape=[jax.ShapeDtypeStruct(curve.shape, f32), jax.ShapeDtypeStruct(grad.shape, f32)],
        grid_spec=pltpu.PrefetchScalarGridSpec(
            num_scalar_prefetch=2,
            grid=(1,),
            in_specs=[pl.BlockSpec((1, 512, 768), lambda i, *scalars: (1, 0, 0))] + [whole] * 2 + [there] * 2,
            out_specs=[there] * 2,
            scratch_shapes=[
                pltpu.VMEM((8, 48, 384), f32),
                pltpu.VMEM((8, 24, 384), f32),
                pltpu.VMEM((8, 32, 768), f32),
                pltpu.SemaphoreType.DMA((16,)),
            ],
        ),
        input_output_aliases={5: 0, 6: 1},
        compiler_params=pltpu.CompilerParams(vmem_limit_bytes=VMEM_SHARD),
        cost_estimate=pl.CostEstimate(flops=0, bytes_accessed=5 * 10**6, transcendentals=0),
        name="finish_split",
    )(owners, info, acc_h.reshape(2, 512, 768), near_b, extra, curve, grad)


def own_attention_kernel(info, seq_device, seq_length, q_ref, k_ref, v_ref, g_ref, cos_ref, sin_ref, att, gq_out, gk_out, gv_out, mask, buf, gk, gv):
    short = is_short(seq_device, seq_length, info[0], 512)

    @pl.when(pl.program_id(0) == 0)
    def _():
        mask_rows(mask, short, 512)

    cos, sin = cos_ref[short], sin_ref[short]
    buf[...] = q_ref[...]
    rotate_rows(buf, 0, cos, sin, False)
    q_rows = buf[...] * 0.125
    qt = q_rows.astype(bf16)
    qn = jnp.transpose(q_rows).astype(bf16)
    buf[...] = k_ref[...]
    rotate_rows(buf, 0, cos, sin, False)
    kt = buf[...].astype(bf16)
    vt = v_ref[...].astype(bf16)
    gt = g_ref[...].astype(bf16)
    gn = jnp.transpose(g_ref[...]).astype(bf16)
    for block in range(2):
        rows = slice(block * 256, block * 256 + 256)
        wide = block * 256 + 256
        scores = dot_nn(qn[rows, :], kt[:, :wide]) + mask[rows, :wide]
        exp_scores = jnp.exp(scores - jnp.max(scores, axis=1, keepdims=True))
        probs = exp_scores * (1.0 / jnp.sum(exp_scores, axis=1, keepdims=True))
        probs_low = probs.astype(bf16)
        grad_probs = dot_nn(gn[rows, :], vt[:, :wide])
        weighted = probs * grad_probs
        g_scores = (weighted - probs * jnp.sum(weighted, axis=1, keepdims=True)).astype(bf16)
        att[:, rows] = dot_nt(vt[:, :wide], probs_low).astype(bf16)
        buf[:, rows] = dot_nt(kt[:, :wide], g_scores) * 0.125
        part_v = dot_nn(gt[:, rows], probs_low)
        part_k = dot_nn(qt[:, rows], g_scores)
        if block == 0:
            gv[:, :wide] = part_v
            gk[:, :wide] = part_k
            gv[:, wide:] = jnp.zeros((64, 512 - wide), f32)
            gk[:, wide:] = jnp.zeros((64, 512 - wide), f32)
        else:
            gv[:, :wide] += part_v
            gk[:, :wide] += part_k
    rotate_rows(buf, 0, cos, sin, True)
    rotate_rows(gk, 0, cos, sin, True)
    gq_out[...] = buf[...].astype(bf16)
    gk_out[...] = gk[...].astype(bf16)
    gv_out[...] = gv[...].astype(bf16)


def own_attention(scalars, mixed, grad_att, tables):
    def rows_at(offset):
        return pl.BlockSpec((64, 512), lambda i, *scalars: (offset + i, 0))

    whole = pl.BlockSpec(memory_space=pltpu.VMEM)
    return pl.pallas_call(
        own_attention_kernel,
        out_shape=[jax.ShapeDtypeStruct((768, 512), bf16)] * 4,
        grid_spec=pltpu.PrefetchScalarGridSpec(
            num_scalar_prefetch=3,
            grid=(12,),
            in_specs=[rows_at(0), rows_at(12), rows_at(24), rows_at(0), whole, whole],
            out_specs=[rows_at(0)] * 4,
            scratch_shapes=[pltpu.VMEM((512, 512), f32)] + [pltpu.VMEM((64, 512), f32)] * 3,
        ),
        compiler_params=pltpu.CompilerParams(vmem_limit_bytes=16 << 20),
        cost_estimate=pl.CostEstimate(flops=10**10, bytes_accessed=10**7, transcendentals=3 * 10**6),
        name="own_attention",
    )(*scalars, mixed, mixed, mixed, grad_att, *tables)


def lay_rows(table, slot, rows, out, buf):
    for source in range(8):
        for part in range(3):
            start = pl.multiple_of(table[slot, source * 3 + part], 16)
            buf[pl.ds(start, 16), :] = rows(source, part * 16)

    @pl.when(table[slot, 24] == 1)
    def _():
        out[0] = jnp.transpose(buf[...])

    @pl.when(table[slot, 24] == 0)
    def _():
        out[0] = buf[...]


def assemble_kernel(table, pieces, out, buf):
    lay_rows(table, pl.program_id(0), lambda source, at: pieces[source, 0, at : at + 16, :], out, buf)


def assemble(table, pieces):
    slots = pieces.shape[1]
    return pl.pallas_call(
        assemble_kernel,
        out_shape=jax.ShapeDtypeStruct((slots, 384, 384), f32),
        grid_spec=pltpu.PrefetchScalarGridSpec(
            num_scalar_prefetch=1,
            grid=(slots,),
            in_specs=[pl.BlockSpec((8, 1, 48, 384), lambda i, table: (0, i, 0, 0))],
            out_specs=pl.BlockSpec((1, 384, 384), lambda i, table: (i, 0, 0)),
            scratch_shapes=[pltpu.VMEM((384, 384), f32)],
        ),
        compiler_params=pltpu.CompilerParams(vmem_limit_bytes=16 << 20),
        cost_estimate=pl.CostEstimate(flops=0, bytes_accessed=8 * 10**6, transcendentals=0),
        name="assemble",
    )(table, pieces)


def split_two(value):
    high = value.astype(bf16)
    return (high, (value - high.astype(f32)).astype(bf16))


def dot_fine(left, right, dims):
    (a_high, a_low), (b_high, b_low) = left, right

    def dot(a, b):
        return lax.dot_general(a, b, (dims, ((), ())), preferred_element_type=f32)

    return dot(a_high, b_high) + (dot(a_high, b_low) + dot(a_low, b_high))


def update_kernel(table, info, tile, own, own_core, far, far_core, qkv, out_w, up, down, left, right, first, second, grad, new_first, new_second, new_weight, new_low, rows, buf):
    slot = pl.program_id(0)
    core, y = info[3], info[5]
    group = pl.num_programs(0) // 2

    def join(one, two):
        rows[:, pl.ds(pl.multiple_of(core * 24, 8), 24), :] = one[:, 0]
        rows[:, pl.ds(pl.multiple_of(24 - core * 24, 8), 24), :] = two[:, 0]

    @pl.when(slot // group == y)
    def _():
        join(own, own_core)

    @pl.when(slot // group != y)
    def _():
        join(far, far_core)

    lay_rows(table, slot, lambda source, at: rows[source, at : at + 16, :], grad, buf)
    index = tile[slot]

    def weight(low, high, ref):
        @pl.when((index >= low) & (index < high))
        def _():
            buf[...] = ref[...].astype(f32)

    weight(0, 12, qkv)
    weight(12, 16, out_w)
    weight(16, 32, up)
    weight(32, 48, down)
    used = jnp.where(index < 48, 1.0, 0.0)
    l_two, r_two = split_two(left[0]), split_two(right[0])
    turned = dot_fine(l_two, split_two(grad[0]), ((0,), (0,)))
    turned = dot_fine(split_two(turned), r_two, ((1,), (0,)))
    moment = beta_decay * first[0] + (1.0 - beta_decay) * turned
    square = beta_decay * second[0] + (1.0 - beta_decay) * turned * turned
    correction = 1.0 - beta_decay**STEP
    direction = moment / correction / (jnp.sqrt(square / correction) + adam_epsilon)
    new_first[0] = used * moment
    new_second[0] = used * square
    restored = dot_fine(l_two, split_two(direction), ((1,), (0,)))
    restored = dot_fine(split_two(restored), r_two, ((1,), (1,)))
    value = buf[...]
    value = jnp.where(index < 48, value - learning_rate * (restored + weight_decay * value), 0.0)
    new_weight[0] = value
    new_low[0] = value.astype(bf16)


def update(table, info, tile, pieces, weights, states):
    group = pieces[0].shape[1]
    slots = 2 * group
    piece = pl.BlockSpec((8, 1, 24, 384), lambda i, table, info, tile: (0, i % group, 0, 0))
    slab = pl.BlockSpec((1, 384, 384), lambda i, table, info, tile: (i, 0, 0))

    def spec(start, count, columns):
        def at(i, table, info, tile):
            local_tile = jnp.clip(tile[i] - start, 0, count - 1)
            return (local_tile // columns, local_tile % columns)

        return pl.BlockSpec((384, 384), at)

    kinds = [f32, f32, f32, f32, bf16]
    return pl.pallas_call(
        update_kernel,
        out_shape=[jax.ShapeDtypeStruct((slots, 384, 384), kind) for kind in kinds],
        grid_spec=pltpu.PrefetchScalarGridSpec(
            num_scalar_prefetch=3,
            grid=(slots,),
            in_specs=[piece] * 4 + [spec(0, 12, 6), spec(12, 4, 2), spec(16, 16, 8), spec(32, 16, 2)] + [slab] * 4,
            out_specs=[slab] * 5,
            scratch_shapes=[pltpu.VMEM((8, 48, 384), f32), pltpu.VMEM((384, 384), f32)],
        ),
        compiler_params=pltpu.CompilerParams(vmem_limit_bytes=32 << 20),
        cost_estimate=pl.CostEstimate(flops=10**10, bytes_accessed=4 * 10**7, transcendentals=10**6),
        name="update",
    )(table, info, tile, *pieces, *(in_hbm(value) for value in (*weights, *states)))


def small_sums_kernel(info, acc_h, acc_m, acc_c, acc_r, wat, oat, uwt, dwt, out_sum, out):
    device = info[0]
    out[...] = jnp.zeros((32, 768), f32)
    blank = jnp.zeros((8, 768), f32)
    along, curve = blank, acc_r[32:40, :]
    shift_a, shift_m, dshift_a, dshift_m = blank, blank, blank, blank

    def fold(value):
        return jnp.sum(value.reshape(value.shape[0] // 8, 8, 768), axis=0)

    for place in range(2):
        acc = acc_h.at[place * 512 : place * 512 + 512]
        head = info[1 + place]
        row = lax.broadcasted_iota(jnp.int32, (64, 128), 0) + (head % 2) * 64
        pick = lax.broadcasted_iota(jnp.int32, (64, 128), 1) == row
        for kind in range(4):
            at = kind * 128
            if kind < 3:
                base = place * 192 + kind * 64
                w_one, w_drift = wat[base : base + 64, 768:].astype(f32), wat[base : base + 64, :768].astype(f32)
                base = place * 384 + kind * 64
                p_col, q_col = acc_c[base : base + 64, :], acc_c[base + 192 : base + 256, :]
                shift_a += fold(w_one * p_col[:, 0:1])
                dshift_a += fold(w_one * q_col[:, 0:1] + w_drift * p_col[:, 0:1])
                lanes = pl.ds(pl.multiple_of(128 * (head // 2), 128), 128)
                out[4 + kind : 5 + kind, lanes] += jnp.sum(jnp.where(pick, p_col, 0.0), axis=0, keepdims=True)
                out[20 + kind : 21 + kind, lanes] += jnp.sum(jnp.where(pick, q_col, 0.0), axis=0, keepdims=True)
            else:
                w_drift = oat[place * 128 + 64 : place * 128 + 128, :].astype(f32)
            along += fold(acc[at : at + 64, :] * w_drift)
    row = lax.broadcasted_iota(jnp.int32, (48, 384), 0) + device * 48
    pick = lax.broadcasted_iota(jnp.int32, (48, 384), 1) == row
    for block in range(8):
        at = block * 48
        w_one, w_drift = uwt[at : at + 48, :].astype(f32), uwt[384 + at : 432 + at, :].astype(f32)
        d_drift = dwt[384 + at : 432 + at, :].astype(f32)
        p_col, q_col = acc_c[768 + at : 816 + at, 0:1], acc_c[1152 + at : 1200 + at, 0:1]
        shift_m += fold(w_one * p_col)
        dshift_m += fold(w_one * q_col + w_drift * p_col)
        along += fold(acc_m[at : at + 48, :] * w_drift) + fold(acc_m[768 + at : 816 + at, :] * d_drift)
        lanes = slice(384 * (block % 2), 384 * (block % 2) + 384)
        place = 8 + block // 2
        out[place : place + 1, lanes] = jnp.sum(jnp.where(pick, p_col, 0.0), axis=0, keepdims=True)
        out[16 + place : 17 + place, lanes] = jnp.sum(jnp.where(pick, q_col, 0.0), axis=0, keepdims=True)

    def row_sum(value):
        return jnp.sum(value, axis=0, keepdims=True)

    out[0:1, :] = row_sum(acc_r[16:24, :])
    out[1:2, :] = row_sum(shift_a)
    out[2:3, :] = row_sum(acc_r[24:32, :])
    out[3:4, :] = row_sum(shift_m)
    out[7:8, :] = out_sum[...]
    out[12:13, :] = out_sum[...]
    out[16:17, :] = row_sum(acc_r[0:8, :])
    out[17:18, :] = row_sum(dshift_a)
    out[18:19, :] = row_sum(acc_r[8:16, :])
    out[19:20, :] = row_sum(dshift_m)
    lane = lax.broadcasted_iota(jnp.int32, (1, 768), 1)
    out[29:30, :] = jnp.where(lane == 0, jnp.sum(along), jnp.where(lane == 1, jnp.sum(curve), 0.0))


def take_rows(matrix, start, size):
    return lax.dynamic_slice_in_dim(matrix, start, size, axis=0)


def piece_rows(index):
    z, x = index // 2, index % 2
    plain = [48 * index, 48 * index + 16, 48 * index + 32]
    full = [[64 * x + 16 * i for i in range(3)], [64 + 64 * x + 16 * i for i in range(3)]]
    full += [[192 + 64 * x + 16 * i for i in range(3)], [256 + 64 * x + 16 * i for i in range(3)]]
    split = [
        [32 * x, 32 * x + 16, 64 + 64 * x + 48],
        [128 + 32 * x, 144 + 32 * x, 64 * x + 48],
        [192 + 32 * x, 208 + 32 * x, 256 + 64 * x + 48],
        [320 + 32 * x, 336 + 32 * x, 192 + 64 * x + 48],
    ]
    even = z % 2 == 0
    return (full[z] if even else split[z], split[z] if even else full[z], plain)


def local_tp(
    tokens,
    cotangent,
    vec_params,
    qkv_weight,
    out_weight,
    up_weight,
    down_weight,
    probe_vec,
    probe_qkv,
    probe_out,
    probe_up,
    probe_down,
    seq_device,
    seq_length,
    owners,
    left_bases,
    right_bases,
    first_moment,
    second_moment,
    vec_first,
    vec_second,
):
    row_count, width = tokens.shape
    device = lax.axis_index("dp")
    z = device // 2
    probe = lax.axis_index("probe")
    x, y, core = device % 2, probe // 2, probe % 2
    info = lax.dynamic_index_in_dim(jnp.array(device_table(), jnp.int32), device * 4 + probe, 0, keepdims=False)
    scalars = (info, seq_device, seq_length)
    drift_vec, drift_qkv, drift_out = probe_vec[0], probe_qkv[0], probe_out[0]
    drift_up, drift_down = probe_up[0], probe_down[0]
    barrier = lax.optimization_barrier

    across = [(i, i ^ 1) for i in range(8)]
    outer = [(i, i ^ 2) for i in range(8)]
    middle = [(2, 4), (3, 5), (4, 2), (5, 3)]
    outward = [(2, 0), (3, 1), (4, 6), (5, 7)]
    swap_core = [(0, 1), (1, 0), (2, 3), (3, 2)]
    swap_y = [(0, 2), (2, 0), (1, 3), (3, 1)]

    def move(value, pairs):
        return lax.ppermute(value, "dp", pairs)

    def to_core(value):
        return lax.ppermute(value, "probe", swap_core)

    mine = outgoing(info, tokens, cotangent)
    near, centre, cross_0 = move(mine, outer), move(mine, middle), move(mine, across)
    inside = (z == 1) | (z == 2)

    row_index = jnp.arange(row_count, dtype=jnp.int32)
    half_rot = ROT // 2
    frequency = jnp.exp(jnp.arange(half_rot, dtype=f32) * (-2.0 * math.log(10000.0) / ROT))
    position = jnp.stack([row_index, row_index % (row_count // 4)])
    angles = position.astype(f32)[:, None, :] * frequency[None, :, None]
    tables = (jnp.cos(angles), jnp.sin(angles))

    flat_bias = vec_params[4:7].reshape(-1)
    uwt, dwt, bias_u, wat, oat, bias_a = prepare(
        info,
        qkv_weight, drift_qkv, out_weight, drift_out, up_weight, drift_up, down_weight, drift_down, vec_params, drift_vec,
    )
    shared = (vec_params, drift_vec, wat, bias_a, oat, uwt, dwt, bias_u)

    def step(plan, data, old, *how):
        return shard_steps(plan, scalars, data, shared, tables, old, *how)

    acc_h, acc_m, acc_c, acc_r = step(((0, 2),), (tokens, cotangent), None)
    (near, centre, cross_0, acc_r) = barrier((near, centre, cross_0, acc_r))
    edge, middle_near, cross_1 = move(centre, outward), move(near, middle), move(near, across)
    cross_0o, near_o = to_core(cross_0), to_core(near)
    acc_h, acc_m, acc_c, acc_r = step(((1, 2), (4, 1)), (near, near_o, cross_0, cross_0o), (acc_h, acc_m, acc_c, acc_r))

    (edge, middle_near, cross_1, acc_r) = barrier((edge, middle_near, cross_1, acc_r))
    second = jnp.where(inside, centre, edge)
    (middle_near, second) = barrier((middle_near, second))
    edge_far, cross_2 = move(middle_near, outward), move(second, across)
    second_o, cross_1o = to_core(second), to_core(cross_1)
    acc_h, acc_m, acc_c, acc_r = step(((2, 2), (5, 1)), (second, second_o, cross_1, cross_1o), (acc_h, acc_m, acc_c, acc_r))

    (edge_far, cross_2, acc_r) = barrier((edge_far, cross_2, acc_r))
    third = barrier(jnp.where(inside, middle_near, edge_far))
    cross_3, third_o, cross_2o = move(third, across), to_core(third), to_core(cross_2)
    acc_h, acc_m, acc_c, acc_r = step(((3, 2), (6, 1)), (third, third_o, cross_2, cross_2o), (acc_h, acc_m, acc_c, acc_r))
    sends = lax.dynamic_slice(acc_h.reshape(16, 64, width), (8, 32 - 32 * x, 0), (8, 32, width))
    near_b = move(sends, across)
    (tokens, cotangent, cross_3, acc_r) = barrier((tokens, cotangent, cross_3, acc_r))
    cross_3o = to_core(cross_3)
    inputs = tokens.astype(f32)
    cot_rows = cotangent.astype(f32)
    out_sum = jnp.sum(cot_rows, axis=0, keepdims=True)
    normed, norm_scale = normalize(inputs)
    attn_low = (normed * vec_params[0] + vec_params[1]).astype(bf16)
    mlp_low = (normed * vec_params[2] + vec_params[3]).astype(bf16)
    (cross_3, cross_3o, acc_r, attn_low, mlp_low) = barrier((cross_3, cross_3o, acc_r, attn_low, mlp_low))
    acc_h, acc_m, acc_c, acc_r, border = step(((7, 1),), (cross_3, cross_3o), (acc_h, acc_m, acc_c, acc_r), "heads")
    extra = move(border, [(i, i ^ 2) for i in range(8)])

    slot_dev = left_bases.shape[0]
    tile_index, occupied = slot_order(owners, slot_dev * 8)
    curve_slots, grad_slots, vec_all = step(
        ((7, 1),), (cross_3, cross_3o), (acc_h, acc_m, acc_c, acc_r), "close", (owners, slot_dev, out_sum)
    )
    vec_one = move(vec_all, [(i, i ^ 4) for i in range(8)])
    (extra, near_b, vec_all) = barrier((extra, near_b, vec_all))
    curve_slots, grad_slots = finish_split(owners, info, slot_dev, acc_h, near_b, extra, curve_slots, grad_slots)
    curve_slots = curve_slots.reshape(8, slot_dev, 48, 384)
    (attn_low, cotangent, grad_slots) = barrier((attn_low, cotangent, grad_slots))
    grad_slots = lax.all_to_all(grad_slots.reshape(8, slot_dev // 2, 24, 384), "dp", 0, 0)
    curve_slots = lax.all_to_all(curve_slots, "dp", 0, 0)
    mixed = product("kj,tk->jt", qkv_weight, attn_low) + flat_bias[:, None]
    grad_att = product("jk,tk->jt", out_weight, cotangent)
    (mixed, grad_att, vec_all, vec_one) = barrier((mixed, grad_att, vec_all, vec_one))
    vec_all = vec_all + vec_one
    vec_two = move(vec_all, [(i, i ^ 2) for i in range(8)])
    att_t, gq_t, gk_t, gv_t = own_attention(scalars, mixed, grad_att, tables)
    (vec_all, vec_two, att_t) = barrier((vec_all, vec_two, att_t))
    vec_all = vec_all + vec_two
    vec_four = move(vec_all, [(i, i ^ 1) for i in range(8)])

    (grad_slots, att_t, gq_t, gk_t, gv_t) = barrier((grad_slots, att_t, gq_t, gk_t, gv_t))
    far = lax.ppermute(grad_slots, "probe", swap_y)
    own_core = to_core(grad_slots)
    (mlp_low, cotangent, own_core, att_t, gq_t, gk_t, gv_t) = barrier((mlp_low, cotangent, own_core, att_t, gq_t, gk_t, gv_t))
    hidden = product("ij,jk->ik", mlp_low, up_weight) + vec_params[8:12].reshape(-1)
    cumulative = 0.5 * (1.0 + lax.erf(hidden * root_half))
    density = jnp.exp(-0.5 * hidden * hidden) * density_scale
    act_low = (hidden * cumulative).astype(bf16)
    grad_act = product("ij,kj->ik", cotangent, down_weight)
    grad_hidden_low = (grad_act * (cumulative + hidden * density)).astype(bf16)
    mlp_out = product("ij,jk->ik", act_low, down_weight) + vec_params[12]
    (mlp_out, far, grad_hidden_low, att_t) = barrier((mlp_out, far, grad_hidden_low, att_t))
    far_core = to_core(far)
    attn_out = product("jt,jk->tk", att_t, out_weight) + vec_params[7]
    block_output = (inputs + attn_out + mlp_out).astype(bf16)
    grad_mlp_in = product("ij,kj->ik", grad_hidden_low, up_weight)
    grad_attn_in = (
        product("jt,kj->tk", gq_t, qkv_weight[:, :width])
        + product("jt,kj->tk", gk_t, qkv_weight[:, width : 2 * width])
        + product("jt,kj->tk", gv_t, qkv_weight[:, 2 * width :])
    )
    grad_weighted = grad_attn_in * vec_params[0] + grad_mlp_in * vec_params[2]
    input_grad = cot_rows + norm_back(grad_weighted, normed, norm_scale)

    own_index = lax.dynamic_slice_in_dim(tile_index, device * slot_dev, slot_dev)
    kinds = [sum((piece_rows(i)[kind] for i in range(8)), []) for kind in range(3)]
    row_table = jnp.array(kinds, jnp.int32)
    in_qkv, in_out = own_index < 12, (own_index >= 12) & (own_index < 16)
    kind = jnp.where(in_qkv, own_index % 2, jnp.where(in_out, (own_index - 12) // 2, 2))
    turned = in_qkv | ((own_index >= 16) & (own_index < 32))
    table = jnp.concatenate([row_table[kind], turned.astype(jnp.int32)[:, None]], axis=1)
    (far_core, input_grad, block_output) = barrier((far_core, input_grad, block_output))
    own_grad, new_first, new_second, new_weights, new_weights_low = update(
        table,
        info,
        own_index,
        [grad_slots, own_core, far, far_core],
        [qkv_weight, out_weight, up_weight, down_weight],
        [left_bases, right_bases, first_moment, second_moment],
    )
    (vec_all, vec_four, new_first) = barrier((vec_all, vec_four, new_first))
    vec_all = vec_all + vec_four
    vec_total, vec_curve = vec_all[:13], vec_all[16:29]
    own_dots = jnp.stack(
        [vec_all[29, 0] + jnp.sum(vec_total * drift_vec), vec_all[29, 1]]
    )
    all_dots = jnp.where(jnp.arange(8)[:, None] == probe, jnp.pad(own_dots, (0, 126))[None], 0.0)
    all_dots = all_dots + to_core(all_dots)
    all_dots = all_dots + lax.ppermute(all_dots, "probe", swap_y)
    all_dots = all_dots[:4, :2]
    own_curve = assemble(table, curve_slots)
    vec_new_first, vec_new_second, vec_new = plain_adam(vec_total, vec_params, vec_first, vec_second)
    vector_state = jnp.stack([vec_total, vec_new_first], axis=0)
    return (
        block_output,
        input_grad,
        own_grad,
        new_first,
        new_second,
        new_weights,
        new_weights_low,
        own_curve[None],
        vector_state,
        vec_new_second,
        vec_new,
        vec_curve[None],
        all_dots,
    )


def solution(mesh):
    local = local_tp if fits_tp(mesh) else local_any
    return jax.shard_map(
        local,
        mesh=mesh,
        in_specs=(
            P("dp", None),
            P("dp", None),
            P(),
            P(),
            P(),
            P(),
            P(),
            P("probe", None, None),
            P("probe", None, None),
            P("probe", None, None),
            P("probe", None, None),
            P("probe", None, None),
            P(),
            P(),
            P(),
            P("dp", None, None),
            P("dp", None, None),
            P("dp", None, None),
            P("dp", None, None),
            P(),
            P(),
        ),
        out_specs=(
            P("dp", None),
            P("dp", None),
            P("dp", None, None),
            P("dp", None, None),
            P("dp", None, None),
            P("dp", None, None),
            P("dp", None, None),
            P("probe", "dp", None, None),
            P(),
            P(),
            P(),
            P("probe", None, None),
            P(),
        ),
        check_vma=False,
    )
```

```python
import math

import jax
import jax.numpy as jnp
from jax import lax
from jax.experimental import pallas as pl
from jax.experimental.pallas import tpu as pltpu
from jax.sharding import PartitionSpec as P

HEAD = 64
ROT = 16
BLK = 384
STEP = 4


beta_decay = 0.5
learning_rate = 0.05
weight_decay = 0.01
adam_epsilon = 1e-08
norm_epsilon = 1e-05
root_half = 0.7071067811865476
density_scale = 0.3989422804014327
masked_score = -1e30


def product(pattern, left_side, right_side):
    if left_side.dtype == jnp.bfloat16 and right_side.dtype == jnp.bfloat16:
        return jnp.einsum(pattern, left_side, right_side, preferred_element_type=jnp.float32)
    return jnp.einsum(
        pattern,
        left_side,
        right_side,
        precision=lax.Precision.HIGHEST,
        preferred_element_type=jnp.float32,
    )


def normalize(inputs):
    mean_row = jnp.mean(inputs, axis=1, keepdims=True)
    centred = inputs - mean_row
    variance = jnp.mean(centred * centred, axis=1, keepdims=True)
    norm_scale = lax.rsqrt(variance + norm_epsilon)
    return (centred * norm_scale, norm_scale)


def norm_back(grad_normed, normed, norm_scale):
    mean_grad = jnp.mean(grad_normed, axis=1, keepdims=True)
    mean_cross = jnp.mean(grad_normed * normed, axis=1, keepdims=True)
    return norm_scale * (grad_normed - mean_grad - normed * mean_cross)


def row_layout(device, seq_device, seq_length, row_count):
    present = (seq_device == device).astype(jnp.int32)
    taken_rows = present * seq_length
    start_row = jnp.cumsum(taken_rows) - taken_rows
    row_index = jnp.arange(row_count, dtype=jnp.int32)[:, None]
    inside = (
        (present[None, :] > 0)
        & (row_index >= start_row[None, :])
        & (row_index < (start_row + taken_rows)[None, :])
    ).astype(jnp.int32)
    number = jnp.arange(seq_device.shape[0], dtype=jnp.int32)
    segment = jnp.sum(inside * number[None, :], axis=1)
    position = jnp.sum(inside * (row_index - start_row[None, :]), axis=1)
    return (segment, position)


def rotary_table(position):
    half_rot = ROT // 2
    frequency = jnp.exp(jnp.arange(half_rot, dtype=jnp.float32) * (-2.0 * math.log(10000.0) / ROT))
    angles = position.astype(jnp.float32)[:, None] * frequency[None, :]
    return (jnp.cos(angles), jnp.sin(angles))


def rotate(values, cosine_table, sine_table, reverse):
    half_rot = cosine_table.shape[1]
    first_half = values[..., :half_rot]
    second = values[..., half_rot : 2 * half_rot]
    cos_wide = cosine_table[:, None, :]
    sin_wide = sine_table[:, None, :]
    if reverse:
        new_first = first_half * cos_wide + second * sin_wide
        new_second = second * cos_wide - first_half * sin_wide
    else:
        new_first = first_half * cos_wide - second * sin_wide
        new_second = second * cos_wide + first_half * sin_wide
    return jnp.concatenate([new_first, new_second, values[..., 2 * half_rot :]], axis=-1)


def swap_major(values):
    return jnp.transpose(values, (1, 0, 2))


def cut_tiles(matrix):
    height, span_cols = matrix.shape
    return (
        matrix.reshape(height // BLK, BLK, span_cols // BLK, BLK)
        .transpose(0, 2, 1, 3)
        .reshape(-1, BLK, BLK)
    )


def slot_order(owners, slot_total):
    slot_ids = jnp.arange(slot_total, dtype=jnp.int32)
    matches = owners[None, :] == slot_ids[:, None]
    tile_index = jnp.sum(
        jnp.where(matches, jnp.arange(owners.shape[0], dtype=jnp.int32)[None, :], 0), axis=1
    )
    occupied = jnp.any(matches, axis=1)
    return (jnp.where(occupied, tile_index, owners.shape[0]), occupied)


def arrange(blocks, tile_index):
    padded = jnp.concatenate([blocks, jnp.zeros((1,) + blocks.shape[1:], blocks.dtype)], axis=0)
    return jnp.take(padded, tile_index, axis=0)


def rotated_adam(gradient, weight, left_basis, right_basis, first_state, second_state, occupied):
    turned = jnp.einsum("sji,sjk->sik", left_basis, gradient, precision=lax.Precision.HIGHEST)
    turned = jnp.einsum("sik,skl->sil", turned, right_basis, precision=lax.Precision.HIGHEST)
    new_first = beta_decay * first_state + (1.0 - beta_decay) * turned
    new_second = beta_decay * second_state + (1.0 - beta_decay) * turned * turned
    correction = 1.0 - beta_decay**STEP
    direction = new_first / correction / (jnp.sqrt(new_second / correction) + adam_epsilon)
    restored = jnp.einsum("sij,sjk->sik", left_basis, direction, precision=lax.Precision.HIGHEST)
    restored = jnp.einsum("sik,slk->sil", restored, right_basis, precision=lax.Precision.HIGHEST)
    new_weight = weight - learning_rate * (restored + weight_decay * weight)
    slot_mask = occupied.astype(jnp.float32)[:, None, None]
    return (slot_mask * new_first, slot_mask * new_second, slot_mask * new_weight)


def plain_adam(gradient, value_rows, first_state, second_state):
    new_first = beta_decay * first_state + (1.0 - beta_decay) * gradient
    new_second = beta_decay * second_state + (1.0 - beta_decay) * gradient * gradient
    correction = 1.0 - beta_decay**STEP
    new_value = value_rows - learning_rate * (new_first / correction) / (
        jnp.sqrt(new_second / correction) + adam_epsilon
    )
    return (new_first, new_second, new_value)


def local_any(
    tokens,
    cotangent,
    vec_params,
    qkv_weight,
    out_weight,
    up_weight,
    down_weight,
    probe_vec,
    probe_qkv,
    probe_out,
    probe_up,
    probe_down,
    seq_device,
    seq_length,
    owners,
    left_bases,
    right_bases,
    first_moment,
    second_moment,
    vec_first,
    vec_second,
):
    row_count, model_width = tokens.shape
    head_count = model_width // HEAD
    up_rows = up_weight.shape[1] // model_width
    device = lax.axis_index("dp")
    segment, position = row_layout(device, seq_device, seq_length, row_count)
    cosine_table, sine_table = rotary_table(position)
    row_index = jnp.arange(row_count, dtype=jnp.int32)
    allowed = (segment[:, None] == segment[None, :]) & (row_index[None, :] <= row_index[:, None])
    drift_vec = probe_vec[0]
    drift_qkv = probe_qkv[0]
    drift_out = probe_out[0]
    drift_up = probe_up[0]
    drift_down = probe_down[0]
    inputs = tokens.astype(jnp.float32)
    cot_rows = cotangent.astype(jnp.float32)
    normed, norm_scale = normalize(inputs)
    attn_in = normed * vec_params[0] + vec_params[1]
    drift_attn_in = normed * drift_vec[0] + drift_vec[1]
    mlp_in = normed * vec_params[2] + vec_params[3]
    drift_mlp_in = normed * drift_vec[2] + drift_vec[3]
    attn_low = attn_in.astype(jnp.bfloat16)
    mlp_low = mlp_in.astype(jnp.bfloat16)
    mixed_rows = product("ij,jk->ik", attn_low, qkv_weight) + vec_params[4:7].reshape(-1)
    drift_mixed = (
        product("ij,jk->ik", drift_attn_in, qkv_weight)
        + product("ij,jk->ik", attn_low, drift_qkv)
        + drift_vec[4:7].reshape(-1)
    )

    def split_heads(matrix, column_group):
        return matrix[:, column_group * model_width : (column_group + 1) * model_width].reshape(
            row_count, head_count, HEAD
        )

    query_rows = rotate(split_heads(mixed_rows, 0), cosine_table, sine_table, False)
    key_rows = rotate(split_heads(mixed_rows, 1), cosine_table, sine_table, False)
    value_rows = split_heads(mixed_rows, 2)
    drift_query = rotate(split_heads(drift_mixed, 0), cosine_table, sine_table, False)
    drift_key = rotate(split_heads(drift_mixed, 1), cosine_table, sine_table, False)
    drift_value = split_heads(drift_mixed, 2)
    grad_att = product("ij,kj->ik", cotangent, out_weight)
    drift_grad_att = product("ij,kj->ik", cotangent, drift_out)
    grad_att_low = grad_att.astype(jnp.bfloat16)

    def attend(pieces):
        query_block, key_block, value_block, drift_q, drift_k, drift_v, grad_out, drift_grad_out = (
            pieces
        )
        scores = product("ij,kj->ik", query_block, key_block) * 0.125
        drift_scores = (
            product("ij,kj->ik", drift_q, key_block) + product("ij,kj->ik", query_block, drift_k)
        ) * 0.125
        scores = jnp.where(allowed, scores, masked_score)
        shifted = scores - jnp.max(scores, axis=1, keepdims=True)
        exp_scores = jnp.exp(shifted)
        probs = exp_scores / jnp.sum(exp_scores, axis=1, keepdims=True)
        drift_probs = probs * (drift_scores - jnp.sum(probs * drift_scores, axis=1, keepdims=True))
        probs_low = probs.astype(jnp.bfloat16)
        attended_head = product("ij,jk->ik", probs_low, value_block)
        drift_attended_head = product("ij,jk->ik", drift_probs, value_block) + product(
            "ij,jk->ik", probs_low, drift_v
        )
        grad_probs = product("ij,kj->ik", grad_out, value_block)
        drift_grad_probs = product("ij,kj->ik", drift_grad_out, value_block) + product(
            "ij,kj->ik", grad_out, drift_v
        )
        grad_value_head = product("ij,ik->jk", probs_low, grad_out)
        drift_grad_value_head = product("ij,ik->jk", drift_probs, grad_out) + product(
            "ij,ik->jk", probs_low, drift_grad_out
        )
        centre = jnp.sum(probs * grad_probs, axis=1, keepdims=True)
        drift_centre = jnp.sum(
            drift_probs * grad_probs + probs * drift_grad_probs, axis=1, keepdims=True
        )
        grad_scores = probs * (grad_probs - centre)
        drift_grad_scores = drift_probs * (grad_probs - centre) + probs * (
            drift_grad_probs - drift_centre
        )
        scores_low = grad_scores.astype(jnp.bfloat16)
        grad_query_head = product("ij,jk->ik", scores_low, key_block) * 0.125
        drift_grad_query_head = (
            product("ij,jk->ik", drift_grad_scores, key_block)
            + product("ij,jk->ik", scores_low, drift_k)
        ) * 0.125
        grad_key_head = product("ij,ik->jk", scores_low, query_block) * 0.125
        drift_grad_key_head = (
            product("ij,ik->jk", drift_grad_scores, query_block)
            + product("ij,ik->jk", scores_low, drift_q)
        ) * 0.125
        return (
            attended_head,
            drift_attended_head,
            grad_query_head,
            grad_key_head,
            grad_value_head,
            drift_grad_query_head,
            drift_grad_key_head,
            drift_grad_value_head,
        )

    results = lax.map(
        attend,
        (
            swap_major(query_rows.astype(jnp.bfloat16)),
            swap_major(key_rows.astype(jnp.bfloat16)),
            swap_major(value_rows.astype(jnp.bfloat16)),
            swap_major(drift_query),
            swap_major(drift_key),
            swap_major(drift_value),
            swap_major(grad_att_low.reshape(row_count, head_count, HEAD)),
            swap_major(drift_grad_att.reshape(row_count, head_count, HEAD)),
        ),
    )
    attended = swap_major(results[0]).reshape(row_count, model_width)
    drift_attended = swap_major(results[1]).reshape(row_count, model_width)
    grad_query = rotate(swap_major(results[2]), cosine_table, sine_table, True).reshape(
        row_count, model_width
    )
    grad_key = rotate(swap_major(results[3]), cosine_table, sine_table, True).reshape(
        row_count, model_width
    )
    grad_value = swap_major(results[4]).reshape(row_count, model_width)
    drift_grad_query = rotate(swap_major(results[5]), cosine_table, sine_table, True).reshape(
        row_count, model_width
    )
    drift_grad_key = rotate(swap_major(results[6]), cosine_table, sine_table, True).reshape(
        row_count, model_width
    )
    drift_grad_value = swap_major(results[7]).reshape(row_count, model_width)
    grad_mixed_low = jnp.concatenate([grad_query, grad_key, grad_value], axis=1).astype(
        jnp.bfloat16
    )
    drift_grad_mixed = jnp.concatenate([drift_grad_query, drift_grad_key, drift_grad_value], axis=1)
    att_low = attended.astype(jnp.bfloat16)
    attn_out = product("ij,jk->ik", att_low, out_weight) + vec_params[7]
    hidden = product("ij,jk->ik", mlp_low, up_weight) + vec_params[8 : 8 + up_rows].reshape(-1)
    drift_hidden = (
        product("ij,jk->ik", drift_mlp_in, up_weight)
        + product("ij,jk->ik", mlp_low, drift_up)
        + drift_vec[8 : 8 + up_rows].reshape(-1)
    )
    cumulative = 0.5 * (1.0 + lax.erf(hidden * root_half))
    density = jnp.exp(-0.5 * hidden * hidden) * density_scale
    activated = hidden * cumulative
    gelu_slope = cumulative + hidden * density
    gelu_bend = density * (2.0 - hidden * hidden)
    act_low = activated.astype(jnp.bfloat16)
    drift_act = gelu_slope * drift_hidden
    mlp_out = product("ij,jk->ik", act_low, down_weight) + vec_params[8 + up_rows]
    block_output = (inputs + attn_out + mlp_out).astype(jnp.bfloat16)
    grad_down = product("ij,ik->jk", act_low, cotangent)
    drift_grad_down = product("ij,ik->jk", drift_act, cotangent)
    grad_act = product("ij,kj->ik", cotangent, down_weight)
    drift_grad_act = product("ij,kj->ik", cotangent, drift_down)
    grad_hidden = grad_act * gelu_slope
    drift_grad_hidden = drift_grad_act * gelu_slope + grad_act * gelu_bend * drift_hidden
    grad_hidden_low = grad_hidden.astype(jnp.bfloat16)
    grad_up = product("ij,ik->jk", mlp_low, grad_hidden_low)
    drift_grad_up = product("ij,ik->jk", drift_mlp_in, grad_hidden_low) + product(
        "ij,ik->jk", mlp_low, drift_grad_hidden
    )
    grad_mlp_in = product("ij,kj->ik", grad_hidden_low, up_weight)
    drift_grad_mlp_in = product("ij,kj->ik", drift_grad_hidden, up_weight) + product(
        "ij,kj->ik", grad_hidden_low, drift_up
    )
    grad_out_w = product("ij,ik->jk", att_low, cotangent)
    drift_grad_out_w = product("ij,ik->jk", drift_attended, cotangent)
    grad_qkv = product("ij,ik->jk", attn_low, grad_mixed_low)
    drift_grad_qkv = product("ij,ik->jk", drift_attn_in, grad_mixed_low) + product(
        "ij,ik->jk", attn_low, drift_grad_mixed
    )
    grad_attn_in = product("ij,kj->ik", grad_mixed_low, qkv_weight)
    drift_grad_attn_in = product("ij,kj->ik", drift_grad_mixed, qkv_weight) + product(
        "ij,kj->ik", grad_mixed_low, drift_qkv
    )
    grad_weighted = grad_attn_in * vec_params[0] + grad_mlp_in * vec_params[2]
    input_grad = cot_rows + norm_back(grad_weighted, normed, norm_scale)
    out_sum = jnp.sum(cot_rows, axis=0)[None]
    zero_row = jnp.zeros((1, model_width), jnp.float32)
    vec_grad = jnp.concatenate(
        [
            jnp.sum(grad_attn_in * normed, axis=0)[None],
            jnp.sum(grad_attn_in, axis=0)[None],
            jnp.sum(grad_mlp_in * normed, axis=0)[None],
            jnp.sum(grad_mlp_in, axis=0)[None],
            jnp.sum(grad_mixed_low, axis=0, dtype=jnp.float32).reshape(3, model_width),
            out_sum,
            jnp.sum(grad_hidden_low, axis=0, dtype=jnp.float32).reshape(up_rows, model_width),
            out_sum,
        ],
        axis=0,
    )
    vec_drift = jnp.concatenate(
        [
            jnp.sum(drift_grad_attn_in * normed, axis=0)[None],
            jnp.sum(drift_grad_attn_in, axis=0)[None],
            jnp.sum(drift_grad_mlp_in * normed, axis=0)[None],
            jnp.sum(drift_grad_mlp_in, axis=0)[None],
            jnp.sum(drift_grad_mixed, axis=0).reshape(3, model_width),
            zero_row,
            jnp.sum(drift_grad_hidden, axis=0).reshape(up_rows, model_width),
            zero_row,
        ],
        axis=0,
    )
    along_probe = jnp.sum(vec_grad * drift_vec)
    curve_probe = jnp.sum(vec_drift * drift_vec)
    for gradient, drift_gradient, direction_set in (
        (grad_qkv, drift_grad_qkv, drift_qkv),
        (grad_out_w, drift_grad_out_w, drift_out),
        (grad_up, drift_grad_up, drift_up),
        (grad_down, drift_grad_down, drift_down),
    ):
        along_probe = along_probe + jnp.sum(gradient * direction_set.astype(jnp.float32))
        curve_probe = curve_probe + jnp.sum(drift_gradient * direction_set.astype(jnp.float32))
    dots = jnp.stack([along_probe, curve_probe])
    grad_tiles = jnp.concatenate(
        [cut_tiles(grad_qkv), cut_tiles(grad_out_w), cut_tiles(grad_up), cut_tiles(grad_down)],
        axis=0,
    )
    curve_tiles = jnp.concatenate(
        [
            cut_tiles(drift_grad_qkv),
            cut_tiles(drift_grad_out_w),
            cut_tiles(drift_grad_up),
            cut_tiles(drift_grad_down),
        ],
        axis=0,
    )
    slot_dev = left_bases.shape[0]
    slot_total = slot_dev * lax.axis_size("dp")
    tile_index, occupied = slot_order(owners, slot_total)
    slot_grad = arrange(grad_tiles, tile_index)
    slot_curve = arrange(curve_tiles, tile_index)
    own_grad, own_curve = (
        lax.psum_scatter(slot_grad, "dp", scatter_dimension=0, tiled=True),
        lax.psum_scatter(slot_curve, "dp", scatter_dimension=0, tiled=True),
    )
    vec_total, vec_curve, dot_total = lax.psum((vec_grad, vec_drift, dots), "dp")
    all_dots = lax.all_gather(dot_total[None, :], "probe", axis=0, tiled=True)
    own_index = lax.dynamic_slice_in_dim(tile_index, device * slot_dev, slot_dev)
    own_used = lax.dynamic_slice_in_dim(occupied, device * slot_dev, slot_dev)
    weight_tiles = jnp.concatenate(
        [
            cut_tiles(qkv_weight),
            cut_tiles(out_weight),
            cut_tiles(up_weight),
            cut_tiles(down_weight),
        ],
        axis=0,
    )
    own_weight = arrange(weight_tiles, own_index).astype(jnp.float32)
    new_first, new_second, new_weights = rotated_adam(
        own_grad, own_weight, left_bases, right_bases, first_moment, second_moment, own_used
    )
    new_weights_low = new_weights.astype(jnp.bfloat16)
    vec_new_first, vec_new_second, vec_new = plain_adam(
        vec_total, vec_params, vec_first, vec_second
    )
    vector_state = jnp.stack([vec_total, vec_new_first], axis=0)
    return (
        block_output,
        input_grad,
        own_grad,
        new_first,
        new_second,
        new_weights,
        new_weights_low,
        own_curve[None],
        vector_state,
        vec_new_second,
        vec_new,
        vec_curve[None],
        all_dots,
    )


f32 = jnp.float32
bf16 = jnp.bfloat16
VMEM_SHARD = 60 << 20
HEAD_A = (0, 1, 7, 8, 3, 4, 10, 11)
HEAD_B = (6, 6, 2, 2, 9, 9, 5, 5)
ARRIVE = ((1, 2, 3), (0, 2, 3), (3, 1, 0), (2, 1, 0))


def fits_tp(mesh):
    return mesh.shape["dp"] == 8 and mesh.shape["probe"] == 4


def device_table():
    rows = []
    for device in range(8):
        z, x = device // 2, device % 2
        levels = (z,) + ARRIVE[z]
        order = [2 * level + x for level in levels] + [2 * level + 1 - x for level in levels]
        for probe in range(4):
            rows.append([device, HEAD_A[device], HEAD_B[device], probe % 2, x, probe // 2, z % 2, 0] + order)
    return rows


def is_short(seq_device, seq_length, group, rows):
    longest = jnp.int32(0)
    for i in range(seq_device.shape[0]):
        longest = jnp.maximum(longest, jnp.where(seq_device[i] == group, seq_length[i], 0))
    return (longest < rows).astype(jnp.int32)


def in_hbm(value):
    return pltpu.with_memory_space_constraint(value, pltpu.HBM)


def dot_nt(left, right):
    return lax.dot_general(left, right, (((1,), (1,)), ((), ())), preferred_element_type=f32)


def dot_nn(left, right):
    return lax.dot_general(left, right, (((1,), (0,)), ((), ())), preferred_element_type=f32)


def rotate_rows(ref, base, cos, sin, reverse):
    up, low = ref[base : base + 8, :], ref[base + 8 : base + 16, :]
    if reverse:
        ref[base : base + 8, :] = up * cos + low * sin
        ref[base + 8 : base + 16, :] = low * cos - up * sin
    else:
        ref[base : base + 8, :] = up * cos - low * sin
        ref[base + 8 : base + 16, :] = low * cos + up * sin


def mask_rows(bias, short, rows):
    for start in range(0, rows, 128):
        row = lax.broadcasted_iota(jnp.int32, (128, rows), 0) + start
        col = lax.broadcasted_iota(jnp.int32, (128, rows), 1)
        first = jnp.where(short == 1, start, 0)
        bias[start : start + 128, :] = jnp.where((col >= first) & (col <= row), 0.0, masked_score)


def prepare_kernel(info, *refs):
    refs = list(refs)
    ups = [[refs.pop(0) for _ in range(6)] for _ in range(8)]
    heads = [[refs.pop(0) for _ in range(2)] for _ in range(6)]
    outs = [[refs.pop(0) for _ in range(2)] for _ in range(2)]
    vec, dvec, uwt, dwt, bias_u, wat, oat, bias_a = refs
    device = info[0]
    row = lax.broadcasted_iota(jnp.int32, (48, 128), 0) + (device * 48) % 128
    lane = lax.broadcasted_iota(jnp.int32, (48, 128), 1)
    here, after = lane == row, lane == row - 128
    pick_0, pick_1 = here.astype(bf16), after.astype(bf16)
    block = (device * 48) // 128
    lanes_0 = pl.multiple_of(128 * block, 128)
    lanes_1 = pl.multiple_of(128 * jnp.minimum(block + 1, 2), 128)
    for j, (up_0, up_1, dup_0, dup_1, down, ddown) in enumerate(ups):
        for part, (first, second, below, bias) in enumerate(((up_0, up_1, down, vec), (dup_0, dup_1, ddown, dvec))):
            uwt[part, j] = (dot_nt(pick_0, first[...]) + dot_nt(pick_1, second[...])).astype(bf16)
            dwt[part, j] = below[...]
            at = slice(8 + j // 2, 9 + j // 2)
            line_0 = bias[at, pl.ds(pl.multiple_of(384 * (j % 2) + lanes_0, 128), 128)]
            line_1 = bias[at, pl.ds(pl.multiple_of(384 * (j % 2) + lanes_1, 128), 128)]
            column = jnp.sum(jnp.where(here, line_0, 0.0) + jnp.where(after, line_1, 0.0), axis=1, keepdims=True)
            bias_u[part, j] = jnp.broadcast_to(column, (48, 128))
    for i, (qkv, dqkv) in enumerate(heads):
        head = info[1 + i // 3]
        row = lax.broadcasted_iota(jnp.int32, (64, 128), 0) + (head % 2) * 64
        place = lax.broadcasted_iota(jnp.int32, (64, 128), 1) == row
        pick = place.astype(bf16)
        wat[i * 64 : i * 64 + 64, :768] = dot_nt(pick, dqkv[...]).astype(bf16)
        wat[i * 64 : i * 64 + 64, 768:] = dot_nt(pick, qkv[...]).astype(bf16)
        for part, bias in enumerate((vec, dvec)):
            line = bias[4 + i % 3 : 5 + i % 3, pl.ds(pl.multiple_of(128 * (head // 2), 128), 128)]
            at = i * 128 + part * 64
            column = jnp.sum(jnp.where(place, line, 0.0), axis=1, keepdims=True)
            bias_a[at : at + 64, :] = jnp.broadcast_to(column, (64, 128))
    for place, (own, drift) in enumerate(outs):
        oat[place * 128 : place * 128 + 64, :] = own[...]
        oat[place * 128 + 64 : place * 128 + 128, :] = drift[...]


def prepare(info, qkv, dqkv, out_w, dout_w, up, dup, down, ddown, vec, dvec):
    whole = pl.BlockSpec(memory_space=pltpu.VMEM)
    specs, operands = [], []
    qkv, dqkv, out_w, dout_w = (in_hbm(value) for value in (qkv, dqkv, out_w, dout_w))
    up, dup, down, ddown = (in_hbm(value) for value in (up, dup, down, ddown))

    def block(shape, at, *arrays):
        for array in arrays:
            specs.append(pl.BlockSpec(shape, at))
            operands.append(array)

    for j in range(8):
        for array in (up, dup):
            block((768, 128), lambda i, info, j=j: (0, 3 * j + (info[0] * 48) // 128), array)
            block((768, 128), lambda i, info, j=j: (0, 3 * j + jnp.minimum((info[0] * 48) // 128 + 1, 2)), array)
        block((48, 768), lambda i, info, j=j: (8 * j + info[0], 0), down, ddown)
    for h in range(6):
        block((768, 128), lambda i, info, h=h: (0, 6 * (h % 3) + info[1 + h // 3] // 2), qkv, dqkv)
    for place in range(2):
        block((64, 768), lambda i, info, place=place: (info[1 + place], 0), out_w, dout_w)
    kinds = [((2, 8, 48, 768), bf16)] * 2 + [((2, 8, 48, 128), f32), ((384, 1536), bf16), ((256, 768), bf16), ((768, 128), f32)]
    uwt, dwt, bias_u, wat, oat, bias_a = pl.pallas_call(
        prepare_kernel,
        out_shape=[jax.ShapeDtypeStruct(*kind) for kind in kinds],
        grid_spec=pltpu.PrefetchScalarGridSpec(
            num_scalar_prefetch=1,
            grid=(1,),
            in_specs=specs + [whole] * 2,
            out_specs=[whole] * 6,
        ),
        compiler_params=pltpu.CompilerParams(vmem_limit_bytes=VMEM_SHARD),
        cost_estimate=pl.CostEstimate(flops=10**9, bytes_accessed=2 * 10**7, transcendentals=0),
        name="prepare",
    )(info, *operands, vec, dvec)
    return (uwt.reshape(768, 768), dwt.reshape(768, 768), bias_u.reshape(768, 128), wat, oat, bias_a)


def outgoing_kernel(info, tokens, cotangent, out):
    def rows_of(i, carry):
        rows = pl.ds(pl.multiple_of(i * 128, 128), 128)
        out[rows, :768] = normalize(tokens[rows, :].astype(f32))[0]
        out[rows, 768:] = cotangent[rows, :].astype(f32)
        return carry

    lax.fori_loop(0, 2, rows_of, 0)


def outgoing(info, tokens, cotangent):
    half = pl.BlockSpec((256, 768), lambda i, info: (info[3], 0))
    return pl.pallas_call(
        outgoing_kernel,
        out_shape=jax.ShapeDtypeStruct((256, 1536), f32),
        grid_spec=pltpu.PrefetchScalarGridSpec(
            num_scalar_prefetch=1,
            grid=(1,),
            in_specs=[half, half],
            out_specs=pl.BlockSpec((256, 1536), lambda i, info: (0, 0)),
        ),
        compiler_params=pltpu.CompilerParams(vmem_limit_bytes=VMEM_SHARD),
        cost_estimate=pl.CostEstimate(flops=10**6, bytes_accessed=3 * 10**6, transcendentals=0),
        name="outgoing",
    )(info, in_hbm(tokens), in_hbm(cotangent))


def wide(column):
    return jnp.concatenate([column] * 4, axis=1)


def shard_kernel(plan, first, parts, slot_dev, *refs):
    refs = list(refs)
    with_heads, with_mlp, with_finish = parts != "close", parts != "heads", parts == "close"
    info, seq_device, seq_length = refs[:3]
    refs = refs[3:]
    owner = refs.pop(0) if with_finish else None
    steps = len(plan)
    data_h = refs[: 2 * steps]
    refs = refs[2 * steps :]
    vec, dvec, cos_ref, sin_ref = refs[:4]
    weights_h = refs[4:10]
    refs = refs[10:]
    old_h = None if first else refs[:4]
    refs = refs if first else refs[4:]
    if with_finish:
        out_sum, curve, grad, sums_out = refs[0], refs[1], refs[2], refs[3]
        out_h = (None,) * 4
    else:
        out_h = refs[:4]
        border = refs[4] if parts == "heads" else None
        refs = refs[:4] + refs[5:] if parts == "heads" else refs
    (mine, other, wat, bias_a, oat, uwt, dwt, bias_u, acc_h, acc_m, acc_c, acc_r, sem) = refs[4:17]
    (nb, nb_low, ones, lhs_a, ml, dm, dm_low, cb, mask, proj, gat, qt, kt, k4, vt, v4, gt, q4, g4, gq, gk, gv, head_g, head_a, hid, act, mlp_a, mlp_g, one, two) = refs[17:]
    new = (acc_h, acc_m, acc_c, acc_r)
    step = pl.program_id(0)
    core = info[3]
    most = max(heads for _, heads in plan)

    def by_step(values):
        result = jnp.int32(values[0])
        for i, value in enumerate(values[1:]):
            result = jnp.where(step > i, value, result)
        return result

    heads_now = by_step([heads for _, heads in plan])
    short = is_short(seq_device, seq_length, info[8 + by_step([index for index, _ in plan])], 512)
    width = 768
    gain_a, shift_a, gain_m, shift_m = (vec[i : i + 1, :] for i in range(4))
    dgain_a, dshift_a, dgain_m, dshift_m = (dvec[i : i + 1, :] for i in range(4))
    wat_h, bias_ah, oat_h, uwt_h, dwt_h, bias_uh = weights_h
    lead = most * 384
    pairs = [(data_h[0], mine.at[0]), (data_h[1], other.at[0])]
    pairs += [(uwt_h, uwt), (dwt_h, dwt), (bias_uh, bias_u)] if with_mlp else []
    for_mlp = range(2, len(pairs))
    held = 2 if with_finish else most
    pairs += [(wat_h.at[: held * 192], wat), (oat_h.at[: held * 128], oat)]
    pairs += [(bias_ah.at[:lead], bias_a)] if with_heads else []
    for_heads = range(for_mlp.stop, len(pairs))
    if not first:
        pairs += [(old_h[1], acc_m)] if with_mlp else []
        pairs += [(old_h[2], acc_c), (old_h[3], acc_r)]
    for_sums = range(for_heads.stop, len(pairs))
    if not first:
        pairs += [(old_h[0].at[: held * 512], acc_h)]
    for_tiles = range(for_sums.stop, len(pairs))
    base_count = len(pairs)
    for i in range(1, steps):
        pairs += [(data_h[2 * i], mine.at[i]), (data_h[2 * i + 1], other.at[i])]
    arrivals = [pltpu.make_async_copy(source, target, sem.at[i]) for i, (source, target) in enumerate(pairs)]

    def at_step(which):
        if steps == 1:
            return lambda body: body()
        return pl.when(step == which)

    @at_step(0)
    def _():
        for copy in arrivals:
            copy.start()

    def arrived(*which):
        @at_step(0)
        def _():
            for i in which:
                if i < base_count:
                    arrivals[i].wait()

    ones[...] = jnp.ones((512, 128), bf16)
    if with_heads:
        mask_rows(mask, short, 512)

    def load(ref, cot_ref, base, count):
        def rows_of(i, carry):
            src = pl.ds(pl.multiple_of(i * 128, 128), 128)
            dst = pl.ds(pl.multiple_of(base + i * 128, 128), 128)
            rows = ref[step, src, :width].astype(f32)
            normed = normalize(rows)[0] if first else rows
            nb[dst, :], nb_low[dst, :] = split_two(normed)
            if with_heads:
                lhs_a[dst, :width] = (normed * gain_a + shift_a).astype(bf16)
                lhs_a[dst, width : 2 * width], lhs_a[dst, 2 * width :] = split_two(normed * dgain_a + dshift_a)
            if with_mlp:
                ml[dst, :] = (normed * gain_m + shift_m).astype(bf16)
                dm[dst, :], dm_low[dst, :] = split_two(normed * dgain_m + dshift_m)
            cb[dst, :] = cot_ref[step, src, :].astype(bf16)
            return carry

        lax.fori_loop(0, count, rows_of, 0)

    if first:
        arrived(0, 1)
        load(mine, other, 0, 4)
    else:
        arrived(0)
        for i in range(1, steps):

            @at_step(i)
            def _(i=i):
                arrivals[base_count + 2 * i - 2].wait()
                arrivals[base_count + 2 * i - 1].wait()

        load(mine, mine.at[:, :, width:], core * 256, 2)
        arrived(1)
        load(other, other.at[:, :, width:], (1 - core) * 256, 2)

    def add(ref, rows, value):
        ref[rows, :] = value if first else ref[rows, :] + value

    def eight(value):
        rows, columns = value.shape
        return jnp.sum(value.reshape(rows // 8, 8, columns), axis=0)

    def fold(carry, ref, at, tops, w_rows, dw_rows, dgain, dshift, c_rows):
        grad_at, curve_at = at
        top, low = tops
        p_two, q_two = two[top, :], two[low, :]
        add(ref, grad_at, one[top, :])
        moved = dgain * p_two + dshift * c_rows
        add(ref, curve_at, one[low, :] + moved)
        w_wide, dw_wide = w_rows.astype(f32), dw_rows.astype(f32)
        drift, plain, dots = carry
        drift = drift + eight(w_wide * q_two + dw_wide * p_two)
        plain = plain + eight(w_wide * p_two)
        dots = dots + eight(dw_wide * (2.0 * moved))
        return (drift, plain, dots)

    blank = jnp.zeros((8, width), f32)
    if with_mlp:
        arrived(*for_mlp)
        hid[...] = dot_nt(uwt[...], ml[...])
        act[...] = dot_nt(dwt[...], cb[...])
        hid[384:, :] += dot_nt(uwt[:384, :], dm[...]) + dot_nt(uwt[:384, :], dm_low[...])

        def gelu(i, carry):
            top = pl.ds(pl.multiple_of(i * 32, 32), 32)
            low = pl.ds(pl.multiple_of(384 + i * 32, 32), 32)
            hidden, dhidden = hid[top, :] + wide(bias_u[top, :]), hid[low, :] + wide(bias_u[low, :])
            grad_act, dgrad_act = act[top, :], act[low, :]
            cumulative = 0.5 * (1.0 + lax.erf(hidden * root_half))
            density = jnp.exp(-0.5 * hidden * hidden) * density_scale
            slope = cumulative + hidden * density
            bend = density * (2.0 - hidden * hidden)
            drift_act = slope * dhidden
            drift_grad = dgrad_act * slope + grad_act * bend * dhidden
            mlp_a[top, :] = (hidden * cumulative).astype(bf16)
            mlp_a[low, :] = drift_act.astype(bf16)
            mlp_g[top, :] = (grad_act * slope).astype(bf16)
            mlp_g[low, :] = drift_grad.astype(bf16)
            return carry + eight(drift_grad * dhidden + drift_act * dgrad_act)

        dots_m = lax.fori_loop(0, 12, gelu, jnp.zeros((8, 512), f32))
        one[...] = dot_nn(mlp_g[...], ml[...])
        two[...] = dot_nn(mlp_g[...], nb[...])
        two[:384, :] += dot_nn(mlp_g[:384, :], nb_low[...])
        sums = dot_nn(mlp_g[...], ones[...])
        arrived(*for_sums)
        add(acc_c, slice(768, 1536), sums)
        proj[0:384, 0:128] = sums[:384, :]

        def fold_m(i, carry):
            top = pl.ds(pl.multiple_of(i * 64, 64), 64)
            low = pl.ds(pl.multiple_of(384 + i * 64, 64), 64)
            return fold(carry, acc_m, (top, low), (top, low), uwt[top, :], uwt[low, :], dgain_m, dshift_m, proj[top, 0:1])

        carry_m = (blank, blank, blank) if first else (acc_r[8:16, :], acc_r[24:32, :], acc_r[32:40, :])
        acc_r[8:16, :], acc_r[24:32, :], acc_r[32:40, :] = lax.fori_loop(0, 6, fold_m, carry_m)
        acc_r[32:40, :512] += dots_m
        one[...] = dot_nn(mlp_a[...], cb[...])
        add(acc_m, slice(768, 1536), one[...])
        if with_finish:
            arrived(*for_heads, *for_tiles)
            finish_kernel(slot_dev, owner, info, acc_h, acc_m, acc_c, acc_r, wat, oat, uwt, dwt, out_sum, curve, grad, sums_out)
            return
        leave_m = pltpu.make_async_copy(acc_m, out_h[1], sem.at[0])

        @at_step(steps - 1)
        def _():
            leave_m.start()

    if not with_mlp:
        arrived(*for_sums)
    arrived(*for_heads, *for_tiles)
    cos, sin = cos_ref[short], sin_ref[short]

    def attend(head, carry):
        base = pl.multiple_of(head * 384, 128)
        w_at = pl.ds(pl.multiple_of(head * 192, 64), 192)
        plain = dot_nt(wat[w_at, width:], lhs_a[:, :width])
        drift = dot_nt(wat[w_at, :], lhs_a[:, : 2 * width]) + dot_nt(wat[w_at, width:], lhs_a[:, 2 * width :])
        for kind in range(3):
            proj[kind * 128 : kind * 128 + 64, :] = plain[kind * 64 : kind * 64 + 64, :]
            proj[kind * 128 + 64 : kind * 128 + 128, :] = drift[kind * 64 : kind * 64 + 64, :]
        proj[...] += wide(bias_a[pl.ds(base, 384), :])
        gat[...] = dot_nt(oat[pl.ds(pl.multiple_of(head * 128, 128), 128), :], cb[...])
        for part in (0, 64, 128, 192):
            rotate_rows(proj, part, cos, sin, False)
        proj[0:128, :] = proj[0:128, :] * 0.125
        rests = []
        for source, flat, tall, back in ((proj.at[0:128], qt, q4, True), (proj.at[128:256], kt, k4, False), (proj.at[256:384], vt, v4, False), (gat, gt, g4, True)):
            own, moved = source[0:64, :], source[64:128, :]
            flat[0:64, :] = own.astype(bf16)
            high, low = split_two(moved)
            flat[64:128, :] = high
            if back:
                low_wide = low.astype(f32)
                rests.append(low_wide)
                tall[...] = jnp.transpose(jnp.concatenate([own, own, high.astype(f32), low_wide], axis=0)).astype(bf16)
            else:
                tall[0:64, :] = high
                tall[64:128, :] = low
                tall[128:192, :] = flat[0:64, :]
                tall[192:256, :] = flat[0:64, :]
        rest_q, rest_g = rests
        for block in range(2):
            rows = slice(block * 256, block * 256 + 256)
            span = block * 256 + 256
            scores = dot_nn(q4[rows, :64], kt[:64, :span]) + mask[rows, :span]
            dscores = dot_nn(q4[rows, :], k4[:, :span])
            exp_scores = jnp.exp(scores - jnp.max(scores, axis=1, keepdims=True))
            probs = exp_scores * (1.0 / jnp.sum(exp_scores, axis=1, keepdims=True))
            dprobs = probs * (dscores - jnp.sum(probs * dscores, axis=1, keepdims=True))
            probs_low, dprobs_low = probs.astype(bf16), dprobs.astype(bf16)
            grad_probs = dot_nn(g4[rows, :64], vt[:64, :span])
            dgrad_probs = dot_nn(g4[rows, :], v4[:, :span])
            centre = jnp.sum(probs * grad_probs, axis=1, keepdims=True)
            dcentre = jnp.sum(dprobs * grad_probs + probs * dgrad_probs, axis=1, keepdims=True)
            rest = grad_probs - centre
            g_scores = (probs * rest).astype(bf16)
            dg_wide = dprobs * rest + probs * (dgrad_probs - dcentre)
            dg_scores = dg_wide.astype(bf16)
            acc_r[32:40, :span] += eight(dprobs * dgrad_probs + dg_wide * dscores)
            out = dot_nt(vt[:, :span], probs_low)
            head_a[0:64, rows] = out[:64, :].astype(bf16)
            head_a[64:128, rows] = (out[64:, :] + dot_nt(vt[:64, :span], dprobs_low)).astype(bf16)
            part_q = dot_nt(kt[:, :span], g_scores)
            acc_r[32:40, rows] += 2.0 * eight(rest_g[:, rows] * out[64:, :] + rest_q[:, rows] * part_q[64:, :])
            gq[:, rows] = part_q * 0.125
            gq[64:, rows] += dot_nt(kt[:64, :span], dg_scores) * 0.125
            part_v = dot_nn(gt[:, rows], probs_low)
            part_dv = dot_nn(gt[:64, rows], dprobs_low)
            part_k = dot_nn(qt[:, rows], g_scores)
            part_dk = dot_nn(qt[:64, rows], dg_scores)
            acc_r[32:40, :span] += 2.0 * eight(proj[320:384, :span] * part_v[64:, :] + proj[192:256, :span] * part_k[64:, :])
            if block == 0:
                gv[:, :span] = part_v
                gk[:, :span] = part_k
                gv[:, span:] = jnp.zeros((128, 512 - span), f32)
                gk[:, span:] = jnp.zeros((128, 512 - span), f32)
            else:
                gv[:, :span] += part_v
                gk[:, :span] += part_k
            gv[64:, :span] += part_dv
            gk[64:, :span] += part_dk
        for part in (0, 64):
            rotate_rows(gq, part, cos, sin, True)
            rotate_rows(gk, part, cos, sin, True)
        for kind, grad in enumerate((gq, gk, gv)):
            head_g[kind * 64 : kind * 64 + 64, :] = grad[:64, :].astype(bf16)
            head_g[192 + kind * 64 : 256 + kind * 64, :] = grad[64:, :].astype(bf16)
        one[:384, :] = dot_nn(head_g[...], lhs_a[:, :width])
        two[:384, :] = dot_nn(head_g[...], nb[...])
        two[:192, :] += dot_nn(head_g[:192, :], nb_low[...])
        sums = dot_nn(head_g[...], ones[...])
        add(acc_c, pl.ds(base, 384), sums)
        for kind in range(3):
            at = pl.multiple_of(head * 512 + kind * 128, 128)
            top, low = slice(kind * 64, kind * 64 + 64), slice(192 + kind * 64, 256 + kind * 64)
            w_rows = pl.ds(pl.multiple_of(head * 192 + kind * 64, 64), 64)
            carry = fold(
                carry, acc_h, (pl.ds(at, 64), pl.ds(at + 64, 64)), (top, low),
                wat[w_rows, width:], wat[w_rows, :width], dgain_a, dshift_a, sums[top, 0:1],
            )
        add(acc_h, pl.ds(pl.multiple_of(head * 512 + 384, 128), 128), dot_nn(head_a[...], cb[...]))
        return carry

    carry_r = (blank, blank, blank) if first else (acc_r[0:8, :], acc_r[16:24, :], blank)
    if most == 1:
        carry_r = attend(0, carry_r)
    else:
        carry_r = lax.fori_loop(0, heads_now, attend, carry_r)
    acc_r[0:8, :], acc_r[16:24, :] = carry_r[:2]
    acc_r[32:40, :] += carry_r[2]
    if parts == "heads":
        for index in range(8):
            border[index] = acc_h[index * 64 + 48 : index * 64 + 64, :]
    leaves = [
        pltpu.make_async_copy(acc_c, out_h[2], sem.at[1]),
        pltpu.make_async_copy(acc_r, out_h[3], sem.at[2]),
        pltpu.make_async_copy(acc_h.at[: most * 512], out_h[0].at[: most * 512], sem.at[3]),
    ]

    @at_step(steps - 1)
    def _():
        for copy in leaves:
            copy.start()
        if with_mlp:
            leave_m.wait()
        for copy in leaves:
            copy.wait()


def shard_steps(plan, scalars, data, shared, tables, old, parts="both", close=None):
    first = old is None
    sizes = [(1024, 768), (1536, 768), (1536, 128), (40, 768)]
    steps = len(plan)
    most = max(heads for _, heads in plan)
    whole = pl.BlockSpec(memory_space=pltpu.VMEM)
    there = pl.BlockSpec(memory_space=pltpu.HBM)
    specs = [pl.BlockSpec(memory_space=pl.ANY)] * (2 * steps) + [whole] * 4 + [there] * 6
    vec, dvec, wat, bias_a, oat, uwt, dwt, bias_u = shared
    operands = [*data, vec, dvec, *tables, wat, bias_a, oat, uwt, dwt, bias_u]
    aliases = {}
    if not first:
        aliases = {3 + len(operands) + i: i for i in range(len(sizes))}
        specs += [there] * len(sizes)
        operands += list(old)
    held = most
    outs, out_specs, slot_dev = sizes, [there] * len(sizes), None
    if parts == "close":
        owners, slot_dev, out_sum = close
        held, aliases, scalars = 2, {}, (*scalars, owners)
        specs.append(whole)
        operands.append(out_sum)
        outs, out_specs = [(8 * slot_dev, 48, 384), (4 * slot_dev, 24, 384), (32, 768)], [whole] * 3
    if parts == "heads":
        outs, out_specs = sizes + [(8, 16, 768)], out_specs + [whole]
    scratch = [((steps, *data[0].shape), data[0].dtype), ((steps, *data[1].shape), data[1].dtype)]
    scratch += [((held * 192, 1536), bf16), ((most * 384, 128), f32), ((held * 128, 768), bf16)]
    scratch += [((768, 768), bf16)] * 2 + [((768, 128), f32)]
    scratch += [((held * 512, 768), f32)] + [(size, f32) for size in sizes[1:]] + [None]
    scratch += [
        ((512, 768), bf16),
        ((512, 768), bf16),
        ((512, 128), bf16),
        ((512, 2304), bf16),
        ((512, 768), bf16),
        ((512, 768), bf16),
        ((512, 768), bf16),
        ((512, 768), bf16),
        ((512, 512), f32),
        ((384, 512), f32),
        ((128, 512), f32),
    ]
    flat, tall, back = ((128, 512), bf16), ((256, 512), bf16), ((512, 256), bf16)
    scratch += [flat, flat, tall, flat, tall, flat, back, back] + [((128, 512), f32)] * 3
    scratch += [((384, 512), bf16), ((128, 512), bf16)]
    scratch += [((768, 512), f32)] * 2 + [((768, 512), bf16)] * 2 + [((768, 768), f32)] * 2
    return pl.pallas_call(
        lambda *refs: shard_kernel(plan, first, parts, slot_dev, *refs),
        out_shape=[jax.ShapeDtypeStruct(size, f32) for size in outs],
        grid_spec=pltpu.PrefetchScalarGridSpec(
            num_scalar_prefetch=len(scalars),
            grid=(steps,),
            in_specs=specs,
            out_specs=out_specs,
            scratch_shapes=[pltpu.SemaphoreType.DMA((16,)) if one is None else pltpu.VMEM(*one) for one in scratch],
        ),
        input_output_aliases=aliases,
        compiler_params=pltpu.CompilerParams(vmem_limit_bytes=VMEM_SHARD),
        cost_estimate=pl.CostEstimate(
            flops=sum(heads * 2 * 10**9 + 5 * 10**9 for _, heads in plan), bytes_accessed=2 * 10**7, transcendentals=10**6
        ),
        name="shards_" + parts + "".join(str(heads) for _, heads in plan),
    )(*scalars, *operands)


def put_tile(slot_dev, owner, y, tile, curve, grad, curve_rows, grad_rows):
    group = slot_dev // 2
    slot = owner[tile]
    curve_rows(curve.at[slot])
    home, place = slot // slot_dev, slot % slot_dev

    @pl.when(place // group == y)
    def _():
        grad_rows(grad.at[home * group + place % group])


def tile_at(kind, side):
    return (side * 6 + 2 * kind, 1) if kind < 3 else (12 + side, 2)


def finish_kernel(slot_dev, owner, info, acc_h, acc_m, acc_c, acc_r, wat, oat, uwt, dwt, out_sum, curve, grad, sums):
    core, y, odd = info[3], info[5], info[6]
    if slot_dev * 8 > 48:
        curve[...] = jnp.zeros(curve.shape, f32)
        grad[...] = jnp.zeros(grad.shape, f32)

    def put(tile, columns, source, curve_at, grad_at):
        def curve_rows(ref):
            ref[...] = source[curve_at : curve_at + 48, columns]

        def grad_rows(ref):
            ref[...] = source[pl.ds(pl.multiple_of(grad_at + core * 24, 8), 24), columns]

        put_tile(slot_dev, owner, y, tile, curve, grad, curve_rows, grad_rows)

    for side in range(2):
        columns = slice(side * 384, side * 384 + 384)
        for kind in range(4):
            lower, step = tile_at(kind, side)
            put(lower + odd * step, columns, acc_h, kind * 128 + 64, kind * 128)
        for block in range(8):
            at = block * 48
            put(16 + side * 8 + block, columns, acc_m, 384 + at, at)
            put(32 + block * 2 + side, columns, acc_m, 1152 + at, 768 + at)
    small_sums_kernel(info, acc_h, acc_m, acc_c, acc_r, wat, oat, uwt, dwt, out_sum, sums)


def finish_split_kernel(slot_dev, owner, info, own_b, far_b, extra, old_curve, old_grad, curve, grad, new_curve, new_grad, near_b, sem):
    core, x, y, odd = info[3], info[4], info[5], info[6]
    group = slot_dev // 2
    for index in range(8):
        near_b[index] = far_b[index] + own_b[0, pl.ds(pl.multiple_of(index * 64 + x * 32, 32), 32), :]
    copies, later = [], []
    for kind in range(4):
        for side in range(2):
            columns = slice(side * 384, side * 384 + 384)
            lower, step = tile_at(kind, side)
            slot = owner[lower + (1 - odd) * step]
            place = kind * 2 + side
            new_curve[place, 0:32, :] = near_b[kind * 2 + 1, :, columns]
            new_curve[place, 32:48, :] = extra[kind * 2 + 1, :, columns]
            copy = pltpu.make_async_copy(new_curve.at[place], curve.at[slot], sem.at[place])
            copy.start()
            copies.append(copy)

            @pl.when(core == 0)
            def _(place=place, kind=kind, columns=columns):
                new_grad[place] = near_b[kind * 2, 0:24, columns]

            @pl.when(core == 1)
            def _(place=place, kind=kind, columns=columns):
                new_grad[place, 0:8, :] = near_b[kind * 2, 24:32, columns]
                new_grad[place, 8:24, :] = extra[kind * 2, :, columns]

            home, spot = slot // slot_dev, slot % slot_dev

            @pl.when(spot // group == y)
            def _(place=place, home=home, spot=spot):
                pltpu.make_async_copy(new_grad.at[place], grad.at[home * group + spot % group], sem.at[8 + place]).start()

            later.append((place, home * group + spot % group, spot // group == y))

    for copy in copies:
        copy.wait()
    for place, target, mine in later:

        @pl.when(mine)
        def _(place=place, target=target):
            pltpu.make_async_copy(new_grad.at[place], grad.at[target], sem.at[8 + place]).wait()


def finish_split(owners, info, slot_dev, acc_h, near_b, extra, curve, grad):
    whole = pl.BlockSpec(memory_space=pltpu.VMEM)
    there = pl.BlockSpec(memory_space=pltpu.HBM)
    return pl.pallas_call(
        lambda *refs: finish_split_kernel(slot_dev, *refs),
        out_shape=[jax.ShapeDtypeStruct(curve.shape, f32), jax.ShapeDtypeStruct(grad.shape, f32)],
        grid_spec=pltpu.PrefetchScalarGridSpec(
            num_scalar_prefetch=2,
            grid=(1,),
            in_specs=[pl.BlockSpec((1, 512, 768), lambda i, *scalars: (1, 0, 0))] + [whole] * 2 + [there] * 2,
            out_specs=[there] * 2,
            scratch_shapes=[
                pltpu.VMEM((8, 48, 384), f32),
                pltpu.VMEM((8, 24, 384), f32),
                pltpu.VMEM((8, 32, 768), f32),
                pltpu.SemaphoreType.DMA((16,)),
            ],
        ),
        input_output_aliases={5: 0, 6: 1},
        compiler_params=pltpu.CompilerParams(vmem_limit_bytes=VMEM_SHARD),
        cost_estimate=pl.CostEstimate(flops=0, bytes_accessed=5 * 10**6, transcendentals=0),
        name="finish_split",
    )(owners, info, acc_h.reshape(2, 512, 768), near_b, extra, curve, grad)


def own_attention_kernel(info, seq_device, seq_length, q_ref, k_ref, v_ref, g_ref, cos_ref, sin_ref, att, gq_out, gk_out, gv_out, mask, buf, gk, gv):
    short = is_short(seq_device, seq_length, info[0], 512)

    @pl.when(pl.program_id(0) == 0)
    def _():
        mask_rows(mask, short, 512)

    cos, sin = cos_ref[short], sin_ref[short]
    buf[...] = q_ref[...]
    rotate_rows(buf, 0, cos, sin, False)
    q_rows = buf[...] * 0.125
    qt = q_rows.astype(bf16)
    qn = jnp.transpose(q_rows).astype(bf16)
    buf[...] = k_ref[...]
    rotate_rows(buf, 0, cos, sin, False)
    kt = buf[...].astype(bf16)
    vt = v_ref[...].astype(bf16)
    gt = g_ref[...].astype(bf16)
    gn = jnp.transpose(g_ref[...]).astype(bf16)
    for block in range(2):
        rows = slice(block * 256, block * 256 + 256)
        wide = block * 256 + 256
        scores = dot_nn(qn[rows, :], kt[:, :wide]) + mask[rows, :wide]
        exp_scores = jnp.exp(scores - jnp.max(scores, axis=1, keepdims=True))
        probs = exp_scores * (1.0 / jnp.sum(exp_scores, axis=1, keepdims=True))
        probs_low = probs.astype(bf16)
        grad_probs = dot_nn(gn[rows, :], vt[:, :wide])
        weighted = probs * grad_probs
        g_scores = (weighted - probs * jnp.sum(weighted, axis=1, keepdims=True)).astype(bf16)
        att[:, rows] = dot_nt(vt[:, :wide], probs_low).astype(bf16)
        buf[:, rows] = dot_nt(kt[:, :wide], g_scores) * 0.125
        part_v = dot_nn(gt[:, rows], probs_low)
        part_k = dot_nn(qt[:, rows], g_scores)
        if block == 0:
            gv[:, :wide] = part_v
            gk[:, :wide] = part_k
            gv[:, wide:] = jnp.zeros((64, 512 - wide), f32)
            gk[:, wide:] = jnp.zeros((64, 512 - wide), f32)
        else:
            gv[:, :wide] += part_v
            gk[:, :wide] += part_k
    rotate_rows(buf, 0, cos, sin, True)
    rotate_rows(gk, 0, cos, sin, True)
    gq_out[...] = buf[...].astype(bf16)
    gk_out[...] = gk[...].astype(bf16)
    gv_out[...] = gv[...].astype(bf16)


def own_attention(scalars, mixed, grad_att, tables):
    def rows_at(offset):
        return pl.BlockSpec((64, 512), lambda i, *scalars: (offset + i, 0))

    whole = pl.BlockSpec(memory_space=pltpu.VMEM)
    return pl.pallas_call(
        own_attention_kernel,
        out_shape=[jax.ShapeDtypeStruct((768, 512), bf16)] * 4,
        grid_spec=pltpu.PrefetchScalarGridSpec(
            num_scalar_prefetch=3,
            grid=(12,),
            in_specs=[rows_at(0), rows_at(12), rows_at(24), rows_at(0), whole, whole],
            out_specs=[rows_at(0)] * 4,
            scratch_shapes=[pltpu.VMEM((512, 512), f32)] + [pltpu.VMEM((64, 512), f32)] * 3,
        ),
        compiler_params=pltpu.CompilerParams(vmem_limit_bytes=16 << 20),
        cost_estimate=pl.CostEstimate(flops=10**10, bytes_accessed=10**7, transcendentals=3 * 10**6),
        name="own_attention",
    )(*scalars, mixed, mixed, mixed, grad_att, *tables)


def lay_rows(table, slot, rows, out, buf):
    for source in range(8):
        for part in range(3):
            start = pl.multiple_of(table[slot, source * 3 + part], 16)
            buf[pl.ds(start, 16), :] = rows(source, part * 16)

    @pl.when(table[slot, 24] == 1)
    def _():
        out[0] = jnp.transpose(buf[...])

    @pl.when(table[slot, 24] == 0)
    def _():
        out[0] = buf[...]


def assemble_kernel(table, pieces, out, buf):
    lay_rows(table, pl.program_id(0), lambda source, at: pieces[source, 0, at : at + 16, :], out, buf)


def assemble(table, pieces):
    slots = pieces.shape[1]
    return pl.pallas_call(
        assemble_kernel,
        out_shape=jax.ShapeDtypeStruct((slots, 384, 384), f32),
        grid_spec=pltpu.PrefetchScalarGridSpec(
            num_scalar_prefetch=1,
            grid=(slots,),
            in_specs=[pl.BlockSpec((8, 1, 48, 384), lambda i, table: (0, i, 0, 0))],
            out_specs=pl.BlockSpec((1, 384, 384), lambda i, table: (i, 0, 0)),
            scratch_shapes=[pltpu.VMEM((384, 384), f32)],
        ),
        compiler_params=pltpu.CompilerParams(vmem_limit_bytes=16 << 20),
        cost_estimate=pl.CostEstimate(flops=0, bytes_accessed=8 * 10**6, transcendentals=0),
        name="assemble",
    )(table, pieces)


def split_two(value):
    high = value.astype(bf16)
    return (high, (value - high.astype(f32)).astype(bf16))


def dot_fine(left, right, dims):
    (a_high, a_low), (b_high, b_low) = left, right

    def dot(a, b):
        return lax.dot_general(a, b, (dims, ((), ())), preferred_element_type=f32)

    return dot(a_high, b_high) + (dot(a_high, b_low) + dot(a_low, b_high))


def update_kernel(table, info, tile, own, own_core, far, far_core, qkv, out_w, up, down, left, right, first, second, grad, new_first, new_second, new_weight, new_low, rows, buf):
    slot = pl.program_id(0)
    core, y = info[3], info[5]
    group = pl.num_programs(0) // 2

    def join(one, two):
        rows[:, pl.ds(pl.multiple_of(core * 24, 8), 24), :] = one[:, 0]
        rows[:, pl.ds(pl.multiple_of(24 - core * 24, 8), 24), :] = two[:, 0]

    @pl.when(slot // group == y)
    def _():
        join(own, own_core)

    @pl.when(slot // group != y)
    def _():
        join(far, far_core)

    lay_rows(table, slot, lambda source, at: rows[source, at : at + 16, :], grad, buf)
    index = tile[slot]

    def weight(low, high, ref):
        @pl.when((index >= low) & (index < high))
        def _():
            buf[...] = ref[...].astype(f32)

    weight(0, 12, qkv)
    weight(12, 16, out_w)
    weight(16, 32, up)
    weight(32, 48, down)
    used = jnp.where(index < 48, 1.0, 0.0)
    l_two, r_two = split_two(left[0]), split_two(right[0])
    turned = dot_fine(l_two, split_two(grad[0]), ((0,), (0,)))
    turned = dot_fine(split_two(turned), r_two, ((1,), (0,)))
    moment = beta_decay * first[0] + (1.0 - beta_decay) * turned
    square = beta_decay * second[0] + (1.0 - beta_decay) * turned * turned
    correction = 1.0 - beta_decay**STEP
    direction = moment / correction / (jnp.sqrt(square / correction) + adam_epsilon)
    new_first[0] = used * moment
    new_second[0] = used * square
    restored = dot_fine(l_two, split_two(direction), ((1,), (0,)))
    restored = dot_fine(split_two(restored), r_two, ((1,), (1,)))
    value = buf[...]
    value = jnp.where(index < 48, value - learning_rate * (restored + weight_decay * value), 0.0)
    new_weight[0] = value
    new_low[0] = value.astype(bf16)


def update(table, info, tile, pieces, weights, states):
    group = pieces[0].shape[1]
    slots = 2 * group
    piece = pl.BlockSpec((8, 1, 24, 384), lambda i, table, info, tile: (0, i % group, 0, 0))
    slab = pl.BlockSpec((1, 384, 384), lambda i, table, info, tile: (i, 0, 0))

    def spec(start, count, columns):
        def at(i, table, info, tile):
            local_tile = jnp.clip(tile[i] - start, 0, count - 1)
            return (local_tile // columns, local_tile % columns)

        return pl.BlockSpec((384, 384), at)

    kinds = [f32, f32, f32, f32, bf16]
    return pl.pallas_call(
        update_kernel,
        out_shape=[jax.ShapeDtypeStruct((slots, 384, 384), kind) for kind in kinds],
        grid_spec=pltpu.PrefetchScalarGridSpec(
            num_scalar_prefetch=3,
            grid=(slots,),
            in_specs=[piece] * 4 + [spec(0, 12, 6), spec(12, 4, 2), spec(16, 16, 8), spec(32, 16, 2)] + [slab] * 4,
            out_specs=[slab] * 5,
            scratch_shapes=[pltpu.VMEM((8, 48, 384), f32), pltpu.VMEM((384, 384), f32)],
        ),
        compiler_params=pltpu.CompilerParams(vmem_limit_bytes=32 << 20),
        cost_estimate=pl.CostEstimate(flops=10**10, bytes_accessed=4 * 10**7, transcendentals=10**6),
        name="update",
    )(table, info, tile, *pieces, *(in_hbm(value) for value in (*weights, *states)))


def small_sums_kernel(info, acc_h, acc_m, acc_c, acc_r, wat, oat, uwt, dwt, out_sum, out):
    device = info[0]
    out[...] = jnp.zeros((32, 768), f32)
    blank = jnp.zeros((8, 768), f32)
    along, curve = blank, acc_r[32:40, :]
    shift_a, shift_m, dshift_a, dshift_m = blank, blank, blank, blank

    def fold(value):
        return jnp.sum(value.reshape(value.shape[0] // 8, 8, 768), axis=0)

    for place in range(2):
        acc = acc_h.at[place * 512 : place * 512 + 512]
        head = info[1 + place]
        row = lax.broadcasted_iota(jnp.int32, (64, 128), 0) + (head % 2) * 64
        pick = lax.broadcasted_iota(jnp.int32, (64, 128), 1) == row
        for kind in range(4):
            at = kind * 128
            if kind < 3:
                base = place * 192 + kind * 64
                w_one, w_drift = wat[base : base + 64, 768:].astype(f32), wat[base : base + 64, :768].astype(f32)
                base = place * 384 + kind * 64
                p_col, q_col = acc_c[base : base + 64, :], acc_c[base + 192 : base + 256, :]
                shift_a += fold(w_one * p_col[:, 0:1])
                dshift_a += fold(w_one * q_col[:, 0:1] + w_drift * p_col[:, 0:1])
                lanes = pl.ds(pl.multiple_of(128 * (head // 2), 128), 128)
                out[4 + kind : 5 + kind, lanes] += jnp.sum(jnp.where(pick, p_col, 0.0), axis=0, keepdims=True)
                out[20 + kind : 21 + kind, lanes] += jnp.sum(jnp.where(pick, q_col, 0.0), axis=0, keepdims=True)
            else:
                w_drift = oat[place * 128 + 64 : place * 128 + 128, :].astype(f32)
            along += fold(acc[at : at + 64, :] * w_drift)
    row = lax.broadcasted_iota(jnp.int32, (48, 384), 0) + device * 48
    pick = lax.broadcasted_iota(jnp.int32, (48, 384), 1) == row
    for block in range(8):
        at = block * 48
        w_one, w_drift = uwt[at : at + 48, :].astype(f32), uwt[384 + at : 432 + at, :].astype(f32)
        d_drift = dwt[384 + at : 432 + at, :].astype(f32)
        p_col, q_col = acc_c[768 + at : 816 + at, 0:1], acc_c[1152 + at : 1200 + at, 0:1]
        shift_m += fold(w_one * p_col)
        dshift_m += fold(w_one * q_col + w_drift * p_col)
        along += fold(acc_m[at : at + 48, :] * w_drift) + fold(acc_m[768 + at : 816 + at, :] * d_drift)
        lanes = slice(384 * (block % 2), 384 * (block % 2) + 384)
        place = 8 + block // 2
        out[place : place + 1, lanes] = jnp.sum(jnp.where(pick, p_col, 0.0), axis=0, keepdims=True)
        out[16 + place : 17 + place, lanes] = jnp.sum(jnp.where(pick, q_col, 0.0), axis=0, keepdims=True)

    def row_sum(value):
        return jnp.sum(value, axis=0, keepdims=True)

    out[0:1, :] = row_sum(acc_r[16:24, :])
    out[1:2, :] = row_sum(shift_a)
    out[2:3, :] = row_sum(acc_r[24:32, :])
    out[3:4, :] = row_sum(shift_m)
    out[7:8, :] = out_sum[...]
    out[12:13, :] = out_sum[...]
    out[16:17, :] = row_sum(acc_r[0:8, :])
    out[17:18, :] = row_sum(dshift_a)
    out[18:19, :] = row_sum(acc_r[8:16, :])
    out[19:20, :] = row_sum(dshift_m)
    lane = lax.broadcasted_iota(jnp.int32, (1, 768), 1)
    out[29:30, :] = jnp.where(lane == 0, jnp.sum(along), jnp.where(lane == 1, jnp.sum(curve), 0.0))


def take_rows(matrix, start, size):
    return lax.dynamic_slice_in_dim(matrix, start, size, axis=0)


def piece_rows(index):
    z, x = index // 2, index % 2
    plain = [48 * index, 48 * index + 16, 48 * index + 32]
    full = [[64 * x + 16 * i for i in range(3)], [64 + 64 * x + 16 * i for i in range(3)]]
    full += [[192 + 64 * x + 16 * i for i in range(3)], [256 + 64 * x + 16 * i for i in range(3)]]
    split = [
        [32 * x, 32 * x + 16, 64 + 64 * x + 48],
        [128 + 32 * x, 144 + 32 * x, 64 * x + 48],
        [192 + 32 * x, 208 + 32 * x, 256 + 64 * x + 48],
        [320 + 32 * x, 336 + 32 * x, 192 + 64 * x + 48],
    ]
    even = z % 2 == 0
    return (full[z] if even else split[z], split[z] if even else full[z], plain)


def local_tp(
    tokens,
    cotangent,
    vec_params,
    qkv_weight,
    out_weight,
    up_weight,
    down_weight,
    probe_vec,
    probe_qkv,
    probe_out,
    probe_up,
    probe_down,
    seq_device,
    seq_length,
    owners,
    left_bases,
    right_bases,
    first_moment,
    second_moment,
    vec_first,
    vec_second,
):
    row_count, width = tokens.shape
    device = lax.axis_index("dp")
    z = device // 2
    probe = lax.axis_index("probe")
    x, y, core = device % 2, probe // 2, probe % 2
    info = lax.dynamic_index_in_dim(jnp.array(device_table(), jnp.int32), device * 4 + probe, 0, keepdims=False)
    scalars = (info, seq_device, seq_length)
    drift_vec, drift_qkv, drift_out = probe_vec[0], probe_qkv[0], probe_out[0]
    drift_up, drift_down = probe_up[0], probe_down[0]
    barrier = lax.optimization_barrier

    across = [(i, i ^ 1) for i in range(8)]
    outer = [(i, i ^ 2) for i in range(8)]
    middle = [(2, 4), (3, 5), (4, 2), (5, 3)]
    outward = [(2, 0), (3, 1), (4, 6), (5, 7)]
    swap_core = [(0, 1), (1, 0), (2, 3), (3, 2)]
    swap_y = [(0, 2), (2, 0), (1, 3), (3, 1)]

    def move(value, pairs):
        return lax.ppermute(value, "dp", pairs)

    def to_core(value):
        return lax.ppermute(value, "probe", swap_core)

    mine = outgoing(info, tokens, cotangent)
    near, centre, cross_0 = move(mine, outer), move(mine, middle), move(mine, across)
    inside = (z == 1) | (z == 2)

    row_index = jnp.arange(row_count, dtype=jnp.int32)
    half_rot = ROT // 2
    frequency = jnp.exp(jnp.arange(half_rot, dtype=f32) * (-2.0 * math.log(10000.0) / ROT))
    position = jnp.stack([row_index, row_index % (row_count // 4)])
    angles = position.astype(f32)[:, None, :] * frequency[None, :, None]
    tables = (jnp.cos(angles), jnp.sin(angles))

    flat_bias = vec_params[4:7].reshape(-1)
    uwt, dwt, bias_u, wat, oat, bias_a = prepare(
        info,
        qkv_weight, drift_qkv, out_weight, drift_out, up_weight, drift_up, down_weight, drift_down, vec_params, drift_vec,
    )
    shared = (vec_params, drift_vec, wat, bias_a, oat, uwt, dwt, bias_u)

    def step(plan, data, old, *how):
        return shard_steps(plan, scalars, data, shared, tables, old, *how)

    acc_h, acc_m, acc_c, acc_r = step(((0, 2),), (tokens, cotangent), None)
    (near, centre, cross_0, acc_r) = barrier((near, centre, cross_0, acc_r))
    edge, middle_near, cross_1 = move(centre, outward), move(near, middle), move(near, across)
    cross_0o, near_o = to_core(cross_0), to_core(near)
    acc_h, acc_m, acc_c, acc_r = step(((1, 2), (4, 1)), (near, near_o, cross_0, cross_0o), (acc_h, acc_m, acc_c, acc_r))

    (edge, middle_near, cross_1, acc_r) = barrier((edge, middle_near, cross_1, acc_r))
    second = jnp.where(inside, centre, edge)
    (middle_near, second) = barrier((middle_near, second))
    edge_far, cross_2 = move(middle_near, outward), move(second, across)
    second_o, cross_1o = to_core(second), to_core(cross_1)
    acc_h, acc_m, acc_c, acc_r = step(((2, 2), (5, 1)), (second, second_o, cross_1, cross_1o), (acc_h, acc_m, acc_c, acc_r))

    (edge_far, cross_2, acc_r) = barrier((edge_far, cross_2, acc_r))
    third = barrier(jnp.where(inside, middle_near, edge_far))
    cross_3, third_o, cross_2o = move(third, across), to_core(third), to_core(cross_2)
    acc_h, acc_m, acc_c, acc_r = step(((3, 2), (6, 1)), (third, third_o, cross_2, cross_2o), (acc_h, acc_m, acc_c, acc_r))
    sends = lax.dynamic_slice(acc_h.reshape(16, 64, width), (8, 32 - 32 * x, 0), (8, 32, width))
    near_b = move(sends, across)
    (tokens, cotangent, cross_3, acc_r) = barrier((tokens, cotangent, cross_3, acc_r))
    cross_3o = to_core(cross_3)
    inputs = tokens.astype(f32)
    cot_rows = cotangent.astype(f32)
    out_sum = jnp.sum(cot_rows, axis=0, keepdims=True)
    normed, norm_scale = normalize(inputs)
    attn_low = (normed * vec_params[0] + vec_params[1]).astype(bf16)
    mlp_low = (normed * vec_params[2] + vec_params[3]).astype(bf16)
    (cross_3, cross_3o, acc_r, attn_low, mlp_low) = barrier((cross_3, cross_3o, acc_r, attn_low, mlp_low))
    acc_h, acc_m, acc_c, acc_r, border = step(((7, 1),), (cross_3, cross_3o), (acc_h, acc_m, acc_c, acc_r), "heads")
    extra = move(border, [(i, i ^ 2) for i in range(8)])

    slot_dev = left_bases.shape[0]
    tile_index, occupied = slot_order(owners, slot_dev * 8)
    curve_slots, grad_slots, vec_all = step(
        ((7, 1),), (cross_3, cross_3o), (acc_h, acc_m, acc_c, acc_r), "close", (owners, slot_dev, out_sum)
    )
    vec_one = move(vec_all, [(i, i ^ 4) for i in range(8)])
    (extra, near_b, vec_all) = barrier((extra, near_b, vec_all))
    curve_slots, grad_slots = finish_split(owners, info, slot_dev, acc_h, near_b, extra, curve_slots, grad_slots)
    curve_slots = curve_slots.reshape(8, slot_dev, 48, 384)
    (attn_low, cotangent, grad_slots) = barrier((attn_low, cotangent, grad_slots))
    grad_slots = lax.all_to_all(grad_slots.reshape(8, slot_dev // 2, 24, 384), "dp", 0, 0)
    curve_slots = lax.all_to_all(curve_slots, "dp", 0, 0)
    mixed = product("kj,tk->jt", qkv_weight, attn_low) + flat_bias[:, None]
    grad_att = product("jk,tk->jt", out_weight, cotangent)
    (mixed, grad_att, vec_all, vec_one) = barrier((mixed, grad_att, vec_all, vec_one))
    vec_all = vec_all + vec_one
    vec_two = move(vec_all, [(i, i ^ 2) for i in range(8)])
    att_t, gq_t, gk_t, gv_t = own_attention(scalars, mixed, grad_att, tables)
    (vec_all, vec_two, att_t) = barrier((vec_all, vec_two, att_t))
    vec_all = vec_all + vec_two
    vec_four = move(vec_all, [(i, i ^ 1) for i in range(8)])

    (grad_slots, att_t, gq_t, gk_t, gv_t) = barrier((grad_slots, att_t, gq_t, gk_t, gv_t))
    far = lax.ppermute(grad_slots, "probe", swap_y)
    own_core = to_core(grad_slots)
    (mlp_low, cotangent, own_core, att_t, gq_t, gk_t, gv_t) = barrier((mlp_low, cotangent, own_core, att_t, gq_t, gk_t, gv_t))
    hidden = product("ij,jk->ik", mlp_low, up_weight) + vec_params[8:12].reshape(-1)
    cumulative = 0.5 * (1.0 + lax.erf(hidden * root_half))
    density = jnp.exp(-0.5 * hidden * hidden) * density_scale
    act_low = (hidden * cumulative).astype(bf16)
    grad_act = product("ij,kj->ik", cotangent, down_weight)
    grad_hidden_low = (grad_act * (cumulative + hidden * density)).astype(bf16)
    mlp_out = product("ij,jk->ik", act_low, down_weight) + vec_params[12]
    (mlp_out, far, grad_hidden_low, att_t) = barrier((mlp_out, far, grad_hidden_low, att_t))
    far_core = to_core(far)
    attn_out = product("jt,jk->tk", att_t, out_weight) + vec_params[7]
    block_output = (inputs + attn_out + mlp_out).astype(bf16)
    grad_mlp_in = product("ij,kj->ik", grad_hidden_low, up_weight)
    grad_attn_in = (
        product("jt,kj->tk", gq_t, qkv_weight[:, :width])
        + product("jt,kj->tk", gk_t, qkv_weight[:, width : 2 * width])
        + product("jt,kj->tk", gv_t, qkv_weight[:, 2 * width :])
    )
    grad_weighted = grad_attn_in * vec_params[0] + grad_mlp_in * vec_params[2]
    input_grad = cot_rows + norm_back(grad_weighted, normed, norm_scale)

    own_index = lax.dynamic_slice_in_dim(tile_index, device * slot_dev, slot_dev)
    kinds = [sum((piece_rows(i)[kind] for i in range(8)), []) for kind in range(3)]
    row_table = jnp.array(kinds, jnp.int32)
    in_qkv, in_out = own_index < 12, (own_index >= 12) & (own_index < 16)
    kind = jnp.where(in_qkv, own_index % 2, jnp.where(in_out, (own_index - 12) // 2, 2))
    turned = in_qkv | ((own_index >= 16) & (own_index < 32))
    table = jnp.concatenate([row_table[kind], turned.astype(jnp.int32)[:, None]], axis=1)
    (far_core, input_grad, block_output) = barrier((far_core, input_grad, block_output))
    own_grad, new_first, new_second, new_weights, new_weights_low = update(
        table,
        info,
        own_index,
        [grad_slots, own_core, far, far_core],
        [qkv_weight, out_weight, up_weight, down_weight],
        [left_bases, right_bases, first_moment, second_moment],
    )
    (vec_all, vec_four, new_first) = barrier((vec_all, vec_four, new_first))
    vec_all = vec_all + vec_four
    vec_total, vec_curve = vec_all[:13], vec_all[16:29]
    own_dots = jnp.stack(
        [vec_all[29, 0] + jnp.sum(vec_total * drift_vec), vec_all[29, 1]]
    )
    all_dots = jnp.where(jnp.arange(8)[:, None] == probe, jnp.pad(own_dots, (0, 126))[None], 0.0)
    all_dots = all_dots + to_core(all_dots)
    all_dots = all_dots + lax.ppermute(all_dots, "probe", swap_y)
    all_dots = all_dots[:4, :2]
    own_curve = assemble(table, curve_slots)
    vec_new_first, vec_new_second, vec_new = plain_adam(vec_total, vec_params, vec_first, vec_second)
    vector_state = jnp.stack([vec_total, vec_new_first], axis=0)
    return (
        block_output,
        input_grad,
        own_grad,
        new_first,
        new_second,
        new_weights,
        new_weights_low,
        own_curve[None],
        vector_state,
        vec_new_second,
        vec_new,
        vec_curve[None],
        all_dots,
    )


def solution(mesh):
    local = local_tp if fits_tp(mesh) else local_any
    return jax.shard_map(
        local,
        mesh=mesh,
        in_specs=(
            P("dp", None),
            P("dp", None),
            P(),
            P(),
            P(),
            P(),
            P(),
            P("probe", None, None),
            P("probe", None, None),
            P("probe", None, None),
            P("probe", None, None),
            P("probe", None, None),
            P(),
            P(),
            P(),
            P("dp", None, None),
            P("dp", None, None),
            P("dp", None, None),
            P("dp", None, None),
            P(),
            P(),
        ),
        out_specs=(
            P("dp", None),
            P("dp", None),
            P("dp", None, None),
            P("dp", None, None),
            P("dp", None, None),
            P("dp", None, None),
            P("dp", None, None),
            P("probe", "dp", None, None),
            P(),
            P(),
            P(),
            P("probe", None, None),
            P(),
        ),
        check_vma=False,
    )
```
